8 devices in a mesh: dp: 1 (over z), tp: 2 (over y), sp: 4 (over x, core).
Axes of the slice: x: 2, y: 2, z: 1, core: 2. Of those that a mesh axis runs over, the one named last changes fastest.
Arguments:
- hidden: bfloat16 [128, 8192], P('dp')
- seq_lens: int32 [128], P('dp')
- rope_cos: float32 [128, 64], P('dp')
- rope_sin: float32 [128, 64], P('dp')
- k_cache: bfloat16 [128, 256, 8, 128], P('dp', 'sp', 'tp')
- v_cache: bfloat16 [128, 256, 8, 128], P('dp', 'sp', 'tp')
- norm_gain: bfloat16 [8192], replicated
- w_qkv: bfloat16 [8192, 8, 1280], P(None, 'tp')
- b_qkv: bfloat16 [8, 1280], P('tp')
- sink_logits: float32 [64], P('tp')
- w_o: bfloat16 [8192, 8192], P('tp')
- b_o: bfloat16 [8192], replicated
Outputs:
- output 1: bfloat16 [128, 8192], P('dp')
- output 2: bfloat16 [128, 256, 8, 128], P('dp', 'sp', 'tp')
- output 3: bfloat16 [128, 256, 8, 128], P('dp', 'sp', 'tp')
All inputs are finite; a program needn't handle non-finite values.
Results may differ from the reference program's by a relative error of at most 0.00537465.
Values sent between devices are 32-bit elements.
A program may use at most 1 GiB of HBM per device.

```python
import math
import jax
import jax.numpy as jnp
from jax import lax

D_MODEL = 8192
Q_HEADS = 64
KV_HEADS = 8
HEAD_DIM = 128
SEQ_COUNT = 128
CTX_LEN = 256
ROPE_BASE = 150000
NORM_EPS = 1e-5


def rotate_half(heads_in, cos_part, sin_part):
    half_dim = heads_in.shape[-1] // 2
    first_half = heads_in[..., :half_dim]
    second_half = heads_in[..., half_dim:]
    return jnp.concatenate([first_half * cos_part - second_half * sin_part, second_half * cos_part + first_half * sin_part], axis=-1)


def setup_inputs(seed: int = 0, part: int = 0) -> dict:
    shared_keys = jax.random.split(jax.random.key(seed), 6)
    part_keys = jax.random.split(jax.random.fold_in(jax.random.key(seed + 1), part), 5)
    group_size = Q_HEADS // KV_HEADS
    qkv_width = (group_size + 2) * HEAD_DIM
    key_scale = math.sqrt(math.log(CTX_LEN) / 2.0)
    sink_center = math.log(CTX_LEN / 2.0) + 0.6 * key_scale * key_scale - 1.0
    hidden = (0.5 * jax.random.normal(part_keys[0], (SEQ_COUNT, D_MODEL), jnp.float32)).astype(jnp.bfloat16)
    drawn_lens = jax.random.randint(part_keys[1], (SEQ_COUNT,), 0, CTX_LEN, jnp.int32)
    full_row = jax.random.randint(part_keys[2], (), 0, SEQ_COUNT, jnp.int32)
    seq_lens = jnp.where(jnp.arange(SEQ_COUNT) == full_row, CTX_LEN - 1, drawn_lens).astype(jnp.int32)
    inv_freq = jnp.exp(jnp.arange(HEAD_DIM // 2, dtype=jnp.float32) * (-2.0 * math.log(ROPE_BASE) / HEAD_DIM))
    angles = seq_lens.astype(jnp.float32)[:, None] * inv_freq[None, :]
    cache_shape = (SEQ_COUNT, CTX_LEN, KV_HEADS, HEAD_DIM)
    k_cache = (key_scale * jax.random.normal(part_keys[3], cache_shape, jnp.float32)).astype(jnp.bfloat16)
    v_cache = jax.random.normal(part_keys[4], cache_shape, jnp.float32).astype(jnp.bfloat16)
    norm_gain = (1.0 + 0.2 * jax.random.normal(shared_keys[0], (D_MODEL,), jnp.float32)).astype(jnp.bfloat16)
    w_qkv = (D_MODEL ** -0.5 * jax.random.normal(shared_keys[1], (D_MODEL, KV_HEADS, qkv_width), jnp.float32)).astype(jnp.bfloat16)
    b_qkv = (0.5 * jax.random.normal(shared_keys[2], (KV_HEADS, qkv_width), jnp.float32)).astype(jnp.bfloat16)
    sink_logits = sink_center + jax.random.normal(shared_keys[3], (Q_HEADS,), jnp.float32)
    w_o = (4.0 * (Q_HEADS * HEAD_DIM) ** -0.5 * jax.random.normal(shared_keys[4], (Q_HEADS * HEAD_DIM, D_MODEL), jnp.float32)).astype(jnp.bfloat16)
    b_o = (0.3 * jax.random.normal(shared_keys[5], (D_MODEL,), jnp.float32)).astype(jnp.bfloat16)
    return {"hidden": hidden, "seq_lens": seq_lens, "rope_cos": jnp.cos(angles), "rope_sin": jnp.sin(angles), "k_cache": k_cache, "v_cache": v_cache, "norm_gain": norm_gain, "w_qkv": w_qkv, "b_qkv": b_qkv, "sink_logits": sink_logits, "w_o": w_o, "b_o": b_o}


def reference(hidden, seq_lens, rope_cos, rope_sin, k_cache, v_cache, norm_gain, w_qkv, b_qkv, sink_logits, w_o, b_o):
    group_size = Q_HEADS // KV_HEADS
    x_wide = hidden.astype(jnp.float32)
    inv_rms = lax.rsqrt(jnp.mean(x_wide * x_wide, axis=-1, keepdims=True) + NORM_EPS)
    normed = (x_wide * inv_rms * norm_gain.astype(jnp.float32)).astype(jnp.bfloat16)
    qkv_all = jnp.dot(normed, w_qkv.reshape(D_MODEL, KV_HEADS * (group_size + 2) * HEAD_DIM), preferred_element_type=jnp.float32)
    qkv_all = (qkv_all + b_qkv.astype(jnp.float32).reshape(-1)).reshape(SEQ_COUNT, KV_HEADS, group_size + 2, HEAD_DIM)
    q_rot = rotate_half(qkv_all[:, :, :group_size], rope_cos[:, None, None, :], rope_sin[:, None, None, :]).astype(jnp.bfloat16)
    k_new = rotate_half(qkv_all[:, :, group_size], rope_cos[:, None, :], rope_sin[:, None, :]).astype(jnp.bfloat16)
    v_new = qkv_all[:, :, group_size + 1].astype(jnp.bfloat16)
    positions = jnp.arange(CTX_LEN)
    is_new = (positions[None, :] == seq_lens[:, None])[:, :, None, None]
    k_out = jnp.where(is_new, k_new[:, None], k_cache)
    v_out = jnp.where(is_new, v_new[:, None], v_cache)
    sink_kg = sink_logits.reshape(KV_HEADS, group_size)
    logit_scale = HEAD_DIM ** -0.5

    def one_sequence(per_seq):
        q_seq, k_seq, v_seq, len_seq = per_seq
        logits = jnp.einsum("kgd,lkd->kgl", q_seq.astype(jnp.float32), k_seq.astype(jnp.float32)) * logit_scale
        logits = jnp.where((positions <= len_seq)[None, None, :], logits, -jnp.inf)
        row_max = jnp.maximum(jnp.max(logits, axis=-1), sink_kg)
        weights = jnp.exp(logits - row_max[..., None])
        denominator = jnp.sum(weights, axis=-1) + jnp.exp(sink_kg - row_max)
        weighted = jnp.einsum("kgl,lkd->kgd", weights.astype(jnp.bfloat16).astype(jnp.float32), v_seq.astype(jnp.float32))
        return weighted / denominator[..., None]

    head_out = lax.map(one_sequence, (q_rot, k_out, v_out, seq_lens))
    attn_out = jnp.dot(head_out.astype(jnp.bfloat16).reshape(SEQ_COUNT, Q_HEADS * HEAD_DIM), w_o, preferred_element_type=jnp.float32)
    out_hidden = (x_wide + attn_out + b_o.astype(jnp.float32)).astype(jnp.bfloat16)
    return out_hidden, k_out, v_out
```

```python
import functools

import jax
import jax.numpy as jnp
from jax import lax
from jax.experimental import pallas as pl
from jax.experimental.pallas import tpu as pltpu
from jax.sharding import PartitionSpec as P

NORM_EPS = 1e-5
F32 = jnp.float32
BF16 = jnp.bfloat16
MESH = pl.DeviceIdType.MESH


def sp_place():
    sp = lax.axis_index("sp")
    return lax.div(sp, 2), lax.rem(sp, 2)


def remote(src, dst, send_sem, recv_sem, where):
    return pltpu.make_async_remote_copy(src_ref=src, dst_ref=dst, send_sem=send_sem, recv_sem=recv_sem, device_id=where, device_id_type=MESH)


QKV_ROWS = 512
QKV_SLOTS = 3


def qkv_kernel(x_ref, gain_ref, cos_ref, sin_ref, bias_ref, w_ref, out_ref, normed, heads, acc_q, acc_e, wq_buf, we_buf, wq_sem, we_sem, send_sem, recv_sem, out_sem):
    chip, core = sp_place()
    partner = {"sp": 2 * chip + (1 - core)}
    num_seqs, depth = x_ref.shape
    head_dim = acc_e.shape[2]
    q_cols = acc_q.shape[2]
    kv_local = acc_q.shape[0]
    per_core = q_cols // head_dim
    group = 2 * per_core
    steps = depth // QKV_ROWS

    def fetch(step, slot):
        rows = pl.ds(step * QKV_ROWS, QKV_ROWS)
        cq = pltpu.make_async_copy(w_ref.at[rows, :, pl.ds(pl.multiple_of(core * q_cols, 128), q_cols)], wq_buf.at[slot], wq_sem.at[slot])
        ce = pltpu.make_async_copy(w_ref.at[rows, :, pl.ds(pl.multiple_of((group + core) * head_dim, 128), head_dim)], we_buf.at[slot], we_sem.at[slot])
        return cq, ce

    for s in range(QKV_SLOTS - 1):
        for c in fetch(s, s):
            c.start()

    barrier = pltpu.get_barrier_semaphore()
    pl.semaphore_signal(barrier, inc=1, device_id=partner, device_id_type=MESH)

    def norm_rows(r, _):
        rows = pl.ds(pl.multiple_of(r * 16, 16), 16)
        xw = x_ref[rows, :].astype(F32)
        inv = lax.rsqrt(jnp.mean(xw * xw, axis=-1, keepdims=True) + NORM_EPS)
        normed[rows, :] = (xw * inv * gain_ref[...].astype(F32)).astype(BF16)
        return 0

    lax.fori_loop(0, num_seqs // 16, norm_rows, 0)
    acc_q[...] = jnp.zeros_like(acc_q)
    acc_e[...] = jnp.zeros_like(acc_e)

    def step_fn(step, _):
        slot = lax.rem(step, QKV_SLOTS)
        for c in fetch(step, slot):
            c.wait()

        @pl.when(step + QKV_SLOTS - 1 < steps)
        def _():
            for c in fetch(step + QKV_SLOTS - 1, lax.rem(step + QKV_SLOTS - 1, QKV_SLOTS)):
                c.start()

        h = normed[:, pl.ds(pl.multiple_of(step * QKV_ROWS, 128), QKV_ROWS)]
        wq = jnp.swapaxes(wq_buf[slot], 0, 1)
        we = jnp.swapaxes(we_buf[slot], 0, 1)
        for k in range(kv_local):
            acc_q[k] += jnp.dot(h, wq[k], preferred_element_type=F32)
            acc_e[k] += jnp.dot(h, we[k], preferred_element_type=F32)
        return 0

    lax.fori_loop(0, steps, step_fn, 0)

    cos_t = cos_ref[...].T
    sin_t = sin_ref[...].T
    cos2 = jnp.concatenate([cos_t, cos_t], axis=1)
    sin2 = jnp.concatenate([-sin_t, sin_t], axis=1)
    is_key = core == 0
    cos_e = jnp.where(is_key, cos2, jnp.ones_like(cos2))
    sin_e = jnp.where(is_key, sin2, jnp.zeros_like(sin2))

    def rotate(v, c, s):
        r = v * c + pltpu.roll(v, head_dim // 2, 1) * s
        return r.astype(BF16).astype(F32)

    pl.semaphore_wait(barrier, 1)
    copies = []
    for k in range(kv_local):
        bias_q = bias_ref[k : k + 1, pl.ds(pl.multiple_of(core * q_cols, 128), q_cols)].astype(F32)
        for g in range(per_core):
            cols = slice(g * head_dim, (g + 1) * head_dim)
            heads[k * group + per_core * core + g] = rotate(acc_q[k, :, cols] + bias_q[:, cols], cos2, sin2)
        part = heads.at[pl.ds(k * group + per_core * core, per_core)]
        copies.append(remote(part, part, send_sem.at[k], recv_sem.at[k], partner))
        copies[-1].start()
    for k in range(kv_local):
        bias_e = bias_ref[k : k + 1, pl.ds(pl.multiple_of((group + core) * head_dim, 128), head_dim)].astype(F32)
        heads[kv_local * group + kv_local * core + k] = rotate(acc_e[k] + bias_e, cos_e, sin_e)
    part = heads.at[pl.ds(kv_local * group + kv_local * core, kv_local)]
    copies.append(remote(part, part, send_sem.at[kv_local], recv_sem.at[kv_local], partner))
    copies[-1].start()
    for c in copies:
        c.wait()
    done = pltpu.make_async_copy(heads, out_ref, out_sem)
    done.start()
    done.wait()


def qkv_heads(hidden, rope_cos, rope_sin, norm_gain, w_qkv, b_qkv, head_dim):
    num_seqs, depth = hidden.shape
    kv_local = w_qkv.shape[1]
    per_core = (w_qkv.shape[2] // head_dim - 2) // 2
    rows = kv_local * (2 * per_core + 2)
    vmem = pl.BlockSpec(memory_space=pltpu.VMEM)
    anyspace = pl.BlockSpec(memory_space=pl.ANY)
    return pl.pallas_call(
        qkv_kernel,
        out_shape=jax.ShapeDtypeStruct((rows, num_seqs, head_dim), F32),
        in_specs=[vmem] * 5 + [anyspace],
        out_specs=anyspace,
        scratch_shapes=[
            pltpu.VMEM((num_seqs, depth), BF16),
            pltpu.VMEM((rows, num_seqs, head_dim), F32),
            pltpu.VMEM((kv_local, num_seqs, per_core * head_dim), F32),
            pltpu.VMEM((kv_local, num_seqs, head_dim), F32),
            pltpu.VMEM((QKV_SLOTS, QKV_ROWS, kv_local, per_core * head_dim), BF16),
            pltpu.VMEM((QKV_SLOTS, QKV_ROWS, kv_local, head_dim), BF16),
            pltpu.SemaphoreType.DMA((QKV_SLOTS,)),
            pltpu.SemaphoreType.DMA((QKV_SLOTS,)),
            pltpu.SemaphoreType.DMA((kv_local + 1,)),
            pltpu.SemaphoreType.DMA((kv_local + 1,)),
            pltpu.SemaphoreType.DMA,
        ],
        compiler_params=pltpu.CompilerParams(collective_id=0, has_side_effects=True, vmem_limit_bytes=56 << 20),
        name="qkv_heads",
    )(hidden, norm_gain.reshape(1, depth), rope_cos.T, rope_sin.T, b_qkv, w_qkv)


ATT_SEQS = 8


def attend_kernel(lens_ref, heads_ref, sink_ref, k_ref, v_ref, k_out, v_out, num_ref, ml_ref):
    step = pl.program_id(0)
    q_rows = num_ref.shape[0]
    kv_local = (heads_ref.shape[0] - q_rows) // 2
    group = q_rows // kv_local
    rows, head_dim = k_ref.shape[1:]
    ctx_local = rows // kv_local
    base = lax.axis_index("sp") * ctx_local
    scale = head_dim**-0.5
    col = lax.broadcasted_iota(jnp.int32, (q_rows, rows), 1)
    kv_row = lax.div(lax.broadcasted_iota(jnp.int32, (q_rows, rows), 0), group)
    col_pos = jnp.where(lax.rem(col, kv_local) == kv_row, lax.div(col, kv_local), ctx_local * 1024)
    sub_pos = lax.div(lax.broadcasted_iota(jnp.int32, (16, head_dim), 0), kv_local)
    lane = lax.broadcasted_iota(jnp.int32, (q_rows, head_dim), 1)
    sink = sink_ref[...]

    @pl.when(step == 0)
    def _():
        ml_ref[...] = jnp.zeros_like(ml_ref)

    m_all = ml_ref[0:q_rows]
    l_all = ml_ref[q_rows : 2 * q_rows]
    for s in range(ATT_SEQS):
        seq = step * ATT_SEQS + s
        n = lens_ref[seq] - base
        inside = jnp.logical_and(n >= 0, n < ctx_local)
        at = jnp.where(inside, n, 0)
        start = pl.multiple_of(lax.div(at * kv_local, 16) * 16, 16)
        hit = jnp.logical_and(sub_pos == lax.rem(at, 16 // kv_local), inside)
        for cache, out, lo in ((k_ref, k_out, q_rows), (v_ref, v_out, q_rows + kv_local)):
            out[s] = cache[s]
            new = heads_ref[lo : lo + kv_local, s, :]
            new = jnp.concatenate([new] * (16 // kv_local), axis=0)
            old = cache[s, pl.ds(start, 16), :].astype(F32)
            out[s, pl.ds(start, 16), :] = jnp.where(hit, new, old).astype(BF16)
        q = heads_ref[0:q_rows, s, :].astype(BF16)
        logits = lax.dot_general(q, k_out[s], (((1,), (1,)), ((), ())), preferred_element_type=F32) * scale
        logits = jnp.where(col_pos <= n, logits, -jnp.inf)
        m = jnp.maximum(jnp.max(logits, axis=1, keepdims=True), sink)
        e = jnp.exp(logits - m[:, 0:1])
        total = jnp.sum(e, axis=1, keepdims=True)
        num_ref[:, s, :] = jnp.dot(e.astype(BF16), v_out[s], preferred_element_type=F32)
        here = lane == seq
        m_all = jnp.where(here, m, m_all)
        l_all = jnp.where(here, total, l_all)
    ml_ref[0:q_rows] = m_all
    ml_ref[q_rows : 2 * q_rows] = l_all


def attend(seq_lens, heads, sink_wide, k_rows, v_rows):
    num_seqs, rows, head_dim = k_rows.shape
    q_rows = sink_wide.shape[0]
    cache = pl.BlockSpec((ATT_SEQS, rows, head_dim), lambda i, lens: (i, 0, 0))
    return pl.pallas_call(
        attend_kernel,
        grid_spec=pltpu.PrefetchScalarGridSpec(
            num_scalar_prefetch=1,
            grid=(num_seqs // ATT_SEQS,),
            in_specs=[
                pl.BlockSpec((heads.shape[0], ATT_SEQS, head_dim), lambda i, lens: (0, i, 0)),
                pl.BlockSpec((q_rows, head_dim), lambda i, lens: (0, 0)),
                cache,
                cache,
            ],
            out_specs=[
                cache,
                cache,
                pl.BlockSpec((q_rows, ATT_SEQS, head_dim), lambda i, lens: (0, i, 0)),
                pl.BlockSpec((2 * q_rows, num_seqs), lambda i, lens: (0, 0)),
            ],
        ),
        out_shape=[
            jax.ShapeDtypeStruct(k_rows.shape, BF16),
            jax.ShapeDtypeStruct(v_rows.shape, BF16),
            jax.ShapeDtypeStruct((q_rows, num_seqs, head_dim), F32),
            jax.ShapeDtypeStruct((2 * q_rows, num_seqs), F32),
        ],
        compiler_params=pltpu.CompilerParams(dimension_semantics=("arbitrary",), vmem_limit_bytes=40 << 20),
        name="attend",
    )(seq_lens, heads, sink_wide, k_rows, v_rows)


OUT_COLS = 256
HEAD_GROUPS = 4
LAG_Y = 4
LAG_X = 3


def finish_kernel(num_ref, ml_ref, sink_ref, hid_ref, bo_ref, wo_ref, y_ref,
                  w_buf, x_buf, r1, r1ml, own, away, away_ml, r2, r2ml, fac, o_buf, r3, o_all,
                  y_send, y_recv, z_buf, x_recv, p1, p2,
                  w_sem, h_sem, s1_send, s1_recv, s2_send, s2_recv, s3_send, s3_recv,
                  y_ss, y_rs, x_ss, x_rs, p1_ss, p1_rs, p2_ss, p2_rs):
    chip, core = sp_place()
    tp = lax.axis_index("tp")
    partner = {"sp": 2 * chip + (1 - core)}
    across_x = {"sp": 2 * (1 - chip) + core}
    across_y = {"tp": 1 - tp}
    q_rows, num_seqs, head_dim = num_ref.shape
    half_h = q_rows // 2
    half_s = num_seqs // 2
    cols = w_buf.shape[1]
    chunks = cols // OUT_COLS
    per_group = half_h // HEAD_GROUPS
    mine = pl.multiple_of(core * half_h, half_h)
    theirs = pl.multiple_of((1 - core) * half_h, half_h)
    here = pl.ds(pl.multiple_of(chip * half_s, half_s), half_s)
    there = pl.ds(pl.multiple_of((1 - chip) * half_s, half_s), half_s)

    barrier = pltpu.get_barrier_semaphore()
    for peer in (partner, across_x, across_y):
        pl.semaphore_signal(barrier, inc=1, device_id=peer, device_id_type=MESH)

    parts = w_sem.shape[0]
    w_rows = w_buf.shape[0] // parts
    w_copies = []
    my_cols = pl.ds(pl.multiple_of(core * cols, 128), cols)
    for p in range(parts):
        rows = pl.ds(p * w_rows, w_rows)
        w_copies.append(pltpu.make_async_copy(wo_ref.at[rows, my_cols], w_buf.at[rows], w_sem.at[p]))
        w_copies[-1].start()
    h_copy = pltpu.make_async_copy(hid_ref.at[here, my_cols], x_buf, h_sem)
    h_copy.start()

    pl.semaphore_wait(barrier, 3)

    c_ml = remote(ml_ref, r1ml, s1_send.at[0], s1_recv.at[0], partner)
    c_there = remote(num_ref.at[pl.ds(theirs, half_h), there], r1.at[:, there], s1_send.at[1], s1_recv.at[1], partner)
    c_here = remote(num_ref.at[pl.ds(theirs, half_h), here], r1.at[:, here], s1_send.at[2], s1_recv.at[2], partner)
    for c in (c_ml, c_there, c_here):
        c.start()

    c_ml.wait_recv()
    m_a, l_a = ml_ref[pl.ds(mine, half_h)], ml_ref[pl.ds(q_rows + mine, half_h)]
    m_b, l_b = r1ml[pl.ds(mine, half_h)], r1ml[pl.ds(q_rows + mine, half_h)]
    m_chip = jnp.maximum(m_a, m_b)
    f_a = jnp.exp(m_a - m_chip)
    f_b = jnp.exp(m_b - m_chip)
    l_chip = l_a * f_a + l_b * f_b
    fac[0] = f_a.T
    fac[1] = f_b.T
    away_ml[0:half_h] = m_chip
    away_ml[half_h : 2 * half_h] = l_chip
    c2_ml = remote(away_ml, r2ml, s2_send.at[HEAD_GROUPS], s2_recv.at[HEAD_GROUPS], across_x)
    c2_ml.start()

    c_there.wait_recv()
    fa, fb = fac[0, there, :], fac[1, there, :]
    c2 = []
    for g in range(HEAD_GROUPS):
        for h in range(g * per_group, (g + 1) * per_group):
            away[h] = num_ref[mine + h, there, :] * fa[:, h : h + 1] + r1[h, there, :] * fb[:, h : h + 1]
        part = pl.ds(g * per_group, per_group)
        c2.append(remote(away.at[part], r2.at[part], s2_send.at[g], s2_recv.at[g], across_x))
        c2[-1].start()
    c_here.wait_recv()
    fa, fb = fac[0, here, :], fac[1, here, :]
    for h in range(half_h):
        own[h] = num_ref[mine + h, here, :] * fa[:, h : h + 1] + r1[h, here, :] * fb[:, h : h + 1]

    c2_ml.wait_recv()
    m_o, l_o = r2ml[0:half_h], r2ml[half_h : 2 * half_h]
    m_top = jnp.maximum(m_chip, m_o)
    f_a = jnp.exp(m_chip - m_top)
    f_b = jnp.exp(m_o - m_top)
    den = l_chip * f_a + l_o * f_b + jnp.exp(sink_ref[pl.ds(mine, half_h)] - m_top)
    fac[2] = (f_a / den).T
    fac[3] = (f_b / den).T
    fa, fb = fac[2, here, :], fac[3, here, :]
    c3 = []
    width = per_group * head_dim
    for g in range(HEAD_GROUPS):
        c2[g].wait_recv()
        for i in range(per_group):
            h = g * per_group + i
            o_buf[g, :, i * head_dim : (i + 1) * head_dim] = own[h] * fa[:, h : h + 1] + r2[h] * fb[:, h : h + 1]
        c3.append(remote(o_buf.at[g], r3.at[g], s3_send.at[g], s3_recv.at[g], partner))
        c3[-1].start()
        o_all[:, pl.ds(pl.multiple_of(core * half_h * head_dim + g * width, 128), width)] = o_buf[g].astype(BF16)
    for g in range(HEAD_GROUPS):
        c3[g].wait_recv()
        o_all[:, pl.ds(pl.multiple_of((1 - core) * half_h * head_dim + g * width, 128), width)] = r3[g].astype(BF16)
    for c in w_copies:
        c.wait()
    h_copy.wait()

    def y_copy(j):
        return remote(y_send.at[j], y_recv.at[j], y_ss.at[j], y_rs.at[j], across_y)

    def x_copy(j):
        return remote(z_buf.at[j], x_recv.at[j], x_ss.at[j], x_rs.at[j], across_x)

    def p1_copy(j):
        return remote(z_buf.at[j], p1.at[j], p1_ss.at[j], p1_rs.at[j], partner)

    def p2_copy(j):
        return remote(x_recv.at[j], p2.at[j], p2_ss.at[j], p2_rs.at[j], partner)

    def at_col(which, j):
        return pl.ds(pl.multiple_of(which * cols + j * OUT_COLS, 128), OUT_COLS)

    def body(t, _):
        @pl.when(t < chunks)
        def _():
            j = t
            w = w_buf[:, pl.ds(pl.multiple_of(j * OUT_COLS, 128), OUT_COLS)]
            y_send[j] = jnp.dot(o_all[...], w, preferred_element_type=F32)
            y_copy(j).start()

        @pl.when(jnp.logical_and(t >= LAG_Y, t < chunks + LAG_Y))
        def _():
            j = t - LAG_Y
            y_copy(j).wait_recv()
            x_part = x_buf[:, pl.ds(pl.multiple_of(j * OUT_COLS, 128), OUT_COLS)].astype(F32)
            z = (x_part + (y_send[j] + y_recv[j]) + bo_ref[:, at_col(core, j)].astype(F32)).astype(BF16)
            z_buf[j] = z.astype(F32)
            x_copy(j).start()
            p1_copy(j).start()
            y_ref[here, at_col(core, j)] = z

        @pl.when(t >= LAG_Y + LAG_X)
        def _():
            j = t - (LAG_Y + LAG_X)
            x_copy(j).wait_recv()
            p2_copy(j).start()
            y_ref[there, at_col(core, j)] = x_recv[j].astype(BF16)
            p1_copy(j).wait_recv()
            y_ref[here, at_col(1 - core, j)] = p1[j].astype(BF16)

        return 0

    lax.fori_loop(0, chunks + LAG_Y + LAG_X, body, 0)

    def tail(j, _):
        p2_copy(j).wait_recv()
        y_ref[there, at_col(1 - core, j)] = p2[j].astype(BF16)
        y_copy(j).wait_send()
        x_copy(j).wait_send()
        p1_copy(j).wait_send()
        p2_copy(j).wait_send()
        return 0

    lax.fori_loop(0, chunks, tail, 0)
    for c in (c_ml, c_there, c_here, c2_ml, *c2, *c3):
        c.wait_send()


def finish(num, ml, sink_wide, hidden, b_o, w_o):
    q_rows, num_seqs, head_dim = num.shape
    half_h, half_s = q_rows // 2, num_seqs // 2
    width = w_o.shape[1]
    cols = width // 2
    chunks = cols // OUT_COLS
    group_cols = half_h // HEAD_GROUPS * head_dim
    vmem = pl.BlockSpec(memory_space=pltpu.VMEM)
    anyspace = pl.BlockSpec(memory_space=pl.ANY)
    chunked = pltpu.VMEM((chunks, half_s, OUT_COLS), F32)
    dma = pltpu.SemaphoreType.DMA
    return pl.pallas_call(
        finish_kernel,
        out_shape=jax.ShapeDtypeStruct((num_seqs, width), BF16),
        in_specs=[vmem, vmem, vmem, anyspace, vmem, anyspace],
        out_specs=vmem,
        scratch_shapes=[
            pltpu.VMEM((w_o.shape[0], cols), BF16),
            pltpu.VMEM((half_s, cols), BF16),
            pltpu.VMEM((half_h, num_seqs, head_dim), F32),
            pltpu.VMEM((2 * q_rows, num_seqs), F32),
            pltpu.VMEM((half_h, half_s, head_dim), F32),
            pltpu.VMEM((half_h, half_s, head_dim), F32),
            pltpu.VMEM((2 * half_h, num_seqs), F32),
            pltpu.VMEM((half_h, half_s, head_dim), F32),
            pltpu.VMEM((2 * half_h, num_seqs), F32),
            pltpu.VMEM((4, num_seqs, half_h), F32),
            pltpu.VMEM((HEAD_GROUPS, half_s, group_cols), F32),
            pltpu.VMEM((HEAD_GROUPS, half_s, group_cols), F32),
            pltpu.VMEM((half_s, q_rows * head_dim), BF16),
            chunked, chunked, chunked, chunked, chunked, chunked,
            dma((4,)), dma,
            dma((3,)), dma((3,)),
            dma((HEAD_GROUPS + 1,)), dma((HEAD_GROUPS + 1,)),
            dma((HEAD_GROUPS,)), dma((HEAD_GROUPS,)),
            *[dma((chunks,))] * 8,
        ],
        compiler_params=pltpu.CompilerParams(collective_id=1, has_side_effects=True, vmem_limit_bytes=60 << 20),
        name="finish",
    )(num, ml, sink_wide, hidden, b_o.reshape(1, width), w_o)


def solution(mesh):
    cache_spec = P("dp", "sp", "tp", None)

    def block_step(hidden, seq_lens, rope_cos, rope_sin, k_cache, v_cache, norm_gain, w_qkv, b_qkv, sink_logits, w_o, b_o):
        num_seqs, ctx_local, kv_local, head_dim = k_cache.shape
        heads = qkv_heads(hidden, rope_cos, rope_sin, norm_gain, w_qkv, b_qkv, head_dim)
        sink_wide = jnp.broadcast_to(sink_logits[:, None], (sink_logits.shape[0], num_seqs))
        rows = (num_seqs, ctx_local * kv_local, head_dim)
        k_out, v_out, num, ml = attend(seq_lens, heads, sink_wide, k_cache.reshape(rows), v_cache.reshape(rows))
        out_hidden = finish(num, ml, sink_wide, hidden, b_o, w_o)
        return out_hidden, k_out.reshape(k_cache.shape), v_out.reshape(v_cache.shape)

    return jax.shard_map(block_step, mesh=mesh, in_specs=(P("dp", None), P("dp"), P("dp", None), P("dp", None), cache_spec, cache_spec, P(None), P(None, "tp", None), P("tp", None), P("tp"), P("tp", None), P(None)), out_specs=(P("dp", None), cache_spec, cache_spec), check_vma=False)
```

```python
import functools

import jax
import jax.numpy as jnp
from jax import lax
from jax.experimental import pallas as pl
from jax.experimental.pallas import tpu as pltpu
from jax.sharding import PartitionSpec as P

NORM_EPS = 1e-5
F32 = jnp.float32
BF16 = jnp.bfloat16
MESH = pl.DeviceIdType.MESH


def sp_place():
    sp = lax.axis_index("sp")
    return lax.div(sp, 2), lax.rem(sp, 2)


def remote(src, dst, send_sem, recv_sem, where):
    return pltpu.make_async_remote_copy(src_ref=src, dst_ref=dst, send_sem=send_sem, recv_sem=recv_sem, device_id=where, device_id_type=MESH)


def column(row_ref, count):
    wide = jnp.broadcast_to(row_ref[...], (count, count))
    same = lax.broadcasted_iota(jnp.int32, (count, count), 0) == lax.broadcasted_iota(jnp.int32, (count, count), 1)
    return jnp.sum(jnp.where(same, wide, 0.0), axis=1, keepdims=True)


QKV_ROWS = 512
QKV_SLOTS = 3


def qkv_kernel(x_ref, gain_ref, cos_ref, sin_ref, bias_ref, w_ref, out_ref, normed, gain, heads, acc_q, acc_e, wq_buf, we_buf, wq_sem, we_sem, send_sem, recv_sem, out_sem):
    chip, core = sp_place()
    partner = {"sp": 2 * chip + (1 - core)}
    num_seqs, depth = x_ref.shape
    head_dim = acc_e.shape[2]
    q_cols = acc_q.shape[2]
    kv_local = acc_q.shape[0]
    per_core = q_cols // head_dim
    group = 2 * per_core
    steps = depth // QKV_ROWS

    def fetch(step, slot):
        rows = pl.ds(step * QKV_ROWS, QKV_ROWS)
        cq = pltpu.make_async_copy(w_ref.at[rows, :, pl.ds(pl.multiple_of(core * q_cols, 128), q_cols)], wq_buf.at[slot], wq_sem.at[slot])
        ce = pltpu.make_async_copy(w_ref.at[rows, :, pl.ds(pl.multiple_of((group + core) * head_dim, 128), head_dim)], we_buf.at[slot], we_sem.at[slot])
        return cq, ce

    for s in range(QKV_SLOTS - 1):
        for c in fetch(s, s):
            c.start()

    barrier = pltpu.get_barrier_semaphore()
    pl.semaphore_signal(barrier, inc=1, device_id=partner, device_id_type=MESH)

    gain[...] = gain_ref[...].astype(F32)

    def norm_rows(r, _):
        rows = pl.ds(pl.multiple_of(r * 16, 16), 16)
        xw = x_ref[rows, :].astype(F32)
        inv = lax.rsqrt(jnp.mean(xw * xw, axis=-1, keepdims=True) + NORM_EPS)
        for t in range(depth // head_dim):
            cols = slice(t * head_dim, (t + 1) * head_dim)
            normed[rows, cols] = (xw[:, cols] * inv * gain[t : t + 1, :]).astype(BF16)
        return 0

    lax.fori_loop(0, num_seqs // 16, norm_rows, 0)
    acc_q[...] = jnp.zeros_like(acc_q)
    acc_e[...] = jnp.zeros_like(acc_e)

    def step_fn(step, _):
        slot = lax.rem(step, QKV_SLOTS)
        for c in fetch(step, slot):
            c.wait()

        @pl.when(step + QKV_SLOTS - 1 < steps)
        def _():
            for c in fetch(step + QKV_SLOTS - 1, lax.rem(step + QKV_SLOTS - 1, QKV_SLOTS)):
                c.start()

        h = normed[:, pl.ds(pl.multiple_of(step * QKV_ROWS, 128), QKV_ROWS)]
        wq = jnp.swapaxes(wq_buf[slot], 0, 1)
        we = jnp.swapaxes(we_buf[slot], 0, 1)
        for k in range(kv_local):
            acc_q[k] += jnp.dot(h, wq[k], preferred_element_type=F32)
            acc_e[k] += jnp.dot(h, we[k], preferred_element_type=F32)
        return 0

    lax.fori_loop(0, steps, step_fn, 0)

    cos_t = cos_ref[...].T
    sin_t = sin_ref[...].T
    cos2 = jnp.concatenate([cos_t, cos_t], axis=1)
    sin2 = jnp.concatenate([-sin_t, sin_t], axis=1)
    is_key = core == 0
    cos_e = jnp.where(is_key, cos2, jnp.ones_like(cos2))
    sin_e = jnp.where(is_key, sin2, jnp.zeros_like(sin2))

    def rotate(v, c, s):
        r = v * c + pltpu.roll(v, head_dim // 2, 1) * s
        return r.astype(BF16).astype(F32)

    pl.semaphore_wait(barrier, 1)
    copies = []
    for k in range(kv_local):
        bias_q = bias_ref[k : k + 1, pl.ds(pl.multiple_of(core * q_cols, 128), q_cols)].astype(F32)
        for g in range(per_core):
            cols = slice(g * head_dim, (g + 1) * head_dim)
            heads[k * group + per_core * core + g] = rotate(acc_q[k, :, cols] + bias_q[:, cols], cos2, sin2)
        part = heads.at[pl.ds(k * group + per_core * core, per_core)]
        copies.append(remote(part, part, send_sem.at[k], recv_sem.at[k], partner))
        copies[-1].start()
    for k in range(kv_local):
        bias_e = bias_ref[k : k + 1, pl.ds(pl.multiple_of((group + core) * head_dim, 128), head_dim)].astype(F32)
        heads[kv_local * group + kv_local * core + k] = rotate(acc_e[k] + bias_e, cos_e, sin_e)
    part = heads.at[pl.ds(kv_local * group + kv_local * core, kv_local)]
    copies.append(remote(part, part, send_sem.at[kv_local], recv_sem.at[kv_local], partner))
    copies[-1].start()
    for c in copies:
        c.wait()
    done = pltpu.make_async_copy(heads, out_ref, out_sem)
    done.start()
    done.wait()


def qkv_heads(hidden, rope_cos, rope_sin, norm_gain, w_qkv, b_qkv, head_dim):
    num_seqs, depth = hidden.shape
    kv_local = w_qkv.shape[1]
    per_core = (w_qkv.shape[2] // head_dim - 2) // 2
    rows = kv_local * (2 * per_core + 2)
    vmem = pl.BlockSpec(memory_space=pltpu.VMEM)
    anyspace = pl.BlockSpec(memory_space=pl.ANY)
    return pl.pallas_call(
        qkv_kernel,
        out_shape=jax.ShapeDtypeStruct((rows, num_seqs, head_dim), F32),
        in_specs=[vmem] * 5 + [anyspace],
        out_specs=anyspace,
        scratch_shapes=[
            pltpu.VMEM((num_seqs, depth), BF16),
            pltpu.VMEM((depth // head_dim, head_dim), F32),
            pltpu.VMEM((rows, num_seqs, head_dim), F32),
            pltpu.VMEM((kv_local, num_seqs, per_core * head_dim), F32),
            pltpu.VMEM((kv_local, num_seqs, head_dim), F32),
            pltpu.VMEM((QKV_SLOTS, QKV_ROWS, kv_local, per_core * head_dim), BF16),
            pltpu.VMEM((QKV_SLOTS, QKV_ROWS, kv_local, head_dim), BF16),
            pltpu.SemaphoreType.DMA((QKV_SLOTS,)),
            pltpu.SemaphoreType.DMA((QKV_SLOTS,)),
            pltpu.SemaphoreType.DMA((kv_local + 1,)),
            pltpu.SemaphoreType.DMA((kv_local + 1,)),
            pltpu.SemaphoreType.DMA,
        ],
        compiler_params=pltpu.CompilerParams(collective_id=0, has_side_effects=True, vmem_limit_bytes=56 << 20),
        name="qkv_heads",
    )(hidden, norm_gain.reshape(depth // head_dim, head_dim), rope_cos.T, rope_sin.T, b_qkv, w_qkv)


ATT_SEQS = 8


def attend_kernel(lens_ref, heads_ref, sink_ref, k_ref, v_ref, k_out, v_out, num_ref, ml_ref):
    step = pl.program_id(0)
    q_rows = num_ref.shape[0]
    kv_local = (heads_ref.shape[0] - q_rows) // 2
    group = q_rows // kv_local
    rows, head_dim = k_ref.shape[1:]
    ctx_local = rows // kv_local
    base = lax.axis_index("sp") * ctx_local
    scale = head_dim**-0.5
    col = lax.broadcasted_iota(jnp.int32, (q_rows, rows), 1)
    kv_row = lax.div(lax.broadcasted_iota(jnp.int32, (q_rows, rows), 0), group)
    col_pos = jnp.where(lax.rem(col, kv_local) == kv_row, lax.div(col, kv_local), ctx_local * 1024)
    sub_pos = lax.div(lax.broadcasted_iota(jnp.int32, (16, head_dim), 0), kv_local)
    lane = lax.broadcasted_iota(jnp.int32, (q_rows, ml_ref.shape[1]), 1)

    @pl.when(step == 0)
    def _():
        ml_ref[...] = jnp.zeros_like(ml_ref)

    seqs = range(ATT_SEQS)
    rel = []
    for s in seqs:
        k_out[s] = k_ref[s]
        v_out[s] = v_ref[s]
    for s in seqs:
        n = lens_ref[step * ATT_SEQS + s] - base
        rel.append(n)
        inside = jnp.logical_and(n >= 0, n < ctx_local)
        at = jnp.where(inside, n, 0)
        start = pl.multiple_of(lax.div(at * kv_local, 16) * 16, 16)
        hit = jnp.logical_and(sub_pos == lax.rem(at, 16 // kv_local), inside)
        for cache, out, lo in ((k_ref, k_out, q_rows), (v_ref, v_out, q_rows + kv_local)):
            new = heads_ref[lo : lo + kv_local, s, :]
            new = jnp.concatenate([new] * (16 // kv_local), axis=0)
            old = cache[s, pl.ds(start, 16), :].astype(F32)
            out[s, pl.ds(start, 16), :] = jnp.where(hit, new, old).astype(BF16)
    sink = column(sink_ref, q_rows)
    queries = [heads_ref[0:q_rows, s, :].astype(BF16) for s in seqs]
    logits = [lax.dot_general(queries[s], k_out[s], (((1,), (1,)), ((), ())), preferred_element_type=F32) for s in seqs]
    logits = [jnp.where(col_pos <= rel[s], logits[s] * scale, -jnp.inf) for s in seqs]
    tops = [jnp.maximum(jnp.max(logits[s], axis=1, keepdims=True), sink) for s in seqs]
    weights = [jnp.exp(logits[s] - tops[s]) for s in seqs]
    totals = [jnp.sum(weights[s], axis=1, keepdims=True) for s in seqs]
    sums = [jnp.dot(weights[s].astype(BF16), v_out[s], preferred_element_type=F32) for s in seqs]
    m_all = ml_ref[0:q_rows]
    l_all = ml_ref[q_rows : 2 * q_rows]
    for s in seqs:
        num_ref[:, s, :] = sums[s]
        here = lane == step * ATT_SEQS + s
        m_all = jnp.where(here, tops[s], m_all)
        l_all = jnp.where(here, totals[s], l_all)
    ml_ref[0:q_rows] = m_all
    ml_ref[q_rows : 2 * q_rows] = l_all


def attend(seq_lens, heads, sinks, k_rows, v_rows):
    num_seqs, rows, head_dim = k_rows.shape
    q_rows = sinks.shape[1]
    cache = pl.BlockSpec((ATT_SEQS, rows, head_dim), lambda i, lens: (i, 0, 0))
    return pl.pallas_call(
        attend_kernel,
        grid_spec=pltpu.PrefetchScalarGridSpec(
            num_scalar_prefetch=1,
            grid=(num_seqs // ATT_SEQS,),
            in_specs=[
                pl.BlockSpec((heads.shape[0], ATT_SEQS, head_dim), lambda i, lens: (0, i, 0)),
                pl.BlockSpec((1, q_rows), lambda i, lens: (0, 0)),
                cache,
                cache,
            ],
            out_specs=[
                cache,
                cache,
                pl.BlockSpec((q_rows, ATT_SEQS, head_dim), lambda i, lens: (0, i, 0)),
                pl.BlockSpec((2 * q_rows, num_seqs), lambda i, lens: (0, 0)),
            ],
        ),
        out_shape=[
            jax.ShapeDtypeStruct(k_rows.shape, BF16),
            jax.ShapeDtypeStruct(v_rows.shape, BF16),
            jax.ShapeDtypeStruct((q_rows, num_seqs, head_dim), F32),
            jax.ShapeDtypeStruct((2 * q_rows, num_seqs), F32),
        ],
        compiler_params=pltpu.CompilerParams(dimension_semantics=("arbitrary",), vmem_limit_bytes=60 << 20),
        name="attend",
    )(seq_lens, heads, sinks, k_rows, v_rows)


OUT_COLS = 256
HEAD_GROUPS = 4
LAG_Y = 4
LAG_X = 3


def finish_kernel(num_ref, ml_ref, sink_ref, hid_ref, bo_ref, wo_ref, y_ref,
                  w_buf, x_buf, sink_col, bo_f32, r1, r1ml, own, away, away_ml, r2, r2ml, fac, o_buf, r3, o_all,
                  y_send, y_recv, z_buf, x_recv, p1, p2,
                  w_sem, h_sem, s1_send, s1_recv, s2_send, s2_recv, s3_send, s3_recv,
                  y_ss, y_rs, x_ss, x_rs, p1_ss, p1_rs, p2_ss, p2_rs):
    chip, core = sp_place()
    tp = lax.axis_index("tp")
    partner = {"sp": 2 * chip + (1 - core)}
    across_x = {"sp": 2 * (1 - chip) + core}
    across_y = {"tp": 1 - tp}
    q_rows, num_seqs, head_dim = num_ref.shape
    half_h = q_rows // 2
    half_s = num_seqs // 2
    cols = w_buf.shape[1]
    chunks = cols // OUT_COLS
    per_group = half_h // HEAD_GROUPS
    mine = pl.multiple_of(core * half_h, half_h)
    theirs = pl.multiple_of((1 - core) * half_h, half_h)
    here = pl.ds(pl.multiple_of(chip * half_s, half_s), half_s)
    there = pl.ds(pl.multiple_of((1 - chip) * half_s, half_s), half_s)

    barrier = pltpu.get_barrier_semaphore()
    for peer in (partner, across_x, across_y):
        pl.semaphore_signal(barrier, inc=1, device_id=peer, device_id_type=MESH)

    parts = w_sem.shape[0]
    w_rows = w_buf.shape[0] // parts
    w_copies = []
    my_cols = pl.ds(pl.multiple_of(core * cols, 128), cols)
    for p in range(parts):
        rows = pl.ds(p * w_rows, w_rows)
        w_copies.append(pltpu.make_async_copy(wo_ref.at[rows, my_cols], w_buf.at[rows], w_sem.at[p]))
        w_copies[-1].start()
    h_copy = pltpu.make_async_copy(hid_ref.at[here, my_cols], x_buf, h_sem)
    h_copy.start()

    sink_col[...] = jnp.broadcast_to(column(sink_ref, q_rows), sink_col.shape)
    bo_f32[...] = bo_ref[...].astype(F32)
    pl.semaphore_wait(barrier, 3)

    c_ml = remote(ml_ref, r1ml, s1_send.at[0], s1_recv.at[0], partner)
    c_there = remote(num_ref.at[pl.ds(theirs, half_h), there], r1.at[:, there], s1_send.at[1], s1_recv.at[1], partner)
    c_here = remote(num_ref.at[pl.ds(theirs, half_h), here], r1.at[:, here], s1_send.at[2], s1_recv.at[2], partner)
    for c in (c_ml, c_there, c_here):
        c.start()

    c_ml.wait_recv()
    m_a, l_a = ml_ref[pl.ds(mine, half_h)], ml_ref[pl.ds(q_rows + mine, half_h)]
    m_b, l_b = r1ml[pl.ds(mine, half_h)], r1ml[pl.ds(q_rows + mine, half_h)]
    m_chip = jnp.maximum(m_a, m_b)
    f_a = jnp.exp(m_a - m_chip)
    f_b = jnp.exp(m_b - m_chip)
    l_chip = l_a * f_a + l_b * f_b
    fac[0] = f_a.T
    fac[1] = f_b.T
    away_ml[0:half_h] = m_chip
    away_ml[half_h : 2 * half_h] = l_chip
    c2_ml = remote(away_ml, r2ml, s2_send.at[HEAD_GROUPS], s2_recv.at[HEAD_GROUPS], across_x)
    c2_ml.start()

    c_there.wait_recv()
    fa, fb = fac[0, there, :], fac[1, there, :]
    c2 = []
    for g in range(HEAD_GROUPS):
        for h in range(g * per_group, (g + 1) * per_group):
            away[h] = num_ref[mine + h, there, :] * fa[:, h : h + 1] + r1[h, there, :] * fb[:, h : h + 1]
        part = pl.ds(g * per_group, per_group)
        c2.append(remote(away.at[part], r2.at[part], s2_send.at[g], s2_recv.at[g], across_x))
        c2[-1].start()
    c_here.wait_recv()
    fa, fb = fac[0, here, :], fac[1, here, :]
    for h in range(half_h):
        own[h] = num_ref[mine + h, here, :] * fa[:, h : h + 1] + r1[h, here, :] * fb[:, h : h + 1]

    c2_ml.wait_recv()
    m_o, l_o = r2ml[0:half_h], r2ml[half_h : 2 * half_h]
    m_top = jnp.maximum(m_chip, m_o)
    f_a = jnp.exp(m_chip - m_top)
    f_b = jnp.exp(m_o - m_top)
    den = l_chip * f_a + l_o * f_b + jnp.exp(sink_col[pl.ds(mine, half_h)] - m_top)
    fac[2] = (f_a / den).T
    fac[3] = (f_b / den).T
    fa, fb = fac[2, here, :], fac[3, here, :]
    c3 = []
    width = per_group * head_dim
    for g in range(HEAD_GROUPS):
        c2[g].wait_recv()
        for i in range(per_group):
            h = g * per_group + i
            o_buf[g, :, i * head_dim : (i + 1) * head_dim] = own[h] * fa[:, h : h + 1] + r2[h] * fb[:, h : h + 1]
        c3.append(remote(o_buf.at[g], r3.at[g], s3_send.at[g], s3_recv.at[g], partner))
        c3[-1].start()
        o_all[:, pl.ds(pl.multiple_of(core * half_h * head_dim + g * width, 128), width)] = o_buf[g].astype(BF16)
    for g in range(HEAD_GROUPS):
        c3[g].wait_recv()
        o_all[:, pl.ds(pl.multiple_of((1 - core) * half_h * head_dim + g * width, 128), width)] = r3[g].astype(BF16)
    for c in w_copies:
        c.wait()
    h_copy.wait()

    def y_copy(j):
        return remote(y_send.at[j], y_recv.at[j], y_ss.at[j], y_rs.at[j], across_y)

    def x_copy(j):
        return remote(z_buf.at[j], x_recv.at[j], x_ss.at[j], x_rs.at[j], across_x)

    def p1_copy(j):
        return remote(z_buf.at[j], p1.at[j], p1_ss.at[j], p1_rs.at[j], partner)

    def p2_copy(j):
        return remote(x_recv.at[j], p2.at[j], p2_ss.at[j], p2_rs.at[j], partner)

    def at_col(which, j):
        return pl.ds(pl.multiple_of(which * cols + j * OUT_COLS, 128), OUT_COLS)

    def body(t, _):
        @pl.when(t < chunks)
        def _():
            j = t
            w = w_buf[:, pl.ds(pl.multiple_of(j * OUT_COLS, 128), OUT_COLS)]
            y_send[j] = jnp.dot(o_all[...], w, preferred_element_type=F32)
            y_copy(j).start()

        @pl.when(jnp.logical_and(t >= LAG_Y, t < chunks + LAG_Y))
        def _():
            j = t - LAG_Y
            y_copy(j).wait_recv()
            x_part = x_buf[:, pl.ds(pl.multiple_of(j * OUT_COLS, 128), OUT_COLS)].astype(F32)
            row = (core * cols + j * OUT_COLS) // head_dim
            bias = jnp.concatenate([bo_f32[pl.ds(row + i, 1), :] for i in range(OUT_COLS // head_dim)], axis=1)
            z = (x_part + (y_send[j] + y_recv[j]) + bias).astype(BF16)
            z_buf[j] = z.astype(F32)
            x_copy(j).start()
            p1_copy(j).start()
            y_ref[here, at_col(core, j)] = z

        @pl.when(t >= LAG_Y + LAG_X)
        def _():
            j = t - (LAG_Y + LAG_X)
            x_copy(j).wait_recv()
            p2_copy(j).start()
            y_ref[there, at_col(core, j)] = x_recv[j].astype(BF16)
            p1_copy(j).wait_recv()
            y_ref[here, at_col(1 - core, j)] = p1[j].astype(BF16)

        return 0

    lax.fori_loop(0, chunks + LAG_Y + LAG_X, body, 0)

    def tail(j, _):
        p2_copy(j).wait_recv()
        y_ref[there, at_col(1 - core, j)] = p2[j].astype(BF16)
        y_copy(j).wait_send()
        x_copy(j).wait_send()
        p1_copy(j).wait_send()
        p2_copy(j).wait_send()
        return 0

    lax.fori_loop(0, chunks, tail, 0)
    for c in (c_ml, c_there, c_here, c2_ml, *c2, *c3):
        c.wait_send()


def finish(num, ml, sinks, hidden, b_o, w_o):
    q_rows, num_seqs, head_dim = num.shape
    half_h, half_s = q_rows // 2, num_seqs // 2
    width = w_o.shape[1]
    cols = width // 2
    chunks = cols // OUT_COLS
    group_cols = half_h // HEAD_GROUPS * head_dim
    vmem = pl.BlockSpec(memory_space=pltpu.VMEM)
    anyspace = pl.BlockSpec(memory_space=pl.ANY)
    chunked = pltpu.VMEM((chunks, half_s, OUT_COLS), F32)
    dma = pltpu.SemaphoreType.DMA
    return pl.pallas_call(
        finish_kernel,
        out_shape=jax.ShapeDtypeStruct((num_seqs, width), BF16),
        in_specs=[vmem, vmem, vmem, anyspace, vmem, anyspace],
        out_specs=vmem,
        scratch_shapes=[
            pltpu.VMEM((w_o.shape[0], cols), BF16),
            pltpu.VMEM((half_s, cols), BF16),
            pltpu.VMEM((q_rows, num_seqs), F32),
            pltpu.VMEM((width // head_dim, head_dim), F32),
            pltpu.VMEM((half_h, num_seqs, head_dim), F32),
            pltpu.VMEM((2 * q_rows, num_seqs), F32),
            pltpu.VMEM((half_h, half_s, head_dim), F32),
            pltpu.VMEM((half_h, half_s, head_dim), F32),
            pltpu.VMEM((2 * half_h, num_seqs), F32),
            pltpu.VMEM((half_h, half_s, head_dim), F32),
            pltpu.VMEM((2 * half_h, num_seqs), F32),
            pltpu.VMEM((4, num_seqs, half_h), F32),
            pltpu.VMEM((HEAD_GROUPS, half_s, group_cols), F32),
            pltpu.VMEM((HEAD_GROUPS, half_s, group_cols), F32),
            pltpu.VMEM((half_s, q_rows * head_dim), BF16),
            chunked, chunked, chunked, chunked, chunked, chunked,
            dma((4,)), dma,
            dma((3,)), dma((3,)),
            dma((HEAD_GROUPS + 1,)), dma((HEAD_GROUPS + 1,)),
            dma((HEAD_GROUPS,)), dma((HEAD_GROUPS,)),
            *[dma((chunks,))] * 8,
        ],
        compiler_params=pltpu.CompilerParams(collective_id=1, has_side_effects=True, vmem_limit_bytes=60 << 20),
        name="finish",
    )(num, ml, sinks, hidden, b_o.reshape(width // head_dim, head_dim), w_o)


def solution(mesh):
    cache_spec = P("dp", "sp", "tp", None)

    def block_step(hidden, seq_lens, rope_cos, rope_sin, k_cache, v_cache, norm_gain, w_qkv, b_qkv, sink_logits, w_o, b_o):
        num_seqs, ctx_local, kv_local, head_dim = k_cache.shape
        heads = qkv_heads(hidden, rope_cos, rope_sin, norm_gain, w_qkv, b_qkv, head_dim)
        sinks = sink_logits.reshape(1, sink_logits.shape[0])
        rows = (num_seqs, ctx_local * kv_local, head_dim)
        k_out, v_out, num, ml = attend(seq_lens, heads, sinks, k_cache.reshape(rows), v_cache.reshape(rows))
        out_hidden = finish(num, ml, sinks, hidden, b_o, w_o)
        return out_hidden, k_out.reshape(k_cache.shape), v_out.reshape(v_cache.shape)

    return jax.shard_map(block_step, mesh=mesh, in_specs=(P("dp", None), P("dp"), P("dp", None), P("dp", None), cache_spec, cache_spec, P(None), P(None, "tp", None), P("tp", None), P("tp"), P("tp", None), P(None)), out_specs=(P("dp", None), cache_spec, cache_spec), check_vma=False)
```

```python
import functools

import jax
import jax.numpy as jnp
from jax import lax
from jax.experimental import pallas as pl
from jax.experimental.pallas import tpu as pltpu
from jax.sharding import PartitionSpec as P

NORM_EPS = 1e-5
F32 = jnp.float32
BF16 = jnp.bfloat16
MESH = pl.DeviceIdType.MESH


def sp_place():
    sp = lax.axis_index("sp")
    return lax.div(sp, 2), lax.rem(sp, 2)


def remote(src, dst, send_sem, recv_sem, where):
    return pltpu.make_async_remote_copy(src_ref=src, dst_ref=dst, send_sem=send_sem, recv_sem=recv_sem, device_id=where, device_id_type=MESH)


def column(row_ref, count):
    wide = jnp.broadcast_to(row_ref[...], (count, count))
    same = lax.broadcasted_iota(jnp.int32, (count, count), 0) == lax.broadcasted_iota(jnp.int32, (count, count), 1)
    return jnp.sum(jnp.where(same, wide, 0.0), axis=1, keepdims=True)


QKV_ROWS = 512
QKV_SLOTS = 3


def qkv_kernel(x_ref, gain_ref, cos_ref, sin_ref, bias_ref, w_ref, out_ref, normed, gain, heads, acc_q, acc_e, wq_buf, we_buf, wq_sem, we_sem, send_sem, recv_sem, out_sem):
    chip, core = sp_place()
    partner = {"sp": 2 * chip + (1 - core)}
    num_seqs, depth = x_ref.shape
    head_dim = acc_e.shape[2]
    q_cols = acc_q.shape[2]
    kv_local = acc_q.shape[0]
    per_core = q_cols // head_dim
    group = 2 * per_core
    steps = depth // QKV_ROWS

    def fetch(step, slot):
        rows = pl.ds(step * QKV_ROWS, QKV_ROWS)
        cq = pltpu.make_async_copy(w_ref.at[rows, :, pl.ds(pl.multiple_of(core * q_cols, 128), q_cols)], wq_buf.at[slot], wq_sem.at[slot])
        ce = pltpu.make_async_copy(w_ref.at[rows, :, pl.ds(pl.multiple_of((group + core) * head_dim, 128), head_dim)], we_buf.at[slot], we_sem.at[slot])
        return cq, ce

    for s in range(QKV_SLOTS - 1):
        for c in fetch(s, s):
            c.start()

    barrier = pltpu.get_barrier_semaphore()
    pl.semaphore_signal(barrier, inc=1, device_id=partner, device_id_type=MESH)

    gain[...] = gain_ref[...].astype(F32)

    def norm_rows(r, _):
        rows = pl.ds(pl.multiple_of(r * 16, 16), 16)
        xw = x_ref[rows, :].astype(F32)
        inv = lax.rsqrt(jnp.mean(xw * xw, axis=-1, keepdims=True) + NORM_EPS)
        for t in range(depth // head_dim):
            cols = slice(t * head_dim, (t + 1) * head_dim)
            normed[rows, cols] = (xw[:, cols] * inv * gain[t : t + 1, :]).astype(BF16)
        return 0

    lax.fori_loop(0, num_seqs // 16, norm_rows, 0)
    acc_q[...] = jnp.zeros_like(acc_q)
    acc_e[...] = jnp.zeros_like(acc_e)

    def step_fn(step, _):
        slot = lax.rem(step, QKV_SLOTS)
        for c in fetch(step, slot):
            c.wait()

        @pl.when(step + QKV_SLOTS - 1 < steps)
        def _():
            for c in fetch(step + QKV_SLOTS - 1, lax.rem(step + QKV_SLOTS - 1, QKV_SLOTS)):
                c.start()

        h = normed[:, pl.ds(pl.multiple_of(step * QKV_ROWS, 128), QKV_ROWS)]
        wq = jnp.swapaxes(wq_buf[slot], 0, 1)
        we = jnp.swapaxes(we_buf[slot], 0, 1)
        for k in range(kv_local):
            acc_q[k] += jnp.dot(h, wq[k], preferred_element_type=F32)
            acc_e[k] += jnp.dot(h, we[k], preferred_element_type=F32)
        return 0

    lax.fori_loop(0, steps, step_fn, 0)

    cos_t = cos_ref[...].T
    sin_t = sin_ref[...].T
    cos2 = jnp.concatenate([cos_t, cos_t], axis=1)
    sin2 = jnp.concatenate([-sin_t, sin_t], axis=1)
    is_key = core == 0
    cos_e = jnp.where(is_key, cos2, jnp.ones_like(cos2))
    sin_e = jnp.where(is_key, sin2, jnp.zeros_like(sin2))

    def rotate(v, c, s):
        r = v * c + pltpu.roll(v, head_dim // 2, 1) * s
        return r.astype(BF16).astype(F32)

    pl.semaphore_wait(barrier, 1)
    copies = []
    for k in range(kv_local):
        bias_q = bias_ref[k : k + 1, pl.ds(pl.multiple_of(core * q_cols, 128), q_cols)].astype(F32)
        for g in range(per_core):
            cols = slice(g * head_dim, (g + 1) * head_dim)
            heads[k * group + per_core * core + g] = rotate(acc_q[k, :, cols] + bias_q[:, cols], cos2, sin2)
        part = heads.at[pl.ds(k * group + per_core * core, per_core)]
        copies.append(remote(part, part, send_sem.at[k], recv_sem.at[k], partner))
        copies[-1].start()
    for k in range(kv_local):
        bias_e = bias_ref[k : k + 1, pl.ds(pl.multiple_of((group + core) * head_dim, 128), head_dim)].astype(F32)
        heads[kv_local * group + kv_local * core + k] = rotate(acc_e[k] + bias_e, cos_e, sin_e)
    part = heads.at[pl.ds(kv_local * group + kv_local * core, kv_local)]
    copies.append(remote(part, part, send_sem.at[kv_local], recv_sem.at[kv_local], partner))
    copies[-1].start()
    for c in copies:
        c.wait()
    done = pltpu.make_async_copy(heads, out_ref, out_sem)
    done.start()
    done.wait()


def qkv_heads(hidden, rope_cos, rope_sin, norm_gain, w_qkv, b_qkv, head_dim):
    num_seqs, depth = hidden.shape
    kv_local = w_qkv.shape[1]
    per_core = (w_qkv.shape[2] // head_dim - 2) // 2
    rows = kv_local * (2 * per_core + 2)
    vmem = pl.BlockSpec(memory_space=pltpu.VMEM)
    anyspace = pl.BlockSpec(memory_space=pl.ANY)
    return pl.pallas_call(
        qkv_kernel,
        out_shape=jax.ShapeDtypeStruct((rows, num_seqs, head_dim), F32),
        in_specs=[vmem] * 5 + [anyspace],
        out_specs=anyspace,
        scratch_shapes=[
            pltpu.VMEM((num_seqs, depth), BF16),
            pltpu.VMEM((depth // head_dim, head_dim), F32),
            pltpu.VMEM((rows, num_seqs, head_dim), F32),
            pltpu.VMEM((kv_local, num_seqs, per_core * head_dim), F32),
            pltpu.VMEM((kv_local, num_seqs, head_dim), F32),
            pltpu.VMEM((QKV_SLOTS, QKV_ROWS, kv_local, per_core * head_dim), BF16),
            pltpu.VMEM((QKV_SLOTS, QKV_ROWS, kv_local, head_dim), BF16),
            pltpu.SemaphoreType.DMA((QKV_SLOTS,)),
            pltpu.SemaphoreType.DMA((QKV_SLOTS,)),
            pltpu.SemaphoreType.DMA((kv_local + 1,)),
            pltpu.SemaphoreType.DMA((kv_local + 1,)),
            pltpu.SemaphoreType.DMA,
        ],
        compiler_params=pltpu.CompilerParams(collective_id=0, has_side_effects=True, vmem_limit_bytes=56 << 20),
        name="qkv_heads",
    )(hidden, norm_gain.reshape(depth // head_dim, head_dim), rope_cos.T, rope_sin.T, b_qkv, w_qkv)


ATT_SEQS = 8


def attend_kernel(lens_ref, heads_ref, sink_ref, k_ref, v_ref, k_out, v_out, num_ref, ml_ref, k_buf, v_buf, h_buf, n_buf, k_in, v_in, h_in, k_back, v_back, n_back):
    num_seqs, rows, head_dim = k_buf.shape
    q_rows = n_buf.shape[0]
    kv_local = (h_buf.shape[0] - q_rows) // 2
    group = q_rows // kv_local
    ctx_local = rows // kv_local
    steps = num_seqs // ATT_SEQS
    base = lax.axis_index("sp") * ctx_local
    scale = head_dim**-0.5

    def block(step):
        return pl.ds(pl.multiple_of(step * ATT_SEQS, ATT_SEQS), ATT_SEQS)

    def loads(step):
        at = block(step)
        return (
            pltpu.make_async_copy(heads_ref.at[:, at], h_buf.at[:, at], h_in.at[step]),
            pltpu.make_async_copy(k_ref.at[at], k_buf.at[at], k_in.at[step]),
            pltpu.make_async_copy(v_ref.at[at], v_buf.at[at], v_in.at[step]),
        )

    def stores(step):
        at = block(step)
        return (
            pltpu.make_async_copy(k_buf.at[at], k_out.at[at], k_back.at[step]),
            pltpu.make_async_copy(v_buf.at[at], v_out.at[at], v_back.at[step]),
            pltpu.make_async_copy(n_buf.at[:, at], num_ref.at[:, at], n_back.at[step]),
        )

    for step in range(steps):
        for c in loads(step):
            c.start()

    col = lax.broadcasted_iota(jnp.int32, (q_rows, rows), 1)
    kv_row = lax.div(lax.broadcasted_iota(jnp.int32, (q_rows, rows), 0), group)
    col_pos = jnp.where(lax.rem(col, kv_local) == kv_row, lax.div(col, kv_local), ctx_local * 1024)
    sub_pos = lax.div(lax.broadcasted_iota(jnp.int32, (16, head_dim), 0), kv_local)
    lane = lax.broadcasted_iota(jnp.int32, (q_rows, num_seqs), 1)
    sink = column(sink_ref, q_rows)
    seqs = range(ATT_SEQS)

    def step_fn(step, carry):
        m_all, l_all = carry
        for c in loads(step):
            c.wait()
        first = step * ATT_SEQS
        heads = h_buf.at[:, block(step)]
        rel = []
        for s in seqs:
            n = lens_ref[first + s] - base
            rel.append(n)
            inside = jnp.logical_and(n >= 0, n < ctx_local)
            at = jnp.where(inside, n, 0)
            start = pl.multiple_of(lax.div(at * kv_local, 16) * 16, 16)
            hit = jnp.logical_and(sub_pos == lax.rem(at, 16 // kv_local), inside)
            for cache, lo in ((k_buf, q_rows), (v_buf, q_rows + kv_local)):
                new = heads[lo : lo + kv_local, s, :]
                new = jnp.concatenate([new] * (16 // kv_local), axis=0)
                old = cache[first + s, pl.ds(start, 16), :].astype(F32)
                cache[first + s, pl.ds(start, 16), :] = jnp.where(hit, new, old).astype(BF16)
        queries = [heads[0:q_rows, s, :].astype(BF16) for s in seqs]
        logits = [lax.dot_general(queries[s], k_buf[first + s], (((1,), (1,)), ((), ())), preferred_element_type=F32) for s in seqs]
        logits = [jnp.where(col_pos <= rel[s], logits[s] * scale, -jnp.inf) for s in seqs]
        tops = [jnp.maximum(jnp.max(logits[s], axis=1, keepdims=True), sink) for s in seqs]
        weights = [jnp.exp(logits[s] - tops[s]) for s in seqs]
        totals = [jnp.sum(weights[s], axis=1, keepdims=True) for s in seqs]
        sums = [jnp.dot(weights[s].astype(BF16), v_buf[first + s], preferred_element_type=F32) for s in seqs]
        for s in seqs:
            here = lane == first + s
            m_all = jnp.where(here, tops[s], m_all)
            l_all = jnp.where(here, totals[s], l_all)
        out = n_buf.at[:, block(step)]
        for s in seqs:
            out[:, s, :] = sums[s]
        for c in stores(step):
            c.start()
        return m_all, l_all

    zero = jnp.zeros((q_rows, num_seqs), F32)
    m_all, l_all = lax.fori_loop(0, steps, step_fn, (zero, zero))
    ml_ref[0:q_rows] = m_all
    ml_ref[q_rows : 2 * q_rows] = l_all
    for step in range(steps):
        for c in stores(step):
            c.wait()


def attend(seq_lens, heads, sinks, k_rows, v_rows):
    num_seqs, rows, head_dim = k_rows.shape
    q_rows = sinks.shape[1]
    vmem = pl.BlockSpec(memory_space=pltpu.VMEM)
    anyspace = pl.BlockSpec(memory_space=pl.ANY)
    dma = pltpu.SemaphoreType.DMA((num_seqs // ATT_SEQS,))
    return pl.pallas_call(
        attend_kernel,
        in_specs=[pl.BlockSpec(memory_space=pltpu.SMEM), anyspace, vmem, anyspace, anyspace],
        out_specs=[anyspace, anyspace, anyspace, vmem],
        out_shape=[
            jax.ShapeDtypeStruct(k_rows.shape, BF16),
            jax.ShapeDtypeStruct(v_rows.shape, BF16),
            jax.ShapeDtypeStruct((q_rows, num_seqs, head_dim), F32),
            jax.ShapeDtypeStruct((2 * q_rows, num_seqs), F32),
        ],
        scratch_shapes=[
            pltpu.VMEM((num_seqs, rows, head_dim), BF16),
            pltpu.VMEM((num_seqs, rows, head_dim), BF16),
            pltpu.VMEM(heads.shape, F32),
            pltpu.VMEM((q_rows, num_seqs, head_dim), F32),
        ] + [dma] * 6,
        compiler_params=pltpu.CompilerParams(vmem_limit_bytes=60 << 20),
        name="attend",
    )(seq_lens, heads, sinks, k_rows, v_rows)


OUT_COLS = 256
SEQ_GROUPS = 2
W_PARTS = 4
LAG_Y = 6
LAG_X = 5


def finish_kernel(num_hbm, ml_ref, sink_ref, hid_ref, bo_ref, wo_ref, y_ref,
                  w_buf, x_buf, num, sink_col, bo_f32, r1, r1ml, own, away, away_ml, r2, r2ml, fac, o_buf, r3, o_all,
                  y_send, y_recv, z_buf, x_recv, p1, p2,
                  w_sem, h_sem, n_sem, s1_send, s1_recv, s2_send, s2_recv, s3_send, s3_recv, ml_send, ml_recv,
                  y_ss, y_rs, x_ss, x_rs, p1_ss, p1_rs, p2_ss, p2_rs):
    chip, core = sp_place()
    tp = lax.axis_index("tp")
    partner = {"sp": 2 * chip + (1 - core)}
    across_x = {"sp": 2 * (1 - chip) + core}
    across_y = {"tp": 1 - tp}
    q_rows, num_seqs, head_dim = num.shape
    half_h = q_rows // 2
    half_s = num_seqs // 2
    some = half_s // SEQ_GROUPS
    cols = w_buf.shape[1]
    chunks = cols // OUT_COLS
    total = SEQ_GROUPS * chunks
    mine = pl.multiple_of(core * half_h, half_h)
    theirs = pl.multiple_of((1 - core) * half_h, half_h)

    def seqs(which, g):
        return pl.ds(pl.multiple_of(which * half_s + g * some, some), some)

    barrier = pltpu.get_barrier_semaphore()
    for peer in (partner, across_x, across_y):
        pl.semaphore_signal(barrier, inc=1, device_id=peer, device_id_type=MESH)

    n_copies = []
    for i, h in enumerate((theirs, mine)):
        part = pl.ds(h, half_h)
        n_copies.append(pltpu.make_async_copy(num_hbm.at[part], num.at[part], n_sem.at[i]))
        n_copies[-1].start()
    my_cols = pl.ds(pl.multiple_of(core * cols, 128), cols)
    h_copy = pltpu.make_async_copy(hid_ref.at[pl.ds(pl.multiple_of(chip * half_s, half_s), half_s), my_cols], x_buf, h_sem)
    h_copy.start()
    w_cols = cols // W_PARTS
    w_chunks = w_cols // OUT_COLS

    def w_copy(p):
        return pltpu.make_async_copy(wo_ref.at[:, pl.ds(pl.multiple_of(core * cols + p * w_cols, 128), w_cols)], w_buf.at[:, pl.ds(pl.multiple_of(p * w_cols, 128), w_cols)], w_sem.at[p])

    sink_col[...] = jnp.broadcast_to(column(sink_ref, q_rows), sink_col.shape)
    bo_f32[...] = bo_ref[...].astype(F32)
    n_copies[0].wait()
    for p in range(W_PARTS):
        w_copy(p).start()
    pl.semaphore_wait(barrier, 3)

    c_ml = remote(ml_ref, r1ml, ml_send.at[0], ml_recv.at[0], partner)
    c_ml.start()
    c1 = []
    for g in range(SEQ_GROUPS):
        for i, which in enumerate((1 - chip, chip)):
            c1.append(remote(num.at[pl.ds(theirs, half_h), seqs(which, g)], r1.at[:, seqs(which, g)], s1_send.at[2 * g + i], s1_recv.at[2 * g + i], partner))
            c1[-1].start()

    c_ml.wait_recv()
    m_a, l_a = ml_ref[pl.ds(mine, half_h)], ml_ref[pl.ds(q_rows + mine, half_h)]
    m_b, l_b = r1ml[pl.ds(mine, half_h)], r1ml[pl.ds(q_rows + mine, half_h)]
    m_chip = jnp.maximum(m_a, m_b)
    f_a = jnp.exp(m_a - m_chip)
    f_b = jnp.exp(m_b - m_chip)
    l_chip = l_a * f_a + l_b * f_b
    fac[0] = f_a.T
    fac[1] = f_b.T
    away_ml[0:half_h] = m_chip
    away_ml[half_h : 2 * half_h] = l_chip
    n_copies[1].wait()

    c2_ml = remote(away_ml, r2ml, ml_send.at[1], ml_recv.at[1], across_x)
    c2 = []
    for g in range(SEQ_GROUPS):
        c1[2 * g].wait_recv()
        at = seqs(1 - chip, g)
        fa, fb = fac[0, at, :], fac[1, at, :]
        for h in range(half_h):
            away[g, h] = num[mine + h, at, :] * fa[:, h : h + 1] + r1[h, at, :] * fb[:, h : h + 1]
        if g == 0:
            c2_ml.start()
        c2.append(remote(away.at[g], r2.at[g], s2_send.at[g], s2_recv.at[g], across_x))
        c2[-1].start()
    for g in range(SEQ_GROUPS):
        c1[2 * g + 1].wait_recv()
        at = seqs(chip, g)
        fa, fb = fac[0, at, :], fac[1, at, :]
        for h in range(half_h):
            own[g, h] = num[mine + h, at, :] * fa[:, h : h + 1] + r1[h, at, :] * fb[:, h : h + 1]

    c2_ml.wait_recv()
    m_o, l_o = r2ml[0:half_h], r2ml[half_h : 2 * half_h]
    m_top = jnp.maximum(m_chip, m_o)
    f_a = jnp.exp(m_chip - m_top)
    f_b = jnp.exp(m_o - m_top)
    den = l_chip * f_a + l_o * f_b + jnp.exp(sink_col[pl.ds(mine, half_h)] - m_top)
    fac[2] = (f_a / den).T
    fac[3] = (f_b / den).T
    width = half_h * head_dim

    def heads_start(g):
        at = seqs(chip, g)
        fa, fb = fac[2, at, :], fac[3, at, :]
        c2[g].wait_recv()
        for h in range(half_h):
            o_buf[g, :, h * head_dim : (h + 1) * head_dim] = own[g, h] * fa[:, h : h + 1] + r2[g, h] * fb[:, h : h + 1]
        c = remote(o_buf.at[g], r3.at[g], s3_send.at[g], s3_recv.at[g], partner)
        c.start()
        o_all[g, :, pl.ds(pl.multiple_of(core * width, 128), width)] = o_buf[g].astype(BF16)
        return c

    def heads_end(g, c):
        c.wait_recv()
        o_all[g, :, pl.ds(pl.multiple_of((1 - core) * width, 128), width)] = r3[g].astype(BF16)

    def y_copy(t):
        return remote(y_send.at[t], y_recv.at[t], y_ss.at[t], y_rs.at[t], across_y)

    def x_copy(t):
        return remote(z_buf.at[t], x_recv.at[t], x_ss.at[t], x_rs.at[t], across_x)

    def p1_copy(t):
        return remote(z_buf.at[t], p1.at[t], p1_ss.at[t], p1_rs.at[t], partner)

    def p2_copy(t):
        return remote(x_recv.at[t], p2.at[t], p2_ss.at[t], p2_rs.at[t], partner)

    def place(which_seqs, which_cols, t):
        g, j = lax.div(t, chunks), lax.rem(t, chunks)
        return seqs(which_seqs, g), pl.ds(pl.multiple_of(which_cols * cols + j * OUT_COLS, 128), OUT_COLS)

    def body(t, _):
        @pl.when(t < total)
        def _():
            g, j = lax.div(t, chunks), lax.rem(t, chunks)

            @pl.when(jnp.logical_and(g == 0, lax.rem(j, w_chunks) == 0))
            def _():
                w_copy(lax.div(j, w_chunks)).wait()

            w = w_buf[:, pl.ds(pl.multiple_of(j * OUT_COLS, 128), OUT_COLS)]
            y_send[t] = jnp.dot(o_all[g], w, preferred_element_type=F32)
            y_copy(t).start()

        @pl.when(jnp.logical_and(t >= LAG_Y, t < total + LAG_Y))
        def _():
            u = t - LAG_Y
            g, j = lax.div(u, chunks), lax.rem(u, chunks)
            y_copy(u).wait_recv()
            x_part = x_buf[pl.ds(pl.multiple_of(g * some, some), some), pl.ds(pl.multiple_of(j * OUT_COLS, 128), OUT_COLS)].astype(F32)
            row = (core * cols + j * OUT_COLS) // head_dim
            bias = jnp.concatenate([bo_f32[pl.ds(row + i, 1), :] for i in range(OUT_COLS // head_dim)], axis=1)
            z = (x_part + (y_send[u] + y_recv[u]) + bias).astype(BF16)
            z_buf[u] = z.astype(F32)
            x_copy(u).start()
            p1_copy(u).start()
            rows_at, cols_at = place(chip, core, u)
            y_ref[rows_at, cols_at] = z

        @pl.when(t >= LAG_Y + LAG_X)
        def _():
            u = t - (LAG_Y + LAG_X)
            x_copy(u).wait_recv()
            p2_copy(u).start()
            rows_at, cols_at = place(1 - chip, core, u)
            y_ref[rows_at, cols_at] = x_recv[u].astype(BF16)
            p1_copy(u).wait_recv()
            rows_at, cols_at = place(chip, 1 - core, u)
            y_ref[rows_at, cols_at] = p1[u].astype(BF16)

        return 0

    c3 = [heads_start(0)]
    heads_end(0, c3[0])
    h_copy.wait()
    lax.fori_loop(0, 8, body, 0)
    c3.append(heads_start(1))
    lax.fori_loop(8, 12, body, 0)
    heads_end(1, c3[1])
    lax.fori_loop(12, total + LAG_Y + LAG_X, body, 0)

    def tail(t, _):
        p2_copy(t).wait_recv()
        rows_at, cols_at = place(1 - chip, 1 - core, t)
        y_ref[rows_at, cols_at] = p2[t].astype(BF16)
        y_copy(t).wait_send()
        x_copy(t).wait_send()
        p1_copy(t).wait_send()
        p2_copy(t).wait_send()
        return 0

    lax.fori_loop(0, total, tail, 0)
    for c in (c_ml, c2_ml, *c1, *c2, *c3):
        c.wait_send()


def finish(num, ml, sinks, hidden, b_o, w_o):
    q_rows, num_seqs, head_dim = num.shape
    half_h, half_s = q_rows // 2, num_seqs // 2
    some = half_s // SEQ_GROUPS
    width = w_o.shape[1]
    cols = width // 2
    total = SEQ_GROUPS * (cols // OUT_COLS)
    vmem = pl.BlockSpec(memory_space=pltpu.VMEM)
    anyspace = pl.BlockSpec(memory_space=pl.ANY)
    chunked = pltpu.VMEM((total, some, OUT_COLS), F32)
    dma = pltpu.SemaphoreType.DMA
    return pl.pallas_call(
        finish_kernel,
        out_shape=jax.ShapeDtypeStruct((num_seqs, width), BF16),
        in_specs=[anyspace, vmem, vmem, anyspace, vmem, anyspace],
        out_specs=vmem,
        scratch_shapes=[
            pltpu.VMEM((w_o.shape[0], cols), BF16),
            pltpu.VMEM((half_s, cols), BF16),
            pltpu.VMEM(num.shape, F32),
            pltpu.VMEM((q_rows, num_seqs), F32),
            pltpu.VMEM((width // head_dim, head_dim), F32),
            pltpu.VMEM((half_h, num_seqs, head_dim), F32),
            pltpu.VMEM((2 * q_rows, num_seqs), F32),
            pltpu.VMEM((SEQ_GROUPS, half_h, some, head_dim), F32),
            pltpu.VMEM((SEQ_GROUPS, half_h, some, head_dim), F32),
            pltpu.VMEM((2 * half_h, num_seqs), F32),
            pltpu.VMEM((SEQ_GROUPS, half_h, some, head_dim), F32),
            pltpu.VMEM((2 * half_h, num_seqs), F32),
            pltpu.VMEM((4, num_seqs, half_h), F32),
            pltpu.VMEM((SEQ_GROUPS, some, half_h * head_dim), F32),
            pltpu.VMEM((SEQ_GROUPS, some, half_h * head_dim), F32),
            pltpu.VMEM((SEQ_GROUPS, some, q_rows * head_dim), BF16),
            chunked, chunked, chunked, chunked, chunked, chunked,
            dma((W_PARTS,)), dma, dma((2,)),
            dma((2 * SEQ_GROUPS,)), dma((2 * SEQ_GROUPS,)),
            dma((SEQ_GROUPS,)), dma((SEQ_GROUPS,)),
            dma((SEQ_GROUPS,)), dma((SEQ_GROUPS,)),
            dma((2,)), dma((2,)),
            *[dma((total,))] * 8,
        ],
        compiler_params=pltpu.CompilerParams(collective_id=1, has_side_effects=True, vmem_limit_bytes=56 << 20),
        name="finish",
    )(num, ml, sinks, hidden, b_o.reshape(width // head_dim, head_dim), w_o)


def solution(mesh):
    cache_spec = P("dp", "sp", "tp", None)

    def block_step(hidden, seq_lens, rope_cos, rope_sin, k_cache, v_cache, norm_gain, w_qkv, b_qkv, sink_logits, w_o, b_o):
        num_seqs, ctx_local, kv_local, head_dim = k_cache.shape
        heads = qkv_heads(hidden, rope_cos, rope_sin, norm_gain, w_qkv, b_qkv, head_dim)
        sinks = sink_logits.reshape(1, sink_logits.shape[0])
        rows = (num_seqs, ctx_local * kv_local, head_dim)
        k_out, v_out, num, ml = attend(seq_lens, heads, sinks, k_cache.reshape(rows), v_cache.reshape(rows))
        out_hidden = finish(num, ml, sinks, hidden, b_o, w_o)
        return out_hidden, k_out.reshape(k_cache.shape), v_out.reshape(v_cache.shape)

    return jax.shard_map(block_step, mesh=mesh, in_specs=(P("dp", None), P("dp"), P("dp", None), P("dp", None), cache_spec, cache_spec, P(None), P(None, "tp", None), P("tp", None), P("tp"), P("tp", None), P(None)), out_specs=(P("dp", None), cache_spec, cache_spec), check_vma=False)
```

```python
import functools

import jax
import jax.numpy as jnp
from jax import lax
from jax.experimental import pallas as pl
from jax.experimental.pallas import tpu as pltpu
from jax.sharding import PartitionSpec as P

NORM_EPS = 1e-5
F32 = jnp.float32
BF16 = jnp.bfloat16
MESH = pl.DeviceIdType.MESH


def sp_place():
    sp = lax.axis_index("sp")
    return lax.div(sp, 2), lax.rem(sp, 2)


def remote(src, dst, send_sem, recv_sem, where):
    return pltpu.make_async_remote_copy(src_ref=src, dst_ref=dst, send_sem=send_sem, recv_sem=recv_sem, device_id=where, device_id_type=MESH)


def sink_column(row_ref, count, halves, group):
    row = lax.broadcasted_iota(jnp.int32, (count, count), 0)
    per_half = count // halves
    part = group // halves
    head = lax.div(lax.rem(row, per_half), part) * group + lax.div(row, per_half) * part + lax.rem(row, part)
    same = head == lax.broadcasted_iota(jnp.int32, (count, count), 1)
    return jnp.sum(jnp.where(same, jnp.broadcast_to(row_ref[...], (count, count)), 0.0), axis=1, keepdims=True)


QKV_ROWS = 512
QKV_SLOTS = 3
CACHE_SEQS = 8
CACHE_AHEAD = 4


def project_kernel(x_ref, gain_ref, cos_ref, sin_ref, bias_ref, w_ref, k_ref, v_ref, out_ref, k_out, v_out,
                   normed, gain, heads, acc_q, acc_e, wq_buf, we_buf, k_buf, v_buf, wq_sem, we_sem, out_sem, k_in, v_in, k_back, v_back):
    _, core = sp_place()
    num_seqs, depth = x_ref.shape
    head_dim = acc_e.shape[2]
    q_cols = acc_q.shape[2]
    kv_local = acc_q.shape[0]
    per_core = q_cols // head_dim
    group = 2 * per_core
    steps = depth // QKV_ROWS
    blocks = num_seqs // CACHE_SEQS

    def fetch(step, slot):
        rows = pl.ds(step * QKV_ROWS, QKV_ROWS)
        cq = pltpu.make_async_copy(w_ref.at[rows, :, pl.ds(pl.multiple_of(core * q_cols, 128), q_cols)], wq_buf.at[slot], wq_sem.at[slot])
        ce = pltpu.make_async_copy(w_ref.at[rows, :, pl.ds(pl.multiple_of((group + core) * head_dim, 128), head_dim)], we_buf.at[slot], we_sem.at[slot])
        return cq, ce

    def cache_in(i):
        at = pl.ds(i * CACHE_SEQS, CACHE_SEQS)
        return pltpu.make_async_copy(k_ref.at[at], k_buf.at[at], k_in.at[i]), pltpu.make_async_copy(v_ref.at[at], v_buf.at[at], v_in.at[i])

    def cache_back(i):
        at = pl.ds(i * CACHE_SEQS, CACHE_SEQS)
        return pltpu.make_async_copy(k_buf.at[at], k_out.at[at], k_back.at[i]), pltpu.make_async_copy(v_buf.at[at], v_out.at[at], v_back.at[i])

    for s in range(QKV_SLOTS - 1):
        for c in fetch(s, s):
            c.start()
    for i in range(CACHE_AHEAD):
        for c in cache_in(i):
            c.start()

    gain[...] = gain_ref[...].astype(F32)

    def norm_rows(r, _):
        rows = pl.ds(pl.multiple_of(r * 16, 16), 16)
        xw = x_ref[rows, :].astype(F32)
        inv = lax.rsqrt(jnp.mean(xw * xw, axis=-1, keepdims=True) + NORM_EPS)
        for t in range(depth // head_dim):
            cols = slice(t * head_dim, (t + 1) * head_dim)
            normed[rows, cols] = (xw[:, cols] * inv * gain[t : t + 1, :]).astype(BF16)
        return 0

    lax.fori_loop(0, num_seqs // 16, norm_rows, 0)
    acc_q[...] = jnp.zeros_like(acc_q)
    acc_e[...] = jnp.zeros_like(acc_e)

    def step_fn(step, _):
        slot = lax.rem(step, QKV_SLOTS)

        @pl.when(step + CACHE_AHEAD < blocks)
        def _():
            for c in cache_in(step + CACHE_AHEAD):
                c.start()

        for c in fetch(step, slot):
            c.wait()

        @pl.when(step + QKV_SLOTS - 1 < steps)
        def _():
            for c in fetch(step + QKV_SLOTS - 1, lax.rem(step + QKV_SLOTS - 1, QKV_SLOTS)):
                c.start()

        for c in cache_in(step):
            c.wait()
        for c in cache_back(step):
            c.start()

        h = normed[:, pl.ds(pl.multiple_of(step * QKV_ROWS, 128), QKV_ROWS)]
        wq = jnp.swapaxes(wq_buf[slot], 0, 1)
        we = jnp.swapaxes(we_buf[slot], 0, 1)
        for k in range(kv_local):
            acc_q[k] += jnp.dot(h, wq[k], preferred_element_type=F32)
            acc_e[k] += jnp.dot(h, we[k], preferred_element_type=F32)
        return 0

    lax.fori_loop(0, steps, step_fn, 0)

    cos_t = cos_ref[...].T
    sin_t = sin_ref[...].T
    cos2 = jnp.concatenate([cos_t, cos_t], axis=1)
    sin2 = jnp.concatenate([-sin_t, sin_t], axis=1)
    is_key = core == 0
    cos_e = jnp.where(is_key, cos2, jnp.ones_like(cos2))
    sin_e = jnp.where(is_key, sin2, jnp.zeros_like(sin2))

    def rotate(v, c, s):
        r = v * c + pltpu.roll(v, head_dim // 2, 1) * s
        return r.astype(BF16).astype(F32)

    for k in range(kv_local):
        bias_q = bias_ref[k : k + 1, pl.ds(pl.multiple_of(core * q_cols, 128), q_cols)].astype(F32)
        for g in range(per_core):
            cols = slice(g * head_dim, (g + 1) * head_dim)
            heads[k * per_core + g] = rotate(acc_q[k, :, cols] + bias_q[:, cols], cos2, sin2)
        bias_e = bias_ref[k : k + 1, pl.ds(pl.multiple_of((group + core) * head_dim, 128), head_dim)].astype(F32)
        heads[kv_local * per_core + k] = rotate(acc_e[k] + bias_e, cos_e, sin_e)
    done = pltpu.make_async_copy(heads, out_ref, out_sem)
    done.start()
    for i in range(blocks):
        for c in cache_back(i):
            c.wait()
    done.wait()


def project(hidden, rope_cos, rope_sin, norm_gain, w_qkv, b_qkv, k_rows, v_rows):
    num_seqs, depth = hidden.shape
    head_dim = k_rows.shape[2]
    kv_local = w_qkv.shape[1]
    per_core = (w_qkv.shape[2] // head_dim - 2) // 2
    rows = kv_local * (per_core + 1)
    blocks = num_seqs // CACHE_SEQS
    assert blocks == depth // QKV_ROWS
    vmem = pl.BlockSpec(memory_space=pltpu.VMEM)
    anyspace = pl.BlockSpec(memory_space=pl.ANY)
    dma = pltpu.SemaphoreType.DMA
    return pl.pallas_call(
        project_kernel,
        out_shape=[
            jax.ShapeDtypeStruct((rows, num_seqs, head_dim), F32),
            jax.ShapeDtypeStruct(k_rows.shape, BF16),
            jax.ShapeDtypeStruct(v_rows.shape, BF16),
        ],
        in_specs=[vmem] * 5 + [anyspace] * 3,
        out_specs=[anyspace] * 3,
        scratch_shapes=[
            pltpu.VMEM((num_seqs, depth), BF16),
            pltpu.VMEM((depth // head_dim, head_dim), F32),
            pltpu.VMEM((rows, num_seqs, head_dim), F32),
            pltpu.VMEM((kv_local, num_seqs, per_core * head_dim), F32),
            pltpu.VMEM((kv_local, num_seqs, head_dim), F32),
            pltpu.VMEM((QKV_SLOTS, QKV_ROWS, kv_local, per_core * head_dim), BF16),
            pltpu.VMEM((QKV_SLOTS, QKV_ROWS, kv_local, head_dim), BF16),
            pltpu.VMEM(k_rows.shape, BF16),
            pltpu.VMEM(v_rows.shape, BF16),
            dma((QKV_SLOTS,)), dma((QKV_SLOTS,)), dma,
            dma((blocks,)), dma((blocks,)), dma((blocks,)), dma((blocks,)),
        ],
        compiler_params=pltpu.CompilerParams(vmem_limit_bytes=60 << 20),
        name="project",
    )(hidden, norm_gain.reshape(depth // head_dim, head_dim), rope_cos.T, rope_sin.T, b_qkv, w_qkv, k_rows, v_rows)


ATT_SEQS = 8
ATT_SLOTS = 5
OUT_COLS = 256
SEQ_GROUPS = 2
W_PARTS = 4
LAG_Y = 6
LAG_X = 5


def finish_kernel(lens_ref, half_hbm, sink_ref, hid_ref, bo_ref, wo_ref, k_hbm, v_hbm, y_ref, new_ref,
                  w_buf, x_buf, h_buf, k_ring, v_ring, pos_ref, num, ml, sink_col, bo_f32, r1, r1ml, own, own_ml, away, away_ml, r2, r2ml, o_buf, r3, o_all,
                  y_send, y_recv, z_buf, x_recv, p1, p2,
                  w_sem, x_sem, k_sem, v_sem, h_in, h_send, h_recv, s1_send, s1_recv, s2_send, s2_recv, s3_send, s3_recv,
                  y_ss, y_rs, x_ss, x_rs, p1_ss, p1_rs, p2_ss, p2_rs):
    chip, core = sp_place()
    tp = lax.axis_index("tp")
    partner = {"sp": 2 * chip + (1 - core)}
    across_x = {"sp": 2 * (1 - chip) + core}
    across_y = {"tp": 1 - tp}
    groups, q_rows, some, head_dim = num.shape
    num_seqs = h_buf.shape[1]
    kv_local = (h_buf.shape[0] - q_rows) // 2
    rows = k_ring.shape[2]
    ctx_local = rows // kv_local
    half_h = q_rows // 2
    half_s = num_seqs // 2
    part_h = half_h // kv_local
    cols = w_buf.shape[1]
    chunks = cols // OUT_COLS
    total = SEQ_GROUPS * chunks
    mine = pl.multiple_of(core * half_h, half_h)
    theirs = pl.multiple_of((1 - core) * half_h, half_h)

    def seqs(which, g):
        return pl.ds(pl.multiple_of(which * half_s + g * some, some), some)

    barrier = pltpu.get_barrier_semaphore()
    for peer in (partner, across_x, across_y):
        pl.semaphore_signal(barrier, inc=1, device_id=peer, device_id_type=MESH)

    order = [(1 - chip, g) for g in range(SEQ_GROUPS)] + [(chip, g) for g in range(SEQ_GROUPS)]
    own_rows = (pl.ds(mine, half_h), pl.ds(pl.multiple_of(q_rows + kv_local * core, kv_local), kv_local))
    src_rows = (pl.ds(0, half_h), pl.ds(half_h, kv_local))
    h_local, h_remote = [], []
    for i, (which, g) in enumerate(order):
        at = seqs(which, g)
        for j in range(2):
            h_local.append(pltpu.make_async_copy(half_hbm.at[src_rows[j], at], h_buf.at[own_rows[j], at], h_in.at[2 * i + j]))
            h_local[-1].start()
            h_remote.append(remote(half_hbm.at[src_rows[j], at], h_buf.at[own_rows[j], at], h_send.at[2 * i + j], h_recv.at[2 * i + j], partner))

    steps = num_seqs // ATT_SEQS
    per_group = some // ATT_SEQS

    def block(p):
        return lax.rem(p + (1 - chip) * (steps // 2), steps) * ATT_SEQS

    def kv_load(p):
        at = pl.ds(pl.multiple_of(block(p), ATT_SEQS), ATT_SEQS)
        slot = lax.rem(p, ATT_SLOTS)
        return pltpu.make_async_copy(k_hbm.at[at], k_ring.at[slot], k_sem.at[slot]), pltpu.make_async_copy(v_hbm.at[at], v_ring.at[slot], v_sem.at[slot])

    for p in range(ATT_SLOTS):
        for c in kv_load(p):
            c.start()
    my_cols = pl.ds(pl.multiple_of(core * cols, 128), cols)
    x_copy_in = pltpu.make_async_copy(hid_ref.at[pl.ds(pl.multiple_of(chip * half_s, half_s), half_s), my_cols], x_buf, x_sem)
    w_cols = cols // W_PARTS
    w_chunks = w_cols // OUT_COLS

    def w_copy(p):
        return pltpu.make_async_copy(wo_ref.at[:, pl.ds(pl.multiple_of(core * cols + p * w_cols, 128), w_cols)], w_buf.at[:, pl.ds(pl.multiple_of(p * w_cols, 128), w_cols)], w_sem.at[p])

    sink = sink_column(sink_ref, q_rows, 2, 2 * part_h)
    sink_col[...] = jnp.broadcast_to(sink, sink_col.shape)
    bo_f32[...] = bo_ref[...].astype(F32)
    pos_ref[...] = lax.div(lax.broadcasted_iota(jnp.int32, pos_ref.shape, 0), kv_local).astype(F32).astype(BF16)
    pl.semaphore_wait(barrier, 3)
    for c in h_remote:
        c.start()

    base = lax.axis_index("sp") * ctx_local
    scale = head_dim**-0.5
    col = lax.broadcasted_iota(jnp.int32, (q_rows, rows), 1)
    kv_row = lax.div(lax.rem(lax.broadcasted_iota(jnp.int32, (q_rows, rows), 0), half_h), part_h)
    col_pos = jnp.where(lax.rem(col, kv_local) == kv_row, lax.div(col, kv_local), ctx_local * 1024)
    lane = lax.broadcasted_iota(jnp.int32, (q_rows, ml.shape[2]), 1)
    batch = range(ATT_SEQS)

    def attend(i, first, last, carry):
        def step_fn(t, carry):
            m_all, l_all = carry
            p = i * per_group + t
            slot = lax.rem(p, ATT_SLOTS)
            for c in kv_load(p):
                c.wait()
            start = block(p)
            heads = h_buf.at[:, pl.ds(pl.multiple_of(start, ATT_SEQS), ATT_SEQS)]
            rel = [lens_ref[start + s] - base for s in batch]
            keys, values = [], []
            for s in batch:
                n = jnp.full((16, head_dim), rel[s].astype(F32)).astype(BF16)
                hit = pos_ref[...].reshape(rows // 16, 16, head_dim) == n[None]
                for j, (ring, out) in enumerate(((k_ring, keys), (v_ring, values))):
                    new = heads[q_rows + j * kv_local : q_rows + (j + 1) * kv_local, s, :].astype(BF16)
                    new_ref[j, start + s] = new
                    new = jnp.concatenate([new] * (16 // kv_local), axis=0)
                    old = ring[slot, s].reshape(rows // 16, 16, head_dim)
                    out.append(jnp.where(hit, new[None], old).reshape(rows, head_dim))
            queries = [heads[0:q_rows, s, :].astype(BF16) for s in batch]
            logits = [lax.dot_general(queries[s], keys[s], (((1,), (1,)), ((), ())), preferred_element_type=F32) for s in batch]
            logits = [jnp.where(col_pos <= rel[s], logits[s] * scale, -jnp.inf) for s in batch]
            tops = [jnp.maximum(jnp.max(logits[s], axis=1, keepdims=True), sink) for s in batch]
            weights = [jnp.exp(logits[s] - tops[s]) for s in batch]
            totals = [jnp.sum(weights[s], axis=1, keepdims=True) for s in batch]
            sums = [jnp.dot(weights[s].astype(BF16), values[s], preferred_element_type=F32) for s in batch]
            out = num.at[i, :, pl.ds(pl.multiple_of(t * ATT_SEQS, ATT_SEQS), ATT_SEQS)]
            for s in batch:
                here = lane == t * ATT_SEQS + s
                m_all = jnp.where(here, tops[s], m_all)
                l_all = jnp.where(here, totals[s], l_all)
                out[:, s, :] = sums[s]

            @pl.when(p + ATT_SLOTS < steps)
            def _():
                for c in kv_load(p + ATT_SLOTS):
                    c.start()

            return m_all, l_all

        return lax.fori_loop(first, last, step_fn, carry)

    def heads_wait(i):
        for j in range(2):
            h_local[2 * i + j].wait()
            h_remote[2 * i + j].wait_recv()

    zero = jnp.zeros((q_rows, ml.shape[2]), F32)
    c1 = []

    def to_partner(i, carry):
        ml[i, 0:q_rows] = carry[0]
        ml[i, q_rows : 2 * q_rows] = carry[1]
        c1.append((
            remote(ml.at[i], r1ml.at[i], s1_send.at[2 * i], s1_recv.at[2 * i], partner),
            remote(num.at[i, pl.ds(theirs, half_h)], r1.at[i], s1_send.at[2 * i + 1], s1_recv.at[2 * i + 1], partner),
        ))
        for c in c1[-1]:
            c.start()

    def combine(i, dst, dst_ml):
        for c in c1[i]:
            c.wait_recv()
        m_a, l_a = ml[i, pl.ds(mine, half_h)], ml[i, pl.ds(q_rows + mine, half_h)]
        m_b, l_b = r1ml[i, pl.ds(mine, half_h)], r1ml[i, pl.ds(q_rows + mine, half_h)]
        m_chip = jnp.maximum(m_a, m_b)
        f_a = jnp.exp(m_a - m_chip)
        f_b = jnp.exp(m_b - m_chip)
        dst_ml[0:half_h] = m_chip
        dst_ml[half_h : 2 * half_h] = l_a * f_a + l_b * f_b
        f_a, f_b = f_a.T, f_b.T
        for h in range(half_h):
            dst[h] = num[i, mine + h] * f_a[0:some, h : h + 1] + r1[i, h] * f_b[0:some, h : h + 1]

    c2 = []

    def across(g):
        combine(g, away.at[g], away_ml.at[g])
        c2.append((
            remote(away_ml.at[g], r2ml.at[g], s2_send.at[2 * g], s2_recv.at[2 * g], across_x),
            remote(away.at[g], r2.at[g], s2_send.at[2 * g + 1], s2_recv.at[2 * g + 1], across_x),
        ))
        for c in c2[-1]:
            c.start()

    width = half_h * head_dim
    part_w = part_h * head_dim

    def o_place(which_half, k):
        return pl.ds(pl.multiple_of(2 * k * part_w + which_half * part_w, 128), part_w)

    def heads_start(g):
        for c in c2[g]:
            c.wait_recv()
        m_a, l_a = own_ml[g, 0:half_h], own_ml[g, half_h : 2 * half_h]
        m_b, l_b = r2ml[g, 0:half_h], r2ml[g, half_h : 2 * half_h]
        m_top = jnp.maximum(m_a, m_b)
        f_a = jnp.exp(m_a - m_top)
        f_b = jnp.exp(m_b - m_top)
        den = l_a * f_a + l_b * f_b + jnp.exp(sink_col[pl.ds(mine, half_h)] - m_top)
        f_a, f_b = (f_a / den).T, (f_b / den).T
        for h in range(half_h):
            o_buf[g, :, h * head_dim : (h + 1) * head_dim] = own[g, h] * f_a[0:some, h : h + 1] + r2[g, h] * f_b[0:some, h : h + 1]
        c = remote(o_buf.at[g], r3.at[g], s3_send.at[g], s3_recv.at[g], partner)
        c.start()
        for k in range(kv_local):
            o_all[g, :, o_place(core, k)] = o_buf[g, :, k * part_w : (k + 1) * part_w].astype(BF16)
        return c

    def heads_end(g, c):
        c.wait_recv()
        for k in range(kv_local):
            o_all[g, :, o_place(1 - core, k)] = r3[g, :, k * part_w : (k + 1) * part_w].astype(BF16)

    def y_copy(t):
        return remote(y_send.at[t], y_recv.at[t], y_ss.at[t], y_rs.at[t], across_y)

    def x_copy(t):
        return remote(z_buf.at[t], x_recv.at[t], x_ss.at[t], x_rs.at[t], across_x)

    def p1_copy(t):
        return remote(z_buf.at[t], p1.at[t], p1_ss.at[t], p1_rs.at[t], partner)

    def p2_copy(t):
        return remote(x_recv.at[t], p2.at[t], p2_ss.at[t], p2_rs.at[t], partner)

    def place(which_seqs, which_cols, t):
        g, j = lax.div(t, chunks), lax.rem(t, chunks)
        return seqs(which_seqs, g), pl.ds(pl.multiple_of(which_cols * cols + j * OUT_COLS, 128), OUT_COLS)

    def body(t, _):
        @pl.when(t < total)
        def _():
            g, j = lax.div(t, chunks), lax.rem(t, chunks)

            @pl.when(jnp.logical_and(g == 0, lax.rem(j, w_chunks) == 0))
            def _():
                w_copy(lax.div(j, w_chunks)).wait()

            w = w_buf[:, pl.ds(pl.multiple_of(j * OUT_COLS, 128), OUT_COLS)]
            y_send[t] = jnp.dot(o_all[g], w, preferred_element_type=F32)
            y_copy(t).start()

        @pl.when(jnp.logical_and(t >= LAG_Y, t < total + LAG_Y))
        def _():
            u = t - LAG_Y
            g, j = lax.div(u, chunks), lax.rem(u, chunks)
            y_copy(u).wait_recv()
            x_part = x_buf[pl.ds(pl.multiple_of(g * some, some), some), pl.ds(pl.multiple_of(j * OUT_COLS, 128), OUT_COLS)].astype(F32)
            row = (core * cols + j * OUT_COLS) // head_dim
            bias = jnp.concatenate([bo_f32[pl.ds(row + i, 1), :] for i in range(OUT_COLS // head_dim)], axis=1)
            z = (x_part + (y_send[u] + y_recv[u]) + bias).astype(BF16)
            z_buf[u] = z.astype(F32)
            x_copy(u).start()
            p1_copy(u).start()
            rows_at, cols_at = place(chip, core, u)
            y_ref[rows_at, cols_at] = z

        @pl.when(t >= LAG_Y + LAG_X)
        def _():
            u = t - (LAG_Y + LAG_X)
            x_copy(u).wait_recv()
            p2_copy(u).start()
            rows_at, cols_at = place(1 - chip, core, u)
            y_ref[rows_at, cols_at] = x_recv[u].astype(BF16)
            p1_copy(u).wait_recv()
            rows_at, cols_at = place(chip, 1 - core, u)
            y_ref[rows_at, cols_at] = p1[u].astype(BF16)

        return 0

    half_group = per_group // 2
    heads_wait(0)
    carry = attend(0, 0, per_group, (zero, zero))
    to_partner(0, carry)
    x_copy_in.start()
    for p in range(W_PARTS // 2):
        w_copy(p).start()
    heads_wait(1)
    carry = attend(1, 0, half_group, (zero, zero))
    across(0)
    carry = attend(1, half_group, per_group, carry)
    to_partner(1, carry)
    for p in range(W_PARTS // 2, W_PARTS):
        w_copy(p).start()
    heads_wait(2)
    carry = attend(2, 0, half_group, (zero, zero))
    across(1)
    carry = attend(2, half_group, per_group, carry)
    to_partner(2, carry)
    heads_wait(3)
    carry = attend(3, 0, per_group, (zero, zero))
    to_partner(3, carry)
    combine(2, own.at[0], own_ml.at[0])
    combine(3, own.at[1], own_ml.at[1])

    c3 = [heads_start(0)]
    heads_end(0, c3[0])
    x_copy_in.wait()
    lax.fori_loop(0, 8, body, 0)
    c3.append(heads_start(1))
    lax.fori_loop(8, 12, body, 0)
    heads_end(1, c3[1])
    lax.fori_loop(12, total + LAG_Y + LAG_X, body, 0)

    def tail(t, _):
        p2_copy(t).wait_recv()
        rows_at, cols_at = place(1 - chip, 1 - core, t)
        y_ref[rows_at, cols_at] = p2[t].astype(BF16)
        y_copy(t).wait_send()
        x_copy(t).wait_send()
        p1_copy(t).wait_send()
        p2_copy(t).wait_send()
        return 0

    lax.fori_loop(0, total, tail, 0)
    for c in (*h_remote, *(c for pair in c1 + c2 for c in pair), *c3):
        c.wait_send()


def finish(seq_lens, half, sinks, hidden, b_o, w_o, k_rows, v_rows):
    num_seqs, rows, head_dim = k_rows.shape
    q_rows = sinks.shape[1]
    half_h, half_s = q_rows // 2, num_seqs // 2
    kv_local = half.shape[0] - half_h
    some = half_s // SEQ_GROUPS
    groups = 2 * SEQ_GROUPS
    width = w_o.shape[1]
    cols = width // 2
    total = SEQ_GROUPS * (cols // OUT_COLS)
    vmem = pl.BlockSpec(memory_space=pltpu.VMEM)
    anyspace = pl.BlockSpec(memory_space=pl.ANY)
    chunked = pltpu.VMEM((total, some, OUT_COLS), F32)
    parts = pltpu.VMEM((SEQ_GROUPS, half_h, some, head_dim), F32)
    parts_ml = pltpu.VMEM((SEQ_GROUPS, 2 * half_h, 128), F32)
    ring = pltpu.VMEM((ATT_SLOTS, ATT_SEQS, rows, head_dim), BF16)
    dma = pltpu.SemaphoreType.DMA
    return pl.pallas_call(
        finish_kernel,
        out_shape=[
            jax.ShapeDtypeStruct((num_seqs, width), BF16),
            jax.ShapeDtypeStruct((2, num_seqs, kv_local, head_dim), BF16),
        ],
        in_specs=[pl.BlockSpec(memory_space=pltpu.SMEM), anyspace, vmem, anyspace, vmem, anyspace, anyspace, anyspace],
        out_specs=[vmem, vmem],
        scratch_shapes=[
            pltpu.VMEM((w_o.shape[0], cols), BF16),
            pltpu.VMEM((half_s, cols), BF16),
            pltpu.VMEM((q_rows + 2 * kv_local, num_seqs, head_dim), F32),
            ring, ring,
            pltpu.VMEM((rows, head_dim), BF16),
            pltpu.VMEM((groups, q_rows, some, head_dim), F32),
            pltpu.VMEM((groups, 2 * q_rows, 128), F32),
            pltpu.VMEM((q_rows, 128), F32),
            pltpu.VMEM((width // head_dim, head_dim), F32),
            pltpu.VMEM((groups, half_h, some, head_dim), F32),
            pltpu.VMEM((groups, 2 * q_rows, 128), F32),
            parts, parts_ml, parts, parts_ml, parts, parts_ml,
            pltpu.VMEM((SEQ_GROUPS, some, half_h * head_dim), F32),
            pltpu.VMEM((SEQ_GROUPS, some, half_h * head_dim), F32),
            pltpu.VMEM((SEQ_GROUPS, some, q_rows * head_dim), BF16),
            chunked, chunked, chunked, chunked, chunked, chunked,
            dma((W_PARTS,)), dma, dma((ATT_SLOTS,)), dma((ATT_SLOTS,)),
            dma((2 * groups,)), dma((2 * groups,)), dma((2 * groups,)),
            dma((2 * groups,)), dma((2 * groups,)),
            dma((groups,)), dma((groups,)),
            dma((SEQ_GROUPS,)), dma((SEQ_GROUPS,)),
            *[dma((total,))] * 8,
        ],
        compiler_params=pltpu.CompilerParams(collective_id=1, has_side_effects=True, vmem_limit_bytes=62 << 20),
        name="finish",
    )(seq_lens, half, sinks, hidden, b_o.reshape(width // head_dim, head_dim), w_o, k_rows, v_rows)


LAST_PARTS = 4


def last_kernel(lens_ref, y_hbm, new_ref, k_in, v_in, y_out, k_out, v_out, y_buf, in_sem, out_sem, k_sem, v_sem):
    num_seqs, ctx_local = k_out.shape[:2]
    base = lax.axis_index("sp") * ctx_local
    rows = y_hbm.shape[0] // LAST_PARTS
    loads, stores = [], []
    for p in range(LAST_PARTS):
        at = pl.ds(p * rows, rows)
        loads.append(pltpu.make_async_copy(y_hbm.at[at], y_buf.at[at], in_sem.at[p]))
        stores.append(pltpu.make_async_copy(y_buf.at[at], y_out.at[at], out_sem.at[p]))
        loads[-1].start()

    def copies(b, n):
        return pltpu.make_async_copy(new_ref.at[0, b], k_out.at[b, n], k_sem), pltpu.make_async_copy(new_ref.at[1, b], v_out.at[b, n], v_sem)

    def put(b, _):
        n = lens_ref[b] - base

        @pl.when(jnp.logical_and(n >= 0, n < ctx_local))
        def _():
            for c in copies(b, n):
                c.start()

        return 0

    lax.fori_loop(0, num_seqs, put, 0)
    for p in range(LAST_PARTS):
        loads[p].wait()
        stores[p].start()

    def settle(b, _):
        n = lens_ref[b] - base

        @pl.when(jnp.logical_and(n >= 0, n < ctx_local))
        def _():
            for c in copies(b, n):
                c.wait()

        return 0

    lax.fori_loop(0, num_seqs, settle, 0)
    for c in stores:
        c.wait()


def last(seq_lens, y, new, k_copy, v_copy):
    vmem = pl.BlockSpec(memory_space=pltpu.VMEM)
    anyspace = pl.BlockSpec(memory_space=pl.ANY)
    dma = pltpu.SemaphoreType.DMA
    return pl.pallas_call(
        last_kernel,
        out_shape=[jax.ShapeDtypeStruct(a.shape, a.dtype) for a in (y, k_copy, v_copy)],
        in_specs=[pl.BlockSpec(memory_space=pltpu.SMEM), anyspace, vmem, anyspace, anyspace],
        out_specs=[anyspace] * 3,
        scratch_shapes=[pltpu.VMEM(y.shape, y.dtype), dma((LAST_PARTS,)), dma((LAST_PARTS,)), dma, dma],
        input_output_aliases={3: 1, 4: 2},
        compiler_params=pltpu.CompilerParams(vmem_limit_bytes=60 << 20),
        name="last",
    )(seq_lens, y, new, k_copy, v_copy)


def solution(mesh):
    cache_spec = P("dp", "sp", "tp", None)

    def block_step(hidden, seq_lens, rope_cos, rope_sin, k_cache, v_cache, norm_gain, w_qkv, b_qkv, sink_logits, w_o, b_o):
        num_seqs, ctx_local, kv_local, head_dim = k_cache.shape
        rows = (num_seqs, ctx_local * kv_local, head_dim)
        k_rows, v_rows = k_cache.reshape(rows), v_cache.reshape(rows)
        half, k_copy, v_copy = project(hidden, rope_cos, rope_sin, norm_gain, w_qkv, b_qkv, k_rows, v_rows)
        sinks = sink_logits.reshape(1, sink_logits.shape[0])
        y, new = finish(seq_lens, half, sinks, hidden, b_o, w_o, k_rows, v_rows)
        return last(seq_lens, y, new, k_copy.reshape(k_cache.shape), v_copy.reshape(v_cache.shape))

    return jax.shard_map(block_step, mesh=mesh, in_specs=(P("dp", None), P("dp"), P("dp", None), P("dp", None), cache_spec, cache_spec, P(None), P(None, "tp", None), P("tp", None), P("tp"), P("tp", None), P(None)), out_specs=(P("dp", None), cache_spec, cache_spec), check_vma=False)
```

```python
import functools

import jax
import jax.numpy as jnp
from jax import lax
from jax.experimental import pallas as pl
from jax.experimental.pallas import tpu as pltpu
from jax.sharding import PartitionSpec as P

NORM_EPS = 1e-5
F32 = jnp.float32
BF16 = jnp.bfloat16
MESH = pl.DeviceIdType.MESH


def sp_place():
    sp = lax.axis_index("sp")
    return lax.div(sp, 2), lax.rem(sp, 2)


def remote(src, dst, send_sem, recv_sem, where):
    return pltpu.make_async_remote_copy(src_ref=src, dst_ref=dst, send_sem=send_sem, recv_sem=recv_sem, device_id=where, device_id_type=MESH)


def sink_column(row_ref, count, halves, group):
    row = lax.broadcasted_iota(jnp.int32, (count, count), 0)
    per_half = count // halves
    part = group // halves
    head = lax.div(lax.rem(row, per_half), part) * group + lax.div(row, per_half) * part + lax.rem(row, part)
    same = head == lax.broadcasted_iota(jnp.int32, (count, count), 1)
    return jnp.sum(jnp.where(same, jnp.broadcast_to(row_ref[...], (count, count)), 0.0), axis=1, keepdims=True)


QKV_ROWS = 512
QKV_SLOTS = 3
CACHE_SEQS = 8
CACHE_AHEAD = 4


def project_kernel(x_ref, gain_ref, cos_ref, sin_ref, bias_ref, w_ref, k_ref, v_ref, out_ref, k_out, v_out,
                   normed, gain, heads, acc_q, acc_e, wq_buf, we_buf, k_buf, v_buf, wq_sem, we_sem, out_sem, k_in, v_in, k_back, v_back):
    _, core = sp_place()
    num_seqs, depth = x_ref.shape
    head_dim = acc_e.shape[2]
    q_cols = acc_q.shape[2]
    kv_local = acc_q.shape[0]
    per_core = q_cols // head_dim
    group = 2 * per_core
    steps = depth // QKV_ROWS
    blocks = num_seqs // CACHE_SEQS

    def fetch(step, slot):
        rows = pl.ds(step * QKV_ROWS, QKV_ROWS)
        cq = pltpu.make_async_copy(w_ref.at[rows, :, pl.ds(pl.multiple_of(core * q_cols, 128), q_cols)], wq_buf.at[slot], wq_sem.at[slot])
        ce = pltpu.make_async_copy(w_ref.at[rows, :, pl.ds(pl.multiple_of((group + core) * head_dim, 128), head_dim)], we_buf.at[slot], we_sem.at[slot])
        return cq, ce

    def cache_in(i):
        at = pl.ds(i * CACHE_SEQS, CACHE_SEQS)
        return pltpu.make_async_copy(k_ref.at[at], k_buf.at[at], k_in.at[i]), pltpu.make_async_copy(v_ref.at[at], v_buf.at[at], v_in.at[i])

    def cache_back(i):
        at = pl.ds(i * CACHE_SEQS, CACHE_SEQS)
        return pltpu.make_async_copy(k_buf.at[at], k_out.at[at], k_back.at[i]), pltpu.make_async_copy(v_buf.at[at], v_out.at[at], v_back.at[i])

    for s in range(QKV_SLOTS - 1):
        for c in fetch(s, s):
            c.start()
    for i in range(CACHE_AHEAD):
        for c in cache_in(i):
            c.start()

    gain[...] = gain_ref[...].astype(F32)

    def norm_rows(r, _):
        rows = pl.ds(pl.multiple_of(r * 16, 16), 16)
        xw = x_ref[rows, :].astype(F32)
        inv = lax.rsqrt(jnp.mean(xw * xw, axis=-1, keepdims=True) + NORM_EPS)
        for t in range(depth // head_dim):
            cols = slice(t * head_dim, (t + 1) * head_dim)
            normed[rows, cols] = (xw[:, cols] * inv * gain[t : t + 1, :]).astype(BF16)
        return 0

    lax.fori_loop(0, num_seqs // 16, norm_rows, 0)
    acc_q[...] = jnp.zeros_like(acc_q)
    acc_e[...] = jnp.zeros_like(acc_e)

    def step_fn(step, _):
        slot = lax.rem(step, QKV_SLOTS)

        @pl.when(step + CACHE_AHEAD < blocks)
        def _():
            for c in cache_in(step + CACHE_AHEAD):
                c.start()

        for c in fetch(step, slot):
            c.wait()

        @pl.when(step + QKV_SLOTS - 1 < steps)
        def _():
            for c in fetch(step + QKV_SLOTS - 1, lax.rem(step + QKV_SLOTS - 1, QKV_SLOTS)):
                c.start()

        for c in cache_in(step):
            c.wait()
        for c in cache_back(step):
            c.start()

        h = normed[:, pl.ds(pl.multiple_of(step * QKV_ROWS, 128), QKV_ROWS)]
        wq = jnp.swapaxes(wq_buf[slot], 0, 1)
        we = jnp.swapaxes(we_buf[slot], 0, 1)
        for k in range(kv_local):
            acc_q[k] += jnp.dot(h, wq[k], preferred_element_type=F32)
            acc_e[k] += jnp.dot(h, we[k], preferred_element_type=F32)
        return 0

    lax.fori_loop(0, steps, step_fn, 0)

    cos_t = cos_ref[...].T
    sin_t = sin_ref[...].T
    cos2 = jnp.concatenate([cos_t, cos_t], axis=1)
    sin2 = jnp.concatenate([-sin_t, sin_t], axis=1)
    is_key = core == 0
    cos_e = jnp.where(is_key, cos2, jnp.ones_like(cos2))
    sin_e = jnp.where(is_key, sin2, jnp.zeros_like(sin2))

    def rotate(v, c, s):
        r = v * c + pltpu.roll(v, head_dim // 2, 1) * s
        return r.astype(BF16).astype(F32)

    for k in range(kv_local):
        bias_q = bias_ref[k : k + 1, pl.ds(pl.multiple_of(core * q_cols, 128), q_cols)].astype(F32)
        for g in range(per_core):
            cols = slice(g * head_dim, (g + 1) * head_dim)
            heads[k * per_core + g] = rotate(acc_q[k, :, cols] + bias_q[:, cols], cos2, sin2)
        bias_e = bias_ref[k : k + 1, pl.ds(pl.multiple_of((group + core) * head_dim, 128), head_dim)].astype(F32)
        heads[kv_local * per_core + k] = rotate(acc_e[k] + bias_e, cos_e, sin_e)
    done = pltpu.make_async_copy(heads, out_ref, out_sem)
    done.start()
    for i in range(blocks):
        for c in cache_back(i):
            c.wait()
    done.wait()


def project(hidden, rope_cos, rope_sin, norm_gain, w_qkv, b_qkv, k_rows, v_rows):
    num_seqs, depth = hidden.shape
    head_dim = k_rows.shape[2]
    kv_local = w_qkv.shape[1]
    per_core = (w_qkv.shape[2] // head_dim - 2) // 2
    rows = kv_local * (per_core + 1)
    blocks = num_seqs // CACHE_SEQS
    assert blocks == depth // QKV_ROWS
    vmem = pl.BlockSpec(memory_space=pltpu.VMEM)
    anyspace = pl.BlockSpec(memory_space=pl.ANY)
    dma = pltpu.SemaphoreType.DMA
    return pl.pallas_call(
        project_kernel,
        out_shape=[
            jax.ShapeDtypeStruct((rows, num_seqs, head_dim), F32),
            jax.ShapeDtypeStruct(k_rows.shape, BF16),
            jax.ShapeDtypeStruct(v_rows.shape, BF16),
        ],
        in_specs=[vmem] * 5 + [anyspace] * 3,
        out_specs=[anyspace] * 3,
        scratch_shapes=[
            pltpu.VMEM((num_seqs, depth), BF16),
            pltpu.VMEM((depth // head_dim, head_dim), F32),
            pltpu.VMEM((rows, num_seqs, head_dim), F32),
            pltpu.VMEM((kv_local, num_seqs, per_core * head_dim), F32),
            pltpu.VMEM((kv_local, num_seqs, head_dim), F32),
            pltpu.VMEM((QKV_SLOTS, QKV_ROWS, kv_local, per_core * head_dim), BF16),
            pltpu.VMEM((QKV_SLOTS, QKV_ROWS, kv_local, head_dim), BF16),
            pltpu.VMEM(k_rows.shape, BF16),
            pltpu.VMEM(v_rows.shape, BF16),
            dma((QKV_SLOTS,)), dma((QKV_SLOTS,)), dma,
            dma((blocks,)), dma((blocks,)), dma((blocks,)), dma((blocks,)),
        ],
        compiler_params=pltpu.CompilerParams(vmem_limit_bytes=60 << 20),
        name="project",
    )(hidden, norm_gain.reshape(depth // head_dim, head_dim), rope_cos.T, rope_sin.T, b_qkv, w_qkv, k_rows, v_rows)


ATT_SEQS = 8
ATT_SLOTS = 6
OUT_COLS = 256
SEQ_GROUPS = 2
W_PARTS = 8
LAG_Y = 6
LAG_X = 5


def finish_kernel(lens_ref, half_hbm, sink_ref, hid_ref, bo_ref, wo_ref, k_hbm, v_hbm, y_ref, new_ref,
                  w_buf, x_buf, h_buf, k_ring, v_ring, pos_ref, num, ml, sink_col, bo_f32, r1, r1ml, own, own_ml, away, away_ml, r2, r2ml, o_buf, r3, o_all,
                  y_send, y_recv, z_buf, x_recv, p1, p2,
                  w_sem, x_sem, k_sem, v_sem, h_in, h_send, h_recv, s1_send, s1_recv, s2_send, s2_recv, s3_send, s3_recv,
                  y_ss, y_rs, x_ss, x_rs, p1_ss, p1_rs, p2_ss, p2_rs):
    chip, core = sp_place()
    tp = lax.axis_index("tp")
    partner = {"sp": 2 * chip + (1 - core)}
    across_x = {"sp": 2 * (1 - chip) + core}
    across_y = {"tp": 1 - tp}
    groups, q_rows, some, head_dim = num.shape
    num_seqs = h_buf.shape[1]
    kv_local = (h_buf.shape[0] - q_rows) // 2
    rows = k_ring.shape[2]
    ctx_local = rows // kv_local
    half_h = q_rows // 2
    half_s = num_seqs // 2
    part_h = half_h // kv_local
    cols = w_buf.shape[1]
    chunks = cols // OUT_COLS
    total = SEQ_GROUPS * chunks
    mine = pl.multiple_of(core * half_h, half_h)
    theirs = pl.multiple_of((1 - core) * half_h, half_h)

    def seqs(which, g):
        return pl.ds(pl.multiple_of(which * half_s + g * some, some), some)

    barrier = pltpu.get_barrier_semaphore()
    for peer in (partner, across_x, across_y):
        pl.semaphore_signal(barrier, inc=1, device_id=peer, device_id_type=MESH)

    order = [(1 - chip, g) for g in range(SEQ_GROUPS)] + [(chip, g) for g in range(SEQ_GROUPS)]
    own_rows = (pl.ds(mine, half_h), pl.ds(pl.multiple_of(q_rows + kv_local * core, kv_local), kv_local))
    src_rows = (pl.ds(0, half_h), pl.ds(half_h, kv_local))
    h_local, h_remote = [], []
    for i, (which, g) in enumerate(order):
        at = seqs(which, g)
        for j in range(2):
            h_local.append(pltpu.make_async_copy(half_hbm.at[src_rows[j], at], h_buf.at[own_rows[j], at], h_in.at[2 * i + j]))
            h_local[-1].start()
            h_remote.append(remote(half_hbm.at[src_rows[j], at], h_buf.at[own_rows[j], at], h_send.at[2 * i + j], h_recv.at[2 * i + j], partner))

    steps = num_seqs // ATT_SEQS
    per_group = some // ATT_SEQS

    def block(p):
        return lax.rem(p + (1 - chip) * (steps // 2), steps) * ATT_SEQS

    def kv_load(p):
        at = pl.ds(pl.multiple_of(block(p), ATT_SEQS), ATT_SEQS)
        slot = lax.rem(p, ATT_SLOTS)
        return pltpu.make_async_copy(k_hbm.at[at], k_ring.at[slot], k_sem.at[slot]), pltpu.make_async_copy(v_hbm.at[at], v_ring.at[slot], v_sem.at[slot])

    for p in range(ATT_SLOTS):
        for c in kv_load(p):
            c.start()
    my_cols = pl.ds(pl.multiple_of(core * cols, 128), cols)
    x_copy_in = pltpu.make_async_copy(hid_ref.at[pl.ds(pl.multiple_of(chip * half_s, half_s), half_s), my_cols], x_buf, x_sem)
    w_cols = cols // W_PARTS
    w_chunks = w_cols // OUT_COLS

    def w_copy(p):
        return pltpu.make_async_copy(wo_ref.at[:, pl.ds(pl.multiple_of(core * cols + p * w_cols, 128), w_cols)], w_buf.at[:, pl.ds(pl.multiple_of(p * w_cols, 128), w_cols)], w_sem.at[p])

    sink = sink_column(sink_ref, q_rows, 2, 2 * part_h)
    sink_col[...] = jnp.broadcast_to(sink, sink_col.shape)
    bo_f32[...] = bo_ref[...].astype(F32)
    pos_ref[...] = lax.div(lax.broadcasted_iota(jnp.int32, pos_ref.shape, 0), kv_local).astype(F32).astype(BF16)
    pl.semaphore_wait(barrier, 3)
    for c in h_remote:
        c.start()

    base = lax.axis_index("sp") * ctx_local
    scale = head_dim**-0.5
    col = lax.broadcasted_iota(jnp.int32, (q_rows, rows), 1)
    kv_row = lax.div(lax.rem(lax.broadcasted_iota(jnp.int32, (q_rows, rows), 0), half_h), part_h)
    col_pos = jnp.where(lax.rem(col, kv_local) == kv_row, lax.div(col, kv_local), ctx_local * 1024)
    lane = lax.broadcasted_iota(jnp.int32, (q_rows, ml.shape[2]), 1)
    batch = range(ATT_SEQS)

    def attend(i, first, last, carry):
        def step_fn(t, carry):
            m_all, l_all = carry
            p = i * per_group + t
            slot = lax.rem(p, ATT_SLOTS)
            for c in kv_load(p):
                c.wait()
            start = block(p)
            heads = h_buf.at[:, pl.ds(pl.multiple_of(start, ATT_SEQS), ATT_SEQS)]
            rel = [lens_ref[start + s] - base for s in batch]
            keys, values = [], []
            for s in batch:
                n = jnp.full((16, head_dim), rel[s].astype(F32)).astype(BF16)
                hit = pos_ref[...].reshape(rows // 16, 16, head_dim) == n[None]
                for j, (ring, out) in enumerate(((k_ring, keys), (v_ring, values))):
                    new = heads[q_rows + j * kv_local : q_rows + (j + 1) * kv_local, s, :].astype(BF16)
                    new_ref[j, start + s] = new
                    new = jnp.concatenate([new] * (16 // kv_local), axis=0)
                    old = ring[slot, s].reshape(rows // 16, 16, head_dim)
                    out.append(jnp.where(hit, new[None], old).reshape(rows, head_dim))
            queries = [heads[0:q_rows, s, :].astype(BF16) for s in batch]
            logits = [lax.dot_general(queries[s], keys[s], (((1,), (1,)), ((), ())), preferred_element_type=F32) for s in batch]
            logits = [jnp.where(col_pos <= rel[s], logits[s] * scale, -jnp.inf) for s in batch]
            tops = [jnp.maximum(jnp.max(logits[s], axis=1, keepdims=True), sink) for s in batch]
            weights = [jnp.exp(logits[s] - tops[s]) for s in batch]
            totals = [jnp.sum(weights[s], axis=1, keepdims=True) for s in batch]
            sums = [jnp.dot(weights[s].astype(BF16), values[s], preferred_element_type=F32) for s in batch]
            out = num.at[i, :, pl.ds(pl.multiple_of(t * ATT_SEQS, ATT_SEQS), ATT_SEQS)]
            for s in batch:
                here = lane == t * ATT_SEQS + s
                m_all = jnp.where(here, tops[s], m_all)
                l_all = jnp.where(here, totals[s], l_all)
                out[:, s, :] = sums[s]

            @pl.when(p + ATT_SLOTS < steps)
            def _():
                for c in kv_load(p + ATT_SLOTS):
                    c.start()

            return m_all, l_all

        return lax.fori_loop(first, last, step_fn, carry)

    def heads_wait(i):
        for j in range(2):
            h_local[2 * i + j].wait()
            h_remote[2 * i + j].wait_recv()

    zero = jnp.zeros((q_rows, ml.shape[2]), F32)
    c1 = []

    def to_partner(i, carry):
        ml[i, 0:q_rows] = carry[0]
        ml[i, q_rows : 2 * q_rows] = carry[1]
        c1.append((
            remote(ml.at[i], r1ml.at[i], s1_send.at[2 * i], s1_recv.at[2 * i], partner),
            remote(num.at[i, pl.ds(theirs, half_h)], r1.at[i], s1_send.at[2 * i + 1], s1_recv.at[2 * i + 1], partner),
        ))
        for c in c1[-1]:
            c.start()

    def combine(i, dst, dst_ml):
        for c in c1[i]:
            c.wait_recv()
        m_a, l_a = ml[i, pl.ds(mine, half_h)], ml[i, pl.ds(q_rows + mine, half_h)]
        m_b, l_b = r1ml[i, pl.ds(mine, half_h)], r1ml[i, pl.ds(q_rows + mine, half_h)]
        m_chip = jnp.maximum(m_a, m_b)
        f_a = jnp.exp(m_a - m_chip)
        f_b = jnp.exp(m_b - m_chip)
        dst_ml[0:half_h] = m_chip
        dst_ml[half_h : 2 * half_h] = l_a * f_a + l_b * f_b
        f_a, f_b = f_a.T, f_b.T
        for h in range(half_h):
            dst[h] = num[i, mine + h] * f_a[0:some, h : h + 1] + r1[i, h] * f_b[0:some, h : h + 1]

    c2 = []

    def across(g):
        combine(g, away.at[g], away_ml.at[g])
        c2.append((
            remote(away_ml.at[g], r2ml.at[g], s2_send.at[2 * g], s2_recv.at[2 * g], across_x),
            remote(away.at[g], r2.at[g], s2_send.at[2 * g + 1], s2_recv.at[2 * g + 1], across_x),
        ))
        for c in c2[-1]:
            c.start()

    width = half_h * head_dim
    part_w = part_h * head_dim

    def o_place(which_half, k):
        return pl.ds(pl.multiple_of(2 * k * part_w + which_half * part_w, 128), part_w)

    def heads_start(g):
        for c in c2[g]:
            c.wait_recv()
        m_a, l_a = own_ml[g, 0:half_h], own_ml[g, half_h : 2 * half_h]
        m_b, l_b = r2ml[g, 0:half_h], r2ml[g, half_h : 2 * half_h]
        m_top = jnp.maximum(m_a, m_b)
        f_a = jnp.exp(m_a - m_top)
        f_b = jnp.exp(m_b - m_top)
        den = l_a * f_a + l_b * f_b + jnp.exp(sink_col[pl.ds(mine, half_h)] - m_top)
        f_a, f_b = (f_a / den).T, (f_b / den).T
        for h in range(half_h):
            o_buf[g, :, h * head_dim : (h + 1) * head_dim] = own[g, h] * f_a[0:some, h : h + 1] + r2[g, h] * f_b[0:some, h : h + 1]
        c = remote(o_buf.at[g], r3.at[g], s3_send.at[g], s3_recv.at[g], partner)
        c.start()
        for k in range(kv_local):
            o_all[g, :, o_place(core, k)] = o_buf[g, :, k * part_w : (k + 1) * part_w].astype(BF16)
        return c

    def heads_end(g, c):
        c.wait_recv()
        for k in range(kv_local):
            o_all[g, :, o_place(1 - core, k)] = r3[g, :, k * part_w : (k + 1) * part_w].astype(BF16)

    def y_copy(t):
        return remote(y_send.at[t], y_recv.at[t], y_ss.at[t], y_rs.at[t], across_y)

    def x_copy(t):
        return remote(z_buf.at[t], x_recv.at[t], x_ss.at[t], x_rs.at[t], across_x)

    def p1_copy(t):
        return remote(z_buf.at[t], p1.at[t], p1_ss.at[t], p1_rs.at[t], partner)

    def p2_copy(t):
        return remote(x_recv.at[t], p2.at[t], p2_ss.at[t], p2_rs.at[t], partner)

    def place(which_seqs, which_cols, t):
        g, j = lax.div(t, chunks), lax.rem(t, chunks)
        return seqs(which_seqs, g), pl.ds(pl.multiple_of(which_cols * cols + j * OUT_COLS, 128), OUT_COLS)

    def body(t, _):
        @pl.when(t < total)
        def _():
            g, j = lax.div(t, chunks), lax.rem(t, chunks)

            @pl.when(jnp.logical_and(g == 0, lax.rem(j, w_chunks) == 0))
            def _():
                w_copy(lax.div(j, w_chunks)).wait()

            w = w_buf[:, pl.ds(pl.multiple_of(j * OUT_COLS, 128), OUT_COLS)]
            y_send[t] = jnp.dot(o_all[g], w, preferred_element_type=F32)
            y_copy(t).start()

        @pl.when(jnp.logical_and(t >= LAG_Y, t < total + LAG_Y))
        def _():
            u = t - LAG_Y
            g, j = lax.div(u, chunks), lax.rem(u, chunks)
            y_copy(u).wait_recv()
            x_part = x_buf[pl.ds(pl.multiple_of(g * some, some), some), pl.ds(pl.multiple_of(j * OUT_COLS, 128), OUT_COLS)].astype(F32)
            row = (core * cols + j * OUT_COLS) // head_dim
            bias = jnp.concatenate([bo_f32[pl.ds(row + i, 1), :] for i in range(OUT_COLS // head_dim)], axis=1)
            z = (x_part + (y_send[u] + y_recv[u]) + bias).astype(BF16)
            z_buf[u] = z.astype(F32)
            x_copy(u).start()
            p1_copy(u).start()
            rows_at, cols_at = place(chip, core, u)
            y_ref[rows_at, cols_at] = z

        @pl.when(t >= LAG_Y + LAG_X)
        def _():
            u = t - (LAG_Y + LAG_X)
            x_copy(u).wait_recv()
            p2_copy(u).start()
            rows_at, cols_at = place(1 - chip, core, u)
            y_ref[rows_at, cols_at] = x_recv[u].astype(BF16)
            p1_copy(u).wait_recv()
            rows_at, cols_at = place(chip, 1 - core, u)
            y_ref[rows_at, cols_at] = p1[u].astype(BF16)

        return 0

    half_group = per_group // 2
    heads_wait(0)
    carry = attend(0, 0, per_group, (zero, zero))
    to_partner(0, carry)
    x_copy_in.start()
    heads_wait(1)
    carry = attend(1, 0, half_group, (zero, zero))
    across(0)
    carry = attend(1, half_group, per_group, carry)
    to_partner(1, carry)
    w_copy(0).start()
    heads_wait(2)
    carry = attend(2, 0, half_group, (zero, zero))
    across(1)
    w_copy(1).start()
    carry = attend(2, half_group, per_group, carry)
    to_partner(2, carry)
    for p in range(2, W_PARTS):
        w_copy(p).start()
    heads_wait(3)
    carry = attend(3, 0, per_group, (zero, zero))
    to_partner(3, carry)
    combine(2, own.at[0], own_ml.at[0])
    combine(3, own.at[1], own_ml.at[1])

    c3 = [heads_start(0)]
    heads_end(0, c3[0])
    x_copy_in.wait()
    lax.fori_loop(0, 8, body, 0)
    c3.append(heads_start(1))
    lax.fori_loop(8, 12, body, 0)
    heads_end(1, c3[1])
    lax.fori_loop(12, total + LAG_Y + LAG_X, body, 0)

    def tail(t, _):
        p2_copy(t).wait_recv()
        rows_at, cols_at = place(1 - chip, 1 - core, t)
        y_ref[rows_at, cols_at] = p2[t].astype(BF16)
        y_copy(t).wait_send()
        x_copy(t).wait_send()
        p1_copy(t).wait_send()
        p2_copy(t).wait_send()
        return 0

    lax.fori_loop(0, total, tail, 0)
    for c in (*h_remote, *(c for pair in c1 + c2 for c in pair), *c3):
        c.wait_send()


def finish(seq_lens, half, sinks, hidden, b_o, w_o, k_rows, v_rows):
    num_seqs, rows, head_dim = k_rows.shape
    q_rows = sinks.shape[1]
    half_h, half_s = q_rows // 2, num_seqs // 2
    kv_local = half.shape[0] - half_h
    some = half_s // SEQ_GROUPS
    groups = 2 * SEQ_GROUPS
    width = w_o.shape[1]
    cols = width // 2
    total = SEQ_GROUPS * (cols // OUT_COLS)
    vmem = pl.BlockSpec(memory_space=pltpu.VMEM)
    anyspace = pl.BlockSpec(memory_space=pl.ANY)
    chunked = pltpu.VMEM((total, some, OUT_COLS), F32)
    parts = pltpu.VMEM((SEQ_GROUPS, half_h, some, head_dim), F32)
    parts_ml = pltpu.VMEM((SEQ_GROUPS, 2 * half_h, 128), F32)
    ring = pltpu.VMEM((ATT_SLOTS, ATT_SEQS, rows, head_dim), BF16)
    dma = pltpu.SemaphoreType.DMA
    return pl.pallas_call(
        finish_kernel,
        out_shape=[
            jax.ShapeDtypeStruct((num_seqs, width), BF16),
            jax.ShapeDtypeStruct((2, num_seqs, kv_local, head_dim), BF16),
        ],
        in_specs=[pl.BlockSpec(memory_space=pltpu.SMEM), anyspace, vmem, anyspace, vmem, anyspace, anyspace, anyspace],
        out_specs=[vmem, vmem],
        scratch_shapes=[
            pltpu.VMEM((w_o.shape[0], cols), BF16),
            pltpu.VMEM((half_s, cols), BF16),
            pltpu.VMEM((q_rows + 2 * kv_local, num_seqs, head_dim), F32),
            ring, ring,
            pltpu.VMEM((rows, head_dim), BF16),
            pltpu.VMEM((groups, q_rows, some, head_dim), F32),
            pltpu.VMEM((groups, 2 * q_rows, 128), F32),
            pltpu.VMEM((q_rows, 128), F32),
            pltpu.VMEM((width // head_dim, head_dim), F32),
            pltpu.VMEM((groups, half_h, some, head_dim), F32),
            pltpu.VMEM((groups, 2 * q_rows, 128), F32),
            parts, parts_ml, parts, parts_ml, parts, parts_ml,
            pltpu.VMEM((SEQ_GROUPS, some, half_h * head_dim), F32),
            pltpu.VMEM((SEQ_GROUPS, some, half_h * head_dim), F32),
            pltpu.VMEM((SEQ_GROUPS, some, q_rows * head_dim), BF16),
            chunked, chunked, chunked, chunked, chunked, chunked,
            dma((W_PARTS,)), dma, dma((ATT_SLOTS,)), dma((ATT_SLOTS,)),
            dma((2 * groups,)), dma((2 * groups,)), dma((2 * groups,)),
            dma((2 * groups,)), dma((2 * groups,)),
            dma((groups,)), dma((groups,)),
            dma((SEQ_GROUPS,)), dma((SEQ_GROUPS,)),
            *[dma((total,))] * 8,
        ],
        compiler_params=pltpu.CompilerParams(collective_id=1, has_side_effects=True, vmem_limit_bytes=62 << 20),
        name="finish",
    )(seq_lens, half, sinks, hidden, b_o.reshape(width // head_dim, head_dim), w_o, k_rows, v_rows)


LAST_PARTS = 4


def last_kernel(lens_ref, y_hbm, new_ref, k_in, v_in, y_out, k_out, v_out, y_buf, in_sem, out_sem, k_sem, v_sem):
    num_seqs, ctx_local = k_out.shape[:2]
    base = lax.axis_index("sp") * ctx_local
    rows = y_hbm.shape[0] // LAST_PARTS
    loads, stores = [], []
    for p in range(LAST_PARTS):
        at = pl.ds(p * rows, rows)
        loads.append(pltpu.make_async_copy(y_hbm.at[at], y_buf.at[at], in_sem.at[p]))
        stores.append(pltpu.make_async_copy(y_buf.at[at], y_out.at[at], out_sem.at[p]))
        loads[-1].start()

    def copies(b, n):
        return pltpu.make_async_copy(new_ref.at[0, b], k_out.at[b, n], k_sem), pltpu.make_async_copy(new_ref.at[1, b], v_out.at[b, n], v_sem)

    def put(b, _):
        n = lens_ref[b] - base

        @pl.when(jnp.logical_and(n >= 0, n < ctx_local))
        def _():
            for c in copies(b, n):
                c.start()

        return 0

    lax.fori_loop(0, num_seqs, put, 0)
    for p in range(LAST_PARTS):
        loads[p].wait()
        stores[p].start()

    def settle(b, _):
        n = lens_ref[b] - base

        @pl.when(jnp.logical_and(n >= 0, n < ctx_local))
        def _():
            for c in copies(b, n):
                c.wait()

        return 0

    lax.fori_loop(0, num_seqs, settle, 0)
    for c in stores:
        c.wait()


def last(seq_lens, y, new, k_copy, v_copy):
    vmem = pl.BlockSpec(memory_space=pltpu.VMEM)
    anyspace = pl.BlockSpec(memory_space=pl.ANY)
    dma = pltpu.SemaphoreType.DMA
    return pl.pallas_call(
        last_kernel,
        out_shape=[jax.ShapeDtypeStruct(a.shape, a.dtype) for a in (y, k_copy, v_copy)],
        in_specs=[pl.BlockSpec(memory_space=pltpu.SMEM), anyspace, vmem, anyspace, anyspace],
        out_specs=[anyspace] * 3,
        scratch_shapes=[pltpu.VMEM(y.shape, y.dtype), dma((LAST_PARTS,)), dma((LAST_PARTS,)), dma, dma],
        input_output_aliases={3: 1, 4: 2},
        compiler_params=pltpu.CompilerParams(vmem_limit_bytes=60 << 20),
        name="last",
    )(seq_lens, y, new, k_copy, v_copy)


def solution(mesh):
    cache_spec = P("dp", "sp", "tp", None)

    def block_step(hidden, seq_lens, rope_cos, rope_sin, k_cache, v_cache, norm_gain, w_qkv, b_qkv, sink_logits, w_o, b_o):
        num_seqs, ctx_local, kv_local, head_dim = k_cache.shape
        rows = (num_seqs, ctx_local * kv_local, head_dim)
        k_rows, v_rows = k_cache.reshape(rows), v_cache.reshape(rows)
        half, k_copy, v_copy = project(hidden, rope_cos, rope_sin, norm_gain, w_qkv, b_qkv, k_rows, v_rows)
        sinks = sink_logits.reshape(1, sink_logits.shape[0])
        y, new = finish(seq_lens, half, sinks, hidden, b_o, w_o, k_rows, v_rows)
        return last(seq_lens, y, new, k_copy.reshape(k_cache.shape), v_copy.reshape(v_cache.shape))

    return jax.shard_map(block_step, mesh=mesh, in_specs=(P("dp", None), P("dp"), P("dp", None), P("dp", None), cache_spec, cache_spec, P(None), P(None, "tp", None), P("tp", None), P("tp"), P("tp", None), P(None)), out_specs=(P("dp", None), cache_spec, cache_spec), check_vma=False)
```

```python
import functools

import jax
import jax.numpy as jnp
from jax import lax
from jax.experimental import pallas as pl
from jax.experimental.pallas import tpu as pltpu
from jax.sharding import PartitionSpec as P

NORM_EPS = 1e-5
F32 = jnp.float32
BF16 = jnp.bfloat16
MESH = pl.DeviceIdType.MESH


def sp_place():
    sp = lax.axis_index("sp")
    return lax.div(sp, 2), lax.rem(sp, 2)


def remote(src, dst, send_sem, recv_sem, where):
    return pltpu.make_async_remote_copy(src_ref=src, dst_ref=dst, send_sem=send_sem, recv_sem=recv_sem, device_id=where, device_id_type=MESH)


def sink_column(row_ref, count, halves, group):
    row = lax.broadcasted_iota(jnp.int32, (count, count), 0)
    per_half = count // halves
    part = group // halves
    head = lax.div(lax.rem(row, per_half), part) * group + lax.div(row, per_half) * part + lax.rem(row, part)
    same = head == lax.broadcasted_iota(jnp.int32, (count, count), 1)
    return jnp.sum(jnp.where(same, jnp.broadcast_to(row_ref[...], (count, count)), 0.0), axis=1, keepdims=True)


QKV_ROWS = 512
QKV_SLOTS = 4
CACHE_SEQS = 8
CACHE_AHEAD = 6
CACHE_FIRST = 3
X_PARTS = 4


def project_kernel(x_hbm, gain_hbm, cos_hbm, sin_hbm, bias_hbm, w_ref, k_ref, v_ref, out_ref, k_out, v_out,
                   x_ref, gain_ref, cos_ref, sin_ref, bias_ref, x_sem, small_sem, normed, gain, heads, acc_q, acc_e, wq_buf, we_buf, k_buf, v_buf, wq_sem, we_sem, out_sem, k_in, v_in, k_back, v_back):
    _, core = sp_place()
    num_seqs, depth = x_ref.shape
    head_dim = acc_e.shape[2]
    q_cols = acc_q.shape[2]
    kv_local = acc_q.shape[0]
    per_core = q_cols // head_dim
    group = 2 * per_core
    steps = depth // QKV_ROWS
    x_rows = num_seqs // X_PARTS
    blocks = num_seqs // CACHE_SEQS

    def fetch(step, slot):
        rows = pl.ds(step * QKV_ROWS, QKV_ROWS)
        cq = pltpu.make_async_copy(w_ref.at[rows, :, pl.ds(pl.multiple_of(core * q_cols, 128), q_cols)], wq_buf.at[slot], wq_sem.at[slot])
        ce = pltpu.make_async_copy(w_ref.at[rows, :, pl.ds(pl.multiple_of((group + core) * head_dim, 128), head_dim)], we_buf.at[slot], we_sem.at[slot])
        return cq, ce

    def cache_in(i):
        at = pl.ds(i * CACHE_SEQS, CACHE_SEQS)
        return pltpu.make_async_copy(k_ref.at[at], k_buf.at[at], k_in.at[i]), pltpu.make_async_copy(v_ref.at[at], v_buf.at[at], v_in.at[i])

    def cache_back(i):
        at = pl.ds(i * CACHE_SEQS, CACHE_SEQS)
        return pltpu.make_async_copy(k_buf.at[at], k_out.at[at], k_back.at[i]), pltpu.make_async_copy(v_buf.at[at], v_out.at[at], v_back.at[i])

    small = [pltpu.make_async_copy(src, dst, small_sem.at[i]) for i, (src, dst) in enumerate(((gain_hbm, gain_ref), (cos_hbm, cos_ref), (sin_hbm, sin_ref), (bias_hbm, bias_ref)))]
    small[0].start()
    x_copies = []
    for p in range(X_PARTS):
        at = pl.ds(p * x_rows, x_rows)
        x_copies.append(pltpu.make_async_copy(x_hbm.at[at], x_ref.at[at], x_sem.at[p]))
        x_copies[-1].start()
    for c in fetch(0, 0):
        c.start()
    for i in range(CACHE_FIRST):
        for c in cache_in(i):
            c.start()
    for s in range(1, QKV_SLOTS - 1):
        for c in fetch(s, s):
            c.start()
    for i in range(CACHE_FIRST, CACHE_AHEAD):
        for c in cache_in(i):
            c.start()
    for c in small[1:]:
        c.start()

    small[0].wait()
    gain[...] = gain_ref[...].astype(F32)

    def norm_rows(r, _):
        rows = pl.ds(pl.multiple_of(r * 16, 16), 16)
        xw = x_ref[rows, :].astype(F32)
        inv = lax.rsqrt(jnp.mean(xw * xw, axis=-1, keepdims=True) + NORM_EPS)
        for t in range(depth // head_dim):
            cols = slice(t * head_dim, (t + 1) * head_dim)
            normed[rows, cols] = (xw[:, cols] * inv * gain[t : t + 1, :]).astype(BF16)
        return 0

    for p in range(X_PARTS):
        x_copies[p].wait()
        lax.fori_loop(p * x_rows // 16, (p + 1) * x_rows // 16, norm_rows, 0)
    for i in range(CACHE_FIRST):
        for c in cache_in(i):
            c.wait()
        for c in cache_back(i):
            c.start()
    acc_q[...] = jnp.zeros_like(acc_q)
    acc_e[...] = jnp.zeros_like(acc_e)

    def step_fn(step, _):
        slot = lax.rem(step, QKV_SLOTS)

        @pl.when(step + CACHE_AHEAD < blocks)
        def _():
            for c in cache_in(step + CACHE_AHEAD):
                c.start()

        for c in fetch(step, slot):
            c.wait()

        @pl.when(step + QKV_SLOTS - 1 < steps)
        def _():
            for c in fetch(step + QKV_SLOTS - 1, lax.rem(step + QKV_SLOTS - 1, QKV_SLOTS)):
                c.start()

        @pl.when(step + CACHE_FIRST < blocks)
        def _():
            for c in cache_in(step + CACHE_FIRST):
                c.wait()
            for c in cache_back(step + CACHE_FIRST):
                c.start()

        h = normed[:, pl.ds(pl.multiple_of(step * QKV_ROWS, 128), QKV_ROWS)]
        wq = jnp.swapaxes(wq_buf[slot], 0, 1)
        we = jnp.swapaxes(we_buf[slot], 0, 1)
        for k in range(kv_local):
            acc_q[k] += jnp.dot(h, wq[k], preferred_element_type=F32)
            acc_e[k] += jnp.dot(h, we[k], preferred_element_type=F32)
        return 0

    lax.fori_loop(0, steps, step_fn, 0)

    for c in small[1:]:
        c.wait()
    cos_t = cos_ref[...].T
    sin_t = sin_ref[...].T
    cos2 = jnp.concatenate([cos_t, cos_t], axis=1)
    sin2 = jnp.concatenate([-sin_t, sin_t], axis=1)
    is_key = core == 0
    cos_e = jnp.where(is_key, cos2, jnp.ones_like(cos2))
    sin_e = jnp.where(is_key, sin2, jnp.zeros_like(sin2))

    def rotate(v, c, s):
        r = v * c + pltpu.roll(v, head_dim // 2, 1) * s
        return r.astype(BF16).astype(F32)

    for k in range(kv_local):
        bias_q = bias_ref[k : k + 1, pl.ds(pl.multiple_of(core * q_cols, 128), q_cols)].astype(F32)
        for g in range(per_core):
            cols = slice(g * head_dim, (g + 1) * head_dim)
            heads[k * per_core + g] = rotate(acc_q[k, :, cols] + bias_q[:, cols], cos2, sin2)
        bias_e = bias_ref[k : k + 1, pl.ds(pl.multiple_of((group + core) * head_dim, 128), head_dim)].astype(F32)
        heads[kv_local * per_core + k] = rotate(acc_e[k] + bias_e, cos_e, sin_e)
    done = pltpu.make_async_copy(heads, out_ref, out_sem)
    done.start()
    for i in range(blocks):
        for c in cache_back(i):
            c.wait()
    done.wait()


def project(hidden, rope_cos, rope_sin, norm_gain, w_qkv, b_qkv, k_rows, v_rows):
    num_seqs, depth = hidden.shape
    head_dim = k_rows.shape[2]
    kv_local = w_qkv.shape[1]
    per_core = (w_qkv.shape[2] // head_dim - 2) // 2
    rows = kv_local * (per_core + 1)
    blocks = num_seqs // CACHE_SEQS
    assert blocks <= depth // QKV_ROWS + CACHE_FIRST
    anyspace = pl.BlockSpec(memory_space=pl.ANY)
    dma = pltpu.SemaphoreType.DMA
    return pl.pallas_call(
        project_kernel,
        out_shape=[
            jax.ShapeDtypeStruct((rows, num_seqs, head_dim), F32),
            jax.ShapeDtypeStruct(k_rows.shape, BF16),
            jax.ShapeDtypeStruct(v_rows.shape, BF16),
        ],
        in_specs=[anyspace] * 8,
        out_specs=[anyspace] * 3,
        scratch_shapes=[
            pltpu.VMEM((num_seqs, depth), BF16),
            pltpu.VMEM((depth // head_dim, head_dim), BF16),
            pltpu.VMEM((head_dim // 2, num_seqs), F32),
            pltpu.VMEM((head_dim // 2, num_seqs), F32),
            pltpu.VMEM(b_qkv.shape, BF16),
            dma((X_PARTS,)),
            dma((4,)),
            pltpu.VMEM((num_seqs, depth), BF16),
            pltpu.VMEM((depth // head_dim, head_dim), F32),
            pltpu.VMEM((rows, num_seqs, head_dim), F32),
            pltpu.VMEM((kv_local, num_seqs, per_core * head_dim), F32),
            pltpu.VMEM((kv_local, num_seqs, head_dim), F32),
            pltpu.VMEM((QKV_SLOTS, QKV_ROWS, kv_local, per_core * head_dim), BF16),
            pltpu.VMEM((QKV_SLOTS, QKV_ROWS, kv_local, head_dim), BF16),
            pltpu.VMEM(k_rows.shape, BF16),
            pltpu.VMEM(v_rows.shape, BF16),
            dma((QKV_SLOTS,)), dma((QKV_SLOTS,)), dma,
            dma((blocks,)), dma((blocks,)), dma((blocks,)), dma((blocks,)),
        ],
        compiler_params=pltpu.CompilerParams(vmem_limit_bytes=60 << 20),
        name="project",
    )(hidden, norm_gain.reshape(depth // head_dim, head_dim), rope_cos.T, rope_sin.T, b_qkv, w_qkv, k_rows, v_rows)


ATT_SEQS = 8
ATT_SLOTS = 6
OUT_COLS = 256
SEQ_GROUPS = 2
W_PARTS = 8
LAG_Y = 6
LAG_X = 5
LAG_P = 2
OUT_CHUNKS = 4


def finish_kernel(lens_ref, half_hbm, sink_ref, hid_ref, bo_ref, wo_ref, k_hbm, v_hbm, y_out, new_ref,
                  y_ref, w_buf, x_buf, h_buf, k_ring, v_ring, num, ml, sink_col, bo_f32, r1, r1ml, own, own_ml, away, away_ml, r2, r2ml, o_buf, r3, o_all,
                  y_send, y_recv, z_buf, x_recv, p1, p2,
                  w_sem, x_sem, k_sem, v_sem, h_in, h_send, h_recv, s1_send, s1_recv, s2_send, s2_recv, s3_send, s3_recv,
                  y_ss, y_rs, x_ss, x_rs, p1_ss, p1_rs, p2_ss, p2_rs, o_sem):
    chip, core = sp_place()
    tp = lax.axis_index("tp")
    partner = {"sp": 2 * chip + (1 - core)}
    across_x = {"sp": 2 * (1 - chip) + core}
    across_y = {"tp": 1 - tp}
    groups, q_rows, some, head_dim = num.shape
    num_seqs = h_buf.shape[1]
    kv_local = (h_buf.shape[0] - q_rows) // 2
    rows = k_ring.shape[2]
    ctx_local = rows // kv_local
    half_h = q_rows // 2
    half_s = num_seqs // 2
    part_h = half_h // kv_local
    cols = w_buf.shape[1]
    chunks = cols // OUT_COLS
    total = SEQ_GROUPS * chunks
    mine = pl.multiple_of(core * half_h, half_h)
    theirs = pl.multiple_of((1 - core) * half_h, half_h)

    def seqs(which, g):
        return pl.ds(pl.multiple_of(which * half_s + g * some, some), some)

    barrier = pltpu.get_barrier_semaphore()
    for peer in (partner, across_x, across_y):
        pl.semaphore_signal(barrier, inc=1, device_id=peer, device_id_type=MESH)

    order = [(1 - chip, g) for g in range(SEQ_GROUPS)] + [(chip, g) for g in range(SEQ_GROUPS)]
    own_rows = (pl.ds(mine, half_h), pl.ds(pl.multiple_of(q_rows + kv_local * core, kv_local), kv_local))
    src_rows = (pl.ds(0, half_h), pl.ds(half_h, kv_local))
    h_local, h_remote = [], []
    for i, (which, g) in enumerate(order):
        at = seqs(which, g)
        for j in range(2):
            h_local.append(pltpu.make_async_copy(half_hbm.at[src_rows[j], at], h_buf.at[own_rows[j], at], h_in.at[2 * i + j]))
            h_local[-1].start()
            h_remote.append(remote(half_hbm.at[src_rows[j], at], h_buf.at[own_rows[j], at], h_send.at[2 * i + j], h_recv.at[2 * i + j], partner))

    steps = num_seqs // ATT_SEQS
    per_group = some // ATT_SEQS

    def block(p):
        return lax.rem(p + (1 - chip) * (steps // 2), steps) * ATT_SEQS

    def kv_load(p):
        at = pl.ds(pl.multiple_of(block(p), ATT_SEQS), ATT_SEQS)
        slot = lax.rem(p, ATT_SLOTS)
        return pltpu.make_async_copy(k_hbm.at[at], k_ring.at[slot], k_sem.at[slot]), pltpu.make_async_copy(v_hbm.at[at], v_ring.at[slot], v_sem.at[slot])

    for p in range(ATT_SLOTS):
        for c in kv_load(p):
            c.start()
    my_cols = pl.ds(pl.multiple_of(core * cols, 128), cols)
    x_copy_in = pltpu.make_async_copy(hid_ref.at[pl.ds(pl.multiple_of(chip * half_s, half_s), half_s), my_cols], x_buf, x_sem)
    w_cols = cols // W_PARTS
    w_chunks = w_cols // OUT_COLS

    def w_copy(p):
        return pltpu.make_async_copy(wo_ref.at[:, pl.ds(pl.multiple_of(core * cols + p * w_cols, 128), w_cols)], w_buf.at[:, pl.ds(pl.multiple_of(p * w_cols, 128), w_cols)], w_sem.at[p])

    sink = sink_column(sink_ref, q_rows, 2, 2 * part_h)
    sink_col[...] = jnp.broadcast_to(sink, sink_col.shape)
    bo_f32[...] = bo_ref[...].astype(F32)
    pl.semaphore_wait(barrier, 3)
    for c in h_remote:
        c.start()

    base = lax.axis_index("sp") * ctx_local
    scale = head_dim**-0.5
    col = lax.broadcasted_iota(jnp.int32, (q_rows, rows), 1)
    kv_row = lax.div(lax.rem(lax.broadcasted_iota(jnp.int32, (q_rows, rows), 0), half_h), part_h)
    col_pos = jnp.where(lax.rem(col, kv_local) == kv_row, lax.div(col, kv_local), ctx_local * 1024)
    lane = lax.broadcasted_iota(jnp.int32, (q_rows, ml.shape[2]), 1)
    batch = range(ATT_SEQS)
    over_d = (((1,), (1,)), ((), ()))
    new_code = jnp.where(lax.broadcasted_iota(jnp.int32, (q_rows, 16), 1) == lax.div(lax.rem(lax.broadcasted_iota(jnp.int32, (q_rows, 16), 0), half_h), part_h), 1, 2)

    def attend(i, first, last, carry):
        def step_fn(t, carry):
            m_all, l_all = carry
            p = i * per_group + t
            slot = lax.rem(p, ATT_SLOTS)
            for c in kv_load(p):
                c.wait()
            start = block(p)
            heads = h_buf.at[:, pl.ds(pl.multiple_of(start, ATT_SEQS), ATT_SEQS)]
            rel = [lens_ref[start + s] - base for s in batch]
            inside = [jnp.where(jnp.logical_and(r >= 0, r < ctx_local), 1, 0) for r in rel]
            queries = [heads[0:q_rows, s, :].astype(BF16) for s in batch]
            new_k, new_v = ([jnp.concatenate([heads[lo : lo + kv_local, s, :]] * (16 // kv_local), axis=0).astype(BF16) for s in batch] for lo in (q_rows, q_rows + kv_local))
            logits = [lax.dot_general(queries[s], k_ring[slot, s], over_d, preferred_element_type=F32) for s in batch]
            extra = [lax.dot_general(queries[s], new_k[s], over_d, preferred_element_type=F32) for s in batch]
            logits = [jnp.where(col_pos < rel[s], logits[s] * scale, -jnp.inf) for s in batch]
            extra = [jnp.where(new_code == inside[s], extra[s] * scale, -jnp.inf) for s in batch]
            tops = [jnp.maximum(jnp.maximum(jnp.max(logits[s], axis=1, keepdims=True), jnp.max(extra[s], axis=1, keepdims=True)), sink) for s in batch]
            weights = [jnp.exp(logits[s] - tops[s]) for s in batch]
            extra = [jnp.exp(extra[s] - tops[s]) for s in batch]
            totals = [jnp.sum(weights[s], axis=1, keepdims=True) + jnp.sum(extra[s], axis=1, keepdims=True) for s in batch]
            sums = [jnp.dot(weights[s].astype(BF16), v_ring[slot, s], preferred_element_type=F32) for s in batch]
            sums = [sums[s] + jnp.dot(extra[s].astype(BF16), new_v[s], preferred_element_type=F32) for s in batch]
            out = num.at[i, :, pl.ds(pl.multiple_of(t * ATT_SEQS, ATT_SEQS), ATT_SEQS)]
            for s in batch:
                here = lane == t * ATT_SEQS + s
                m_all = jnp.where(here, tops[s], m_all)
                l_all = jnp.where(here, totals[s], l_all)
                out[:, s, :] = sums[s]
            for s in batch:
                for j in range(2):
                    new_ref[j, start + s] = heads[q_rows + j * kv_local : q_rows + (j + 1) * kv_local, s, :].astype(BF16)

            @pl.when(p + ATT_SLOTS < steps)
            def _():
                for c in kv_load(p + ATT_SLOTS):
                    c.start()

            return m_all, l_all

        return lax.fori_loop(first, last, step_fn, carry)

    def heads_wait(i):
        for j in range(2):
            h_local[2 * i + j].wait()
            h_remote[2 * i + j].wait_recv()

    zero = jnp.zeros((q_rows, ml.shape[2]), F32)
    c1 = []

    def to_partner(i, carry):
        ml[i, 0:q_rows] = carry[0]
        ml[i, q_rows : 2 * q_rows] = carry[1]
        c1.append((
            remote(ml.at[i], r1ml.at[i], s1_send.at[2 * i], s1_recv.at[2 * i], partner),
            remote(num.at[i, pl.ds(theirs, half_h)], r1.at[i], s1_send.at[2 * i + 1], s1_recv.at[2 * i + 1], partner),
        ))
        for c in c1[-1]:
            c.start()

    def combine(i, dst, dst_ml):
        for c in c1[i]:
            c.wait_recv()
        m_a, l_a = ml[i, pl.ds(mine, half_h)], ml[i, pl.ds(q_rows + mine, half_h)]
        m_b, l_b = r1ml[i, pl.ds(mine, half_h)], r1ml[i, pl.ds(q_rows + mine, half_h)]
        m_chip = jnp.maximum(m_a, m_b)
        f_a = jnp.exp(m_a - m_chip)
        f_b = jnp.exp(m_b - m_chip)
        dst_ml[0:half_h] = m_chip
        dst_ml[half_h : 2 * half_h] = l_a * f_a + l_b * f_b
        f_a, f_b = f_a.T, f_b.T
        for h in range(half_h):
            dst[h] = num[i, mine + h] * f_a[0:some, h : h + 1] + r1[i, h] * f_b[0:some, h : h + 1]

    c2 = []

    def across(g):
        combine(g, away.at[g], away_ml.at[g])
        c2.append((
            remote(away_ml.at[g], r2ml.at[g], s2_send.at[2 * g], s2_recv.at[2 * g], across_x),
            remote(away.at[g], r2.at[g], s2_send.at[2 * g + 1], s2_recv.at[2 * g + 1], across_x),
        ))
        for c in c2[-1]:
            c.start()

    width = half_h * head_dim
    part_w = part_h * head_dim

    def o_place(which_half, k):
        return pl.ds(pl.multiple_of(2 * k * part_w + which_half * part_w, 128), part_w)

    def heads_start(g):
        for c in c2[g]:
            c.wait_recv()
        m_a, l_a = own_ml[g, 0:half_h], own_ml[g, half_h : 2 * half_h]
        m_b, l_b = r2ml[g, 0:half_h], r2ml[g, half_h : 2 * half_h]
        m_top = jnp.maximum(m_a, m_b)
        f_a = jnp.exp(m_a - m_top)
        f_b = jnp.exp(m_b - m_top)
        den = l_a * f_a + l_b * f_b + jnp.exp(sink_col[pl.ds(mine, half_h)] - m_top)
        f_a, f_b = (f_a / den).T, (f_b / den).T
        for h in range(half_h):
            o_buf[g, :, h * head_dim : (h + 1) * head_dim] = own[g, h] * f_a[0:some, h : h + 1] + r2[g, h] * f_b[0:some, h : h + 1]
        c = remote(o_buf.at[g], r3.at[g], s3_send.at[g], s3_recv.at[g], partner)
        c.start()
        for k in range(kv_local):
            o_all[g, :, o_place(core, k)] = o_buf[g, :, k * part_w : (k + 1) * part_w].astype(BF16)
        return c

    def heads_end(g, c):
        c.wait_recv()
        for k in range(kv_local):
            o_all[g, :, o_place(1 - core, k)] = r3[g, :, k * part_w : (k + 1) * part_w].astype(BF16)

    def y_copy(t):
        return remote(y_send.at[t], y_recv.at[t], y_ss.at[t], y_rs.at[t], across_y)

    def x_copy(t):
        return remote(z_buf.at[t], x_recv.at[t], x_ss.at[t], x_rs.at[t], across_x)

    def p1_copy(t):
        return remote(z_buf.at[t], p1.at[t], p1_ss.at[t], p1_rs.at[t], partner)

    def p2_copy(t):
        return remote(x_recv.at[t], p2.at[t], p2_ss.at[t], p2_rs.at[t], partner)

    def place(which_seqs, which_cols, t):
        g, j = lax.div(t, chunks), lax.rem(t, chunks)
        return seqs(which_seqs, g), pl.ds(pl.multiple_of(which_cols * cols + j * OUT_COLS, 128), OUT_COLS)

    def out_copy(kind, q):
        which_seqs, which_cols = ((chip, core), (1 - chip, core), (chip, 1 - core), (1 - chip, 1 - core))[kind]
        rows_at, _ = place(which_seqs, which_cols, q * OUT_CHUNKS)
        j = lax.rem(q * OUT_CHUNKS, chunks)
        cols_at = pl.ds(pl.multiple_of(which_cols * cols + j * OUT_COLS, 128), OUT_CHUNKS * OUT_COLS)
        return pltpu.make_async_copy(y_ref.at[rows_at, cols_at], y_out.at[rows_at, cols_at], o_sem.at[kind, q])

    def put_out(u, kinds):
        @pl.when(lax.rem(u, OUT_CHUNKS) == OUT_CHUNKS - 1)
        def _():
            for kind in kinds:
                out_copy(kind, lax.div(u, OUT_CHUNKS)).start()

    def body(t, _):
        @pl.when(t < total)
        def _():
            g, j = lax.div(t, chunks), lax.rem(t, chunks)

            @pl.when(jnp.logical_and(g == 0, lax.rem(j, w_chunks) == 0))
            def _():
                w_copy(lax.div(j, w_chunks)).wait()

            w = w_buf[:, pl.ds(pl.multiple_of(j * OUT_COLS, 128), OUT_COLS)]
            y_send[t] = jnp.dot(o_all[g], w, preferred_element_type=F32)
            y_copy(t).start()

        @pl.when(jnp.logical_and(t >= LAG_Y, t < total + LAG_Y))
        def _():
            u = t - LAG_Y
            g, j = lax.div(u, chunks), lax.rem(u, chunks)
            y_copy(u).wait_recv()
            x_part = x_buf[pl.ds(pl.multiple_of(g * some, some), some), pl.ds(pl.multiple_of(j * OUT_COLS, 128), OUT_COLS)].astype(F32)
            row = (core * cols + j * OUT_COLS) // head_dim
            bias = jnp.concatenate([bo_f32[pl.ds(row + i, 1), :] for i in range(OUT_COLS // head_dim)], axis=1)
            z = (x_part + (y_send[u] + y_recv[u]) + bias).astype(BF16)
            z_buf[u] = z.astype(F32)
            x_copy(u).start()
            p1_copy(u).start()
            rows_at, cols_at = place(chip, core, u)
            y_ref[rows_at, cols_at] = z
            put_out(u, (0,))

        @pl.when(jnp.logical_and(t >= LAG_Y + LAG_X, t < total + LAG_Y + LAG_X))
        def _():
            u = t - (LAG_Y + LAG_X)
            x_copy(u).wait_recv()
            p2_copy(u).start()
            rows_at, cols_at = place(1 - chip, core, u)
            y_ref[rows_at, cols_at] = x_recv[u].astype(BF16)
            p1_copy(u).wait_recv()
            rows_at, cols_at = place(chip, 1 - core, u)
            y_ref[rows_at, cols_at] = p1[u].astype(BF16)
            put_out(u, (1, 2))

        @pl.when(t >= LAG_Y + LAG_X + LAG_P)
        def _():
            u = t - (LAG_Y + LAG_X + LAG_P)
            p2_copy(u).wait_recv()
            rows_at, cols_at = place(1 - chip, 1 - core, u)
            y_ref[rows_at, cols_at] = p2[u].astype(BF16)
            put_out(u, (3,))

        return 0

    half_group = per_group // 2
    heads_wait(0)
    carry = attend(0, 0, per_group, (zero, zero))
    to_partner(0, carry)
    x_copy_in.start()
    heads_wait(1)
    carry = attend(1, 0, half_group, (zero, zero))
    across(0)
    carry = attend(1, half_group, per_group, carry)
    to_partner(1, carry)
    w_copy(0).start()
    heads_wait(2)
    carry = attend(2, 0, half_group, (zero, zero))
    across(1)
    w_copy(1).start()
    carry = attend(2, half_group, per_group, carry)
    to_partner(2, carry)
    for p in range(2, W_PARTS):
        w_copy(p).start()
    heads_wait(3)
    carry = attend(3, 0, per_group, (zero, zero))
    to_partner(3, carry)
    combine(2, own.at[0], own_ml.at[0])
    combine(3, own.at[1], own_ml.at[1])

    c3 = [heads_start(0)]
    heads_end(0, c3[0])
    x_copy_in.wait()
    lax.fori_loop(0, 8, body, 0)
    c3.append(heads_start(1))
    lax.fori_loop(8, 12, body, 0)
    heads_end(1, c3[1])
    lax.fori_loop(12, total + LAG_Y + LAG_X + LAG_P, body, 0)

    def tail(t, _):
        y_copy(t).wait_send()
        x_copy(t).wait_send()
        p1_copy(t).wait_send()
        p2_copy(t).wait_send()
        return 0

    lax.fori_loop(0, total, tail, 0)

    def settle(q, _):
        for kind in range(4):
            out_copy(kind, q).wait()
        return 0

    lax.fori_loop(0, total // OUT_CHUNKS, settle, 0)
    for c in (*h_remote, *(c for pair in c1 + c2 for c in pair), *c3):
        c.wait_send()


def finish(seq_lens, half, sinks, hidden, b_o, w_o, k_rows, v_rows):
    num_seqs, rows, head_dim = k_rows.shape
    q_rows = sinks.shape[1]
    half_h, half_s = q_rows // 2, num_seqs // 2
    kv_local = half.shape[0] - half_h
    some = half_s // SEQ_GROUPS
    groups = 2 * SEQ_GROUPS
    width = w_o.shape[1]
    cols = width // 2
    total = SEQ_GROUPS * (cols // OUT_COLS)
    vmem = pl.BlockSpec(memory_space=pltpu.VMEM)
    anyspace = pl.BlockSpec(memory_space=pl.ANY)
    chunked = pltpu.VMEM((total, some, OUT_COLS), F32)
    parts = pltpu.VMEM((SEQ_GROUPS, half_h, some, head_dim), F32)
    parts_ml = pltpu.VMEM((SEQ_GROUPS, 2 * half_h, 128), F32)
    ring = pltpu.VMEM((ATT_SLOTS, ATT_SEQS, rows, head_dim), BF16)
    dma = pltpu.SemaphoreType.DMA
    return pl.pallas_call(
        finish_kernel,
        out_shape=[
            jax.ShapeDtypeStruct((num_seqs, width), BF16),
            jax.ShapeDtypeStruct((2, num_seqs, kv_local, head_dim), BF16),
        ],
        in_specs=[pl.BlockSpec(memory_space=pltpu.SMEM), anyspace, vmem, anyspace, vmem, anyspace, anyspace, anyspace],
        out_specs=[anyspace, vmem],
        scratch_shapes=[
            pltpu.VMEM((num_seqs, width), BF16),
            pltpu.VMEM((w_o.shape[0], cols), BF16),
            pltpu.VMEM((half_s, cols), BF16),
            pltpu.VMEM((q_rows + 2 * kv_local, num_seqs, head_dim), F32),
            ring, ring,
            pltpu.VMEM((groups, q_rows, some, head_dim), F32),
            pltpu.VMEM((groups, 2 * q_rows, 128), F32),
            pltpu.VMEM((q_rows, 128), F32),
            pltpu.VMEM((width // head_dim, head_dim), F32),
            pltpu.VMEM((groups, half_h, some, head_dim), F32),
            pltpu.VMEM((groups, 2 * q_rows, 128), F32),
            parts, parts_ml, parts, parts_ml, parts, parts_ml,
            pltpu.VMEM((SEQ_GROUPS, some, half_h * head_dim), F32),
            pltpu.VMEM((SEQ_GROUPS, some, half_h * head_dim), F32),
            pltpu.VMEM((SEQ_GROUPS, some, q_rows * head_dim), BF16),
            chunked, chunked, chunked, chunked, chunked, chunked,
            dma((W_PARTS,)), dma, dma((ATT_SLOTS,)), dma((ATT_SLOTS,)),
            dma((2 * groups,)), dma((2 * groups,)), dma((2 * groups,)),
            dma((2 * groups,)), dma((2 * groups,)),
            dma((groups,)), dma((groups,)),
            dma((SEQ_GROUPS,)), dma((SEQ_GROUPS,)),
            *[dma((total,))] * 8,
            dma((4, total // OUT_CHUNKS)),
        ],
        compiler_params=pltpu.CompilerParams(collective_id=1, has_side_effects=True, vmem_limit_bytes=62 << 20),
        name="finish",
    )(seq_lens, half, sinks, hidden, b_o.reshape(width // head_dim, head_dim), w_o, k_rows, v_rows)


LAST_PARTS = 4
LAST_UNROLL = 8


def last_kernel(lens_ref, y_hbm, new_hbm, k_in, v_in, y_out, k_out, v_out, y_buf, new_ref, in_sem, out_sem, new_sem, k_sem, v_sem):
    num_seqs, ctx_local = k_out.shape[:2]
    base = lax.axis_index("sp") * ctx_local
    rows = y_hbm.shape[0] // LAST_PARTS
    new_copy = pltpu.make_async_copy(new_hbm, new_ref, new_sem)
    new_copy.start()
    loads, stores = [], []
    for p in range(LAST_PARTS):
        at = pl.ds(p * rows, rows)
        loads.append(pltpu.make_async_copy(y_hbm.at[at], y_buf.at[at], in_sem.at[p]))
        stores.append(pltpu.make_async_copy(y_buf.at[at], y_out.at[at], out_sem.at[p]))
        loads[-1].start()

    def for_new_rows(act):
        def step(i, _):
            for b in (i * LAST_UNROLL + r for r in range(LAST_UNROLL)):
                n = lens_ref[b] - base

                @pl.when(jnp.logical_and(n >= 0, n < ctx_local))
                def _():
                    act(pltpu.make_async_copy(new_ref.at[0, b], k_out.at[b, n], k_sem))
                    act(pltpu.make_async_copy(new_ref.at[1, b], v_out.at[b, n], v_sem))

            return 0

        lax.fori_loop(0, num_seqs // LAST_UNROLL, step, 0)

    new_copy.wait()
    for_new_rows(lambda c: c.start())
    for p in range(LAST_PARTS):
        loads[p].wait()
        stores[p].start()
    for_new_rows(lambda c: c.wait())
    for c in stores:
        c.wait()


def last(seq_lens, y, new, k_copy, v_copy):
    anyspace = pl.BlockSpec(memory_space=pl.ANY)
    dma = pltpu.SemaphoreType.DMA
    return pl.pallas_call(
        last_kernel,
        out_shape=[jax.ShapeDtypeStruct(a.shape, a.dtype) for a in (y, k_copy, v_copy)],
        in_specs=[pl.BlockSpec(memory_space=pltpu.SMEM)] + [anyspace] * 4,
        out_specs=[anyspace] * 3,
        scratch_shapes=[pltpu.VMEM(y.shape, y.dtype), pltpu.VMEM(new.shape, new.dtype), dma((LAST_PARTS,)), dma((LAST_PARTS,)), dma, dma, dma],
        input_output_aliases={3: 1, 4: 2},
        compiler_params=pltpu.CompilerParams(vmem_limit_bytes=60 << 20),
        name="last",
    )(seq_lens, y, new, k_copy, v_copy)


def solution(mesh):
    cache_spec = P("dp", "sp", "tp", None)

    def block_step(hidden, seq_lens, rope_cos, rope_sin, k_cache, v_cache, norm_gain, w_qkv, b_qkv, sink_logits, w_o, b_o):
        num_seqs, ctx_local, kv_local, head_dim = k_cache.shape
        rows = (num_seqs, ctx_local * kv_local, head_dim)
        k_rows, v_rows = k_cache.reshape(rows), v_cache.reshape(rows)
        half, k_copy, v_copy = project(hidden, rope_cos, rope_sin, norm_gain, w_qkv, b_qkv, k_rows, v_rows)
        sinks = sink_logits.reshape(1, sink_logits.shape[0])
        y, new = finish(seq_lens, half, sinks, hidden, b_o, w_o, k_rows, v_rows)
        return last(seq_lens, y, new, k_copy.reshape(k_cache.shape), v_copy.reshape(v_cache.shape))

    return jax.shard_map(block_step, mesh=mesh, in_specs=(P("dp", None), P("dp"), P("dp", None), P("dp", None), cache_spec, cache_spec, P(None), P(None, "tp", None), P("tp", None), P("tp"), P("tp", None), P(None)), out_specs=(P("dp", None), cache_spec, cache_spec), check_vma=False)
```

```python
import functools

import jax
import jax.numpy as jnp
from jax import lax
from jax.experimental import pallas as pl
from jax.experimental.pallas import tpu as pltpu
from jax.sharding import PartitionSpec as P

NORM_EPS = 1e-5
F32 = jnp.float32
BF16 = jnp.bfloat16
MESH = pl.DeviceIdType.MESH


def sp_place():
    sp = lax.axis_index("sp")
    return lax.div(sp, 2), lax.rem(sp, 2)


def remote(src, dst, send_sem, recv_sem, where):
    return pltpu.make_async_remote_copy(src_ref=src, dst_ref=dst, send_sem=send_sem, recv_sem=recv_sem, device_id=where, device_id_type=MESH)


def sink_column(row_ref, count, halves, group):
    row = lax.broadcasted_iota(jnp.int32, (count, count), 0)
    per_half = count // halves
    part = group // halves
    head = lax.div(lax.rem(row, per_half), part) * group + lax.div(row, per_half) * part + lax.rem(row, part)
    same = head == lax.broadcasted_iota(jnp.int32, (count, count), 1)
    return jnp.sum(jnp.where(same, jnp.broadcast_to(row_ref[...], (count, count)), 0.0), axis=1, keepdims=True)


QKV_ROWS = 1024
QKV_SLOTS = 3
CACHE_SEQS = 16
CACHE_AHEAD = 2
CACHE_FIRST = 0
X_PARTS = 4


def project_kernel(x_hbm, gain_hbm, cos_hbm, sin_hbm, bias_hbm, w_ref, k_ref, v_ref, out_ref, k_out, v_out,
                   x_ref, gain_ref, cos_ref, sin_ref, bias_ref, x_sem, small_sem, normed, gain, heads, acc_q, acc_e, wq_buf, we_buf, k_buf, v_buf, wq_sem, we_sem, out_sem, k_in, v_in, k_back, v_back):
    _, core = sp_place()
    num_seqs, depth = x_ref.shape
    head_dim = acc_e.shape[2]
    q_cols = acc_q.shape[2]
    kv_local = acc_q.shape[0]
    per_core = q_cols // head_dim
    group = 2 * per_core
    steps = depth // QKV_ROWS
    x_rows = num_seqs // X_PARTS
    blocks = num_seqs // CACHE_SEQS

    def fetch(step, slot):
        rows = pl.ds(step * QKV_ROWS, QKV_ROWS)
        cq = pltpu.make_async_copy(w_ref.at[rows, :, pl.ds(pl.multiple_of(core * q_cols, 128), q_cols)], wq_buf.at[slot], wq_sem.at[slot])
        ce = pltpu.make_async_copy(w_ref.at[rows, :, pl.ds(pl.multiple_of((group + core) * head_dim, 128), head_dim)], we_buf.at[slot], we_sem.at[slot])
        return cq, ce

    def cache_in(i):
        at = pl.ds(i * CACHE_SEQS, CACHE_SEQS)
        return pltpu.make_async_copy(k_ref.at[at], k_buf.at[at], k_in.at[i]), pltpu.make_async_copy(v_ref.at[at], v_buf.at[at], v_in.at[i])

    def cache_back(i):
        at = pl.ds(i * CACHE_SEQS, CACHE_SEQS)
        return pltpu.make_async_copy(k_buf.at[at], k_out.at[at], k_back.at[i]), pltpu.make_async_copy(v_buf.at[at], v_out.at[at], v_back.at[i])

    small = [pltpu.make_async_copy(src, dst, small_sem.at[i]) for i, (src, dst) in enumerate(((gain_hbm, gain_ref), (cos_hbm, cos_ref), (sin_hbm, sin_ref), (bias_hbm, bias_ref)))]
    small[0].start()
    x_copies = []
    for p in range(X_PARTS):
        at = pl.ds(p * x_rows, x_rows)
        x_copies.append(pltpu.make_async_copy(x_hbm.at[at], x_ref.at[at], x_sem.at[p]))
        x_copies[-1].start()
    for c in fetch(0, 0):
        c.start()
    for i in range(CACHE_FIRST):
        for c in cache_in(i):
            c.start()
    for s in range(1, QKV_SLOTS - 1):
        for c in fetch(s, s):
            c.start()
    for i in range(CACHE_FIRST, CACHE_AHEAD):
        for c in cache_in(i):
            c.start()
    for c in small[1:]:
        c.start()

    small[0].wait()
    gain[...] = gain_ref[...].astype(F32)

    def norm_rows(r, _):
        rows = pl.ds(pl.multiple_of(r * 16, 16), 16)
        xw = x_ref[rows, :].astype(F32)
        inv = lax.rsqrt(jnp.mean(xw * xw, axis=-1, keepdims=True) + NORM_EPS)
        for t in range(depth // head_dim):
            cols = slice(t * head_dim, (t + 1) * head_dim)
            normed[rows, cols] = (xw[:, cols] * inv * gain[t : t + 1, :]).astype(BF16)
        return 0

    for p in range(X_PARTS):
        x_copies[p].wait()
        lax.fori_loop(p * x_rows // 16, (p + 1) * x_rows // 16, norm_rows, 0)
    for i in range(CACHE_FIRST):
        for c in cache_in(i):
            c.wait()
        for c in cache_back(i):
            c.start()
    acc_q[...] = jnp.zeros_like(acc_q)
    acc_e[...] = jnp.zeros_like(acc_e)

    def step_fn(step, _):
        slot = lax.rem(step, QKV_SLOTS)

        @pl.when(step + CACHE_AHEAD < blocks)
        def _():
            for c in cache_in(step + CACHE_AHEAD):
                c.start()

        for c in fetch(step, slot):
            c.wait()

        @pl.when(step + QKV_SLOTS - 1 < steps)
        def _():
            for c in fetch(step + QKV_SLOTS - 1, lax.rem(step + QKV_SLOTS - 1, QKV_SLOTS)):
                c.start()

        @pl.when(step + CACHE_FIRST < blocks)
        def _():
            for c in cache_in(step + CACHE_FIRST):
                c.wait()
            for c in cache_back(step + CACHE_FIRST):
                c.start()

        h = normed[:, pl.ds(pl.multiple_of(step * QKV_ROWS, 128), QKV_ROWS)]
        wq = jnp.swapaxes(wq_buf[slot], 0, 1)
        we = jnp.swapaxes(we_buf[slot], 0, 1)
        for k in range(kv_local):
            acc_q[k] += jnp.dot(h, wq[k], preferred_element_type=F32)
            acc_e[k] += jnp.dot(h, we[k], preferred_element_type=F32)
        return 0

    lax.fori_loop(0, steps, step_fn, 0)

    for c in small[1:]:
        c.wait()
    cos_t = cos_ref[...].T
    sin_t = sin_ref[...].T
    cos2 = jnp.concatenate([cos_t, cos_t], axis=1)
    sin2 = jnp.concatenate([-sin_t, sin_t], axis=1)
    is_key = core == 0
    cos_e = jnp.where(is_key, cos2, jnp.ones_like(cos2))
    sin_e = jnp.where(is_key, sin2, jnp.zeros_like(sin2))

    def rotate(v, c, s):
        r = v * c + pltpu.roll(v, head_dim // 2, 1) * s
        return r.astype(BF16).astype(F32)

    for k in range(kv_local):
        bias_q = bias_ref[k : k + 1, pl.ds(pl.multiple_of(core * q_cols, 128), q_cols)].astype(F32)
        for g in range(per_core):
            cols = slice(g * head_dim, (g + 1) * head_dim)
            heads[k * per_core + g] = rotate(acc_q[k, :, cols] + bias_q[:, cols], cos2, sin2)
        bias_e = bias_ref[k : k + 1, pl.ds(pl.multiple_of((group + core) * head_dim, 128), head_dim)].astype(F32)
        heads[kv_local * per_core + k] = rotate(acc_e[k] + bias_e, cos_e, sin_e)
    done = pltpu.make_async_copy(heads, out_ref, out_sem)
    done.start()
    for i in range(blocks):
        for c in cache_back(i):
            c.wait()
    done.wait()


def project(hidden, rope_cos, rope_sin, norm_gain, w_qkv, b_qkv, k_rows, v_rows):
    num_seqs, depth = hidden.shape
    head_dim = k_rows.shape[2]
    kv_local = w_qkv.shape[1]
    per_core = (w_qkv.shape[2] // head_dim - 2) // 2
    rows = kv_local * (per_core + 1)
    blocks = num_seqs // CACHE_SEQS
    assert blocks <= depth // QKV_ROWS + CACHE_FIRST
    anyspace = pl.BlockSpec(memory_space=pl.ANY)
    dma = pltpu.SemaphoreType.DMA
    return pl.pallas_call(
        project_kernel,
        out_shape=[
            jax.ShapeDtypeStruct((rows, num_seqs, head_dim), F32),
            jax.ShapeDtypeStruct(k_rows.shape, BF16),
            jax.ShapeDtypeStruct(v_rows.shape, BF16),
        ],
        in_specs=[anyspace] * 8,
        out_specs=[anyspace] * 3,
        scratch_shapes=[
            pltpu.VMEM((num_seqs, depth), BF16),
            pltpu.VMEM((depth // head_dim, head_dim), BF16),
            pltpu.VMEM((head_dim // 2, num_seqs), F32),
            pltpu.VMEM((head_dim // 2, num_seqs), F32),
            pltpu.VMEM(b_qkv.shape, BF16),
            dma((X_PARTS,)),
            dma((4,)),
            pltpu.VMEM((num_seqs, depth), BF16),
            pltpu.VMEM((depth // head_dim, head_dim), F32),
            pltpu.VMEM((rows, num_seqs, head_dim), F32),
            pltpu.VMEM((kv_local, num_seqs, per_core * head_dim), F32),
            pltpu.VMEM((kv_local, num_seqs, head_dim), F32),
            pltpu.VMEM((QKV_SLOTS, QKV_ROWS, kv_local, per_core * head_dim), BF16),
            pltpu.VMEM((QKV_SLOTS, QKV_ROWS, kv_local, head_dim), BF16),
            pltpu.VMEM(k_rows.shape, BF16),
            pltpu.VMEM(v_rows.shape, BF16),
            dma((QKV_SLOTS,)), dma((QKV_SLOTS,)), dma,
            dma((blocks,)), dma((blocks,)), dma((blocks,)), dma((blocks,)),
        ],
        compiler_params=pltpu.CompilerParams(vmem_limit_bytes=60 << 20),
        name="project",
    )(hidden, norm_gain.reshape(depth // head_dim, head_dim), rope_cos.T, rope_sin.T, b_qkv, w_qkv, k_rows, v_rows)


ATT_SEQS = 8
ATT_SLOTS = 6
OUT_COLS = 512
SEQ_GROUPS = 2
W_PARTS = 8
LAG_Y = 3
LAG_X = 3
LAG_P = 1
OUT_CHUNKS = 2


def finish_kernel(lens_ref, half_hbm, sink_ref, hid_ref, bo_ref, wo_ref, k_hbm, v_hbm, y_out, new_ref,
                  y_ref, w_buf, x_buf, h_buf, k_ring, v_ring, num, ml, sink_col, bo_f32, r1, r1ml, own, own_ml, away, away_ml, r2, r2ml, o_buf, r3, o_all,
                  y_send, y_recv, z_buf, x_recv, p1, p2,
                  w_sem, x_sem, k_sem, v_sem, h_in, h_send, h_recv, s1_send, s1_recv, s2_send, s2_recv, s3_send, s3_recv,
                  y_ss, y_rs, x_ss, x_rs, p1_ss, p1_rs, p2_ss, p2_rs, o_sem):
    chip, core = sp_place()
    tp = lax.axis_index("tp")
    partner = {"sp": 2 * chip + (1 - core)}
    across_x = {"sp": 2 * (1 - chip) + core}
    across_y = {"tp": 1 - tp}
    groups, q_rows, some, head_dim = num.shape
    num_seqs = h_buf.shape[1]
    kv_local = (h_buf.shape[0] - q_rows) // 2
    rows = k_ring.shape[2]
    ctx_local = rows // kv_local
    half_h = q_rows // 2
    half_s = num_seqs // 2
    part_h = half_h // kv_local
    cols = w_buf.shape[1]
    chunks = cols // OUT_COLS
    total = SEQ_GROUPS * chunks
    mine = pl.multiple_of(core * half_h, half_h)
    theirs = pl.multiple_of((1 - core) * half_h, half_h)

    def seqs(which, g):
        return pl.ds(pl.multiple_of(which * half_s + g * some, some), some)

    barrier = pltpu.get_barrier_semaphore()
    for peer in (partner, across_x, across_y):
        pl.semaphore_signal(barrier, inc=1, device_id=peer, device_id_type=MESH)

    order = [(1 - chip, g) for g in range(SEQ_GROUPS)] + [(chip, g) for g in range(SEQ_GROUPS)]
    own_rows = (pl.ds(mine, half_h), pl.ds(pl.multiple_of(q_rows + kv_local * core, kv_local), kv_local))
    src_rows = (pl.ds(0, half_h), pl.ds(half_h, kv_local))
    h_local, h_remote = [], []
    for i, (which, g) in enumerate(order):
        at = seqs(which, g)
        for j in range(2):
            h_local.append(pltpu.make_async_copy(half_hbm.at[src_rows[j], at], h_buf.at[own_rows[j], at], h_in.at[2 * i + j]))
            h_local[-1].start()
            h_remote.append(remote(half_hbm.at[src_rows[j], at], h_buf.at[own_rows[j], at], h_send.at[2 * i + j], h_recv.at[2 * i + j], partner))

    steps = num_seqs // ATT_SEQS
    per_group = some // ATT_SEQS

    def block(p):
        return lax.rem(p + (1 - chip) * (steps // 2), steps) * ATT_SEQS

    def kv_load(p):
        at = pl.ds(pl.multiple_of(block(p), ATT_SEQS), ATT_SEQS)
        slot = lax.rem(p, ATT_SLOTS)
        return pltpu.make_async_copy(k_hbm.at[at], k_ring.at[slot], k_sem.at[slot]), pltpu.make_async_copy(v_hbm.at[at], v_ring.at[slot], v_sem.at[slot])

    for p in range(ATT_SLOTS):
        for c in kv_load(p):
            c.start()
    my_cols = pl.ds(pl.multiple_of(core * cols, 128), cols)
    x_copy_in = pltpu.make_async_copy(hid_ref.at[pl.ds(pl.multiple_of(chip * half_s, half_s), half_s), my_cols], x_buf, x_sem)
    w_cols = cols // W_PARTS
    w_chunks = w_cols // OUT_COLS

    def w_copy(p):
        return pltpu.make_async_copy(wo_ref.at[:, pl.ds(pl.multiple_of(core * cols + p * w_cols, 128), w_cols)], w_buf.at[:, pl.ds(pl.multiple_of(p * w_cols, 128), w_cols)], w_sem.at[p])

    sink = sink_column(sink_ref, q_rows, 2, 2 * part_h)
    sink_col[...] = jnp.broadcast_to(sink, sink_col.shape)
    bo_f32[...] = bo_ref[...].astype(F32)
    pl.semaphore_wait(barrier, 3)
    for c in h_remote:
        c.start()

    base = lax.axis_index("sp") * ctx_local
    scale = head_dim**-0.5
    col = lax.broadcasted_iota(jnp.int32, (q_rows, rows), 1)
    kv_row = lax.div(lax.rem(lax.broadcasted_iota(jnp.int32, (q_rows, rows), 0), half_h), part_h)
    col_pos = jnp.where(lax.rem(col, kv_local) == kv_row, lax.div(col, kv_local), ctx_local * 1024)
    lane = lax.broadcasted_iota(jnp.int32, (q_rows, ml.shape[2]), 1)
    batch = range(ATT_SEQS)
    over_d = (((1,), (1,)), ((), ()))
    new_code = jnp.where(lax.broadcasted_iota(jnp.int32, (q_rows, 16), 1) == lax.div(lax.rem(lax.broadcasted_iota(jnp.int32, (q_rows, 16), 0), half_h), part_h), 1, 2)

    def attend(i, first, last, carry):
        def step_fn(t, carry):
            m_all, l_all = carry
            p = i * per_group + t
            slot = lax.rem(p, ATT_SLOTS)
            for c in kv_load(p):
                c.wait()
            start = block(p)
            heads = h_buf.at[:, pl.ds(pl.multiple_of(start, ATT_SEQS), ATT_SEQS)]
            rel = [lens_ref[start + s] - base for s in batch]
            inside = [jnp.where(jnp.logical_and(r >= 0, r < ctx_local), 1, 0) for r in rel]
            queries = [heads[0:q_rows, s, :].astype(BF16) for s in batch]
            new_k, new_v = ([jnp.concatenate([heads[lo : lo + kv_local, s, :]] * (16 // kv_local), axis=0).astype(BF16) for s in batch] for lo in (q_rows, q_rows + kv_local))
            logits = [lax.dot_general(queries[s], k_ring[slot, s], over_d, preferred_element_type=F32) for s in batch]
            extra = [lax.dot_general(queries[s], new_k[s], over_d, preferred_element_type=F32) for s in batch]
            logits = [jnp.where(col_pos < rel[s], logits[s] * scale, -jnp.inf) for s in batch]
            extra = [jnp.where(new_code == inside[s], extra[s] * scale, -jnp.inf) for s in batch]
            tops = [jnp.maximum(jnp.maximum(jnp.max(logits[s], axis=1, keepdims=True), jnp.max(extra[s], axis=1, keepdims=True)), sink) for s in batch]
            weights = [jnp.exp(logits[s] - tops[s]) for s in batch]
            extra = [jnp.exp(extra[s] - tops[s]) for s in batch]
            totals = [jnp.sum(weights[s], axis=1, keepdims=True) + jnp.sum(extra[s], axis=1, keepdims=True) for s in batch]
            sums = [jnp.dot(weights[s].astype(BF16), v_ring[slot, s], preferred_element_type=F32) for s in batch]
            sums = [sums[s] + jnp.dot(extra[s].astype(BF16), new_v[s], preferred_element_type=F32) for s in batch]
            out = num.at[i, :, pl.ds(pl.multiple_of(t * ATT_SEQS, ATT_SEQS), ATT_SEQS)]
            for s in batch:
                here = lane == t * ATT_SEQS + s
                m_all = jnp.where(here, tops[s], m_all)
                l_all = jnp.where(here, totals[s], l_all)
                out[:, s, :] = sums[s]
            for s in batch:
                for j in range(2):
                    new_ref[j, start + s] = heads[q_rows + j * kv_local : q_rows + (j + 1) * kv_local, s, :].astype(BF16)

            @pl.when(p + ATT_SLOTS < steps)
            def _():
                for c in kv_load(p + ATT_SLOTS):
                    c.start()

            return m_all, l_all

        return lax.fori_loop(first, last, step_fn, carry)

    def heads_wait(i):
        for j in range(2):
            h_local[2 * i + j].wait()
            h_remote[2 * i + j].wait_recv()

    zero = jnp.zeros((q_rows, ml.shape[2]), F32)
    c1 = []

    def to_partner(i, carry):
        ml[i, 0:q_rows] = carry[0]
        ml[i, q_rows : 2 * q_rows] = carry[1]
        c1.append((
            remote(ml.at[i], r1ml.at[i], s1_send.at[2 * i], s1_recv.at[2 * i], partner),
            remote(num.at[i, pl.ds(theirs, half_h)], r1.at[i], s1_send.at[2 * i + 1], s1_recv.at[2 * i + 1], partner),
        ))
        for c in c1[-1]:
            c.start()

    def combine(i, dst, dst_ml):
        for c in c1[i]:
            c.wait_recv()
        m_a, l_a = ml[i, pl.ds(mine, half_h)], ml[i, pl.ds(q_rows + mine, half_h)]
        m_b, l_b = r1ml[i, pl.ds(mine, half_h)], r1ml[i, pl.ds(q_rows + mine, half_h)]
        m_chip = jnp.maximum(m_a, m_b)
        f_a = jnp.exp(m_a - m_chip)
        f_b = jnp.exp(m_b - m_chip)
        dst_ml[0:half_h] = m_chip
        dst_ml[half_h : 2 * half_h] = l_a * f_a + l_b * f_b
        f_a, f_b = f_a.T, f_b.T
        for h in range(half_h):
            dst[h] = num[i, mine + h] * f_a[0:some, h : h + 1] + r1[i, h] * f_b[0:some, h : h + 1]

    c2 = []

    def across(g):
        combine(g, away.at[g], away_ml.at[g])
        c2.append((
            remote(away_ml.at[g], r2ml.at[g], s2_send.at[2 * g], s2_recv.at[2 * g], across_x),
            remote(away.at[g], r2.at[g], s2_send.at[2 * g + 1], s2_recv.at[2 * g + 1], across_x),
        ))
        for c in c2[-1]:
            c.start()

    width = half_h * head_dim
    part_w = part_h * head_dim

    def o_place(which_half, k):
        return pl.ds(pl.multiple_of(2 * k * part_w + which_half * part_w, 128), part_w)

    def heads_start(g):
        for c in c2[g]:
            c.wait_recv()
        m_a, l_a = own_ml[g, 0:half_h], own_ml[g, half_h : 2 * half_h]
        m_b, l_b = r2ml[g, 0:half_h], r2ml[g, half_h : 2 * half_h]
        m_top = jnp.maximum(m_a, m_b)
        f_a = jnp.exp(m_a - m_top)
        f_b = jnp.exp(m_b - m_top)
        den = l_a * f_a + l_b * f_b + jnp.exp(sink_col[pl.ds(mine, half_h)] - m_top)
        f_a, f_b = (f_a / den).T, (f_b / den).T
        for h in range(half_h):
            o_buf[g, :, h * head_dim : (h + 1) * head_dim] = own[g, h] * f_a[0:some, h : h + 1] + r2[g, h] * f_b[0:some, h : h + 1]
        c = remote(o_buf.at[g], r3.at[g], s3_send.at[g], s3_recv.at[g], partner)
        c.start()
        for k in range(kv_local):
            o_all[g, :, o_place(core, k)] = o_buf[g, :, k * part_w : (k + 1) * part_w].astype(BF16)
        return c

    def heads_end(g, c):
        c.wait_recv()
        for k in range(kv_local):
            o_all[g, :, o_place(1 - core, k)] = r3[g, :, k * part_w : (k + 1) * part_w].astype(BF16)

    def y_copy(t):
        return remote(y_send.at[t], y_recv.at[t], y_ss.at[t], y_rs.at[t], across_y)

    def x_copy(t):
        return remote(z_buf.at[t], x_recv.at[t], x_ss.at[t], x_rs.at[t], across_x)

    def p1_copy(t):
        return remote(z_buf.at[t], p1.at[t], p1_ss.at[t], p1_rs.at[t], partner)

    def p2_copy(t):
        return remote(x_recv.at[t], p2.at[t], p2_ss.at[t], p2_rs.at[t], partner)

    def place(which_seqs, which_cols, t):
        g, j = lax.div(t, chunks), lax.rem(t, chunks)
        return seqs(which_seqs, g), pl.ds(pl.multiple_of(which_cols * cols + j * OUT_COLS, 128), OUT_COLS)

    def out_copy(kind, q):
        which_seqs, which_cols = ((chip, core), (1 - chip, core), (chip, 1 - core), (1 - chip, 1 - core))[kind]
        rows_at, _ = place(which_seqs, which_cols, q * OUT_CHUNKS)
        j = lax.rem(q * OUT_CHUNKS, chunks)
        cols_at = pl.ds(pl.multiple_of(which_cols * cols + j * OUT_COLS, 128), OUT_CHUNKS * OUT_COLS)
        return pltpu.make_async_copy(y_ref.at[rows_at, cols_at], y_out.at[rows_at, cols_at], o_sem.at[kind, q])

    def put_out(u, kinds):
        @pl.when(lax.rem(u, OUT_CHUNKS) == OUT_CHUNKS - 1)
        def _():
            for kind in kinds:
                out_copy(kind, lax.div(u, OUT_CHUNKS)).start()

    def body(t, _):
        @pl.when(t < total)
        def _():
            g, j = lax.div(t, chunks), lax.rem(t, chunks)

            @pl.when(jnp.logical_and(g == 0, lax.rem(j, w_chunks) == 0))
            def _():
                w_copy(lax.div(j, w_chunks)).wait()

            w = w_buf[:, pl.ds(pl.multiple_of(j * OUT_COLS, 128), OUT_COLS)]
            y_send[t] = jnp.dot(o_all[g], w, preferred_element_type=F32)
            y_copy(t).start()

        @pl.when(jnp.logical_and(t >= LAG_Y, t < total + LAG_Y))
        def _():
            u = t - LAG_Y
            g, j = lax.div(u, chunks), lax.rem(u, chunks)
            y_copy(u).wait_recv()
            x_part = x_buf[pl.ds(pl.multiple_of(g * some, some), some), pl.ds(pl.multiple_of(j * OUT_COLS, 128), OUT_COLS)].astype(F32)
            row = (core * cols + j * OUT_COLS) // head_dim
            bias = jnp.concatenate([bo_f32[pl.ds(row + i, 1), :] for i in range(OUT_COLS // head_dim)], axis=1)
            z = (x_part + (y_send[u] + y_recv[u]) + bias).astype(BF16)
            z_buf[u] = z.astype(F32)
            x_copy(u).start()
            p1_copy(u).start()
            rows_at, cols_at = place(chip, core, u)
            y_ref[rows_at, cols_at] = z
            put_out(u, (0,))

        @pl.when(jnp.logical_and(t >= LAG_Y + LAG_X, t < total + LAG_Y + LAG_X))
        def _():
            u = t - (LAG_Y + LAG_X)
            x_copy(u).wait_recv()
            p2_copy(u).start()
            rows_at, cols_at = place(1 - chip, core, u)
            y_ref[rows_at, cols_at] = x_recv[u].astype(BF16)
            p1_copy(u).wait_recv()
            rows_at, cols_at = place(chip, 1 - core, u)
            y_ref[rows_at, cols_at] = p1[u].astype(BF16)
            put_out(u, (1, 2))

        @pl.when(t >= LAG_Y + LAG_X + LAG_P)
        def _():
            u = t - (LAG_Y + LAG_X + LAG_P)
            p2_copy(u).wait_recv()
            rows_at, cols_at = place(1 - chip, 1 - core, u)
            y_ref[rows_at, cols_at] = p2[u].astype(BF16)
            put_out(u, (3,))

        return 0

    half_group = per_group // 2
    heads_wait(0)
    carry = attend(0, 0, per_group, (zero, zero))
    to_partner(0, carry)
    x_copy_in.start()
    heads_wait(1)
    carry = attend(1, 0, half_group, (zero, zero))
    across(0)
    carry = attend(1, half_group, per_group, carry)
    to_partner(1, carry)
    w_copy(0).start()
    heads_wait(2)
    carry = attend(2, 0, half_group, (zero, zero))
    across(1)
    w_copy(1).start()
    carry = attend(2, half_group, per_group, carry)
    to_partner(2, carry)
    for p in range(2, W_PARTS):
        w_copy(p).start()
    heads_wait(3)
    carry = attend(3, 0, per_group, (zero, zero))
    to_partner(3, carry)
    combine(2, own.at[0], own_ml.at[0])
    combine(3, own.at[1], own_ml.at[1])

    c3 = [heads_start(0)]
    heads_end(0, c3[0])
    x_copy_in.wait()
    lax.fori_loop(0, chunks // 2, body, 0)
    c3.append(heads_start(1))
    lax.fori_loop(chunks // 2, 3 * chunks // 4, body, 0)
    heads_end(1, c3[1])
    lax.fori_loop(3 * chunks // 4, total + LAG_Y + LAG_X + LAG_P, body, 0)

    def tail(t, _):
        y_copy(t).wait_send()
        x_copy(t).wait_send()
        p1_copy(t).wait_send()
        p2_copy(t).wait_send()
        return 0

    lax.fori_loop(0, total, tail, 0)

    def settle(q, _):
        for kind in range(4):
            out_copy(kind, q).wait()
        return 0

    lax.fori_loop(0, total // OUT_CHUNKS, settle, 0)
    for c in (*h_remote, *(c for pair in c1 + c2 for c in pair), *c3):
        c.wait_send()


def finish(seq_lens, half, sinks, hidden, b_o, w_o, k_rows, v_rows):
    num_seqs, rows, head_dim = k_rows.shape
    q_rows = sinks.shape[1]
    half_h, half_s = q_rows // 2, num_seqs // 2
    kv_local = half.shape[0] - half_h
    some = half_s // SEQ_GROUPS
    groups = 2 * SEQ_GROUPS
    width = w_o.shape[1]
    cols = width // 2
    total = SEQ_GROUPS * (cols // OUT_COLS)
    vmem = pl.BlockSpec(memory_space=pltpu.VMEM)
    anyspace = pl.BlockSpec(memory_space=pl.ANY)
    chunked = pltpu.VMEM((total, some, OUT_COLS), F32)
    parts = pltpu.VMEM((SEQ_GROUPS, half_h, some, head_dim), F32)
    parts_ml = pltpu.VMEM((SEQ_GROUPS, 2 * half_h, 128), F32)
    ring = pltpu.VMEM((ATT_SLOTS, ATT_SEQS, rows, head_dim), BF16)
    dma = pltpu.SemaphoreType.DMA
    return pl.pallas_call(
        finish_kernel,
        out_shape=[
            jax.ShapeDtypeStruct((num_seqs, width), BF16),
            jax.ShapeDtypeStruct((2, num_seqs, kv_local, head_dim), BF16),
        ],
        in_specs=[pl.BlockSpec(memory_space=pltpu.SMEM), anyspace, vmem, anyspace, vmem, anyspace, anyspace, anyspace],
        out_specs=[anyspace, vmem],
        scratch_shapes=[
            pltpu.VMEM((num_seqs, width), BF16),
            pltpu.VMEM((w_o.shape[0], cols), BF16),
            pltpu.VMEM((half_s, cols), BF16),
            pltpu.VMEM((q_rows + 2 * kv_local, num_seqs, head_dim), F32),
            ring, ring,
            pltpu.VMEM((groups, q_rows, some, head_dim), F32),
            pltpu.VMEM((groups, 2 * q_rows, 128), F32),
            pltpu.VMEM((q_rows, 128), F32),
            pltpu.VMEM((width // head_dim, head_dim), F32),
            pltpu.VMEM((groups, half_h, some, head_dim), F32),
            pltpu.VMEM((groups, 2 * q_rows, 128), F32),
            parts, parts_ml, parts, parts_ml, parts, parts_ml,
            pltpu.VMEM((SEQ_GROUPS, some, half_h * head_dim), F32),
            pltpu.VMEM((SEQ_GROUPS, some, half_h * head_dim), F32),
            pltpu.VMEM((SEQ_GROUPS, some, q_rows * head_dim), BF16),
            chunked, chunked, chunked, chunked, chunked, chunked,
            dma((W_PARTS,)), dma, dma((ATT_SLOTS,)), dma((ATT_SLOTS,)),
            dma((2 * groups,)), dma((2 * groups,)), dma((2 * groups,)),
            dma((2 * groups,)), dma((2 * groups,)),
            dma((groups,)), dma((groups,)),
            dma((SEQ_GROUPS,)), dma((SEQ_GROUPS,)),
            *[dma((total,))] * 8,
            dma((4, total // OUT_CHUNKS)),
        ],
        compiler_params=pltpu.CompilerParams(collective_id=1, has_side_effects=True, vmem_limit_bytes=62 << 20),
        name="finish",
    )(seq_lens, half, sinks, hidden, b_o.reshape(width // head_dim, head_dim), w_o, k_rows, v_rows)


LAST_PARTS = 4
LAST_UNROLL = 8


def last_kernel(lens_ref, y_hbm, new_hbm, k_in, v_in, y_out, k_out, v_out, y_buf, new_ref, in_sem, out_sem, new_sem, k_sem, v_sem):
    num_seqs, ctx_local = k_out.shape[:2]
    base = lax.axis_index("sp") * ctx_local
    rows = y_hbm.shape[0] // LAST_PARTS
    new_copy = pltpu.make_async_copy(new_hbm, new_ref, new_sem)
    new_copy.start()
    loads, stores = [], []
    for p in range(LAST_PARTS):
        at = pl.ds(p * rows, rows)
        loads.append(pltpu.make_async_copy(y_hbm.at[at], y_buf.at[at], in_sem.at[p]))
        stores.append(pltpu.make_async_copy(y_buf.at[at], y_out.at[at], out_sem.at[p]))
        loads[-1].start()

    def for_new_rows(act):
        def step(i, _):
            for b in (i * LAST_UNROLL + r for r in range(LAST_UNROLL)):
                n = lens_ref[b] - base

                @pl.when(jnp.logical_and(n >= 0, n < ctx_local))
                def _():
                    act(pltpu.make_async_copy(new_ref.at[0, b], k_out.at[b, n], k_sem))
                    act(pltpu.make_async_copy(new_ref.at[1, b], v_out.at[b, n], v_sem))

            return 0

        lax.fori_loop(0, num_seqs // LAST_UNROLL, step, 0)

    new_copy.wait()
    for_new_rows(lambda c: c.start())
    for p in range(LAST_PARTS):
        loads[p].wait()
        stores[p].start()
    for_new_rows(lambda c: c.wait())
    for c in stores:
        c.wait()


def last(seq_lens, y, new, k_copy, v_copy):
    anyspace = pl.BlockSpec(memory_space=pl.ANY)
    dma = pltpu.SemaphoreType.DMA
    return pl.pallas_call(
        last_kernel,
        out_shape=[jax.ShapeDtypeStruct(a.shape, a.dtype) for a in (y, k_copy, v_copy)],
        in_specs=[pl.BlockSpec(memory_space=pltpu.SMEM)] + [anyspace] * 4,
        out_specs=[anyspace] * 3,
        scratch_shapes=[pltpu.VMEM(y.shape, y.dtype), pltpu.VMEM(new.shape, new.dtype), dma((LAST_PARTS,)), dma((LAST_PARTS,)), dma, dma, dma],
        input_output_aliases={3: 1, 4: 2},
        compiler_params=pltpu.CompilerParams(vmem_limit_bytes=60 << 20),
        name="last",
    )(seq_lens, y, new, k_copy, v_copy)


def solution(mesh):
    cache_spec = P("dp", "sp", "tp", None)

    def block_step(hidden, seq_lens, rope_cos, rope_sin, k_cache, v_cache, norm_gain, w_qkv, b_qkv, sink_logits, w_o, b_o):
        num_seqs, ctx_local, kv_local, head_dim = k_cache.shape
        rows = (num_seqs, ctx_local * kv_local, head_dim)
        k_rows, v_rows = k_cache.reshape(rows), v_cache.reshape(rows)
        half, k_copy, v_copy = project(hidden, rope_cos, rope_sin, norm_gain, w_qkv, b_qkv, k_rows, v_rows)
        sinks = sink_logits.reshape(1, sink_logits.shape[0])
        y, new = finish(seq_lens, half, sinks, hidden, b_o, w_o, k_rows, v_rows)
        return last(seq_lens, y, new, k_copy.reshape(k_cache.shape), v_copy.reshape(v_cache.shape))

    return jax.shard_map(block_step, mesh=mesh, in_specs=(P("dp", None), P("dp"), P("dp", None), P("dp", None), cache_spec, cache_spec, P(None), P(None, "tp", None), P("tp", None), P("tp"), P("tp", None), P(None)), out_specs=(P("dp", None), cache_spec, cache_spec), check_vma=False)
```

```python
import functools

import jax
import jax.numpy as jnp
from jax import lax
from jax.experimental import pallas as pl
from jax.experimental.pallas import tpu as pltpu
from jax.sharding import PartitionSpec as P

NORM_EPS = 1e-5
F32 = jnp.float32
BF16 = jnp.bfloat16
MESH = pl.DeviceIdType.MESH


def sp_place():
    sp = lax.axis_index("sp")
    return lax.div(sp, 2), lax.rem(sp, 2)


def remote(src, dst, send_sem, recv_sem, where):
    return pltpu.make_async_remote_copy(src_ref=src, dst_ref=dst, send_sem=send_sem, recv_sem=recv_sem, device_id=where, device_id_type=MESH)


def sink_column(row_ref, count, halves, group):
    row = lax.broadcasted_iota(jnp.int32, (count, count), 0)
    per_half = count // halves
    part = group // halves
    head = lax.div(lax.rem(row, per_half), part) * group + lax.div(row, per_half) * part + lax.rem(row, part)
    same = head == lax.broadcasted_iota(jnp.int32, (count, count), 1)
    return jnp.sum(jnp.where(same, jnp.broadcast_to(row_ref[...], (count, count)), 0.0), axis=1, keepdims=True)


QKV_ROWS = 1024
QKV_SLOTS = 3
CACHE_SEQS = 16
CACHE_AHEAD = 1
CACHE_FIRST = 0
X_PARTS = 4


def project_kernel(x_hbm, gain_hbm, cos_hbm, sin_hbm, bias_hbm, w_ref, k_ref, v_ref, out_ref, k_out, v_out,
                   x_ref, gain_ref, cos_ref, sin_ref, bias_ref, x_sem, small_sem, normed, gain, heads, acc_q, acc_e, wq_buf, we_buf, k_buf, v_buf, wq_sem, we_sem, out_sem, k_in, v_in, k_back, v_back):
    _, core = sp_place()
    num_seqs, depth = x_ref.shape
    head_dim = acc_e.shape[2]
    q_cols = acc_q.shape[2]
    kv_local = acc_q.shape[0]
    per_core = q_cols // head_dim
    group = 2 * per_core
    steps = depth // QKV_ROWS
    x_rows = num_seqs // X_PARTS
    blocks = num_seqs // CACHE_SEQS

    def fetch(step, slot):
        rows = pl.ds(step * QKV_ROWS, QKV_ROWS)
        cq = pltpu.make_async_copy(w_ref.at[rows, :, pl.ds(pl.multiple_of(core * q_cols, 128), q_cols)], wq_buf.at[slot], wq_sem.at[slot])
        ce = pltpu.make_async_copy(w_ref.at[rows, :, pl.ds(pl.multiple_of((group + core) * head_dim, 128), head_dim)], we_buf.at[slot], we_sem.at[slot])
        return cq, ce

    def cache_in(i):
        at = pl.ds(i * CACHE_SEQS, CACHE_SEQS)
        return pltpu.make_async_copy(k_ref.at[at], k_buf.at[at], k_in.at[i]), pltpu.make_async_copy(v_ref.at[at], v_buf.at[at], v_in.at[i])

    def cache_back(i):
        at = pl.ds(i * CACHE_SEQS, CACHE_SEQS)
        return pltpu.make_async_copy(k_buf.at[at], k_out.at[at], k_back.at[i]), pltpu.make_async_copy(v_buf.at[at], v_out.at[at], v_back.at[i])

    small = [pltpu.make_async_copy(src, dst, small_sem.at[i]) for i, (src, dst) in enumerate(((gain_hbm, gain_ref), (cos_hbm, cos_ref), (sin_hbm, sin_ref), (bias_hbm, bias_ref)))]
    small[0].start()
    x_copies = []
    for p in range(X_PARTS):
        at = pl.ds(p * x_rows, x_rows)
        x_copies.append(pltpu.make_async_copy(x_hbm.at[at], x_ref.at[at], x_sem.at[p]))
        x_copies[-1].start()
    for c in fetch(0, 0):
        c.start()
    for i in range(CACHE_FIRST):
        for c in cache_in(i):
            c.start()
    for s in range(1, QKV_SLOTS - 1):
        for c in fetch(s, s):
            c.start()
    for i in range(CACHE_FIRST, CACHE_AHEAD):
        for c in cache_in(i):
            c.start()
    for c in small[1:]:
        c.start()

    small[0].wait()
    gain[...] = gain_ref[...].astype(F32)

    def norm_rows(r, _):
        rows = pl.ds(pl.multiple_of(r * 16, 16), 16)
        xw = x_ref[rows, :].astype(F32)
        inv = lax.rsqrt(jnp.mean(xw * xw, axis=-1, keepdims=True) + NORM_EPS)
        for t in range(depth // head_dim):
            cols = slice(t * head_dim, (t + 1) * head_dim)
            normed[rows, cols] = (xw[:, cols] * inv * gain[t : t + 1, :]).astype(BF16)
        return 0

    for p in range(X_PARTS):
        x_copies[p].wait()
        lax.fori_loop(p * x_rows // 16, (p + 1) * x_rows // 16, norm_rows, 0)
    for i in range(CACHE_FIRST):
        for c in cache_in(i):
            c.wait()
        for c in cache_back(i):
            c.start()
    acc_q[...] = jnp.zeros_like(acc_q)
    acc_e[...] = jnp.zeros_like(acc_e)

    def step_fn(step, _):
        slot = lax.rem(step, QKV_SLOTS)

        @pl.when(step + CACHE_AHEAD < blocks)
        def _():
            for c in cache_in(step + CACHE_AHEAD):
                c.start()

        for c in fetch(step, slot):
            c.wait()

        @pl.when(step + QKV_SLOTS - 1 < steps)
        def _():
            for c in fetch(step + QKV_SLOTS - 1, lax.rem(step + QKV_SLOTS - 1, QKV_SLOTS)):
                c.start()

        @pl.when(step + CACHE_FIRST < blocks)
        def _():
            for c in cache_in(step + CACHE_FIRST):
                c.wait()
            for c in cache_back(step + CACHE_FIRST):
                c.start()

        h = normed[:, pl.ds(pl.multiple_of(step * QKV_ROWS, 128), QKV_ROWS)]
        wq = jnp.swapaxes(wq_buf[slot], 0, 1)
        we = jnp.swapaxes(we_buf[slot], 0, 1)
        for k in range(kv_local):
            acc_q[k] += jnp.dot(h, wq[k], preferred_element_type=F32)
            acc_e[k] += jnp.dot(h, we[k], preferred_element_type=F32)
        return 0

    lax.fori_loop(0, steps, step_fn, 0)

    for c in small[1:]:
        c.wait()
    cos_t = cos_ref[...].T
    sin_t = sin_ref[...].T
    cos2 = jnp.concatenate([cos_t, cos_t], axis=1)
    sin2 = jnp.concatenate([-sin_t, sin_t], axis=1)
    is_key = core == 0
    cos_e = jnp.where(is_key, cos2, jnp.ones_like(cos2))
    sin_e = jnp.where(is_key, sin2, jnp.zeros_like(sin2))

    def rotate(v, c, s):
        r = v * c + pltpu.roll(v, head_dim // 2, 1) * s
        return r.astype(BF16).astype(F32)

    for k in range(kv_local):
        bias_q = bias_ref[k : k + 1, pl.ds(pl.multiple_of(core * q_cols, 128), q_cols)].astype(F32)
        for g in range(per_core):
            cols = slice(g * head_dim, (g + 1) * head_dim)
            heads[k * per_core + g] = rotate(acc_q[k, :, cols] + bias_q[:, cols], cos2, sin2)
        bias_e = bias_ref[k : k + 1, pl.ds(pl.multiple_of((group + core) * head_dim, 128), head_dim)].astype(F32)
        heads[kv_local * per_core + k] = rotate(acc_e[k] + bias_e, cos_e, sin_e)
    done = []
    for k in range(kv_local + 1):
        part = pl.ds(k * per_core, per_core)
        done.append(pltpu.make_async_copy(heads.at[part], out_ref.at[part], out_sem.at[k]))
        done[-1].start()
    for i in range(blocks):
        for c in cache_back(i):
            c.wait()
    for c in done:
        c.wait()


def project(hidden, rope_cos, rope_sin, norm_gain, w_qkv, b_qkv, k_rows, v_rows):
    num_seqs, depth = hidden.shape
    head_dim = k_rows.shape[2]
    kv_local = w_qkv.shape[1]
    per_core = (w_qkv.shape[2] // head_dim - 2) // 2
    rows = kv_local * (per_core + 1)
    blocks = num_seqs // CACHE_SEQS
    assert blocks <= depth // QKV_ROWS + CACHE_FIRST
    anyspace = pl.BlockSpec(memory_space=pl.ANY)
    dma = pltpu.SemaphoreType.DMA
    return pl.pallas_call(
        project_kernel,
        out_shape=[
            jax.ShapeDtypeStruct((rows, num_seqs, head_dim), F32),
            jax.ShapeDtypeStruct(k_rows.shape, BF16),
            jax.ShapeDtypeStruct(v_rows.shape, BF16),
        ],
        in_specs=[anyspace] * 8,
        out_specs=[anyspace] * 3,
        scratch_shapes=[
            pltpu.VMEM((num_seqs, depth), BF16),
            pltpu.VMEM((depth // head_dim, head_dim), BF16),
            pltpu.VMEM((head_dim // 2, num_seqs), F32),
            pltpu.VMEM((head_dim // 2, num_seqs), F32),
            pltpu.VMEM(b_qkv.shape, BF16),
            dma((X_PARTS,)),
            dma((4,)),
            pltpu.VMEM((num_seqs, depth), BF16),
            pltpu.VMEM((depth // head_dim, head_dim), F32),
            pltpu.VMEM((rows, num_seqs, head_dim), F32),
            pltpu.VMEM((kv_local, num_seqs, per_core * head_dim), F32),
            pltpu.VMEM((kv_local, num_seqs, head_dim), F32),
            pltpu.VMEM((QKV_SLOTS, QKV_ROWS, kv_local, per_core * head_dim), BF16),
            pltpu.VMEM((QKV_SLOTS, QKV_ROWS, kv_local, head_dim), BF16),
            pltpu.VMEM(k_rows.shape, BF16),
            pltpu.VMEM(v_rows.shape, BF16),
            dma((QKV_SLOTS,)), dma((QKV_SLOTS,)), dma((kv_local + 1,)),
            dma((blocks,)), dma((blocks,)), dma((blocks,)), dma((blocks,)),
        ],
        compiler_params=pltpu.CompilerParams(vmem_limit_bytes=60 << 20),
        name="project",
    )(hidden, norm_gain.reshape(depth // head_dim, head_dim), rope_cos.T, rope_sin.T, b_qkv, w_qkv, k_rows, v_rows)


ATT_SEQS = 8
ATT_SLOTS = 6
OUT_COLS = 512
SEQ_GROUPS = (24, 40)
W_PARTS = 8
LAG_Y = 3
LAG_X = 3
LAG_P = 1


def finish_kernel(lens_hbm, half_hbm, sink_hbm, hid_ref, bo_hbm, wo_ref, k_hbm, v_hbm, y_out, new_ref,
                  lens_ref, sink_ref, bo_ref, small_sem, y_parts, w_buf, x_buf, h_buf, k_ring, v_ring, num, ml, sink_col, bo_f32, r1, r1ml, own, own_ml, away, away_ml, r2, r2ml, o_buf, r3, o_all,
                  y_send, y_recv, z_buf, x_recv, p1, p2,
                  w_sem, x_sem, k_sem, v_sem, h_in, h_send, h_recv, s1_send, s1_recv, s2_send, s2_recv, s3_send, s3_recv,
                  y_ss, y_rs, x_ss, x_rs, p1_ss, p1_rs, p2_ss, p2_rs, o_sem):
    chip, core = sp_place()
    tp = lax.axis_index("tp")
    partner = {"sp": 2 * chip + (1 - core)}
    across_x = {"sp": 2 * (1 - chip) + core}
    across_y = {"tp": 1 - tp}
    q_rows, _, head_dim = num[0].shape
    chip_groups = len(SEQ_GROUPS)
    offsets = [sum(SEQ_GROUPS[:g]) for g in range(chip_groups)]
    num_seqs = h_buf.shape[1]
    kv_local = (h_buf.shape[0] - q_rows) // 2
    rows = k_ring.shape[2]
    ctx_local = rows // kv_local
    half_h = q_rows // 2
    half_s = num_seqs // 2
    part_h = half_h // kv_local
    cols = w_buf.shape[1]
    chunks = cols // OUT_COLS
    total = chip_groups * chunks
    mine = pl.multiple_of(core * half_h, half_h)
    theirs = pl.multiple_of((1 - core) * half_h, half_h)

    def seqs(which, g):
        return pl.ds(pl.multiple_of(which * half_s + offsets[g], 8), SEQ_GROUPS[g])

    small = [pltpu.make_async_copy(src, dst, small_sem.at[i]) for i, (src, dst) in enumerate(((lens_hbm, lens_ref), (sink_hbm, sink_ref), (bo_hbm, bo_ref)))]
    for c in small:
        c.start()
    barrier = pltpu.get_barrier_semaphore()
    for peer in (partner, across_x, across_y):
        pl.semaphore_signal(barrier, inc=1, device_id=peer, device_id_type=MESH)

    order = [(1 - chip, g) for g in range(chip_groups)] + [(chip, g) for g in range(chip_groups)]
    own_rows = (pl.ds(mine, half_h), pl.ds(pl.multiple_of(q_rows + kv_local * core, kv_local), kv_local))
    src_rows = (pl.ds(0, half_h), pl.ds(half_h, kv_local))
    h_local, h_remote = [], []
    for i, (which, g) in enumerate(order):
        at = seqs(which, g)
        for j in range(2):
            h_local.append(pltpu.make_async_copy(half_hbm.at[src_rows[j], at], h_buf.at[own_rows[j], at], h_in.at[2 * i + j]))
            h_local[-1].start()
            h_remote.append(remote(half_hbm.at[src_rows[j], at], h_buf.at[own_rows[j], at], h_send.at[2 * i + j], h_recv.at[2 * i + j], partner))

    steps = num_seqs // ATT_SEQS
    counts = [n // ATT_SEQS for n in SEQ_GROUPS] * 2
    starts = [sum(counts[:i]) for i in range(len(counts))]

    def block(p):
        return lax.rem(p + (1 - chip) * (steps // 2), steps) * ATT_SEQS

    def kv_load(p):
        at = pl.ds(pl.multiple_of(block(p), ATT_SEQS), ATT_SEQS)
        slot = lax.rem(p, ATT_SLOTS)
        return pltpu.make_async_copy(k_hbm.at[at], k_ring.at[slot], k_sem.at[slot]), pltpu.make_async_copy(v_hbm.at[at], v_ring.at[slot], v_sem.at[slot])

    for p in range(ATT_SLOTS):
        for c in kv_load(p):
            c.start()
    my_cols = pl.ds(pl.multiple_of(core * cols, 128), cols)
    x_in = [pltpu.make_async_copy(hid_ref.at[seqs(chip, g), my_cols], x_buf[g], x_sem.at[g]) for g in range(chip_groups)]
    w_cols = cols // W_PARTS
    w_chunks = w_cols // OUT_COLS

    def w_copy(p):
        return pltpu.make_async_copy(wo_ref.at[:, pl.ds(pl.multiple_of(core * cols + p * w_cols, 128), w_cols)], w_buf.at[:, pl.ds(pl.multiple_of(p * w_cols, 128), w_cols)], w_sem.at[p])

    for c in small:
        c.wait()
    sink = sink_column(sink_ref, q_rows, 2, 2 * part_h)
    sink_col[...] = jnp.broadcast_to(sink, sink_col.shape)
    bo_f32[...] = bo_ref[...].astype(F32)
    pl.semaphore_wait(barrier, 3)
    for c in h_remote:
        c.start()

    base = lax.axis_index("sp") * ctx_local
    scale = head_dim**-0.5
    col = lax.broadcasted_iota(jnp.int32, (q_rows, rows), 1)
    kv_row = lax.div(lax.rem(lax.broadcasted_iota(jnp.int32, (q_rows, rows), 0), half_h), part_h)
    col_pos = jnp.where(lax.rem(col, kv_local) == kv_row, lax.div(col, kv_local), ctx_local * 1024)
    lane = lax.broadcasted_iota(jnp.int32, (q_rows, ml.shape[2]), 1)
    batch = range(ATT_SEQS)
    over_d = (((1,), (1,)), ((), ()))
    new_code = jnp.where(lax.broadcasted_iota(jnp.int32, (q_rows, 16), 1) == lax.div(lax.rem(lax.broadcasted_iota(jnp.int32, (q_rows, 16), 0), half_h), part_h), 1, 2)

    def attend(i, first, last, carry):
        def step_fn(t, carry):
            m_all, l_all = carry
            p = starts[i] + t
            slot = lax.rem(p, ATT_SLOTS)
            for c in kv_load(p):
                c.wait()
            start = block(p)
            heads = h_buf.at[:, pl.ds(pl.multiple_of(start, ATT_SEQS), ATT_SEQS)]
            rel = [lens_ref[start + s] - base for s in batch]
            inside = [jnp.where(jnp.logical_and(r >= 0, r < ctx_local), 1, 0) for r in rel]
            queries = [heads[0:q_rows, s, :].astype(BF16) for s in batch]
            new_k, new_v = ([jnp.concatenate([heads[lo : lo + kv_local, s, :]] * (16 // kv_local), axis=0).astype(BF16) for s in batch] for lo in (q_rows, q_rows + kv_local))
            logits = [lax.dot_general(queries[s], k_ring[slot, s], over_d, preferred_element_type=F32) for s in batch]
            extra = [lax.dot_general(queries[s], new_k[s], over_d, preferred_element_type=F32) for s in batch]
            logits = [jnp.where(col_pos < rel[s], logits[s] * scale, -jnp.inf) for s in batch]
            extra = [jnp.where(new_code == inside[s], extra[s] * scale, -jnp.inf) for s in batch]
            tops = [jnp.maximum(jnp.maximum(jnp.max(logits[s], axis=1, keepdims=True), jnp.max(extra[s], axis=1, keepdims=True)), sink) for s in batch]
            weights = [jnp.exp(logits[s] - tops[s]) for s in batch]
            extra = [jnp.exp(extra[s] - tops[s]) for s in batch]
            totals = [jnp.sum(weights[s], axis=1, keepdims=True) + jnp.sum(extra[s], axis=1, keepdims=True) for s in batch]
            sums = [jnp.dot(weights[s].astype(BF16), v_ring[slot, s], preferred_element_type=F32) for s in batch]
            sums = [sums[s] + jnp.dot(extra[s].astype(BF16), new_v[s], preferred_element_type=F32) for s in batch]
            out = num[i].at[:, pl.ds(pl.multiple_of(t * ATT_SEQS, ATT_SEQS), ATT_SEQS)]
            for s in batch:
                here = lane == t * ATT_SEQS + s
                m_all = jnp.where(here, tops[s], m_all)
                l_all = jnp.where(here, totals[s], l_all)
                out[:, s, :] = sums[s]
            for s in batch:
                for j in range(2):
                    new_ref[j, start + s] = heads[q_rows + j * kv_local : q_rows + (j + 1) * kv_local, s, :].astype(BF16)

            @pl.when(p + ATT_SLOTS < steps)
            def _():
                for c in kv_load(p + ATT_SLOTS):
                    c.start()

            return m_all, l_all

        return lax.fori_loop(first, last, step_fn, carry)

    def heads_wait(i):
        for j in range(2):
            h_local[2 * i + j].wait()
            h_remote[2 * i + j].wait_recv()

    zero = jnp.zeros((q_rows, ml.shape[2]), F32)
    c1 = []

    def to_partner(i, carry):
        ml[i, 0:q_rows] = carry[0]
        ml[i, q_rows : 2 * q_rows] = carry[1]
        c1.append((
            remote(ml.at[i], r1ml.at[i], s1_send.at[2 * i], s1_recv.at[2 * i], partner),
            remote(num[i].at[pl.ds(theirs, half_h)], r1[i], s1_send.at[2 * i + 1], s1_recv.at[2 * i + 1], partner),
        ))
        for c in c1[-1]:
            c.start()

    def combine(i, dst, dst_ml):
        for c in c1[i]:
            c.wait_recv()
        m_a, l_a = ml[i, pl.ds(mine, half_h)], ml[i, pl.ds(q_rows + mine, half_h)]
        m_b, l_b = r1ml[i, pl.ds(mine, half_h)], r1ml[i, pl.ds(q_rows + mine, half_h)]
        m_chip = jnp.maximum(m_a, m_b)
        f_a = jnp.exp(m_a - m_chip)
        f_b = jnp.exp(m_b - m_chip)
        dst_ml[0:half_h] = m_chip
        dst_ml[half_h : 2 * half_h] = l_a * f_a + l_b * f_b
        f_a, f_b = f_a.T, f_b.T
        for h in range(half_h):
            dst[h] = num[i][mine + h] * f_a[0 : dst.shape[1], h : h + 1] + r1[i][h] * f_b[0 : dst.shape[1], h : h + 1]

    c2 = []

    def across(g):
        combine(g, away[g], away_ml.at[g])
        c2.append((
            remote(away_ml.at[g], r2ml.at[g], s2_send.at[2 * g], s2_recv.at[2 * g], across_x),
            remote(away[g], r2[g], s2_send.at[2 * g + 1], s2_recv.at[2 * g + 1], across_x),
        ))
        for c in c2[-1]:
            c.start()

    width = half_h * head_dim
    part_w = part_h * head_dim

    def o_place(which_half, k):
        return pl.ds(pl.multiple_of(2 * k * part_w + which_half * part_w, 128), part_w)

    def heads_start(g):
        for c in c2[g]:
            c.wait_recv()
        m_a, l_a = own_ml[g, 0:half_h], own_ml[g, half_h : 2 * half_h]
        m_b, l_b = r2ml[g, 0:half_h], r2ml[g, half_h : 2 * half_h]
        m_top = jnp.maximum(m_a, m_b)
        f_a = jnp.exp(m_a - m_top)
        f_b = jnp.exp(m_b - m_top)
        den = l_a * f_a + l_b * f_b + jnp.exp(sink_col[pl.ds(mine, half_h)] - m_top)
        f_a, f_b = (f_a / den).T, (f_b / den).T
        for h in range(half_h):
            o_buf[g][:, h * head_dim : (h + 1) * head_dim] = own[g][h] * f_a[0 : SEQ_GROUPS[g], h : h + 1] + r2[g][h] * f_b[0 : SEQ_GROUPS[g], h : h + 1]
        c = remote(o_buf[g], r3[g], s3_send.at[g], s3_recv.at[g], partner)
        c.start()
        for k in range(kv_local):
            o_all[g][:, o_place(core, k)] = o_buf[g][:, k * part_w : (k + 1) * part_w].astype(BF16)
        return c

    def heads_end(g, c):
        c.wait_recv()
        for k in range(kv_local):
            o_all[g][:, o_place(1 - core, k)] = r3[g][:, k * part_w : (k + 1) * part_w].astype(BF16)

    def y_copy(g, j):
        t = g * chunks + j
        return remote(y_send[g].at[j], y_recv[g].at[j], y_ss.at[t], y_rs.at[t], across_y)

    def x_copy(g, j):
        t = g * chunks + j
        return remote(z_buf[g].at[j], x_recv[g].at[j], x_ss.at[t], x_rs.at[t], across_x)

    def p1_copy(g, j):
        t = g * chunks + j
        return remote(z_buf[g].at[j], p1[g].at[j], p1_ss.at[t], p1_rs.at[t], partner)

    def p2_copy(g, j):
        t = g * chunks + j
        return remote(x_recv[g].at[j], p2[g].at[j], p2_ss.at[t], p2_rs.at[t], partner)

    def out_copy(kind, g, j):
        which_seqs, which_cols = ((chip, core), (1 - chip, core), (chip, 1 - core), (1 - chip, 1 - core))[kind]
        cols_at = pl.ds(pl.multiple_of(which_cols * cols + j * OUT_COLS, 128), OUT_COLS)
        return pltpu.make_async_copy(y_parts[g].at[kind, j], y_out.at[seqs(which_seqs, g), cols_at], o_sem.at[kind, g * chunks + j])

    def put_out(kind, g, j, value):
        y_parts[g][kind, j] = value
        out_copy(kind, g, j).start()

    def multiply(g, j):
        if g == 0:
            @pl.when(lax.rem(j, w_chunks) == 0)
            def _():
                w_copy(lax.div(j, w_chunks)).wait()

        w = w_buf[:, pl.ds(pl.multiple_of(j * OUT_COLS, 128), OUT_COLS)]
        y_send[g][j] = jnp.dot(o_all[g][...], w, preferred_element_type=F32)
        y_copy(g, j).start()

    def add(g, j):
        y_copy(g, j).wait_recv()
        x_part = x_buf[g][:, pl.ds(pl.multiple_of(j * OUT_COLS, 128), OUT_COLS)].astype(F32)
        row = (core * cols + j * OUT_COLS) // head_dim
        bias = jnp.concatenate([bo_f32[pl.ds(row + i, 1), :] for i in range(OUT_COLS // head_dim)], axis=1)
        z = (x_part + (y_send[g][j] + y_recv[g][j]) + bias).astype(BF16)
        z_buf[g][j] = z.astype(F32)
        x_copy(g, j).start()
        p1_copy(g, j).start()
        put_out(0, g, j, z)

    def spread(g, j):
        x_copy(g, j).wait_recv()
        p2_copy(g, j).start()
        put_out(1, g, j, x_recv[g][j].astype(BF16))
        p1_copy(g, j).wait_recv()
        put_out(2, g, j, p1[g][j].astype(BF16))

    def receive(g, j):
        p2_copy(g, j).wait_recv()
        put_out(3, g, j, p2[g][j].astype(BF16))

    def body(t, _):
        for stage, lag in ((multiply, 0), (add, LAG_Y), (spread, LAG_Y + LAG_X), (receive, LAG_Y + LAG_X + LAG_P)):
            for g in range(chip_groups):
                j = t - lag - g * chunks

                @pl.when(jnp.logical_and(j >= 0, j < chunks))
                def _():
                    stage(g, j)

        return 0

    heads_wait(0)
    carry = attend(0, 0, counts[0], (zero, zero))
    to_partner(0, carry)
    for c in x_in:
        c.start()
    heads_wait(1)
    carry = attend(1, 0, 2, (zero, zero))
    across(0)
    carry = attend(1, 2, counts[1], carry)
    to_partner(1, carry)
    w_copy(0).start()
    heads_wait(2)
    carry = attend(2, 0, 2, (zero, zero))
    across(1)
    w_copy(1).start()
    carry = attend(2, 2, counts[2], carry)
    to_partner(2, carry)
    for p in range(2, W_PARTS):
        w_copy(p).start()
    heads_wait(3)
    carry = attend(3, 0, counts[3], (zero, zero))
    to_partner(3, carry)
    combine(2, own[0], own_ml.at[0])
    combine(3, own[1], own_ml.at[1])

    c3 = [heads_start(0)]
    heads_end(0, c3[0])
    for c in x_in:
        c.wait()
    lax.fori_loop(0, chunks - 3, body, 0)
    c3.append(heads_start(1))
    lax.fori_loop(chunks - 3, chunks - 1, body, 0)
    heads_end(1, c3[1])
    lax.fori_loop(chunks - 1, total + LAG_Y + LAG_X + LAG_P, body, 0)

    for g in range(chip_groups):
        def tail(j, _):
            for copy in (y_copy, x_copy, p1_copy, p2_copy):
                copy(g, j).wait_send()
            for kind in range(4):
                out_copy(kind, g, j).wait()
            return 0

        lax.fori_loop(0, chunks, tail, 0)
    for c in (*h_remote, *(c for pair in c1 + c2 for c in pair), *c3):
        c.wait_send()


def finish(seq_lens, half, sinks, hidden, b_o, w_o, k_rows, v_rows):
    num_seqs, rows, head_dim = k_rows.shape
    q_rows = sinks.shape[1]
    half_h, half_s = q_rows // 2, num_seqs // 2
    kv_local = half.shape[0] - half_h
    assert sum(SEQ_GROUPS) == half_s
    order = SEQ_GROUPS * 2
    chip_groups, groups = len(SEQ_GROUPS), len(order)
    width = w_o.shape[1]
    cols = width // 2
    chunks = cols // OUT_COLS
    total = chip_groups * chunks
    vmem = pl.BlockSpec(memory_space=pltpu.VMEM)
    anyspace = pl.BlockSpec(memory_space=pl.ANY)
    chunked = tuple(pltpu.VMEM((chunks, n, OUT_COLS), F32) for n in SEQ_GROUPS)
    parts = tuple(pltpu.VMEM((half_h, n, head_dim), F32) for n in SEQ_GROUPS)
    parts_ml = pltpu.VMEM((chip_groups, 2 * half_h, 128), F32)
    o_parts = tuple(pltpu.VMEM((n, half_h * head_dim), F32) for n in SEQ_GROUPS)
    ring = pltpu.VMEM((ATT_SLOTS, ATT_SEQS, rows, head_dim), BF16)
    dma = pltpu.SemaphoreType.DMA
    return pl.pallas_call(
        finish_kernel,
        out_shape=[
            jax.ShapeDtypeStruct((num_seqs, width), BF16),
            jax.ShapeDtypeStruct((2, num_seqs, kv_local, head_dim), BF16),
        ],
        in_specs=[anyspace] * 8,
        out_specs=[anyspace, vmem],
        scratch_shapes=[
            pltpu.SMEM((num_seqs,), jnp.int32),
            pltpu.VMEM((1, q_rows), F32),
            pltpu.VMEM((width // head_dim, head_dim), BF16),
            dma((3,)),
            tuple(pltpu.VMEM((4, chunks, n, OUT_COLS), BF16) for n in SEQ_GROUPS),
            pltpu.VMEM((w_o.shape[0], cols), BF16),
            tuple(pltpu.VMEM((n, cols), BF16) for n in SEQ_GROUPS),
            pltpu.VMEM((q_rows + 2 * kv_local, num_seqs, head_dim), F32),
            ring, ring,
            tuple(pltpu.VMEM((q_rows, n, head_dim), F32) for n in order),
            pltpu.VMEM((groups, 2 * q_rows, 128), F32),
            pltpu.VMEM((q_rows, 128), F32),
            pltpu.VMEM((width // head_dim, head_dim), F32),
            tuple(pltpu.VMEM((half_h, n, head_dim), F32) for n in order),
            pltpu.VMEM((groups, 2 * q_rows, 128), F32),
            parts, parts_ml, parts, parts_ml, parts, parts_ml,
            o_parts, o_parts,
            tuple(pltpu.VMEM((n, q_rows * head_dim), BF16) for n in SEQ_GROUPS),
            chunked, chunked, chunked, chunked, chunked, chunked,
            dma((W_PARTS,)), dma((chip_groups,)), dma((ATT_SLOTS,)), dma((ATT_SLOTS,)),
            dma((2 * groups,)), dma((2 * groups,)), dma((2 * groups,)),
            dma((2 * groups,)), dma((2 * groups,)),
            dma((groups,)), dma((groups,)),
            dma((chip_groups,)), dma((chip_groups,)),
            *[dma((total,))] * 8,
            dma((4, total)),
        ],
        compiler_params=pltpu.CompilerParams(collective_id=1, has_side_effects=True, vmem_limit_bytes=62 << 20),
        name="finish",
    )(seq_lens, half, sinks, hidden, b_o.reshape(width // head_dim, head_dim), w_o, k_rows, v_rows)


LAST_PARTS = 8
LAST_UNROLL = 8


def last_kernel(lens_hbm, y_hbm, new_hbm, k_in, v_in, y_out, k_out, v_out, lens_ref, lens_sem, y_buf, new_ref, in_sem, out_sem, new_sem, k_sem, v_sem):
    num_seqs, ctx_local = k_out.shape[:2]
    base = lax.axis_index("sp") * ctx_local
    rows = y_hbm.shape[0] // LAST_PARTS
    new_copy = pltpu.make_async_copy(new_hbm, new_ref, new_sem)
    new_copy.start()
    lens_copy = pltpu.make_async_copy(lens_hbm, lens_ref, lens_sem)
    lens_copy.start()
    loads, stores = [], []
    for p in range(LAST_PARTS):
        at = pl.ds(p * rows, rows)
        loads.append(pltpu.make_async_copy(y_hbm.at[at], y_buf.at[at], in_sem.at[p]))
        stores.append(pltpu.make_async_copy(y_buf.at[at], y_out.at[at], out_sem.at[p]))
        loads[-1].start()

    def for_new_rows(act):
        def step(i, _):
            for b in (i * LAST_UNROLL + r for r in range(LAST_UNROLL)):
                n = lens_ref[b] - base

                @pl.when(jnp.logical_and(n >= 0, n < ctx_local))
                def _():
                    act(pltpu.make_async_copy(new_ref.at[0, b], k_out.at[b, n], k_sem))
                    act(pltpu.make_async_copy(new_ref.at[1, b], v_out.at[b, n], v_sem))

            return 0

        lax.fori_loop(0, num_seqs // LAST_UNROLL, step, 0)

    lens_copy.wait()
    new_copy.wait()
    for_new_rows(lambda c: c.start())
    for p in range(LAST_PARTS):
        loads[p].wait()
        stores[p].start()
    for_new_rows(lambda c: c.wait())
    for c in stores:
        c.wait()


def last(seq_lens, y, new, k_copy, v_copy):
    anyspace = pl.BlockSpec(memory_space=pl.ANY)
    dma = pltpu.SemaphoreType.DMA
    return pl.pallas_call(
        last_kernel,
        out_shape=[jax.ShapeDtypeStruct(a.shape, a.dtype) for a in (y, k_copy, v_copy)],
        in_specs=[anyspace] * 5,
        out_specs=[anyspace] * 3,
        scratch_shapes=[pltpu.SMEM(seq_lens.shape, jnp.int32), dma, pltpu.VMEM(y.shape, y.dtype), pltpu.VMEM(new.shape, new.dtype), dma((LAST_PARTS,)), dma((LAST_PARTS,)), dma, dma, dma],
        input_output_aliases={3: 1, 4: 2},
        compiler_params=pltpu.CompilerParams(vmem_limit_bytes=60 << 20),
        name="last",
    )(seq_lens, y, new, k_copy, v_copy)


def solution(mesh):
    cache_spec = P("dp", "sp", "tp", None)

    def block_step(hidden, seq_lens, rope_cos, rope_sin, k_cache, v_cache, norm_gain, w_qkv, b_qkv, sink_logits, w_o, b_o):
        num_seqs, ctx_local, kv_local, head_dim = k_cache.shape
        rows = (num_seqs, ctx_local * kv_local, head_dim)
        k_rows, v_rows = k_cache.reshape(rows), v_cache.reshape(rows)
        half, k_copy, v_copy = project(hidden, rope_cos, rope_sin, norm_gain, w_qkv, b_qkv, k_rows, v_rows)
        sinks = sink_logits.reshape(1, sink_logits.shape[0])
        y, new = finish(seq_lens, half, sinks, hidden, b_o, w_o, k_rows, v_rows)
        return last(seq_lens, y, new, k_copy.reshape(k_cache.shape), v_copy.reshape(v_cache.shape))

    return jax.shard_map(block_step, mesh=mesh, in_specs=(P("dp", None), P("dp"), P("dp", None), P("dp", None), cache_spec, cache_spec, P(None), P(None, "tp", None), P("tp", None), P("tp"), P("tp", None), P(None)), out_specs=(P("dp", None), cache_spec, cache_spec), check_vma=False)
```

```python
import functools

import jax
import jax.numpy as jnp
from jax import lax
from jax.experimental import pallas as pl
from jax.experimental.pallas import tpu as pltpu
from jax.sharding import PartitionSpec as P

NORM_EPS = 1e-5
F32 = jnp.float32
BF16 = jnp.bfloat16
MESH = pl.DeviceIdType.MESH


def sp_place():
    sp = lax.axis_index("sp")
    return lax.div(sp, 2), lax.rem(sp, 2)


def remote(src, dst, send_sem, recv_sem, where):
    return pltpu.make_async_remote_copy(src_ref=src, dst_ref=dst, send_sem=send_sem, recv_sem=recv_sem, device_id=where, device_id_type=MESH)


def sink_column(row_ref, count, halves, group):
    row = lax.broadcasted_iota(jnp.int32, (count, count), 0)
    per_half = count // halves
    part = group // halves
    head = lax.div(lax.rem(row, per_half), part) * group + lax.div(row, per_half) * part + lax.rem(row, part)
    same = head == lax.broadcasted_iota(jnp.int32, (count, count), 1)
    return jnp.sum(jnp.where(same, jnp.broadcast_to(row_ref[...], (count, count)), 0.0), axis=1, keepdims=True)


QKV_ROWS = 1024
QKV_SLOTS = 3
CACHE_SEQS = 16
CACHE_AHEAD = 4
CACHE_FIRST = 1
X_PARTS = 4


def project_kernel(x_hbm, gain_hbm, cos_hbm, sin_hbm, bias_hbm, w_ref, k_ref, v_ref, out_ref, k_out, v_out,
                   x_ref, gain_ref, cos_ref, sin_ref, bias_ref, x_sem, small_sem, normed, gain, heads, acc_q, acc_e, wq_buf, we_buf, k_buf, v_buf, wq_sem, we_sem, out_sem, k_in, v_in, k_back, v_back):
    _, core = sp_place()
    num_seqs, depth = x_ref.shape
    head_dim = acc_e.shape[2]
    q_cols = acc_q.shape[2]
    kv_local = acc_q.shape[0]
    per_core = q_cols // head_dim
    group = 2 * per_core
    steps = depth // QKV_ROWS
    x_rows = num_seqs // X_PARTS
    blocks = num_seqs // CACHE_SEQS

    def fetch(step, slot):
        rows = pl.ds(step * QKV_ROWS, QKV_ROWS)
        cq = pltpu.make_async_copy(w_ref.at[rows, :, pl.ds(pl.multiple_of(core * q_cols, 128), q_cols)], wq_buf.at[slot], wq_sem.at[slot])
        ce = pltpu.make_async_copy(w_ref.at[rows, :, pl.ds(pl.multiple_of((group + core) * head_dim, 128), head_dim)], we_buf.at[slot], we_sem.at[slot])
        return cq, ce

    def cache_in(i):
        at = pl.ds(i * CACHE_SEQS, CACHE_SEQS)
        return pltpu.make_async_copy(k_ref.at[at], k_buf.at[at], k_in.at[i]), pltpu.make_async_copy(v_ref.at[at], v_buf.at[at], v_in.at[i])

    def cache_back(i):
        at = pl.ds(i * CACHE_SEQS, CACHE_SEQS)
        return pltpu.make_async_copy(k_buf.at[at], k_out.at[at], k_back.at[i]), pltpu.make_async_copy(v_buf.at[at], v_out.at[at], v_back.at[i])

    small = [pltpu.make_async_copy(src, dst, small_sem.at[i]) for i, (src, dst) in enumerate(((gain_hbm, gain_ref), (cos_hbm, cos_ref), (sin_hbm, sin_ref), (bias_hbm, bias_ref)))]
    small[0].start()
    x_copies = []
    for p in range(X_PARTS):
        at = pl.ds(p * x_rows, x_rows)
        x_copies.append(pltpu.make_async_copy(x_hbm.at[at], x_ref.at[at], x_sem.at[p]))
        x_copies[-1].start()
    for c in fetch(0, 0):
        c.start()
    for i in range(CACHE_FIRST):
        for c in cache_in(i):
            c.start()
    for s in range(1, QKV_SLOTS - 1):
        for c in fetch(s, s):
            c.start()
    for i in range(CACHE_FIRST, CACHE_AHEAD):
        for c in cache_in(i):
            c.start()
    for c in small[1:]:
        c.start()

    small[0].wait()
    gain[...] = gain_ref[...].astype(F32)

    def norm_rows(r, _):
        rows = pl.ds(pl.multiple_of(r * 16, 16), 16)
        xw = x_ref[rows, :].astype(F32)
        inv = lax.rsqrt(jnp.mean(xw * xw, axis=-1, keepdims=True) + NORM_EPS)
        for t in range(depth // head_dim):
            cols = slice(t * head_dim, (t + 1) * head_dim)
            normed[rows, cols] = (xw[:, cols] * inv * gain[t : t + 1, :]).astype(BF16)
        return 0

    for p in range(X_PARTS):
        x_copies[p].wait()
        lax.fori_loop(p * x_rows // 16, (p + 1) * x_rows // 16, norm_rows, 0)
    for i in range(CACHE_FIRST):
        for c in cache_in(i):
            c.wait()
        for c in cache_back(i):
            c.start()
    acc_q[...] = jnp.zeros_like(acc_q)
    acc_e[...] = jnp.zeros_like(acc_e)

    def step_fn(step, _):
        slot = lax.rem(step, QKV_SLOTS)

        @pl.when(step + CACHE_AHEAD < blocks)
        def _():
            for c in cache_in(step + CACHE_AHEAD):
                c.start()

        for c in fetch(step, slot):
            c.wait()

        @pl.when(step + QKV_SLOTS - 1 < steps)
        def _():
            for c in fetch(step + QKV_SLOTS - 1, lax.rem(step + QKV_SLOTS - 1, QKV_SLOTS)):
                c.start()

        @pl.when(step + CACHE_FIRST < blocks)
        def _():
            for c in cache_in(step + CACHE_FIRST):
                c.wait()
            for c in cache_back(step + CACHE_FIRST):
                c.start()

        h = normed[:, pl.ds(pl.multiple_of(step * QKV_ROWS, 128), QKV_ROWS)]
        wq = jnp.swapaxes(wq_buf[slot], 0, 1)
        we = jnp.swapaxes(we_buf[slot], 0, 1)
        for k in range(kv_local):
            acc_q[k] += jnp.dot(h, wq[k], preferred_element_type=F32)
            acc_e[k] += jnp.dot(h, we[k], preferred_element_type=F32)
        return 0

    lax.fori_loop(0, steps, step_fn, 0)

    for c in small[1:]:
        c.wait()
    cos_t = cos_ref[...].T
    sin_t = sin_ref[...].T
    cos2 = jnp.concatenate([cos_t, cos_t], axis=1)
    sin2 = jnp.concatenate([-sin_t, sin_t], axis=1)
    is_key = core == 0
    cos_e = jnp.where(is_key, cos2, jnp.ones_like(cos2))
    sin_e = jnp.where(is_key, sin2, jnp.zeros_like(sin2))

    def rotate(v, c, s):
        r = v * c + pltpu.roll(v, head_dim // 2, 1) * s
        return r.astype(BF16).astype(F32)

    for k in range(kv_local):
        bias_q = bias_ref[k : k + 1, pl.ds(pl.multiple_of(core * q_cols, 128), q_cols)].astype(F32)
        for g in range(per_core):
            cols = slice(g * head_dim, (g + 1) * head_dim)
            heads[k * per_core + g] = rotate(acc_q[k, :, cols] + bias_q[:, cols], cos2, sin2)
        bias_e = bias_ref[k : k + 1, pl.ds(pl.multiple_of((group + core) * head_dim, 128), head_dim)].astype(F32)
        heads[kv_local * per_core + k] = rotate(acc_e[k] + bias_e, cos_e, sin_e)
    done = []
    for k in range(kv_local + 1):
        part = pl.ds(k * per_core, per_core)
        done.append(pltpu.make_async_copy(heads.at[part], out_ref.at[part], out_sem.at[k]))
        done[-1].start()
    for i in range(blocks):
        for c in cache_back(i):
            c.wait()
    for c in done:
        c.wait()


def project(hidden, rope_cos, rope_sin, norm_gain, w_qkv, b_qkv, k_rows, v_rows):
    num_seqs, depth = hidden.shape
    head_dim = k_rows.shape[2]
    kv_local = w_qkv.shape[1]
    per_core = (w_qkv.shape[2] // head_dim - 2) // 2
    rows = kv_local * (per_core + 1)
    blocks = num_seqs // CACHE_SEQS
    assert blocks <= depth // QKV_ROWS + CACHE_FIRST
    anyspace = pl.BlockSpec(memory_space=pl.ANY)
    dma = pltpu.SemaphoreType.DMA
    return pl.pallas_call(
        project_kernel,
        out_shape=[
            jax.ShapeDtypeStruct((rows, num_seqs, head_dim), F32),
            jax.ShapeDtypeStruct(k_rows.shape, BF16),
            jax.ShapeDtypeStruct(v_rows.shape, BF16),
        ],
        in_specs=[anyspace] * 8,
        out_specs=[anyspace] * 3,
        scratch_shapes=[
            pltpu.VMEM((num_seqs, depth), BF16),
            pltpu.VMEM((depth // head_dim, head_dim), BF16),
            pltpu.VMEM((head_dim // 2, num_seqs), F32),
            pltpu.VMEM((head_dim // 2, num_seqs), F32),
            pltpu.VMEM(b_qkv.shape, BF16),
            dma((X_PARTS,)),
            dma((4,)),
            pltpu.VMEM((num_seqs, depth), BF16),
            pltpu.VMEM((depth // head_dim, head_dim), F32),
            pltpu.VMEM((rows, num_seqs, head_dim), F32),
            pltpu.VMEM((kv_local, num_seqs, per_core * head_dim), F32),
            pltpu.VMEM((kv_local, num_seqs, head_dim), F32),
            pltpu.VMEM((QKV_SLOTS, QKV_ROWS, kv_local, per_core * head_dim), BF16),
            pltpu.VMEM((QKV_SLOTS, QKV_ROWS, kv_local, head_dim), BF16),
            pltpu.VMEM(k_rows.shape, BF16),
            pltpu.VMEM(v_rows.shape, BF16),
            dma((QKV_SLOTS,)), dma((QKV_SLOTS,)), dma((kv_local + 1,)),
            dma((blocks,)), dma((blocks,)), dma((blocks,)), dma((blocks,)),
        ],
        compiler_params=pltpu.CompilerParams(vmem_limit_bytes=60 << 20),
        name="project",
    )(hidden, norm_gain.reshape(depth // head_dim, head_dim), rope_cos.T, rope_sin.T, b_qkv, w_qkv, k_rows, v_rows)


ATT_SEQS = 8
ATT_SLOTS = 6
OUT_COLS = 512
SEQ_GROUPS = (24, 40)
PIECES = ((0, 0, 8), (0, 8, 16), (1, 0, 40))
W_PARTS = 8
LAG_Y = 3
LAG_X = 3
LAG_P = 1


def finish_kernel(lens_hbm, half_hbm, sink_hbm, hid_ref, bo_hbm, wo_ref, k_hbm, v_hbm, y_out, new_ref,
                  lens_ref, sink_ref, bo_ref, small_sem, y_parts, w_buf, x_buf, h_buf, k_ring, v_ring, num, ml, sink_col, bo_f32, r1, r1ml, own, own_ml, away, away_ml, r2, r2ml, o_buf, r3, o_all,
                  y_send, y_recv, z_buf, x_recv, p1, p2,
                  w_sem, x_sem, k_sem, v_sem, h_in, h_send, h_recv, s1_send, s1_recv, s2_send, s2_recv, s3_send, s3_recv,
                  y_ss, y_rs, x_ss, x_rs, p1_ss, p1_rs, p2_ss, p2_rs, o_sem):
    chip, core = sp_place()
    tp = lax.axis_index("tp")
    partner = {"sp": 2 * chip + (1 - core)}
    across_x = {"sp": 2 * (1 - chip) + core}
    across_y = {"tp": 1 - tp}
    q_rows, _, head_dim = num[0].shape
    chip_groups = len(SEQ_GROUPS)
    offsets = [sum(SEQ_GROUPS[:g]) for g in range(chip_groups)]
    num_seqs = h_buf.shape[1]
    kv_local = (h_buf.shape[0] - q_rows) // 2
    rows = k_ring.shape[2]
    ctx_local = rows // kv_local
    half_h = q_rows // 2
    half_s = num_seqs // 2
    part_h = half_h // kv_local
    cols = w_buf.shape[1]
    chunks = cols // OUT_COLS
    total = chip_groups * chunks
    mine = pl.multiple_of(core * half_h, half_h)
    theirs = pl.multiple_of((1 - core) * half_h, half_h)

    def seqs(which, g, first=0, count=None):
        return pl.ds(pl.multiple_of(which * half_s + offsets[g] + first, 8), SEQ_GROUPS[g] if count is None else count)

    small = [pltpu.make_async_copy(src, dst, small_sem.at[i]) for i, (src, dst) in enumerate(((lens_hbm, lens_ref), (sink_hbm, sink_ref), (bo_hbm, bo_ref)))]
    for c in small:
        c.start()
    barrier = pltpu.get_barrier_semaphore()
    for peer in (partner, across_x, across_y):
        pl.semaphore_signal(barrier, inc=1, device_id=peer, device_id_type=MESH)

    order = [(1 - chip, *piece) for piece in PIECES] + [(chip, g, 0, n) for g, n in enumerate(SEQ_GROUPS)]
    own_rows = (pl.ds(mine, half_h), pl.ds(pl.multiple_of(q_rows + kv_local * core, kv_local), kv_local))
    src_rows = (pl.ds(0, half_h), pl.ds(half_h, kv_local))
    h_local, h_remote = [], []
    for i, piece in enumerate(order):
        at = seqs(*piece)
        for j in range(2):
            h_local.append(pltpu.make_async_copy(half_hbm.at[src_rows[j], at], h_buf.at[own_rows[j], at], h_in.at[2 * i + j]))
            h_local[-1].start()
            h_remote.append(remote(half_hbm.at[src_rows[j], at], h_buf.at[own_rows[j], at], h_send.at[2 * i + j], h_recv.at[2 * i + j], partner))

    steps = num_seqs // ATT_SEQS
    counts = [n // ATT_SEQS for _, _, _, n in order]
    starts = [sum(counts[:i]) for i in range(len(counts))]

    def block(p):
        return lax.rem(p + (1 - chip) * (steps // 2), steps) * ATT_SEQS

    def kv_load(p):
        at = pl.ds(pl.multiple_of(block(p), ATT_SEQS), ATT_SEQS)
        slot = lax.rem(p, ATT_SLOTS)
        return pltpu.make_async_copy(k_hbm.at[at], k_ring.at[slot], k_sem.at[slot]), pltpu.make_async_copy(v_hbm.at[at], v_ring.at[slot], v_sem.at[slot])

    for p in range(ATT_SLOTS):
        for c in kv_load(p):
            c.start()
    my_cols = pl.ds(pl.multiple_of(core * cols, 128), cols)
    x_in = [pltpu.make_async_copy(hid_ref.at[seqs(chip, g), my_cols], x_buf[g], x_sem.at[g]) for g in range(chip_groups)]
    w_cols = cols // W_PARTS
    w_chunks = w_cols // OUT_COLS

    def w_copy(p):
        return pltpu.make_async_copy(wo_ref.at[:, pl.ds(pl.multiple_of(core * cols + p * w_cols, 128), w_cols)], w_buf.at[:, pl.ds(pl.multiple_of(p * w_cols, 128), w_cols)], w_sem.at[p])

    for c in small:
        c.wait()
    sink = sink_column(sink_ref, q_rows, 2, 2 * part_h)
    sink_col[...] = jnp.broadcast_to(sink, sink_col.shape)
    bo_f32[...] = bo_ref[...].astype(F32)
    pl.semaphore_wait(barrier, 3)
    for c in h_remote:
        c.start()

    base = lax.axis_index("sp") * ctx_local
    scale = head_dim**-0.5
    col = lax.broadcasted_iota(jnp.int32, (q_rows, rows), 1)
    kv_row = lax.div(lax.rem(lax.broadcasted_iota(jnp.int32, (q_rows, rows), 0), half_h), part_h)
    col_pos = jnp.where(lax.rem(col, kv_local) == kv_row, lax.div(col, kv_local), ctx_local * 1024)
    lane = lax.broadcasted_iota(jnp.int32, (q_rows, ml.shape[2]), 1)
    batch = range(ATT_SEQS)
    over_d = (((1,), (1,)), ((), ()))
    new_code = jnp.where(lax.broadcasted_iota(jnp.int32, (q_rows, 16), 1) == lax.div(lax.rem(lax.broadcasted_iota(jnp.int32, (q_rows, 16), 0), half_h), part_h), 1, 2)

    def attend(i, first, last, carry):
        def step_fn(t, carry):
            m_all, l_all = carry
            p = starts[i] + t
            slot = lax.rem(p, ATT_SLOTS)
            for c in kv_load(p):
                c.wait()
            start = block(p)
            heads = h_buf.at[:, pl.ds(pl.multiple_of(start, ATT_SEQS), ATT_SEQS)]
            rel = [lens_ref[start + s] - base for s in batch]
            inside = [jnp.where(jnp.logical_and(r >= 0, r < ctx_local), 1, 0) for r in rel]
            queries = [heads[0:q_rows, s, :].astype(BF16) for s in batch]
            new_k, new_v = ([jnp.concatenate([heads[lo : lo + kv_local, s, :]] * (16 // kv_local), axis=0).astype(BF16) for s in batch] for lo in (q_rows, q_rows + kv_local))
            logits = [lax.dot_general(queries[s], k_ring[slot, s], over_d, preferred_element_type=F32) for s in batch]
            extra = [lax.dot_general(queries[s], new_k[s], over_d, preferred_element_type=F32) for s in batch]
            logits = [jnp.where(col_pos < rel[s], logits[s] * scale, -jnp.inf) for s in batch]
            extra = [jnp.where(new_code == inside[s], extra[s] * scale, -jnp.inf) for s in batch]
            tops = [jnp.maximum(jnp.maximum(jnp.max(logits[s], axis=1, keepdims=True), jnp.max(extra[s], axis=1, keepdims=True)), sink) for s in batch]
            weights = [jnp.exp(logits[s] - tops[s]) for s in batch]
            extra = [jnp.exp(extra[s] - tops[s]) for s in batch]
            totals = [jnp.sum(weights[s], axis=1, keepdims=True) + jnp.sum(extra[s], axis=1, keepdims=True) for s in batch]
            sums = [jnp.dot(weights[s].astype(BF16), v_ring[slot, s], preferred_element_type=F32) for s in batch]
            sums = [sums[s] + jnp.dot(extra[s].astype(BF16), new_v[s], preferred_element_type=F32) for s in batch]
            out = num[i].at[:, pl.ds(pl.multiple_of(t * ATT_SEQS, ATT_SEQS), ATT_SEQS)]
            for s in batch:
                here = lane == order[i][2] + t * ATT_SEQS + s
                m_all = jnp.where(here, tops[s], m_all)
                l_all = jnp.where(here, totals[s], l_all)
                out[:, s, :] = sums[s]
            for s in batch:
                for j in range(2):
                    new_ref[j, start + s] = heads[q_rows + j * kv_local : q_rows + (j + 1) * kv_local, s, :].astype(BF16)

            @pl.when(p + ATT_SLOTS < steps)
            def _():
                for c in kv_load(p + ATT_SLOTS):
                    c.start()

            return m_all, l_all

        return lax.fori_loop(first, last, step_fn, carry)

    def heads_wait(i):
        for j in range(2):
            h_local[2 * i + j].wait()
            h_remote[2 * i + j].wait_recv()

    zero = jnp.zeros((q_rows, ml.shape[2]), F32)
    c1 = []

    def to_partner(i, carry):
        ml[i, 0:q_rows] = carry[0]
        ml[i, q_rows : 2 * q_rows] = carry[1]
        c1.append((
            remote(ml.at[i], r1ml.at[i], s1_send.at[2 * i], s1_recv.at[2 * i], partner),
            remote(num[i].at[pl.ds(theirs, half_h)], r1[i], s1_send.at[2 * i + 1], s1_recv.at[2 * i + 1], partner),
        ))
        for c in c1[-1]:
            c.start()

    def combine(i, dst, dst_ml):
        for c in c1[i]:
            c.wait_recv()
        m_a, l_a = ml[i, pl.ds(mine, half_h)], ml[i, pl.ds(q_rows + mine, half_h)]
        m_b, l_b = r1ml[i, pl.ds(mine, half_h)], r1ml[i, pl.ds(q_rows + mine, half_h)]
        m_chip = jnp.maximum(m_a, m_b)
        f_a = jnp.exp(m_a - m_chip)
        f_b = jnp.exp(m_b - m_chip)
        dst_ml[0:half_h] = m_chip
        dst_ml[half_h : 2 * half_h] = l_a * f_a + l_b * f_b
        f_a, f_b = f_a.T, f_b.T
        some = slice(order[i][2], order[i][2] + order[i][3])
        for h in range(half_h):
            dst[h, some] = num[i][mine + h] * f_a[some, h : h + 1] + r1[i][h] * f_b[some, h : h + 1]

    c2 = []

    def across(i):
        _, g, first, count = order[i]
        combine(i, away[g], away_ml.at[i])
        at = pl.ds(first, count)
        c2.append((
            remote(away_ml.at[i], r2ml.at[i], s2_send.at[2 * i], s2_recv.at[2 * i], across_x),
            remote(away[g].at[:, at], r2[g].at[:, at], s2_send.at[2 * i + 1], s2_recv.at[2 * i + 1], across_x),
        ))
        for c in c2[-1]:
            c.start()

    width = half_h * head_dim
    part_w = part_h * head_dim

    def o_place(which_half, k):
        return pl.ds(pl.multiple_of(2 * k * part_w + which_half * part_w, 128), part_w)

    def heads_start(g):
        m_a, l_a = own_ml[g, 0:half_h], own_ml[g, half_h : 2 * half_h]
        m_b, l_b = None, None
        for i, (group, first, _) in enumerate(PIECES):
            if group == g:
                for c in c2[i]:
                    c.wait_recv()
                m_i, l_i = r2ml[i, 0:half_h], r2ml[i, half_h : 2 * half_h]
                if m_b is None:
                    m_b, l_b = m_i, l_i
                else:
                    m_b = jnp.where(lane[0:half_h] < first, m_b, m_i)
                    l_b = jnp.where(lane[0:half_h] < first, l_b, l_i)
        m_top = jnp.maximum(m_a, m_b)
        f_a = jnp.exp(m_a - m_top)
        f_b = jnp.exp(m_b - m_top)
        den = l_a * f_a + l_b * f_b + jnp.exp(sink_col[pl.ds(mine, half_h)] - m_top)
        f_a, f_b = (f_a / den).T, (f_b / den).T
        for h in range(half_h):
            o_buf[g][:, h * head_dim : (h + 1) * head_dim] = own[g][h] * f_a[0 : SEQ_GROUPS[g], h : h + 1] + r2[g][h] * f_b[0 : SEQ_GROUPS[g], h : h + 1]
        c = remote(o_buf[g], r3[g], s3_send.at[g], s3_recv.at[g], partner)
        c.start()
        for k in range(kv_local):
            o_all[g][:, o_place(core, k)] = o_buf[g][:, k * part_w : (k + 1) * part_w].astype(BF16)
        return c

    def heads_end(g, c):
        c.wait_recv()
        for k in range(kv_local):
            o_all[g][:, o_place(1 - core, k)] = r3[g][:, k * part_w : (k + 1) * part_w].astype(BF16)

    def y_copy(g, j):
        t = g * chunks + j
        return remote(y_send[g].at[j], y_recv[g].at[j], y_ss.at[t], y_rs.at[t], across_y)

    def x_copy(g, j):
        t = g * chunks + j
        return remote(z_buf[g].at[j], x_recv[g].at[j], x_ss.at[t], x_rs.at[t], across_x)

    def p1_copy(g, j):
        t = g * chunks + j
        return remote(z_buf[g].at[j], p1[g].at[j], p1_ss.at[t], p1_rs.at[t], partner)

    def p2_copy(g, j):
        t = g * chunks + j
        return remote(x_recv[g].at[j], p2[g].at[j], p2_ss.at[t], p2_rs.at[t], partner)

    def out_copy(kind, g, j):
        which_seqs, which_cols = ((chip, core), (1 - chip, core), (chip, 1 - core), (1 - chip, 1 - core))[kind]
        cols_at = pl.ds(pl.multiple_of(which_cols * cols + j * OUT_COLS, 128), OUT_COLS)
        return pltpu.make_async_copy(y_parts[g].at[kind, j], y_out.at[seqs(which_seqs, g), cols_at], o_sem.at[kind, g * chunks + j])

    def put_out(kind, g, j, value):
        y_parts[g][kind, j] = value
        out_copy(kind, g, j).start()

    def multiply(g, j):
        if g == 0:
            @pl.when(lax.rem(j, w_chunks) == 0)
            def _():
                w_copy(lax.div(j, w_chunks)).wait()

        w = w_buf[:, pl.ds(pl.multiple_of(j * OUT_COLS, 128), OUT_COLS)]
        y_send[g][j] = jnp.dot(o_all[g][...], w, preferred_element_type=F32)
        y_copy(g, j).start()

    def add(g, j):
        y_copy(g, j).wait_recv()
        x_part = x_buf[g][:, pl.ds(pl.multiple_of(j * OUT_COLS, 128), OUT_COLS)].astype(F32)
        row = (core * cols + j * OUT_COLS) // head_dim
        bias = jnp.concatenate([bo_f32[pl.ds(row + i, 1), :] for i in range(OUT_COLS // head_dim)], axis=1)
        z = (x_part + (y_send[g][j] + y_recv[g][j]) + bias).astype(BF16)
        z_buf[g][j] = z.astype(F32)
        x_copy(g, j).start()
        p1_copy(g, j).start()
        put_out(0, g, j, z)

    def spread(g, j):
        x_copy(g, j).wait_recv()
        p2_copy(g, j).start()
        put_out(1, g, j, x_recv[g][j].astype(BF16))
        p1_copy(g, j).wait_recv()
        put_out(2, g, j, p1[g][j].astype(BF16))

    def receive(g, j):
        p2_copy(g, j).wait_recv()
        put_out(3, g, j, p2[g][j].astype(BF16))

    def body(t, _):
        for stage, lag in ((multiply, 0), (add, LAG_Y), (spread, LAG_Y + LAG_X), (receive, LAG_Y + LAG_X + LAG_P)):
            for g in range(chip_groups):
                j = t - lag - g * chunks

                @pl.when(jnp.logical_and(j >= 0, j < chunks))
                def _():
                    stage(g, j)

        return 0

    heads_wait(0)
    to_partner(0, attend(0, 0, counts[0], (zero, zero)))
    heads_wait(1)
    to_partner(1, attend(1, 0, counts[1], (zero, zero)))
    across(0)
    heads_wait(2)
    carry = attend(2, 0, 2, (zero, zero))
    across(1)
    for c in x_in:
        c.start()
    to_partner(2, attend(2, 2, counts[2], carry))
    w_copy(0).start()
    heads_wait(3)
    carry = attend(3, 0, counts[3], (zero, zero))
    across(2)
    w_copy(1).start()
    to_partner(3, carry)
    for p in range(2, W_PARTS):
        w_copy(p).start()
    heads_wait(4)
    to_partner(4, attend(4, 0, counts[4], (zero, zero)))
    combine(3, own[0], own_ml.at[0])
    combine(4, own[1], own_ml.at[1])

    c3 = [heads_start(0)]
    heads_end(0, c3[0])
    for c in x_in:
        c.wait()
    lax.fori_loop(0, chunks - 3, body, 0)
    c3.append(heads_start(1))
    lax.fori_loop(chunks - 3, chunks - 1, body, 0)
    heads_end(1, c3[1])
    lax.fori_loop(chunks - 1, total + LAG_Y + LAG_X + LAG_P, body, 0)

    for g in range(chip_groups):
        def tail(j, _):
            for copy in (y_copy, x_copy, p1_copy, p2_copy):
                copy(g, j).wait_send()
            for kind in range(4):
                out_copy(kind, g, j).wait()
            return 0

        lax.fori_loop(0, chunks, tail, 0)
    for c in (*h_remote, *(c for pair in c1 + c2 for c in pair), *c3):
        c.wait_send()


def finish(seq_lens, half, sinks, hidden, b_o, w_o, k_rows, v_rows):
    num_seqs, rows, head_dim = k_rows.shape
    q_rows = sinks.shape[1]
    half_h, half_s = q_rows // 2, num_seqs // 2
    kv_local = half.shape[0] - half_h
    assert sum(SEQ_GROUPS) == half_s
    order = tuple(n for _, _, n in PIECES) + SEQ_GROUPS
    chip_groups, groups = len(SEQ_GROUPS), len(order)
    width = w_o.shape[1]
    cols = width // 2
    chunks = cols // OUT_COLS
    total = chip_groups * chunks
    vmem = pl.BlockSpec(memory_space=pltpu.VMEM)
    anyspace = pl.BlockSpec(memory_space=pl.ANY)
    chunked = tuple(pltpu.VMEM((chunks, n, OUT_COLS), F32) for n in SEQ_GROUPS)
    parts = tuple(pltpu.VMEM((half_h, n, head_dim), F32) for n in SEQ_GROUPS)
    own_ml = pltpu.VMEM((chip_groups, 2 * half_h, 128), F32)
    piece_ml = pltpu.VMEM((len(PIECES), 2 * half_h, 128), F32)
    o_parts = tuple(pltpu.VMEM((n, half_h * head_dim), F32) for n in SEQ_GROUPS)
    ring = pltpu.VMEM((ATT_SLOTS, ATT_SEQS, rows, head_dim), BF16)
    dma = pltpu.SemaphoreType.DMA
    return pl.pallas_call(
        finish_kernel,
        out_shape=[
            jax.ShapeDtypeStruct((num_seqs, width), BF16),
            jax.ShapeDtypeStruct((2, num_seqs, kv_local, head_dim), BF16),
        ],
        in_specs=[anyspace] * 8,
        out_specs=[anyspace, vmem],
        scratch_shapes=[
            pltpu.SMEM((num_seqs,), jnp.int32),
            pltpu.VMEM((1, q_rows), F32),
            pltpu.VMEM((width // head_dim, head_dim), BF16),
            dma((3,)),
            tuple(pltpu.VMEM((4, chunks, n, OUT_COLS), BF16) for n in SEQ_GROUPS),
            pltpu.VMEM((w_o.shape[0], cols), BF16),
            tuple(pltpu.VMEM((n, cols), BF16) for n in SEQ_GROUPS),
            pltpu.VMEM((q_rows + 2 * kv_local, num_seqs, head_dim), F32),
            ring, ring,
            tuple(pltpu.VMEM((q_rows, n, head_dim), F32) for n in order),
            pltpu.VMEM((groups, 2 * q_rows, 128), F32),
            pltpu.VMEM((q_rows, 128), F32),
            pltpu.VMEM((width // head_dim, head_dim), F32),
            tuple(pltpu.VMEM((half_h, n, head_dim), F32) for n in order),
            pltpu.VMEM((groups, 2 * q_rows, 128), F32),
            parts, own_ml, parts, piece_ml, parts, piece_ml,
            o_parts, o_parts,
            tuple(pltpu.VMEM((n, q_rows * head_dim), BF16) for n in SEQ_GROUPS),
            chunked, chunked, chunked, chunked, chunked, chunked,
            dma((W_PARTS,)), dma((chip_groups,)), dma((ATT_SLOTS,)), dma((ATT_SLOTS,)),
            dma((2 * groups,)), dma((2 * groups,)), dma((2 * groups,)),
            dma((2 * groups,)), dma((2 * groups,)),
            dma((2 * len(PIECES),)), dma((2 * len(PIECES),)),
            dma((chip_groups,)), dma((chip_groups,)),
            *[dma((total,))] * 8,
            dma((4, total)),
        ],
        compiler_params=pltpu.CompilerParams(collective_id=1, has_side_effects=True, vmem_limit_bytes=62 << 20),
        name="finish",
    )(seq_lens, half, sinks, hidden, b_o.reshape(width // head_dim, head_dim), w_o, k_rows, v_rows)


LAST_PARTS = 8
LAST_UNROLL = 8


def last_kernel(lens_hbm, y_hbm, new_hbm, k_in, v_in, y_out, k_out, v_out, lens_ref, lens_sem, y_buf, new_ref, in_sem, out_sem, new_sem, k_sem, v_sem):
    num_seqs, ctx_local = k_out.shape[:2]
    base = lax.axis_index("sp") * ctx_local
    rows = y_hbm.shape[0] // LAST_PARTS
    new_copy = pltpu.make_async_copy(new_hbm, new_ref, new_sem)
    new_copy.start()
    lens_copy = pltpu.make_async_copy(lens_hbm, lens_ref, lens_sem)
    lens_copy.start()
    loads, stores = [], []
    for p in range(LAST_PARTS):
        at = pl.ds(p * rows, rows)
        loads.append(pltpu.make_async_copy(y_hbm.at[at], y_buf.at[at], in_sem.at[p]))
        stores.append(pltpu.make_async_copy(y_buf.at[at], y_out.at[at], out_sem.at[p]))
        loads[-1].start()

    def for_new_rows(act):
        def step(i, _):
            for b in (i * LAST_UNROLL + r for r in range(LAST_UNROLL)):
                n = lens_ref[b] - base

                @pl.when(jnp.logical_and(n >= 0, n < ctx_local))
                def _():
                    act(pltpu.make_async_copy(new_ref.at[0, b], k_out.at[b, n], k_sem))
                    act(pltpu.make_async_copy(new_ref.at[1, b], v_out.at[b, n], v_sem))

            return 0

        lax.fori_loop(0, num_seqs // LAST_UNROLL, step, 0)

    lens_copy.wait()
    new_copy.wait()
    for_new_rows(lambda c: c.start())
    for p in range(LAST_PARTS):
        loads[p].wait()
        stores[p].start()
    for_new_rows(lambda c: c.wait())
    for c in stores:
        c.wait()


def last(seq_lens, y, new, k_copy, v_copy):
    anyspace = pl.BlockSpec(memory_space=pl.ANY)
    dma = pltpu.SemaphoreType.DMA
    return pl.pallas_call(
        last_kernel,
        out_shape=[jax.ShapeDtypeStruct(a.shape, a.dtype) for a in (y, k_copy, v_copy)],
        in_specs=[anyspace] * 5,
        out_specs=[anyspace] * 3,
        scratch_shapes=[pltpu.SMEM(seq_lens.shape, jnp.int32), dma, pltpu.VMEM(y.shape, y.dtype), pltpu.VMEM(new.shape, new.dtype), dma((LAST_PARTS,)), dma((LAST_PARTS,)), dma, dma, dma],
        input_output_aliases={3: 1, 4: 2},
        compiler_params=pltpu.CompilerParams(vmem_limit_bytes=60 << 20),
        name="last",
    )(seq_lens, y, new, k_copy, v_copy)


def solution(mesh):
    cache_spec = P("dp", "sp", "tp", None)

    def block_step(hidden, seq_lens, rope_cos, rope_sin, k_cache, v_cache, norm_gain, w_qkv, b_qkv, sink_logits, w_o, b_o):
        num_seqs, ctx_local, kv_local, head_dim = k_cache.shape
        rows = (num_seqs, ctx_local * kv_local, head_dim)
        k_rows, v_rows = k_cache.reshape(rows), v_cache.reshape(rows)
        half, k_copy, v_copy = project(hidden, rope_cos, rope_sin, norm_gain, w_qkv, b_qkv, k_rows, v_rows)
        sinks = sink_logits.reshape(1, sink_logits.shape[0])
        y, new = finish(seq_lens, half, sinks, hidden, b_o, w_o, k_rows, v_rows)
        return last(seq_lens, y, new, k_copy.reshape(k_cache.shape), v_copy.reshape(v_cache.shape))

    return jax.shard_map(block_step, mesh=mesh, in_specs=(P("dp", None), P("dp"), P("dp", None), P("dp", None), cache_spec, cache_spec, P(None), P(None, "tp", None), P("tp", None), P("tp"), P("tp", None), P(None)), out_specs=(P("dp", None), cache_spec, cache_spec), check_vma=False)
```

```python
import functools

import jax
import jax.numpy as jnp
from jax import lax
from jax.experimental import pallas as pl
from jax.experimental.pallas import tpu as pltpu
from jax.sharding import PartitionSpec as P

NORM_EPS = 1e-5
F32 = jnp.float32
BF16 = jnp.bfloat16
MESH = pl.DeviceIdType.MESH


def sp_place():
    sp = lax.axis_index("sp")
    return lax.div(sp, 2), lax.rem(sp, 2)


def remote(src, dst, send_sem, recv_sem, where):
    return pltpu.make_async_remote_copy(src_ref=src, dst_ref=dst, send_sem=send_sem, recv_sem=recv_sem, device_id=where, device_id_type=MESH)


def sink_column(row_ref, count, halves, group):
    row = lax.broadcasted_iota(jnp.int32, (count, count), 0)
    per_half = count // halves
    part = group // halves
    head = lax.div(lax.rem(row, per_half), part) * group + lax.div(row, per_half) * part + lax.rem(row, part)
    same = head == lax.broadcasted_iota(jnp.int32, (count, count), 1)
    return jnp.sum(jnp.where(same, jnp.broadcast_to(row_ref[...], (count, count)), 0.0), axis=1, keepdims=True)


QKV_ROWS = 1024
QKV_SLOTS = 3
CACHE_SEQS = 16
CACHE_AHEAD = 2
CACHE_FIRST = 0
X_PARTS = 4


def project_kernel(x_hbm, gain_hbm, cos_hbm, sin_hbm, bias_hbm, w_ref, k_ref, v_ref, out_ref, k_out, v_out,
                   x_ref, gain_ref, cos_ref, sin_ref, bias_ref, x_sem, small_sem, normed, gain, heads, acc_q, acc_e, wq_buf, we_buf, k_buf, v_buf, wq_sem, we_sem, out_sem, k_in, v_in, k_back, v_back):
    _, core = sp_place()
    num_seqs, depth = x_ref.shape
    head_dim = acc_e.shape[2]
    q_cols = acc_q.shape[2]
    kv_local = acc_q.shape[0]
    per_core = q_cols // head_dim
    group = 2 * per_core
    steps = depth // QKV_ROWS
    x_rows = num_seqs // X_PARTS
    blocks = num_seqs // CACHE_SEQS

    def fetch(step, slot):
        rows = pl.ds(step * QKV_ROWS, QKV_ROWS)
        cq = pltpu.make_async_copy(w_ref.at[rows, :, pl.ds(pl.multiple_of(core * q_cols, 128), q_cols)], wq_buf.at[slot], wq_sem.at[slot])
        ce = pltpu.make_async_copy(w_ref.at[rows, :, pl.ds(pl.multiple_of((group + core) * head_dim, 128), head_dim)], we_buf.at[slot], we_sem.at[slot])
        return cq, ce

    def cache_in(i):
        at = pl.ds(i * CACHE_SEQS, CACHE_SEQS)
        return pltpu.make_async_copy(k_ref.at[at], k_buf.at[at], k_in.at[i]), pltpu.make_async_copy(v_ref.at[at], v_buf.at[at], v_in.at[i])

    def cache_back(i):
        at = pl.ds(i * CACHE_SEQS, CACHE_SEQS)
        return pltpu.make_async_copy(k_buf.at[at], k_out.at[at], k_back.at[i]), pltpu.make_async_copy(v_buf.at[at], v_out.at[at], v_back.at[i])

    small = [pltpu.make_async_copy(src, dst, small_sem.at[i]) for i, (src, dst) in enumerate(((gain_hbm, gain_ref), (cos_hbm, cos_ref), (sin_hbm, sin_ref), (bias_hbm, bias_ref)))]
    small[0].start()
    x_copies = []
    for p in range(X_PARTS):
        at = pl.ds(p * x_rows, x_rows)
        x_copies.append(pltpu.make_async_copy(x_hbm.at[at], x_ref.at[at], x_sem.at[p]))
        x_copies[-1].start()
    for c in fetch(0, 0):
        c.start()
    for i in range(CACHE_FIRST):
        for c in cache_in(i):
            c.start()
    for s in range(1, QKV_SLOTS - 1):
        for c in fetch(s, s):
            c.start()
    for i in range(CACHE_FIRST, CACHE_AHEAD):
        for c in cache_in(i):
            c.start()
    for c in small[1:]:
        c.start()

    small[0].wait()
    gain[...] = gain_ref[...].astype(F32)

    def norm_rows(r, _):
        rows = pl.ds(pl.multiple_of(r * 16, 16), 16)
        xw = x_ref[rows, :].astype(F32)
        inv = lax.rsqrt(jnp.mean(xw * xw, axis=-1, keepdims=True) + NORM_EPS)
        for t in range(depth // head_dim):
            cols = slice(t * head_dim, (t + 1) * head_dim)
            normed[rows, cols] = (xw[:, cols] * inv * gain[t : t + 1, :]).astype(BF16)
        return 0

    for p in range(X_PARTS):
        x_copies[p].wait()
        lax.fori_loop(p * x_rows // 16, (p + 1) * x_rows // 16, norm_rows, 0)
    for i in range(CACHE_FIRST):
        for c in cache_in(i):
            c.wait()
        for c in cache_back(i):
            c.start()
    acc_q[...] = jnp.zeros_like(acc_q)
    acc_e[...] = jnp.zeros_like(acc_e)

    def step_fn(step, _):
        slot = lax.rem(step, QKV_SLOTS)

        @pl.when(step + CACHE_AHEAD < blocks)
        def _():
            for c in cache_in(step + CACHE_AHEAD):
                c.start()

        for c in fetch(step, slot):
            c.wait()

        @pl.when(step + QKV_SLOTS - 1 < steps)
        def _():
            for c in fetch(step + QKV_SLOTS - 1, lax.rem(step + QKV_SLOTS - 1, QKV_SLOTS)):
                c.start()

        @pl.when(step + CACHE_FIRST < blocks)
        def _():
            for c in cache_in(step + CACHE_FIRST):
                c.wait()
            for c in cache_back(step + CACHE_FIRST):
                c.start()

        h = normed[:, pl.ds(pl.multiple_of(step * QKV_ROWS, 128), QKV_ROWS)]
        wq = jnp.swapaxes(wq_buf[slot], 0, 1)
        we = jnp.swapaxes(we_buf[slot], 0, 1)
        for k in range(kv_local):
            acc_q[k] += jnp.dot(h, wq[k], preferred_element_type=F32)
            acc_e[k] += jnp.dot(h, we[k], preferred_element_type=F32)
        return 0

    lax.fori_loop(0, steps, step_fn, 0)

    for c in small[1:]:
        c.wait()
    cos_t = cos_ref[...].T
    sin_t = sin_ref[...].T
    cos2 = jnp.concatenate([cos_t, cos_t], axis=1)
    sin2 = jnp.concatenate([-sin_t, sin_t], axis=1)
    is_key = core == 0
    cos_e = jnp.where(is_key, cos2, jnp.ones_like(cos2))
    sin_e = jnp.where(is_key, sin2, jnp.zeros_like(sin2))

    def rotate(v, c, s):
        r = v * c + pltpu.roll(v, head_dim // 2, 1) * s
        return r.astype(BF16).astype(F32)

    for k in range(kv_local):
        bias_q = bias_ref[k : k + 1, pl.ds(pl.multiple_of(core * q_cols, 128), q_cols)].astype(F32)
        for g in range(per_core):
            cols = slice(g * head_dim, (g + 1) * head_dim)
            heads[k * per_core + g] = rotate(acc_q[k, :, cols] + bias_q[:, cols], cos2, sin2)
        bias_e = bias_ref[k : k + 1, pl.ds(pl.multiple_of((group + core) * head_dim, 128), head_dim)].astype(F32)
        heads[kv_local * per_core + k] = rotate(acc_e[k] + bias_e, cos_e, sin_e)
    done = []
    for k in range(kv_local + 1):
        part = pl.ds(k * per_core, per_core)
        done.append(pltpu.make_async_copy(heads.at[part], out_ref.at[part], out_sem.at[k]))
        done[-1].start()
    for i in range(blocks):
        for c in cache_back(i):
            c.wait()
    for c in done:
        c.wait()


def project(hidden, rope_cos, rope_sin, norm_gain, w_qkv, b_qkv, k_rows, v_rows):
    num_seqs, depth = hidden.shape
    head_dim = k_rows.shape[2]
    kv_local = w_qkv.shape[1]
    per_core = (w_qkv.shape[2] // head_dim - 2) // 2
    rows = kv_local * (per_core + 1)
    blocks = num_seqs // CACHE_SEQS
    assert blocks <= depth // QKV_ROWS + CACHE_FIRST
    anyspace = pl.BlockSpec(memory_space=pl.ANY)
    dma = pltpu.SemaphoreType.DMA
    return pl.pallas_call(
        project_kernel,
        out_shape=[
            jax.ShapeDtypeStruct((rows, num_seqs, head_dim), F32),
            jax.ShapeDtypeStruct(k_rows.shape, BF16),
            jax.ShapeDtypeStruct(v_rows.shape, BF16),
        ],
        in_specs=[anyspace] * 8,
        out_specs=[anyspace] * 3,
        scratch_shapes=[
            pltpu.VMEM((num_seqs, depth), BF16),
            pltpu.VMEM((depth // head_dim, head_dim), BF16),
            pltpu.VMEM((head_dim // 2, num_seqs), F32),
            pltpu.VMEM((head_dim // 2, num_seqs), F32),
            pltpu.VMEM(b_qkv.shape, BF16),
            dma((X_PARTS,)),
            dma((4,)),
            pltpu.VMEM((num_seqs, depth), BF16),
            pltpu.VMEM((depth // head_dim, head_dim), F32),
            pltpu.VMEM((rows, num_seqs, head_dim), F32),
            pltpu.VMEM((kv_local, num_seqs, per_core * head_dim), F32),
            pltpu.VMEM((kv_local, num_seqs, head_dim), F32),
            pltpu.VMEM((QKV_SLOTS, QKV_ROWS, kv_local, per_core * head_dim), BF16),
            pltpu.VMEM((QKV_SLOTS, QKV_ROWS, kv_local, head_dim), BF16),
            pltpu.VMEM(k_rows.shape, BF16),
            pltpu.VMEM(v_rows.shape, BF16),
            dma((QKV_SLOTS,)), dma((QKV_SLOTS,)), dma((kv_local + 1,)),
            dma((blocks,)), dma((blocks,)), dma((blocks,)), dma((blocks,)),
        ],
        compiler_params=pltpu.CompilerParams(vmem_limit_bytes=60 << 20),
        name="project",
    )(hidden, norm_gain.reshape(depth // head_dim, head_dim), rope_cos.T, rope_sin.T, b_qkv, w_qkv, k_rows, v_rows)


ATT_SEQS = 8
ATT_SLOTS = 6
OUT_COLS = 512
SEQ_GROUPS = (24, 40)
PIECES = ((0, 0, 8), (0, 8, 16), (1, 0, 40))
W_PARTS = 8
LAG_Y = 3
LAG_X = 3
LAG_P = 1


def finish_kernel(lens_hbm, half_hbm, sink_hbm, hid_ref, bo_hbm, wo_ref, k_hbm, v_hbm, y_out, new_ref,
                  lens_ref, sink_ref, bo_ref, small_sem, y_parts, w_buf, x_buf, h_buf, k_ring, v_ring, num, ml, sink_col, bo_f32, r1, r1ml, own, own_ml, away, away_ml, r2, r2ml, o_buf, r3, o_all,
                  y_send, y_recv, z_buf, x_recv, p1, p2,
                  w_sem, x_sem, k_sem, v_sem, h_in, h_send, h_recv, s1_send, s1_recv, s2_send, s2_recv, s3_send, s3_recv,
                  y_ss, y_rs, x_ss, x_rs, p1_ss, p1_rs, p2_ss, p2_rs, o_sem):
    chip, core = sp_place()
    tp = lax.axis_index("tp")
    partner = {"sp": 2 * chip + (1 - core)}
    across_x = {"sp": 2 * (1 - chip) + core}
    across_y = {"tp": 1 - tp}
    q_rows, _, head_dim = num[0].shape
    chip_groups = len(SEQ_GROUPS)
    offsets = [sum(SEQ_GROUPS[:g]) for g in range(chip_groups)]
    num_seqs = h_buf.shape[1]
    kv_local = (h_buf.shape[0] - q_rows) // 2
    rows = k_ring.shape[2]
    ctx_local = rows // kv_local
    half_h = q_rows // 2
    half_s = num_seqs // 2
    part_h = half_h // kv_local
    cols = w_buf.shape[1]
    chunks = cols // OUT_COLS
    total = chip_groups * chunks
    mine = pl.multiple_of(core * half_h, half_h)
    theirs = pl.multiple_of((1 - core) * half_h, half_h)

    def seqs(which, g, first=0, count=None):
        return pl.ds(pl.multiple_of(which * half_s + offsets[g] + first, 8), SEQ_GROUPS[g] if count is None else count)

    small = [pltpu.make_async_copy(src, dst, small_sem.at[i]) for i, (src, dst) in enumerate(((lens_hbm, lens_ref), (sink_hbm, sink_ref), (bo_hbm, bo_ref)))]
    for c in small:
        c.start()
    barrier = pltpu.get_barrier_semaphore()
    for peer in (partner, across_x, across_y):
        pl.semaphore_signal(barrier, inc=1, device_id=peer, device_id_type=MESH)

    order = [(1 - chip, *piece) for piece in PIECES] + [(chip, g, 0, n) for g, n in enumerate(SEQ_GROUPS)]
    own_rows = (pl.ds(mine, half_h), pl.ds(pl.multiple_of(q_rows + kv_local * core, kv_local), kv_local))
    src_rows = (pl.ds(0, half_h), pl.ds(half_h, kv_local))
    h_local, h_remote = [], []
    for i, piece in enumerate(order):
        at = seqs(*piece)
        for j in range(2):
            h_local.append(pltpu.make_async_copy(half_hbm.at[src_rows[j], at], h_buf.at[own_rows[j], at], h_in.at[2 * i + j]))
            h_local[-1].start()
            h_remote.append(remote(half_hbm.at[src_rows[j], at], h_buf.at[own_rows[j], at], h_send.at[2 * i + j], h_recv.at[2 * i + j], partner))

    steps = num_seqs // ATT_SEQS
    counts = [n // ATT_SEQS for _, _, _, n in order]
    starts = [sum(counts[:i]) for i in range(len(counts))]

    def block(p):
        return lax.rem(p + (1 - chip) * (steps // 2), steps) * ATT_SEQS

    def kv_load(p):
        at = pl.ds(pl.multiple_of(block(p), ATT_SEQS), ATT_SEQS)
        slot = lax.rem(p, ATT_SLOTS)
        return pltpu.make_async_copy(k_hbm.at[at], k_ring.at[slot], k_sem.at[slot]), pltpu.make_async_copy(v_hbm.at[at], v_ring.at[slot], v_sem.at[slot])

    for p in range(ATT_SLOTS):
        for c in kv_load(p):
            c.start()
    my_cols = pl.ds(pl.multiple_of(core * cols, 128), cols)
    x_in = [pltpu.make_async_copy(hid_ref.at[seqs(chip, g), my_cols], x_buf[g], x_sem.at[g]) for g in range(chip_groups)]
    w_cols = cols // W_PARTS
    w_chunks = w_cols // OUT_COLS

    def w_copy(p):
        return pltpu.make_async_copy(wo_ref.at[:, pl.ds(pl.multiple_of(core * cols + p * w_cols, 128), w_cols)], w_buf.at[:, pl.ds(pl.multiple_of(p * w_cols, 128), w_cols)], w_sem.at[p])

    w_copy(0).start()
    w_copy(1).start()
    for c in small:
        c.wait()
    sink = sink_column(sink_ref, q_rows, 2, 2 * part_h)
    sink_col[...] = jnp.broadcast_to(sink, sink_col.shape)
    bo_f32[...] = bo_ref[...].astype(F32)
    pl.semaphore_wait(barrier, 3)
    for c in h_remote:
        c.start()

    base = lax.axis_index("sp") * ctx_local
    scale = head_dim**-0.5
    col = lax.broadcasted_iota(jnp.int32, (q_rows, rows), 1)
    kv_row = lax.div(lax.rem(lax.broadcasted_iota(jnp.int32, (q_rows, rows), 0), half_h), part_h)
    col_pos = jnp.where(lax.rem(col, kv_local) == kv_row, lax.div(col, kv_local), ctx_local * 1024)
    lane = lax.broadcasted_iota(jnp.int32, (q_rows, ml.shape[2]), 1)
    batch = range(ATT_SEQS)
    over_d = (((1,), (1,)), ((), ()))
    new_code = jnp.where(lax.broadcasted_iota(jnp.int32, (q_rows, 16), 1) == lax.div(lax.rem(lax.broadcasted_iota(jnp.int32, (q_rows, 16), 0), half_h), part_h), 1, 2)

    def attend(i, first, last, carry):
        def step_fn(t, carry):
            m_all, l_all = carry
            p = starts[i] + t
            slot = lax.rem(p, ATT_SLOTS)
            for c in kv_load(p):
                c.wait()
            start = block(p)
            heads = h_buf.at[:, pl.ds(pl.multiple_of(start, ATT_SEQS), ATT_SEQS)]
            rel = [lens_ref[start + s] - base for s in batch]
            inside = [jnp.where(jnp.logical_and(r >= 0, r < ctx_local), 1, 0) for r in rel]
            queries = [heads[0:q_rows, s, :].astype(BF16) for s in batch]
            new_k, new_v = ([jnp.concatenate([heads[lo : lo + kv_local, s, :]] * (16 // kv_local), axis=0).astype(BF16) for s in batch] for lo in (q_rows, q_rows + kv_local))
            logits = [lax.dot_general(queries[s], k_ring[slot, s], over_d, preferred_element_type=F32) for s in batch]
            extra = [lax.dot_general(queries[s], new_k[s], over_d, preferred_element_type=F32) for s in batch]
            logits = [jnp.where(col_pos < rel[s], logits[s] * scale, -jnp.inf) for s in batch]
            extra = [jnp.where(new_code == inside[s], extra[s] * scale, -jnp.inf) for s in batch]
            tops = [jnp.maximum(jnp.maximum(jnp.max(logits[s], axis=1, keepdims=True), jnp.max(extra[s], axis=1, keepdims=True)), sink) for s in batch]
            weights = [jnp.exp(logits[s] - tops[s]) for s in batch]
            extra = [jnp.exp(extra[s] - tops[s]) for s in batch]
            totals = [jnp.sum(weights[s], axis=1, keepdims=True) + jnp.sum(extra[s], axis=1, keepdims=True) for s in batch]
            sums = [jnp.dot(weights[s].astype(BF16), v_ring[slot, s], preferred_element_type=F32) for s in batch]
            sums = [sums[s] + jnp.dot(extra[s].astype(BF16), new_v[s], preferred_element_type=F32) for s in batch]
            out = num[i].at[:, pl.ds(pl.multiple_of(t * ATT_SEQS, ATT_SEQS), ATT_SEQS)]
            for s in batch:
                here = lane == order[i][2] + t * ATT_SEQS + s
                m_all = jnp.where(here, tops[s], m_all)
                l_all = jnp.where(here, totals[s], l_all)
                out[:, s, :] = sums[s]
            for s in batch:
                for j in range(2):
                    new_ref[j, start + s] = heads[q_rows + j * kv_local : q_rows + (j + 1) * kv_local, s, :].astype(BF16)

            @pl.when(p + ATT_SLOTS < steps)
            def _():
                for c in kv_load(p + ATT_SLOTS):
                    c.start()

            return m_all, l_all

        return lax.fori_loop(first, last, step_fn, carry)

    def heads_wait(i):
        for j in range(2):
            h_local[2 * i + j].wait()
            h_remote[2 * i + j].wait_recv()

    zero = jnp.zeros((q_rows, ml.shape[2]), F32)
    c1 = []

    def to_partner(i, carry):
        ml[i, 0:q_rows] = carry[0]
        ml[i, q_rows : 2 * q_rows] = carry[1]
        c1.append((
            remote(ml.at[i], r1ml.at[i], s1_send.at[2 * i], s1_recv.at[2 * i], partner),
            remote(num[i].at[pl.ds(theirs, half_h)], r1[i], s1_send.at[2 * i + 1], s1_recv.at[2 * i + 1], partner),
        ))
        for c in c1[-1]:
            c.start()

    def combine(i, dst, dst_ml):
        for c in c1[i]:
            c.wait_recv()
        m_a, l_a = ml[i, pl.ds(mine, half_h)], ml[i, pl.ds(q_rows + mine, half_h)]
        m_b, l_b = r1ml[i, pl.ds(mine, half_h)], r1ml[i, pl.ds(q_rows + mine, half_h)]
        m_chip = jnp.maximum(m_a, m_b)
        f_a = jnp.exp(m_a - m_chip)
        f_b = jnp.exp(m_b - m_chip)
        dst_ml[0:half_h] = m_chip
        dst_ml[half_h : 2 * half_h] = l_a * f_a + l_b * f_b
        f_a, f_b = f_a.T, f_b.T
        some = slice(order[i][2], order[i][2] + order[i][3])
        for h in range(half_h):
            dst[h, some] = num[i][mine + h] * f_a[some, h : h + 1] + r1[i][h] * f_b[some, h : h + 1]

    c2 = []

    def across(i):
        _, g, first, count = order[i]
        combine(i, away[g], away_ml.at[i])
        at = pl.ds(first, count)
        c2.append((
            remote(away_ml.at[i], r2ml.at[i], s2_send.at[2 * i], s2_recv.at[2 * i], across_x),
            remote(away[g].at[:, at], r2[g].at[:, at], s2_send.at[2 * i + 1], s2_recv.at[2 * i + 1], across_x),
        ))
        for c in c2[-1]:
            c.start()

    width = half_h * head_dim
    part_w = part_h * head_dim

    def o_place(which_half, k):
        return pl.ds(pl.multiple_of(2 * k * part_w + which_half * part_w, 128), part_w)

    def heads_start(g):
        m_a, l_a = own_ml[g, 0:half_h], own_ml[g, half_h : 2 * half_h]
        m_b, l_b = None, None
        for i, (group, first, _) in enumerate(PIECES):
            if group == g:
                for c in c2[i]:
                    c.wait_recv()
                m_i, l_i = r2ml[i, 0:half_h], r2ml[i, half_h : 2 * half_h]
                if m_b is None:
                    m_b, l_b = m_i, l_i
                else:
                    m_b = jnp.where(lane[0:half_h] < first, m_b, m_i)
                    l_b = jnp.where(lane[0:half_h] < first, l_b, l_i)
        m_top = jnp.maximum(m_a, m_b)
        f_a = jnp.exp(m_a - m_top)
        f_b = jnp.exp(m_b - m_top)
        den = l_a * f_a + l_b * f_b + jnp.exp(sink_col[pl.ds(mine, half_h)] - m_top)
        f_a, f_b = (f_a / den).T, (f_b / den).T
        for h in range(half_h):
            o_buf[g][:, h * head_dim : (h + 1) * head_dim] = own[g][h] * f_a[0 : SEQ_GROUPS[g], h : h + 1] + r2[g][h] * f_b[0 : SEQ_GROUPS[g], h : h + 1]
        c = remote(o_buf[g], r3[g], s3_send.at[g], s3_recv.at[g], partner)
        c.start()
        for k in range(kv_local):
            o_all[g][:, o_place(core, k)] = o_buf[g][:, k * part_w : (k + 1) * part_w].astype(BF16)
        return c

    def heads_end(g, c):
        c.wait_recv()
        for k in range(kv_local):
            o_all[g][:, o_place(1 - core, k)] = r3[g][:, k * part_w : (k + 1) * part_w].astype(BF16)

    def y_copy(g, j):
        t = g * chunks + j
        return remote(y_send[g].at[j], y_recv[g].at[j], y_ss.at[t], y_rs.at[t], across_y)

    def x_copy(g, j):
        t = g * chunks + j
        return remote(z_buf[g].at[j], x_recv[g].at[j], x_ss.at[t], x_rs.at[t], across_x)

    def p1_copy(g, j):
        t = g * chunks + j
        return remote(z_buf[g].at[j], p1[g].at[j], p1_ss.at[t], p1_rs.at[t], partner)

    def p2_copy(g, j):
        t = g * chunks + j
        return remote(x_recv[g].at[j], p2[g].at[j], p2_ss.at[t], p2_rs.at[t], partner)

    def out_copy(kind, g, j):
        which_seqs, which_cols = ((chip, core), (1 - chip, core), (chip, 1 - core), (1 - chip, 1 - core))[kind]
        cols_at = pl.ds(pl.multiple_of(which_cols * cols + j * OUT_COLS, 128), OUT_COLS)
        return pltpu.make_async_copy(y_parts[g].at[kind, j], y_out.at[seqs(which_seqs, g), cols_at], o_sem.at[kind, g * chunks + j])

    def put_out(kind, g, j, value):
        y_parts[g][kind, j] = value
        out_copy(kind, g, j).start()

    def multiply(g, j):
        if g == 0:
            @pl.when(lax.rem(j, w_chunks) == 0)
            def _():
                w_copy(lax.div(j, w_chunks)).wait()

        w = w_buf[:, pl.ds(pl.multiple_of(j * OUT_COLS, 128), OUT_COLS)]
        y_send[g][j] = jnp.dot(o_all[g][...], w, preferred_element_type=F32)
        y_copy(g, j).start()

    def add(g, j):
        y_copy(g, j).wait_recv()
        x_part = x_buf[g][:, pl.ds(pl.multiple_of(j * OUT_COLS, 128), OUT_COLS)].astype(F32)
        row = (core * cols + j * OUT_COLS) // head_dim
        bias = jnp.concatenate([bo_f32[pl.ds(row + i, 1), :] for i in range(OUT_COLS // head_dim)], axis=1)
        z = (x_part + (y_send[g][j] + y_recv[g][j]) + bias).astype(BF16)
        z_buf[g][j] = z.astype(F32)
        x_copy(g, j).start()
        p1_copy(g, j).start()
        put_out(0, g, j, z)

    def spread(g, j):
        x_copy(g, j).wait_recv()
        p2_copy(g, j).start()
        put_out(1, g, j, x_recv[g][j].astype(BF16))
        p1_copy(g, j).wait_recv()
        put_out(2, g, j, p1[g][j].astype(BF16))

    def receive(g, j):
        p2_copy(g, j).wait_recv()
        put_out(3, g, j, p2[g][j].astype(BF16))

    def body(t, _):
        for stage, lag in ((multiply, 0), (add, LAG_Y), (spread, LAG_Y + LAG_X), (receive, LAG_Y + LAG_X + LAG_P)):
            for g in range(chip_groups):
                j = t - lag - g * chunks

                @pl.when(jnp.logical_and(j >= 0, j < chunks))
                def _():
                    stage(g, j)

        return 0

    heads_wait(0)
    to_partner(0, attend(0, 0, counts[0], (zero, zero)))
    heads_wait(1)
    to_partner(1, attend(1, 0, counts[1], (zero, zero)))
    across(0)
    w_copy(2).start()
    heads_wait(2)
    carry = attend(2, 0, 2, (zero, zero))
    across(1)
    for c in x_in:
        c.start()
    w_copy(3).start()
    to_partner(2, attend(2, 2, counts[2], carry))
    w_copy(4).start()
    heads_wait(3)
    carry = attend(3, 0, counts[3], (zero, zero))
    across(2)
    for p in range(5, W_PARTS):
        w_copy(p).start()
    to_partner(3, carry)
    heads_wait(4)
    to_partner(4, attend(4, 0, counts[4], (zero, zero)))
    combine(3, own[0], own_ml.at[0])
    combine(4, own[1], own_ml.at[1])

    c3 = [heads_start(0)]
    heads_end(0, c3[0])
    for c in x_in:
        c.wait()
    lax.fori_loop(0, chunks - 3, body, 0)
    c3.append(heads_start(1))
    lax.fori_loop(chunks - 3, chunks - 1, body, 0)
    heads_end(1, c3[1])
    lax.fori_loop(chunks - 1, total + LAG_Y + LAG_X + LAG_P, body, 0)

    for g in range(chip_groups):
        def tail(j, _):
            for copy in (y_copy, x_copy, p1_copy, p2_copy):
                copy(g, j).wait_send()
            for kind in range(4):
                out_copy(kind, g, j).wait()
            return 0

        lax.fori_loop(0, chunks, tail, 0)
    for c in (*h_remote, *(c for pair in c1 + c2 for c in pair), *c3):
        c.wait_send()


def finish(seq_lens, half, sinks, hidden, b_o, w_o, k_rows, v_rows):
    num_seqs, rows, head_dim = k_rows.shape
    q_rows = sinks.shape[1]
    half_h, half_s = q_rows // 2, num_seqs // 2
    kv_local = half.shape[0] - half_h
    assert sum(SEQ_GROUPS) == half_s
    order = tuple(n for _, _, n in PIECES) + SEQ_GROUPS
    chip_groups, groups = len(SEQ_GROUPS), len(order)
    width = w_o.shape[1]
    cols = width // 2
    chunks = cols // OUT_COLS
    total = chip_groups * chunks
    vmem = pl.BlockSpec(memory_space=pltpu.VMEM)
    anyspace = pl.BlockSpec(memory_space=pl.ANY)
    chunked = tuple(pltpu.VMEM((chunks, n, OUT_COLS), F32) for n in SEQ_GROUPS)
    parts = tuple(pltpu.VMEM((half_h, n, head_dim), F32) for n in SEQ_GROUPS)
    own_ml = pltpu.VMEM((chip_groups, 2 * half_h, 128), F32)
    piece_ml = pltpu.VMEM((len(PIECES), 2 * half_h, 128), F32)
    o_parts = tuple(pltpu.VMEM((n, half_h * head_dim), F32) for n in SEQ_GROUPS)
    ring = pltpu.VMEM((ATT_SLOTS, ATT_SEQS, rows, head_dim), BF16)
    dma = pltpu.SemaphoreType.DMA
    return pl.pallas_call(
        finish_kernel,
        out_shape=[
            jax.ShapeDtypeStruct((num_seqs, width), BF16),
            jax.ShapeDtypeStruct((2, num_seqs, kv_local, head_dim), BF16),
        ],
        in_specs=[anyspace] * 8,
        out_specs=[anyspace, vmem],
        scratch_shapes=[
            pltpu.SMEM((num_seqs,), jnp.int32),
            pltpu.VMEM((1, q_rows), F32),
            pltpu.VMEM((width // head_dim, head_dim), BF16),
            dma((3,)),
            tuple(pltpu.VMEM((4, chunks, n, OUT_COLS), BF16) for n in SEQ_GROUPS),
            pltpu.VMEM((w_o.shape[0], cols), BF16),
            tuple(pltpu.VMEM((n, cols), BF16) for n in SEQ_GROUPS),
            pltpu.VMEM((q_rows + 2 * kv_local, num_seqs, head_dim), F32),
            ring, ring,
            tuple(pltpu.VMEM((q_rows, n, head_dim), F32) for n in order),
            pltpu.VMEM((groups, 2 * q_rows, 128), F32),
            pltpu.VMEM((q_rows, 128), F32),
            pltpu.VMEM((width // head_dim, head_dim), F32),
            tuple(pltpu.VMEM((half_h, n, head_dim), F32) for n in order),
            pltpu.VMEM((groups, 2 * q_rows, 128), F32),
            parts, own_ml, parts, piece_ml, parts, piece_ml,
            o_parts, o_parts,
            tuple(pltpu.VMEM((n, q_rows * head_dim), BF16) for n in SEQ_GROUPS),
            chunked, chunked, chunked, chunked, chunked, chunked,
            dma((W_PARTS,)), dma((chip_groups,)), dma((ATT_SLOTS,)), dma((ATT_SLOTS,)),
            dma((2 * groups,)), dma((2 * groups,)), dma((2 * groups,)),
            dma((2 * groups,)), dma((2 * groups,)),
            dma((2 * len(PIECES),)), dma((2 * len(PIECES),)),
            dma((chip_groups,)), dma((chip_groups,)),
            *[dma((total,))] * 8,
            dma((4, total)),
        ],
        compiler_params=pltpu.CompilerParams(collective_id=1, has_side_effects=True, vmem_limit_bytes=62 << 20),
        name="finish",
    )(seq_lens, half, sinks, hidden, b_o.reshape(width // head_dim, head_dim), w_o, k_rows, v_rows)


LAST_PARTS = 8
LAST_UNROLL = 8


def last_kernel(lens_hbm, y_hbm, new_hbm, k_in, v_in, y_out, k_out, v_out, lens_ref, lens_sem, y_buf, new_ref, in_sem, out_sem, new_sem, k_sem, v_sem):
    num_seqs, ctx_local = k_out.shape[:2]
    base = lax.axis_index("sp") * ctx_local
    rows = y_hbm.shape[0] // LAST_PARTS
    new_copy = pltpu.make_async_copy(new_hbm, new_ref, new_sem)
    new_copy.start()
    lens_copy = pltpu.make_async_copy(lens_hbm, lens_ref, lens_sem)
    lens_copy.start()
    loads, stores = [], []
    for p in range(LAST_PARTS):
        at = pl.ds(p * rows, rows)
        loads.append(pltpu.make_async_copy(y_hbm.at[at], y_buf.at[at], in_sem.at[p]))
        stores.append(pltpu.make_async_copy(y_buf.at[at], y_out.at[at], out_sem.at[p]))
        loads[-1].start()

    def for_new_rows(act):
        def step(i, _):
            for b in (i * LAST_UNROLL + r for r in range(LAST_UNROLL)):
                n = lens_ref[b] - base

                @pl.when(jnp.logical_and(n >= 0, n < ctx_local))
                def _():
                    act(pltpu.make_async_copy(new_ref.at[0, b], k_out.at[b, n], k_sem))
                    act(pltpu.make_async_copy(new_ref.at[1, b], v_out.at[b, n], v_sem))

            return 0

        lax.fori_loop(0, num_seqs // LAST_UNROLL, step, 0)

    lens_copy.wait()
    new_copy.wait()
    for_new_rows(lambda c: c.start())
    for p in range(LAST_PARTS):
        loads[p].wait()
        stores[p].start()
    for_new_rows(lambda c: c.wait())
    for c in stores:
        c.wait()


def last(seq_lens, y, new, k_copy, v_copy):
    anyspace = pl.BlockSpec(memory_space=pl.ANY)
    dma = pltpu.SemaphoreType.DMA
    return pl.pallas_call(
        last_kernel,
        out_shape=[jax.ShapeDtypeStruct(a.shape, a.dtype) for a in (y, k_copy, v_copy)],
        in_specs=[anyspace] * 5,
        out_specs=[anyspace] * 3,
        scratch_shapes=[pltpu.SMEM(seq_lens.shape, jnp.int32), dma, pltpu.VMEM(y.shape, y.dtype), pltpu.VMEM(new.shape, new.dtype), dma((LAST_PARTS,)), dma((LAST_PARTS,)), dma, dma, dma],
        input_output_aliases={3: 1, 4: 2},
        compiler_params=pltpu.CompilerParams(vmem_limit_bytes=60 << 20),
        name="last",
    )(seq_lens, y, new, k_copy, v_copy)


def solution(mesh):
    cache_spec = P("dp", "sp", "tp", None)

    def block_step(hidden, seq_lens, rope_cos, rope_sin, k_cache, v_cache, norm_gain, w_qkv, b_qkv, sink_logits, w_o, b_o):
        num_seqs, ctx_local, kv_local, head_dim = k_cache.shape
        rows = (num_seqs, ctx_local * kv_local, head_dim)
        k_rows, v_rows = k_cache.reshape(rows), v_cache.reshape(rows)
        half, k_copy, v_copy = project(hidden, rope_cos, rope_sin, norm_gain, w_qkv, b_qkv, k_rows, v_rows)
        sinks = sink_logits.reshape(1, sink_logits.shape[0])
        y, new = finish(seq_lens, half, sinks, hidden, b_o, w_o, k_rows, v_rows)
        return last(seq_lens, y, new, k_copy.reshape(k_cache.shape), v_copy.reshape(v_cache.shape))

    return jax.shard_map(block_step, mesh=mesh, in_specs=(P("dp", None), P("dp"), P("dp", None), P("dp", None), cache_spec, cache_spec, P(None), P(None, "tp", None), P("tp", None), P("tp"), P("tp", None), P(None)), out_specs=(P("dp", None), cache_spec, cache_spec), check_vma=False)
```

```python
import functools

import jax
import jax.numpy as jnp
from jax import lax
from jax.experimental import pallas as pl
from jax.experimental.pallas import tpu as pltpu
from jax.sharding import PartitionSpec as P

NORM_EPS = 1e-5
F32 = jnp.float32
BF16 = jnp.bfloat16
MESH = pl.DeviceIdType.MESH


def sp_place():
    sp = lax.axis_index("sp")
    return lax.div(sp, 2), lax.rem(sp, 2)


def remote(src, dst, send_sem, recv_sem, where):
    return pltpu.make_async_remote_copy(src_ref=src, dst_ref=dst, send_sem=send_sem, recv_sem=recv_sem, device_id=where, device_id_type=MESH)


def sink_column(row_ref, count, halves, group):
    row = lax.broadcasted_iota(jnp.int32, (count, count), 0)
    per_half = count // halves
    part = group // halves
    head = lax.div(lax.rem(row, per_half), part) * group + lax.div(row, per_half) * part + lax.rem(row, part)
    same = head == lax.broadcasted_iota(jnp.int32, (count, count), 1)
    return jnp.sum(jnp.where(same, jnp.broadcast_to(row_ref[...], (count, count)), 0.0), axis=1, keepdims=True)


QKV_ROWS = 1024
QKV_SLOTS = 3
CACHE_SEQS = 16
CACHE_AHEAD = 2
CACHE_FIRST = 0
X_PARTS = 4


def project_kernel(x_hbm, gain_hbm, cos_hbm, sin_hbm, bias_hbm, w_ref, k_ref, v_ref, out_ref, k_out, v_out,
                   x_ref, gain_ref, cos_ref, sin_ref, bias_ref, x_sem, small_sem, normed, gain, heads, acc_q, acc_e, wq_buf, we_buf, k_buf, v_buf, wq_sem, we_sem, out_sem, k_in, v_in, k_back, v_back):
    _, core = sp_place()
    num_seqs, depth = x_ref.shape
    head_dim = acc_e.shape[2]
    q_cols = acc_q.shape[2]
    kv_local = acc_q.shape[0]
    per_core = q_cols // head_dim
    group = 2 * per_core
    steps = depth // QKV_ROWS
    x_rows = num_seqs // X_PARTS
    blocks = num_seqs // CACHE_SEQS

    def fetch(step, slot):
        rows = pl.ds(step * QKV_ROWS, QKV_ROWS)
        cq = pltpu.make_async_copy(w_ref.at[rows, :, pl.ds(pl.multiple_of(core * q_cols, 128), q_cols)], wq_buf.at[slot], wq_sem.at[slot])
        ce = pltpu.make_async_copy(w_ref.at[rows, :, pl.ds(pl.multiple_of((group + core) * head_dim, 128), head_dim)], we_buf.at[slot], we_sem.at[slot])
        return cq, ce

    def cache_in(i):
        at = pl.ds(i * CACHE_SEQS, CACHE_SEQS)
        return pltpu.make_async_copy(k_ref.at[at], k_buf.at[at], k_in.at[i]), pltpu.make_async_copy(v_ref.at[at], v_buf.at[at], v_in.at[i])

    def cache_back(i):
        at = pl.ds(i * CACHE_SEQS, CACHE_SEQS)
        return pltpu.make_async_copy(k_buf.at[at], k_out.at[at], k_back.at[i]), pltpu.make_async_copy(v_buf.at[at], v_out.at[at], v_back.at[i])

    small = [pltpu.make_async_copy(src, dst, small_sem.at[i]) for i, (src, dst) in enumerate(((gain_hbm, gain_ref), (cos_hbm, cos_ref), (sin_hbm, sin_ref), (bias_hbm, bias_ref)))]
    small[0].start()
    x_copies = []
    for p in range(X_PARTS):
        at = pl.ds(p * x_rows, x_rows)
        x_copies.append(pltpu.make_async_copy(x_hbm.at[at], x_ref.at[at], x_sem.at[p]))
        x_copies[-1].start()
    for c in fetch(0, 0):
        c.start()
    for i in range(CACHE_FIRST):
        for c in cache_in(i):
            c.start()
    for s in range(1, QKV_SLOTS - 1):
        for c in fetch(s, s):
            c.start()
    for i in range(CACHE_FIRST, CACHE_AHEAD):
        for c in cache_in(i):
            c.start()
    for c in small[1:]:
        c.start()

    small[0].wait()
    gain[...] = gain_ref[...].astype(F32)

    def norm_rows(r, _):
        rows = pl.ds(pl.multiple_of(r * 16, 16), 16)
        xw = x_ref[rows, :].astype(F32)
        inv = lax.rsqrt(jnp.mean(xw * xw, axis=-1, keepdims=True) + NORM_EPS)
        for t in range(depth // head_dim):
            cols = slice(t * head_dim, (t + 1) * head_dim)
            normed[rows, cols] = (xw[:, cols] * inv * gain[t : t + 1, :]).astype(BF16)
        return 0

    for p in range(X_PARTS):
        x_copies[p].wait()
        lax.fori_loop(p * x_rows // 16, (p + 1) * x_rows // 16, norm_rows, 0)
    for i in range(CACHE_FIRST):
        for c in cache_in(i):
            c.wait()
        for c in cache_back(i):
            c.start()
    acc_q[...] = jnp.zeros_like(acc_q)
    acc_e[...] = jnp.zeros_like(acc_e)

    def step_fn(step, _):
        slot = lax.rem(step, QKV_SLOTS)

        @pl.when(step + CACHE_AHEAD < blocks)
        def _():
            for c in cache_in(step + CACHE_AHEAD):
                c.start()

        for c in fetch(step, slot):
            c.wait()

        @pl.when(step + QKV_SLOTS - 1 < steps)
        def _():
            for c in fetch(step + QKV_SLOTS - 1, lax.rem(step + QKV_SLOTS - 1, QKV_SLOTS)):
                c.start()

        @pl.when(step + CACHE_FIRST < blocks)
        def _():
            for c in cache_in(step + CACHE_FIRST):
                c.wait()
            for c in cache_back(step + CACHE_FIRST):
                c.start()

        h = normed[:, pl.ds(pl.multiple_of(step * QKV_ROWS, 128), QKV_ROWS)]
        wq = jnp.swapaxes(wq_buf[slot], 0, 1)
        we = jnp.swapaxes(we_buf[slot], 0, 1)
        for k in range(kv_local):
            acc_q[k] += jnp.dot(h, wq[k], preferred_element_type=F32)
            acc_e[k] += jnp.dot(h, we[k], preferred_element_type=F32)
        return 0

    lax.fori_loop(0, steps, step_fn, 0)

    for c in small[1:]:
        c.wait()
    cos_t = cos_ref[...].T
    sin_t = sin_ref[...].T
    cos2 = jnp.concatenate([cos_t, cos_t], axis=1)
    sin2 = jnp.concatenate([-sin_t, sin_t], axis=1)
    is_key = core == 0
    cos_e = jnp.where(is_key, cos2, jnp.ones_like(cos2))
    sin_e = jnp.where(is_key, sin2, jnp.zeros_like(sin2))

    def rotate(v, c, s):
        r = v * c + pltpu.roll(v, head_dim // 2, 1) * s
        return r.astype(BF16).astype(F32)

    for k in range(kv_local):
        bias_q = bias_ref[k : k + 1, pl.ds(pl.multiple_of(core * q_cols, 128), q_cols)].astype(F32)
        for g in range(per_core):
            cols = slice(g * head_dim, (g + 1) * head_dim)
            heads[k * per_core + g] = rotate(acc_q[k, :, cols] + bias_q[:, cols], cos2, sin2)
        bias_e = bias_ref[k : k + 1, pl.ds(pl.multiple_of((group + core) * head_dim, 128), head_dim)].astype(F32)
        heads[kv_local * per_core + k] = rotate(acc_e[k] + bias_e, cos_e, sin_e)
    done = []
    for k in range(kv_local + 1):
        part = pl.ds(k * per_core, per_core)
        done.append(pltpu.make_async_copy(heads.at[part], out_ref.at[part], out_sem.at[k]))
        done[-1].start()
    for i in range(blocks):
        for c in cache_back(i):
            c.wait()
    for c in done:
        c.wait()


def project(hidden, rope_cos, rope_sin, norm_gain, w_qkv, b_qkv, k_rows, v_rows):
    num_seqs, depth = hidden.shape
    head_dim = k_rows.shape[2]
    kv_local = w_qkv.shape[1]
    per_core = (w_qkv.shape[2] // head_dim - 2) // 2
    rows = kv_local * (per_core + 1)
    blocks = num_seqs // CACHE_SEQS
    assert blocks <= depth // QKV_ROWS + CACHE_FIRST
    anyspace = pl.BlockSpec(memory_space=pl.ANY)
    dma = pltpu.SemaphoreType.DMA
    return pl.pallas_call(
        project_kernel,
        out_shape=[
            jax.ShapeDtypeStruct((rows, num_seqs, head_dim), F32),
            jax.ShapeDtypeStruct(k_rows.shape, BF16),
            jax.ShapeDtypeStruct(v_rows.shape, BF16),
        ],
        in_specs=[anyspace] * 8,
        out_specs=[anyspace] * 3,
        scratch_shapes=[
            pltpu.VMEM((num_seqs, depth), BF16),
            pltpu.VMEM((depth // head_dim, head_dim), BF16),
            pltpu.VMEM((head_dim // 2, num_seqs), F32),
            pltpu.VMEM((head_dim // 2, num_seqs), F32),
            pltpu.VMEM(b_qkv.shape, BF16),
            dma((X_PARTS,)),
            dma((4,)),
            pltpu.VMEM((num_seqs, depth), BF16),
            pltpu.VMEM((depth // head_dim, head_dim), F32),
            pltpu.VMEM((rows, num_seqs, head_dim), F32),
            pltpu.VMEM((kv_local, num_seqs, per_core * head_dim), F32),
            pltpu.VMEM((kv_local, num_seqs, head_dim), F32),
            pltpu.VMEM((QKV_SLOTS, QKV_ROWS, kv_local, per_core * head_dim), BF16),
            pltpu.VMEM((QKV_SLOTS, QKV_ROWS, kv_local, head_dim), BF16),
            pltpu.VMEM(k_rows.shape, BF16),
            pltpu.VMEM(v_rows.shape, BF16),
            dma((QKV_SLOTS,)), dma((QKV_SLOTS,)), dma((kv_local + 1,)),
            dma((blocks,)), dma((blocks,)), dma((blocks,)), dma((blocks,)),
        ],
        compiler_params=pltpu.CompilerParams(vmem_limit_bytes=60 << 20),
        name="project",
    )(hidden, norm_gain.reshape(depth // head_dim, head_dim), rope_cos.T, rope_sin.T, b_qkv, w_qkv, k_rows, v_rows)


ATT_SEQS = 8
ATT_SLOTS = 6
OUT_COLS = 256
SEQ_GROUPS = (24, 40)
PIECES = ((0, 0, 8), (0, 8, 16), (1, 0, 40))
W_PARTS = 8
LAG_Y = 6
LAG_X = 8
LAG_P = 2


def finish_kernel(lens_hbm, half_hbm, sink_hbm, hid_ref, bo_hbm, wo_ref, k_hbm, v_hbm, y_out, new_ref,
                  lens_ref, sink_ref, bo_ref, small_sem, y_parts, w_buf, x_buf, h_buf, k_ring, v_ring, num, ml, sink_col, bo_f32, r1, r1ml, own, own_ml, away, away_ml, r2, r2ml, o_buf, r3, o_all,
                  y_send, y_recv, z_buf, x_recv, p1, p2,
                  w_sem, x_sem, k_sem, v_sem, h_in, h_send, h_recv, s1_send, s1_recv, s2_send, s2_recv, s3_send, s3_recv,
                  y_ss, y_rs, x_ss, x_rs, p1_ss, p1_rs, p2_ss, p2_rs, o_sem):
    chip, core = sp_place()
    tp = lax.axis_index("tp")
    partner = {"sp": 2 * chip + (1 - core)}
    across_x = {"sp": 2 * (1 - chip) + core}
    across_y = {"tp": 1 - tp}
    q_rows, _, head_dim = num[0].shape
    chip_groups = len(SEQ_GROUPS)
    offsets = [sum(SEQ_GROUPS[:g]) for g in range(chip_groups)]
    num_seqs = h_buf.shape[1]
    kv_local = (h_buf.shape[0] - q_rows) // 2
    rows = k_ring.shape[2]
    ctx_local = rows // kv_local
    half_h = q_rows // 2
    half_s = num_seqs // 2
    part_h = half_h // kv_local
    cols = w_buf.shape[1]
    chunks = cols // OUT_COLS
    total = chip_groups * chunks
    mine = pl.multiple_of(core * half_h, half_h)
    theirs = pl.multiple_of((1 - core) * half_h, half_h)

    def seqs(which, g, first=0, count=None):
        return pl.ds(pl.multiple_of(which * half_s + offsets[g] + first, 8), SEQ_GROUPS[g] if count is None else count)

    small = [pltpu.make_async_copy(src, dst, small_sem.at[i]) for i, (src, dst) in enumerate(((lens_hbm, lens_ref), (sink_hbm, sink_ref), (bo_hbm, bo_ref)))]
    for c in small:
        c.start()
    barrier = pltpu.get_barrier_semaphore()
    for peer in (partner, across_x, across_y):
        pl.semaphore_signal(barrier, inc=1, device_id=peer, device_id_type=MESH)

    order = [(1 - chip, *piece) for piece in PIECES] + [(chip, g, 0, n) for g, n in enumerate(SEQ_GROUPS)]
    own_rows = (pl.ds(mine, half_h), pl.ds(pl.multiple_of(q_rows + kv_local * core, kv_local), kv_local))
    src_rows = (pl.ds(0, half_h), pl.ds(half_h, kv_local))
    h_local, h_remote = [], []
    for i, piece in enumerate(order):
        at = seqs(*piece)
        for j in range(2):
            h_local.append(pltpu.make_async_copy(half_hbm.at[src_rows[j], at], h_buf.at[own_rows[j], at], h_in.at[2 * i + j]))
            h_local[-1].start()
            h_remote.append(remote(half_hbm.at[src_rows[j], at], h_buf.at[own_rows[j], at], h_send.at[2 * i + j], h_recv.at[2 * i + j], partner))

    steps = num_seqs // ATT_SEQS
    counts = [n // ATT_SEQS for _, _, _, n in order]
    starts = [sum(counts[:i]) for i in range(len(counts))]

    def block(p):
        return lax.rem(p + (1 - chip) * (steps // 2), steps) * ATT_SEQS

    def kv_load(p):
        at = pl.ds(pl.multiple_of(block(p), ATT_SEQS), ATT_SEQS)
        slot = lax.rem(p, ATT_SLOTS)
        return pltpu.make_async_copy(k_hbm.at[at], k_ring.at[slot], k_sem.at[slot]), pltpu.make_async_copy(v_hbm.at[at], v_ring.at[slot], v_sem.at[slot])

    for p in range(ATT_SLOTS):
        for c in kv_load(p):
            c.start()
    my_cols = pl.ds(pl.multiple_of(core * cols, 128), cols)
    x_in = [pltpu.make_async_copy(hid_ref.at[seqs(chip, g), my_cols], x_buf[g], x_sem.at[g]) for g in range(chip_groups)]
    w_cols = cols // W_PARTS
    w_chunks = w_cols // OUT_COLS

    def w_copy(p):
        return pltpu.make_async_copy(wo_ref.at[:, pl.ds(pl.multiple_of(core * cols + p * w_cols, 128), w_cols)], w_buf.at[:, pl.ds(pl.multiple_of(p * w_cols, 128), w_cols)], w_sem.at[p])

    w_copy(0).start()
    w_copy(1).start()
    for c in small:
        c.wait()
    sink = sink_column(sink_ref, q_rows, 2, 2 * part_h)
    sink_col[...] = jnp.broadcast_to(sink, sink_col.shape)
    bo_f32[...] = bo_ref[...].astype(F32)
    pl.semaphore_wait(barrier, 3)
    for c in h_remote:
        c.start()

    base = lax.axis_index("sp") * ctx_local
    scale = head_dim**-0.5
    col = lax.broadcasted_iota(jnp.int32, (q_rows, rows), 1)
    kv_row = lax.div(lax.rem(lax.broadcasted_iota(jnp.int32, (q_rows, rows), 0), half_h), part_h)
    col_pos = jnp.where(lax.rem(col, kv_local) == kv_row, lax.div(col, kv_local), ctx_local * 1024)
    lane = lax.broadcasted_iota(jnp.int32, (q_rows, ml.shape[2]), 1)
    batch = range(ATT_SEQS)
    over_d = (((1,), (1,)), ((), ()))
    new_code = jnp.where(lax.broadcasted_iota(jnp.int32, (q_rows, 16), 1) == lax.div(lax.rem(lax.broadcasted_iota(jnp.int32, (q_rows, 16), 0), half_h), part_h), 1, 2)

    def attend(i, first, last, carry):
        def step_fn(t, carry):
            m_all, l_all = carry
            p = starts[i] + t
            slot = lax.rem(p, ATT_SLOTS)
            for c in kv_load(p):
                c.wait()
            start = block(p)
            heads = h_buf.at[:, pl.ds(pl.multiple_of(start, ATT_SEQS), ATT_SEQS)]
            rel = [lens_ref[start + s] - base for s in batch]
            inside = [jnp.where(jnp.logical_and(r >= 0, r < ctx_local), 1, 0) for r in rel]
            queries = [heads[0:q_rows, s, :].astype(BF16) for s in batch]
            new_k, new_v = ([jnp.concatenate([heads[lo : lo + kv_local, s, :]] * (16 // kv_local), axis=0).astype(BF16) for s in batch] for lo in (q_rows, q_rows + kv_local))
            logits = [lax.dot_general(queries[s], k_ring[slot, s], over_d, preferred_element_type=F32) for s in batch]
            extra = [lax.dot_general(queries[s], new_k[s], over_d, preferred_element_type=F32) for s in batch]
            logits = [jnp.where(col_pos < rel[s], logits[s] * scale, -jnp.inf) for s in batch]
            extra = [jnp.where(new_code == inside[s], extra[s] * scale, -jnp.inf) for s in batch]
            tops = [jnp.maximum(jnp.maximum(jnp.max(logits[s], axis=1, keepdims=True), jnp.max(extra[s], axis=1, keepdims=True)), sink) for s in batch]
            weights = [jnp.exp(logits[s] - tops[s]) for s in batch]
            extra = [jnp.exp(extra[s] - tops[s]) for s in batch]
            totals = [jnp.sum(weights[s], axis=1, keepdims=True) + jnp.sum(extra[s], axis=1, keepdims=True) for s in batch]
            sums = [jnp.dot(weights[s].astype(BF16), v_ring[slot, s], preferred_element_type=F32) for s in batch]
            sums = [sums[s] + jnp.dot(extra[s].astype(BF16), new_v[s], preferred_element_type=F32) for s in batch]
            out = num[i].at[:, pl.ds(pl.multiple_of(t * ATT_SEQS, ATT_SEQS), ATT_SEQS)]
            for s in batch:
                here = lane == order[i][2] + t * ATT_SEQS + s
                m_all = jnp.where(here, tops[s], m_all)
                l_all = jnp.where(here, totals[s], l_all)
                out[:, s, :] = sums[s]
            for s in batch:
                for j in range(2):
                    new_ref[j, start + s] = heads[q_rows + j * kv_local : q_rows + (j + 1) * kv_local, s, :].astype(BF16)

            @pl.when(p + ATT_SLOTS < steps)
            def _():
                for c in kv_load(p + ATT_SLOTS):
                    c.start()

            return m_all, l_all

        return lax.fori_loop(first, last, step_fn, carry)

    def heads_wait(i):
        for j in range(2):
            h_local[2 * i + j].wait()
            h_remote[2 * i + j].wait_recv()

    zero = jnp.zeros((q_rows, ml.shape[2]), F32)
    c1 = []

    def to_partner(i, carry):
        ml[i, 0:q_rows] = carry[0]
        ml[i, q_rows : 2 * q_rows] = carry[1]
        c1.append((
            remote(ml.at[i], r1ml.at[i], s1_send.at[2 * i], s1_recv.at[2 * i], partner),
            remote(num[i].at[pl.ds(theirs, half_h)], r1[i], s1_send.at[2 * i + 1], s1_recv.at[2 * i + 1], partner),
        ))
        for c in c1[-1]:
            c.start()

    def combine(i, dst, dst_ml):
        for c in c1[i]:
            c.wait_recv()
        m_a, l_a = ml[i, pl.ds(mine, half_h)], ml[i, pl.ds(q_rows + mine, half_h)]
        m_b, l_b = r1ml[i, pl.ds(mine, half_h)], r1ml[i, pl.ds(q_rows + mine, half_h)]
        m_chip = jnp.maximum(m_a, m_b)
        f_a = jnp.exp(m_a - m_chip)
        f_b = jnp.exp(m_b - m_chip)
        dst_ml[0:half_h] = m_chip
        dst_ml[half_h : 2 * half_h] = l_a * f_a + l_b * f_b
        f_a, f_b = f_a.T, f_b.T
        some = slice(order[i][2], order[i][2] + order[i][3])
        for h in range(half_h):
            dst[h, some] = num[i][mine + h] * f_a[some, h : h + 1] + r1[i][h] * f_b[some, h : h + 1]

    c2 = []

    def across(i):
        _, g, first, count = order[i]
        combine(i, away[g], away_ml.at[i])
        at = pl.ds(first, count)
        c2.append((
            remote(away_ml.at[i], r2ml.at[i], s2_send.at[2 * i], s2_recv.at[2 * i], across_x),
            remote(away[g].at[:, at], r2[g].at[:, at], s2_send.at[2 * i + 1], s2_recv.at[2 * i + 1], across_x),
        ))
        for c in c2[-1]:
            c.start()

    width = half_h * head_dim
    part_w = part_h * head_dim

    def o_place(which_half, k):
        return pl.ds(pl.multiple_of(2 * k * part_w + which_half * part_w, 128), part_w)

    def heads_start(g):
        m_a, l_a = own_ml[g, 0:half_h], own_ml[g, half_h : 2 * half_h]
        m_b, l_b = None, None
        for i, (group, first, _) in enumerate(PIECES):
            if group == g:
                for c in c2[i]:
                    c.wait_recv()
                m_i, l_i = r2ml[i, 0:half_h], r2ml[i, half_h : 2 * half_h]
                if m_b is None:
                    m_b, l_b = m_i, l_i
                else:
                    m_b = jnp.where(lane[0:half_h] < first, m_b, m_i)
                    l_b = jnp.where(lane[0:half_h] < first, l_b, l_i)
        m_top = jnp.maximum(m_a, m_b)
        f_a = jnp.exp(m_a - m_top)
        f_b = jnp.exp(m_b - m_top)
        den = l_a * f_a + l_b * f_b + jnp.exp(sink_col[pl.ds(mine, half_h)] - m_top)
        f_a, f_b = (f_a / den).T, (f_b / den).T
        for h in range(half_h):
            o_buf[g][:, h * head_dim : (h + 1) * head_dim] = own[g][h] * f_a[0 : SEQ_GROUPS[g], h : h + 1] + r2[g][h] * f_b[0 : SEQ_GROUPS[g], h : h + 1]
        c = remote(o_buf[g], r3[g], s3_send.at[g], s3_recv.at[g], partner)
        c.start()
        for k in range(kv_local):
            o_all[g][:, o_place(core, k)] = o_buf[g][:, k * part_w : (k + 1) * part_w].astype(BF16)
        return c

    def heads_end(g, c):
        c.wait_recv()
        for k in range(kv_local):
            o_all[g][:, o_place(1 - core, k)] = r3[g][:, k * part_w : (k + 1) * part_w].astype(BF16)

    def y_copy(g, j):
        t = g * chunks + j
        return remote(y_send[g].at[j], y_recv[g].at[j], y_ss.at[t], y_rs.at[t], across_y)

    def x_copy(g, j):
        t = g * chunks + j
        return remote(z_buf[g].at[j], x_recv[g].at[j], x_ss.at[t], x_rs.at[t], across_x)

    def p1_copy(g, j):
        t = g * chunks + j
        return remote(z_buf[g].at[j], p1[g].at[j], p1_ss.at[t], p1_rs.at[t], partner)

    def p2_copy(g, j):
        t = g * chunks + j
        return remote(x_recv[g].at[j], p2[g].at[j], p2_ss.at[t], p2_rs.at[t], partner)

    def out_copy(kind, g, j):
        which_seqs, which_cols = ((chip, core), (1 - chip, core), (chip, 1 - core), (1 - chip, 1 - core))[kind]
        cols_at = pl.ds(pl.multiple_of(which_cols * cols + j * OUT_COLS, 128), OUT_COLS)
        return pltpu.make_async_copy(y_parts[g].at[kind, j], y_out.at[seqs(which_seqs, g), cols_at], o_sem.at[kind, g * chunks + j])

    def put_out(kind, g, j, value):
        y_parts[g][kind, j] = value
        out_copy(kind, g, j).start()

    def multiply(g, j):
        if g == 0:
            @pl.when(lax.rem(j, w_chunks) == 0)
            def _():
                w_copy(lax.div(j, w_chunks)).wait()

        w = w_buf[:, pl.ds(pl.multiple_of(j * OUT_COLS, 128), OUT_COLS)]
        y_send[g][j] = jnp.dot(o_all[g][...], w, preferred_element_type=F32)
        y_copy(g, j).start()

    def add(g, j):
        y_copy(g, j).wait_recv()
        x_part = x_buf[g][:, pl.ds(pl.multiple_of(j * OUT_COLS, 128), OUT_COLS)].astype(F32)
        row = (core * cols + j * OUT_COLS) // head_dim
        bias = jnp.concatenate([bo_f32[pl.ds(row + i, 1), :] for i in range(OUT_COLS // head_dim)], axis=1)
        z = (x_part + (y_send[g][j] + y_recv[g][j]) + bias).astype(BF16)
        z_buf[g][j] = z.astype(F32)
        x_copy(g, j).start()
        p1_copy(g, j).start()
        put_out(0, g, j, z)

    def spread(g, j):
        x_copy(g, j).wait_recv()
        p2_copy(g, j).start()
        put_out(1, g, j, x_recv[g][j].astype(BF16))
        p1_copy(g, j).wait_recv()
        put_out(2, g, j, p1[g][j].astype(BF16))

    def receive(g, j):
        p2_copy(g, j).wait_recv()
        put_out(3, g, j, p2[g][j].astype(BF16))

    def body(t, _):
        for stage, lag in ((multiply, 0), (add, LAG_Y), (spread, LAG_Y + LAG_X), (receive, LAG_Y + LAG_X + LAG_P)):
            for g in range(chip_groups):
                j = t - lag - g * chunks

                @pl.when(jnp.logical_and(j >= 0, j < chunks))
                def _():
                    stage(g, j)

        return 0

    heads_wait(0)
    to_partner(0, attend(0, 0, counts[0], (zero, zero)))
    heads_wait(1)
    to_partner(1, attend(1, 0, counts[1], (zero, zero)))
    across(0)
    w_copy(2).start()
    heads_wait(2)
    carry = attend(2, 0, 2, (zero, zero))
    across(1)
    for c in x_in:
        c.start()
    w_copy(3).start()
    to_partner(2, attend(2, 2, counts[2], carry))
    w_copy(4).start()
    heads_wait(3)
    carry = attend(3, 0, counts[3], (zero, zero))
    across(2)
    for p in range(5, W_PARTS):
        w_copy(p).start()
    to_partner(3, carry)
    heads_wait(4)
    to_partner(4, attend(4, 0, counts[4], (zero, zero)))
    combine(3, own[0], own_ml.at[0])
    combine(4, own[1], own_ml.at[1])

    c3 = [heads_start(0)]
    heads_end(0, c3[0])
    for c in x_in:
        c.wait()
    lax.fori_loop(0, chunks - 6, body, 0)
    c3.append(heads_start(1))
    lax.fori_loop(chunks - 6, chunks - 2, body, 0)
    heads_end(1, c3[1])
    lax.fori_loop(chunks - 2, total + LAG_Y + LAG_X + LAG_P, body, 0)

    for g in range(chip_groups):
        def tail(j, _):
            for copy in (y_copy, x_copy, p1_copy, p2_copy):
                copy(g, j).wait_send()
            for kind in range(4):
                out_copy(kind, g, j).wait()
            return 0

        lax.fori_loop(0, chunks, tail, 0)
    for c in (*h_remote, *(c for pair in c1 + c2 for c in pair), *c3):
        c.wait_send()


def finish(seq_lens, half, sinks, hidden, b_o, w_o, k_rows, v_rows):
    num_seqs, rows, head_dim = k_rows.shape
    q_rows = sinks.shape[1]
    half_h, half_s = q_rows // 2, num_seqs // 2
    kv_local = half.shape[0] - half_h
    assert sum(SEQ_GROUPS) == half_s
    order = tuple(n for _, _, n in PIECES) + SEQ_GROUPS
    chip_groups, groups = len(SEQ_GROUPS), len(order)
    width = w_o.shape[1]
    cols = width // 2
    chunks = cols // OUT_COLS
    total = chip_groups * chunks
    vmem = pl.BlockSpec(memory_space=pltpu.VMEM)
    anyspace = pl.BlockSpec(memory_space=pl.ANY)
    chunked = tuple(pltpu.VMEM((chunks, n, OUT_COLS), F32) for n in SEQ_GROUPS)
    parts = tuple(pltpu.VMEM((half_h, n, head_dim), F32) for n in SEQ_GROUPS)
    own_ml = pltpu.VMEM((chip_groups, 2 * half_h, 128), F32)
    piece_ml = pltpu.VMEM((len(PIECES), 2 * half_h, 128), F32)
    o_parts = tuple(pltpu.VMEM((n, half_h * head_dim), F32) for n in SEQ_GROUPS)
    ring = pltpu.VMEM((ATT_SLOTS, ATT_SEQS, rows, head_dim), BF16)
    dma = pltpu.SemaphoreType.DMA
    return pl.pallas_call(
        finish_kernel,
        out_shape=[
            jax.ShapeDtypeStruct((num_seqs, width), BF16),
            jax.ShapeDtypeStruct((2, num_seqs, kv_local, head_dim), BF16),
        ],
        in_specs=[anyspace] * 8,
        out_specs=[anyspace, vmem],
        scratch_shapes=[
            pltpu.SMEM((num_seqs,), jnp.int32),
            pltpu.VMEM((1, q_rows), F32),
            pltpu.VMEM((width // head_dim, head_dim), BF16),
            dma((3,)),
            tuple(pltpu.VMEM((4, chunks, n, OUT_COLS), BF16) for n in SEQ_GROUPS),
            pltpu.VMEM((w_o.shape[0], cols), BF16),
            tuple(pltpu.VMEM((n, cols), BF16) for n in SEQ_GROUPS),
            pltpu.VMEM((q_rows + 2 * kv_local, num_seqs, head_dim), F32),
            ring, ring,
            tuple(pltpu.VMEM((q_rows, n, head_dim), F32) for n in order),
            pltpu.VMEM((groups, 2 * q_rows, 128), F32),
            pltpu.VMEM((q_rows, 128), F32),
            pltpu.VMEM((width // head_dim, head_dim), F32),
            tuple(pltpu.VMEM((half_h, n, head_dim), F32) for n in order),
            pltpu.VMEM((groups, 2 * q_rows, 128), F32),
            parts, own_ml, parts, piece_ml, parts, piece_ml,
            o_parts, o_parts,
            tuple(pltpu.VMEM((n, q_rows * head_dim), BF16) for n in SEQ_GROUPS),
            chunked, chunked, chunked, chunked, chunked, chunked,
            dma((W_PARTS,)), dma((chip_groups,)), dma((ATT_SLOTS,)), dma((ATT_SLOTS,)),
            dma((2 * groups,)), dma((2 * groups,)), dma((2 * groups,)),
            dma((2 * groups,)), dma((2 * groups,)),
            dma((2 * len(PIECES),)), dma((2 * len(PIECES),)),
            dma((chip_groups,)), dma((chip_groups,)),
            *[dma((total,))] * 8,
            dma((4, total)),
        ],
        compiler_params=pltpu.CompilerParams(collective_id=1, has_side_effects=True, vmem_limit_bytes=62 << 20),
        name="finish",
    )(seq_lens, half, sinks, hidden, b_o.reshape(width // head_dim, head_dim), w_o, k_rows, v_rows)


LAST_PARTS = 8
LAST_UNROLL = 8


def last_kernel(lens_hbm, y_hbm, new_hbm, k_in, v_in, y_out, k_out, v_out, lens_ref, lens_sem, y_buf, new_ref, in_sem, out_sem, new_sem, k_sem, v_sem):
    num_seqs, ctx_local = k_out.shape[:2]
    base = lax.axis_index("sp") * ctx_local
    rows = y_hbm.shape[0] // LAST_PARTS
    new_copy = pltpu.make_async_copy(new_hbm, new_ref, new_sem)
    new_copy.start()
    lens_copy = pltpu.make_async_copy(lens_hbm, lens_ref, lens_sem)
    lens_copy.start()
    loads, stores = [], []
    for p in range(LAST_PARTS):
        at = pl.ds(p * rows, rows)
        loads.append(pltpu.make_async_copy(y_hbm.at[at], y_buf.at[at], in_sem.at[p]))
        stores.append(pltpu.make_async_copy(y_buf.at[at], y_out.at[at], out_sem.at[p]))
        loads[-1].start()

    def for_new_rows(act):
        def step(i, _):
            for b in (i * LAST_UNROLL + r for r in range(LAST_UNROLL)):
                n = lens_ref[b] - base

                @pl.when(jnp.logical_and(n >= 0, n < ctx_local))
                def _():
                    act(pltpu.make_async_copy(new_ref.at[0, b], k_out.at[b, n], k_sem))
                    act(pltpu.make_async_copy(new_ref.at[1, b], v_out.at[b, n], v_sem))

            return 0

        lax.fori_loop(0, num_seqs // LAST_UNROLL, step, 0)

    lens_copy.wait()
    new_copy.wait()
    for_new_rows(lambda c: c.start())
    for p in range(LAST_PARTS):
        loads[p].wait()
        stores[p].start()
    for_new_rows(lambda c: c.wait())
    for c in stores:
        c.wait()


def last(seq_lens, y, new, k_copy, v_copy):
    anyspace = pl.BlockSpec(memory_space=pl.ANY)
    dma = pltpu.SemaphoreType.DMA
    return pl.pallas_call(
        last_kernel,
        out_shape=[jax.ShapeDtypeStruct(a.shape, a.dtype) for a in (y, k_copy, v_copy)],
        in_specs=[anyspace] * 5,
        out_specs=[anyspace] * 3,
        scratch_shapes=[pltpu.SMEM(seq_lens.shape, jnp.int32), dma, pltpu.VMEM(y.shape, y.dtype), pltpu.VMEM(new.shape, new.dtype), dma((LAST_PARTS,)), dma((LAST_PARTS,)), dma, dma, dma],
        input_output_aliases={3: 1, 4: 2},
        compiler_params=pltpu.CompilerParams(vmem_limit_bytes=60 << 20),
        name="last",
    )(seq_lens, y, new, k_copy, v_copy)


def solution(mesh):
    cache_spec = P("dp", "sp", "tp", None)

    def block_step(hidden, seq_lens, rope_cos, rope_sin, k_cache, v_cache, norm_gain, w_qkv, b_qkv, sink_logits, w_o, b_o):
        num_seqs, ctx_local, kv_local, head_dim = k_cache.shape
        rows = (num_seqs, ctx_local * kv_local, head_dim)
        k_rows, v_rows = k_cache.reshape(rows), v_cache.reshape(rows)
        half, k_copy, v_copy = project(hidden, rope_cos, rope_sin, norm_gain, w_qkv, b_qkv, k_rows, v_rows)
        sinks = sink_logits.reshape(1, sink_logits.shape[0])
        y, new = finish(seq_lens, half, sinks, hidden, b_o, w_o, k_rows, v_rows)
        return last(seq_lens, y, new, k_copy.reshape(k_cache.shape), v_copy.reshape(v_cache.shape))

    return jax.shard_map(block_step, mesh=mesh, in_specs=(P("dp", None), P("dp"), P("dp", None), P("dp", None), cache_spec, cache_spec, P(None), P(None, "tp", None), P("tp", None), P("tp"), P("tp", None), P(None)), out_specs=(P("dp", None), cache_spec, cache_spec), check_vma=False)
```

```python
import functools

import jax
import jax.numpy as jnp
from jax import lax
from jax.experimental import pallas as pl
from jax.experimental.pallas import tpu as pltpu
from jax.sharding import PartitionSpec as P

NORM_EPS = 1e-5
F32 = jnp.float32
BF16 = jnp.bfloat16
MESH = pl.DeviceIdType.MESH


def sp_place():
    sp = lax.axis_index("sp")
    return lax.div(sp, 2), lax.rem(sp, 2)


def remote(src, dst, send_sem, recv_sem, where):
    return pltpu.make_async_remote_copy(src_ref=src, dst_ref=dst, send_sem=send_sem, recv_sem=recv_sem, device_id=where, device_id_type=MESH)


def sink_column(row_ref, count, halves, group):
    row = lax.broadcasted_iota(jnp.int32, (count, count), 0)
    per_half = count // halves
    part = group // halves
    head = lax.div(lax.rem(row, per_half), part) * group + lax.div(row, per_half) * part + lax.rem(row, part)
    same = head == lax.broadcasted_iota(jnp.int32, (count, count), 1)
    return jnp.sum(jnp.where(same, jnp.broadcast_to(row_ref[...], (count, count)), 0.0), axis=1, keepdims=True)


QKV_ROWS = 1024
QKV_SLOTS = 3
CACHE_SEQS = 16
CACHE_AHEAD = 2
CACHE_FIRST = 0
X_PARTS = 4


def project_kernel(x_hbm, gain_hbm, cos_hbm, sin_hbm, bias_hbm, w_ref, k_ref, v_ref, out_ref, k_out, v_out,
                   x_ref, gain_ref, cos_ref, sin_ref, bias_ref, x_sem, small_sem, normed, gain, heads, acc_q, acc_e, wq_buf, we_buf, k_buf, v_buf, wq_sem, we_sem, out_sem, k_in, v_in, k_back, v_back):
    _, core = sp_place()
    num_seqs, depth = x_ref.shape
    head_dim = acc_e.shape[2]
    q_cols = acc_q.shape[2]
    kv_local = acc_q.shape[0]
    per_core = q_cols // head_dim
    group = 2 * per_core
    steps = depth // QKV_ROWS
    x_rows = num_seqs // X_PARTS
    blocks = num_seqs // CACHE_SEQS

    def fetch(step, slot):
        rows = pl.ds(step * QKV_ROWS, QKV_ROWS)
        cq = pltpu.make_async_copy(w_ref.at[rows, :, pl.ds(pl.multiple_of(core * q_cols, 128), q_cols)], wq_buf.at[slot], wq_sem.at[slot])
        ce = pltpu.make_async_copy(w_ref.at[rows, :, pl.ds(pl.multiple_of((group + core) * head_dim, 128), head_dim)], we_buf.at[slot], we_sem.at[slot])
        return cq, ce

    def cache_in(i):
        at = pl.ds(i * CACHE_SEQS, CACHE_SEQS)
        return pltpu.make_async_copy(k_ref.at[at], k_buf.at[at], k_in.at[i]), pltpu.make_async_copy(v_ref.at[at], v_buf.at[at], v_in.at[i])

    def cache_back(i):
        at = pl.ds(i * CACHE_SEQS, CACHE_SEQS)
        return pltpu.make_async_copy(k_buf.at[at], k_out.at[at], k_back.at[i]), pltpu.make_async_copy(v_buf.at[at], v_out.at[at], v_back.at[i])

    small = [pltpu.make_async_copy(src, dst, small_sem.at[i]) for i, (src, dst) in enumerate(((gain_hbm, gain_ref), (cos_hbm, cos_ref), (sin_hbm, sin_ref), (bias_hbm, bias_ref)))]
    small[0].start()
    x_copies = []
    for p in range(X_PARTS):
        at = pl.ds(p * x_rows, x_rows)
        x_copies.append(pltpu.make_async_copy(x_hbm.at[at], x_ref.at[at], x_sem.at[p]))
        x_copies[-1].start()
    for c in fetch(0, 0):
        c.start()
    for i in range(CACHE_FIRST):
        for c in cache_in(i):
            c.start()
    for s in range(1, QKV_SLOTS - 1):
        for c in fetch(s, s):
            c.start()
    for i in range(CACHE_FIRST, CACHE_AHEAD):
        for c in cache_in(i):
            c.start()
    for c in small[1:]:
        c.start()

    small[0].wait()
    gain[...] = gain_ref[...].astype(F32)

    def norm_rows(r, _):
        rows = pl.ds(pl.multiple_of(r * 16, 16), 16)
        xw = x_ref[rows, :].astype(F32)
        inv = lax.rsqrt(jnp.mean(xw * xw, axis=-1, keepdims=True) + NORM_EPS)
        for t in range(depth // head_dim):
            cols = slice(t * head_dim, (t + 1) * head_dim)
            normed[rows, cols] = (xw[:, cols] * inv * gain[t : t + 1, :]).astype(BF16)
        return 0

    for p in range(X_PARTS):
        x_copies[p].wait()
        lax.fori_loop(p * x_rows // 16, (p + 1) * x_rows // 16, norm_rows, 0)
    for i in range(CACHE_FIRST):
        for c in cache_in(i):
            c.wait()
        for c in cache_back(i):
            c.start()
    acc_q[...] = jnp.zeros_like(acc_q)
    acc_e[...] = jnp.zeros_like(acc_e)

    def step_fn(step, _):
        slot = lax.rem(step, QKV_SLOTS)

        @pl.when(step + CACHE_AHEAD < blocks)
        def _():
            for c in cache_in(step + CACHE_AHEAD):
                c.start()

        for c in fetch(step, slot):
            c.wait()

        @pl.when(step + QKV_SLOTS - 1 < steps)
        def _():
            for c in fetch(step + QKV_SLOTS - 1, lax.rem(step + QKV_SLOTS - 1, QKV_SLOTS)):
                c.start()

        @pl.when(step + CACHE_FIRST < blocks)
        def _():
            for c in cache_in(step + CACHE_FIRST):
                c.wait()
            for c in cache_back(step + CACHE_FIRST):
                c.start()

        h = normed[:, pl.ds(pl.multiple_of(step * QKV_ROWS, 128), QKV_ROWS)]
        wq = jnp.swapaxes(wq_buf[slot], 0, 1)
        we = jnp.swapaxes(we_buf[slot], 0, 1)
        for k in range(kv_local):
            acc_q[k] += jnp.dot(h, wq[k], preferred_element_type=F32)
            acc_e[k] += jnp.dot(h, we[k], preferred_element_type=F32)
        return 0

    lax.fori_loop(0, steps, step_fn, 0)

    for c in small[1:]:
        c.wait()
    cos_t = cos_ref[...].T
    sin_t = sin_ref[...].T
    cos2 = jnp.concatenate([cos_t, cos_t], axis=1)
    sin2 = jnp.concatenate([-sin_t, sin_t], axis=1)
    is_key = core == 0
    cos_e = jnp.where(is_key, cos2, jnp.ones_like(cos2))
    sin_e = jnp.where(is_key, sin2, jnp.zeros_like(sin2))

    def rotate(v, c, s):
        r = v * c + pltpu.roll(v, head_dim // 2, 1) * s
        return r.astype(BF16).astype(F32)

    for k in range(kv_local):
        bias_q = bias_ref[k : k + 1, pl.ds(pl.multiple_of(core * q_cols, 128), q_cols)].astype(F32)
        for g in range(per_core):
            cols = slice(g * head_dim, (g + 1) * head_dim)
            heads[k * per_core + g] = rotate(acc_q[k, :, cols] + bias_q[:, cols], cos2, sin2)
        bias_e = bias_ref[k : k + 1, pl.ds(pl.multiple_of((group + core) * head_dim, 128), head_dim)].astype(F32)
        heads[kv_local * per_core + k] = rotate(acc_e[k] + bias_e, cos_e, sin_e)
    done = []
    for k in range(kv_local + 1):
        part = pl.ds(k * per_core, per_core)
        done.append(pltpu.make_async_copy(heads.at[part], out_ref.at[part], out_sem.at[k]))
        done[-1].start()
    for i in range(blocks):
        for c in cache_back(i):
            c.wait()
    for c in done:
        c.wait()


def project(hidden, rope_cos, rope_sin, norm_gain, w_qkv, b_qkv, k_rows, v_rows):
    num_seqs, depth = hidden.shape
    head_dim = k_rows.shape[2]
    kv_local = w_qkv.shape[1]
    per_core = (w_qkv.shape[2] // head_dim - 2) // 2
    rows = kv_local * (per_core + 1)
    blocks = num_seqs // CACHE_SEQS
    assert blocks <= depth // QKV_ROWS + CACHE_FIRST
    anyspace = pl.BlockSpec(memory_space=pl.ANY)
    dma = pltpu.SemaphoreType.DMA
    return pl.pallas_call(
        project_kernel,
        out_shape=[
            jax.ShapeDtypeStruct((rows, num_seqs, head_dim), F32),
            jax.ShapeDtypeStruct(k_rows.shape, BF16),
            jax.ShapeDtypeStruct(v_rows.shape, BF16),
        ],
        in_specs=[anyspace] * 8,
        out_specs=[anyspace] * 3,
        scratch_shapes=[
            pltpu.VMEM((num_seqs, depth), BF16),
            pltpu.VMEM((depth // head_dim, head_dim), BF16),
            pltpu.VMEM((head_dim // 2, num_seqs), F32),
            pltpu.VMEM((head_dim // 2, num_seqs), F32),
            pltpu.VMEM(b_qkv.shape, BF16),
            dma((X_PARTS,)),
            dma((4,)),
            pltpu.VMEM((num_seqs, depth), BF16),
            pltpu.VMEM((depth // head_dim, head_dim), F32),
            pltpu.VMEM((rows, num_seqs, head_dim), F32),
            pltpu.VMEM((kv_local, num_seqs, per_core * head_dim), F32),
            pltpu.VMEM((kv_local, num_seqs, head_dim), F32),
            pltpu.VMEM((QKV_SLOTS, QKV_ROWS, kv_local, per_core * head_dim), BF16),
            pltpu.VMEM((QKV_SLOTS, QKV_ROWS, kv_local, head_dim), BF16),
            pltpu.VMEM(k_rows.shape, BF16),
            pltpu.VMEM(v_rows.shape, BF16),
            dma((QKV_SLOTS,)), dma((QKV_SLOTS,)), dma((kv_local + 1,)),
            dma((blocks,)), dma((blocks,)), dma((blocks,)), dma((blocks,)),
        ],
        compiler_params=pltpu.CompilerParams(vmem_limit_bytes=60 << 20),
        name="project",
    )(hidden, norm_gain.reshape(depth // head_dim, head_dim), rope_cos.T, rope_sin.T, b_qkv, w_qkv, k_rows, v_rows)


ATT_SEQS = 8
ATT_SLOTS = 6
OUT_COLS = 512
SEQ_GROUPS = (24, 24, 16)
PIECES = ((0, 0, 8), (0, 8, 16), (1, 0, 24), (2, 0, 16))
W_PARTS = 8
LAG_Y = 4
LAG_X = 4
LAG_P = 1


def finish_kernel(lens_hbm, half_hbm, sink_hbm, hid_ref, bo_hbm, wo_ref, k_hbm, v_hbm, y_out, new_ref,
                  lens_ref, sink_ref, bo_ref, small_sem, y_parts, w_buf, x_buf, h_buf, k_ring, v_ring, num, ml, sink_col, bo_f32, r1, r1ml, own, own_ml, away, away_ml, r2, r2ml, o_buf, r3, o_all,
                  y_send, y_recv, z_buf, x_recv, p1, p2,
                  w_sem, x_sem, k_sem, v_sem, h_in, h_send, h_recv, s1_send, s1_recv, s2_send, s2_recv, s3_send, s3_recv,
                  y_ss, y_rs, x_ss, x_rs, p1_ss, p1_rs, p2_ss, p2_rs, o_sem):
    chip, core = sp_place()
    tp = lax.axis_index("tp")
    partner = {"sp": 2 * chip + (1 - core)}
    across_x = {"sp": 2 * (1 - chip) + core}
    across_y = {"tp": 1 - tp}
    q_rows, _, head_dim = num[0].shape
    chip_groups = len(SEQ_GROUPS)
    offsets = [sum(SEQ_GROUPS[:g]) for g in range(chip_groups)]
    num_seqs = h_buf.shape[1]
    kv_local = (h_buf.shape[0] - q_rows) // 2
    rows = k_ring.shape[2]
    ctx_local = rows // kv_local
    half_h = q_rows // 2
    half_s = num_seqs // 2
    part_h = half_h // kv_local
    cols = w_buf.shape[1]
    chunks = cols // OUT_COLS
    total = chip_groups * chunks
    mine = pl.multiple_of(core * half_h, half_h)
    theirs = pl.multiple_of((1 - core) * half_h, half_h)

    def seqs(which, g, first=0, count=None):
        return pl.ds(pl.multiple_of(which * half_s + offsets[g] + first, 8), SEQ_GROUPS[g] if count is None else count)

    small = [pltpu.make_async_copy(src, dst, small_sem.at[i]) for i, (src, dst) in enumerate(((lens_hbm, lens_ref), (sink_hbm, sink_ref), (bo_hbm, bo_ref)))]
    for c in small:
        c.start()
    barrier = pltpu.get_barrier_semaphore()
    for peer in (partner, across_x, across_y):
        pl.semaphore_signal(barrier, inc=1, device_id=peer, device_id_type=MESH)

    order = [(1 - chip, *piece) for piece in PIECES] + [(chip, g, 0, n) for g, n in enumerate(SEQ_GROUPS)]
    own_rows = (pl.ds(mine, half_h), pl.ds(pl.multiple_of(q_rows + kv_local * core, kv_local), kv_local))
    src_rows = (pl.ds(0, half_h), pl.ds(half_h, kv_local))
    h_local, h_remote = [], []
    for i, piece in enumerate(order):
        at = seqs(*piece)
        for j in range(2):
            h_local.append(pltpu.make_async_copy(half_hbm.at[src_rows[j], at], h_buf.at[own_rows[j], at], h_in.at[2 * i + j]))
            h_local[-1].start()
            h_remote.append(remote(half_hbm.at[src_rows[j], at], h_buf.at[own_rows[j], at], h_send.at[2 * i + j], h_recv.at[2 * i + j], partner))

    steps = num_seqs // ATT_SEQS
    counts = [n // ATT_SEQS for _, _, _, n in order]
    starts = [sum(counts[:i]) for i in range(len(counts))]

    def block(p):
        return lax.rem(p + (1 - chip) * (steps // 2), steps) * ATT_SEQS

    def kv_load(p):
        at = pl.ds(pl.multiple_of(block(p), ATT_SEQS), ATT_SEQS)
        slot = lax.rem(p, ATT_SLOTS)
        return pltpu.make_async_copy(k_hbm.at[at], k_ring.at[slot], k_sem.at[slot]), pltpu.make_async_copy(v_hbm.at[at], v_ring.at[slot], v_sem.at[slot])

    for p in range(ATT_SLOTS):
        for c in kv_load(p):
            c.start()
    my_cols = pl.ds(pl.multiple_of(core * cols, 128), cols)
    x_in = [pltpu.make_async_copy(hid_ref.at[seqs(chip, g), my_cols], x_buf[g], x_sem.at[g]) for g in range(chip_groups)]
    w_cols = cols // W_PARTS
    w_chunks = w_cols // OUT_COLS

    def w_copy(p):
        return pltpu.make_async_copy(wo_ref.at[:, pl.ds(pl.multiple_of(core * cols + p * w_cols, 128), w_cols)], w_buf.at[:, pl.ds(pl.multiple_of(p * w_cols, 128), w_cols)], w_sem.at[p])

    w_copy(0).start()
    w_copy(1).start()
    for c in small:
        c.wait()
    sink = sink_column(sink_ref, q_rows, 2, 2 * part_h)
    sink_col[...] = jnp.broadcast_to(sink, sink_col.shape)
    bo_f32[...] = bo_ref[...].astype(F32)
    pl.semaphore_wait(barrier, 3)
    for c in h_remote:
        c.start()

    base = lax.axis_index("sp") * ctx_local
    scale = head_dim**-0.5
    col = lax.broadcasted_iota(jnp.int32, (q_rows, rows), 1)
    kv_row = lax.div(lax.rem(lax.broadcasted_iota(jnp.int32, (q_rows, rows), 0), half_h), part_h)
    col_pos = jnp.where(lax.rem(col, kv_local) == kv_row, lax.div(col, kv_local), ctx_local * 1024)
    lane = lax.broadcasted_iota(jnp.int32, (q_rows, ml.shape[2]), 1)
    batch = range(ATT_SEQS)
    over_d = (((1,), (1,)), ((), ()))
    new_code = jnp.where(lax.broadcasted_iota(jnp.int32, (q_rows, 16), 1) == lax.div(lax.rem(lax.broadcasted_iota(jnp.int32, (q_rows, 16), 0), half_h), part_h), 1, 2)

    def attend(i, first, last, carry):
        def step_fn(t, carry):
            m_all, l_all = carry
            p = starts[i] + t
            slot = lax.rem(p, ATT_SLOTS)
            for c in kv_load(p):
                c.wait()
            start = block(p)
            heads = h_buf.at[:, pl.ds(pl.multiple_of(start, ATT_SEQS), ATT_SEQS)]
            rel = [lens_ref[start + s] - base for s in batch]
            inside = [jnp.where(jnp.logical_and(r >= 0, r < ctx_local), 1, 0) for r in rel]
            queries = [heads[0:q_rows, s, :].astype(BF16) for s in batch]
            new_k, new_v = ([jnp.concatenate([heads[lo : lo + kv_local, s, :]] * (16 // kv_local), axis=0).astype(BF16) for s in batch] for lo in (q_rows, q_rows + kv_local))
            logits = [lax.dot_general(queries[s], k_ring[slot, s], over_d, preferred_element_type=F32) for s in batch]
            extra = [lax.dot_general(queries[s], new_k[s], over_d, preferred_element_type=F32) for s in batch]
            logits = [jnp.where(col_pos < rel[s], logits[s] * scale, -jnp.inf) for s in batch]
            extra = [jnp.where(new_code == inside[s], extra[s] * scale, -jnp.inf) for s in batch]
            tops = [jnp.maximum(jnp.maximum(jnp.max(logits[s], axis=1, keepdims=True), jnp.max(extra[s], axis=1, keepdims=True)), sink) for s in batch]
            weights = [jnp.exp(logits[s] - tops[s]) for s in batch]
            extra = [jnp.exp(extra[s] - tops[s]) for s in batch]
            totals = [jnp.sum(weights[s], axis=1, keepdims=True) + jnp.sum(extra[s], axis=1, keepdims=True) for s in batch]
            sums = [jnp.dot(weights[s].astype(BF16), v_ring[slot, s], preferred_element_type=F32) for s in batch]
            sums = [sums[s] + jnp.dot(extra[s].astype(BF16), new_v[s], preferred_element_type=F32) for s in batch]
            out = num[i].at[:, pl.ds(pl.multiple_of(t * ATT_SEQS, ATT_SEQS), ATT_SEQS)]
            for s in batch:
                here = lane == order[i][2] + t * ATT_SEQS + s
                m_all = jnp.where(here, tops[s], m_all)
                l_all = jnp.where(here, totals[s], l_all)
                out[:, s, :] = sums[s]
            for s in batch:
                for j in range(2):
                    new_ref[j, start + s] = heads[q_rows + j * kv_local : q_rows + (j + 1) * kv_local, s, :].astype(BF16)

            @pl.when(p + ATT_SLOTS < steps)
            def _():
                for c in kv_load(p + ATT_SLOTS):
                    c.start()

            return m_all, l_all

        return lax.fori_loop(first, last, step_fn, carry)

    def heads_wait(i):
        for j in range(2):
            h_local[2 * i + j].wait()
            h_remote[2 * i + j].wait_recv()

    zero = jnp.zeros((q_rows, ml.shape[2]), F32)
    c1 = []

    def to_partner(i, carry):
        ml[i, 0:q_rows] = carry[0]
        ml[i, q_rows : 2 * q_rows] = carry[1]
        c1.append((
            remote(ml.at[i], r1ml.at[i], s1_send.at[2 * i], s1_recv.at[2 * i], partner),
            remote(num[i].at[pl.ds(theirs, half_h)], r1[i], s1_send.at[2 * i + 1], s1_recv.at[2 * i + 1], partner),
        ))
        for c in c1[-1]:
            c.start()

    def combine(i, dst, dst_ml):
        for c in c1[i]:
            c.wait_recv()
        m_a, l_a = ml[i, pl.ds(mine, half_h)], ml[i, pl.ds(q_rows + mine, half_h)]
        m_b, l_b = r1ml[i, pl.ds(mine, half_h)], r1ml[i, pl.ds(q_rows + mine, half_h)]
        m_chip = jnp.maximum(m_a, m_b)
        f_a = jnp.exp(m_a - m_chip)
        f_b = jnp.exp(m_b - m_chip)
        dst_ml[0:half_h] = m_chip
        dst_ml[half_h : 2 * half_h] = l_a * f_a + l_b * f_b
        f_a, f_b = f_a.T, f_b.T
        some = slice(order[i][2], order[i][2] + order[i][3])
        for h in range(half_h):
            dst[h, some] = num[i][mine + h] * f_a[some, h : h + 1] + r1[i][h] * f_b[some, h : h + 1]

    c2 = []

    def across(i):
        _, g, first, count = order[i]
        combine(i, away[g], away_ml.at[i])
        at = pl.ds(first, count)
        c2.append((
            remote(away_ml.at[i], r2ml.at[i], s2_send.at[2 * i], s2_recv.at[2 * i], across_x),
            remote(away[g].at[:, at], r2[g].at[:, at], s2_send.at[2 * i + 1], s2_recv.at[2 * i + 1], across_x),
        ))
        for c in c2[-1]:
            c.start()

    width = half_h * head_dim
    part_w = part_h * head_dim

    def o_place(which_half, k):
        return pl.ds(pl.multiple_of(2 * k * part_w + which_half * part_w, 128), part_w)

    def heads_start(g):
        m_a, l_a = own_ml[g, 0:half_h], own_ml[g, half_h : 2 * half_h]
        m_b, l_b = None, None
        for i, (group, first, _) in enumerate(PIECES):
            if group == g:
                for c in c2[i]:
                    c.wait_recv()
                m_i, l_i = r2ml[i, 0:half_h], r2ml[i, half_h : 2 * half_h]
                if m_b is None:
                    m_b, l_b = m_i, l_i
                else:
                    m_b = jnp.where(lane[0:half_h] < first, m_b, m_i)
                    l_b = jnp.where(lane[0:half_h] < first, l_b, l_i)
        m_top = jnp.maximum(m_a, m_b)
        f_a = jnp.exp(m_a - m_top)
        f_b = jnp.exp(m_b - m_top)
        den = l_a * f_a + l_b * f_b + jnp.exp(sink_col[pl.ds(mine, half_h)] - m_top)
        f_a, f_b = (f_a / den).T, (f_b / den).T
        for h in range(half_h):
            o_buf[g][:, h * head_dim : (h + 1) * head_dim] = own[g][h] * f_a[0 : SEQ_GROUPS[g], h : h + 1] + r2[g][h] * f_b[0 : SEQ_GROUPS[g], h : h + 1]
        c = remote(o_buf[g], r3[g], s3_send.at[g], s3_recv.at[g], partner)
        c.start()
        for k in range(kv_local):
            o_all[g][:, o_place(core, k)] = o_buf[g][:, k * part_w : (k + 1) * part_w].astype(BF16)
        return c

    def heads_end(g, c):
        c.wait_recv()
        for k in range(kv_local):
            o_all[g][:, o_place(1 - core, k)] = r3[g][:, k * part_w : (k + 1) * part_w].astype(BF16)

    def y_copy(g, j):
        t = g * chunks + j
        return remote(y_send[g].at[j], y_recv[g].at[j], y_ss.at[t], y_rs.at[t], across_y)

    def x_copy(g, j):
        t = g * chunks + j
        return remote(z_buf[g].at[j], x_recv[g].at[j], x_ss.at[t], x_rs.at[t], across_x)

    def p1_copy(g, j):
        t = g * chunks + j
        return remote(z_buf[g].at[j], p1[g].at[j], p1_ss.at[t], p1_rs.at[t], partner)

    def p2_copy(g, j):
        t = g * chunks + j
        return remote(x_recv[g].at[j], p2[g].at[j], p2_ss.at[t], p2_rs.at[t], partner)

    def out_copy(kind, g, j):
        which_seqs, which_cols = ((chip, core), (1 - chip, core), (chip, 1 - core), (1 - chip, 1 - core))[kind]
        cols_at = pl.ds(pl.multiple_of(which_cols * cols + j * OUT_COLS, 128), OUT_COLS)
        return pltpu.make_async_copy(y_parts[g].at[kind, j], y_out.at[seqs(which_seqs, g), cols_at], o_sem.at[kind, g * chunks + j])

    def put_out(kind, g, j, value):
        y_parts[g][kind, j] = value
        out_copy(kind, g, j).start()

    def multiply(g, j):
        if g == 0:
            @pl.when(lax.rem(j, w_chunks) == 0)
            def _():
                w_copy(lax.div(j, w_chunks)).wait()

        w = w_buf[:, pl.ds(pl.multiple_of(j * OUT_COLS, 128), OUT_COLS)]
        y_send[g][j] = jnp.dot(o_all[g][...], w, preferred_element_type=F32)
        y_copy(g, j).start()

    def add(g, j):
        y_copy(g, j).wait_recv()
        x_part = x_buf[g][:, pl.ds(pl.multiple_of(j * OUT_COLS, 128), OUT_COLS)].astype(F32)
        row = (core * cols + j * OUT_COLS) // head_dim
        bias = jnp.concatenate([bo_f32[pl.ds(row + i, 1), :] for i in range(OUT_COLS // head_dim)], axis=1)
        z = (x_part + (y_send[g][j] + y_recv[g][j]) + bias).astype(BF16)
        z_buf[g][j] = z.astype(F32)
        x_copy(g, j).start()
        p1_copy(g, j).start()
        put_out(0, g, j, z)

    def spread(g, j):
        x_copy(g, j).wait_recv()
        p2_copy(g, j).start()
        put_out(1, g, j, x_recv[g][j].astype(BF16))
        p1_copy(g, j).wait_recv()
        put_out(2, g, j, p1[g][j].astype(BF16))

    def receive(g, j):
        p2_copy(g, j).wait_recv()
        put_out(3, g, j, p2[g][j].astype(BF16))

    def body(t, _):
        for stage, lag in ((multiply, 0), (add, LAG_Y), (spread, LAG_Y + LAG_X), (receive, LAG_Y + LAG_X + LAG_P)):
            for g in range(chip_groups):
                j = t - lag - g * chunks

                @pl.when(jnp.logical_and(j >= 0, j < chunks))
                def _():
                    stage(g, j)

        return 0

    heads_wait(0)
    to_partner(0, attend(0, 0, counts[0], (zero, zero)))
    heads_wait(1)
    to_partner(1, attend(1, 0, counts[1], (zero, zero)))
    across(0)
    w_copy(2).start()
    heads_wait(2)
    carry = attend(2, 0, 2, (zero, zero))
    across(1)
    for c in x_in:
        c.start()
    w_copy(3).start()
    to_partner(2, attend(2, 2, counts[2], carry))
    w_copy(4).start()
    heads_wait(3)
    carry = attend(3, 0, counts[3], (zero, zero))
    across(2)
    to_partner(3, carry)
    for p in range(5, W_PARTS):
        w_copy(p).start()
    heads_wait(4)
    carry = attend(4, 0, counts[4], (zero, zero))
    across(3)
    to_partner(4, carry)
    for i in (5, 6):
        heads_wait(i)
        to_partner(i, attend(i, 0, counts[i], (zero, zero)))
    for g in range(chip_groups):
        combine(len(PIECES) + g, own[g], own_ml.at[g])

    c3 = [heads_start(0)]
    heads_end(0, c3[0])
    for c in x_in:
        c.wait()
    done = 0
    for g in range(1, chip_groups):
        lax.fori_loop(done, g * chunks - 4, body, 0)
        c3.append(heads_start(g))
        lax.fori_loop(g * chunks - 4, g * chunks - 2, body, 0)
        heads_end(g, c3[g])
        done = g * chunks - 2
    lax.fori_loop(done, total + LAG_Y + LAG_X + LAG_P, body, 0)

    for g in range(chip_groups):
        def tail(j, _):
            for copy in (y_copy, x_copy, p1_copy, p2_copy):
                copy(g, j).wait_send()
            for kind in range(4):
                out_copy(kind, g, j).wait()
            return 0

        lax.fori_loop(0, chunks, tail, 0)
    for c in (*h_remote, *(c for pair in c1 + c2 for c in pair), *c3):
        c.wait_send()


def finish(seq_lens, half, sinks, hidden, b_o, w_o, k_rows, v_rows):
    num_seqs, rows, head_dim = k_rows.shape
    q_rows = sinks.shape[1]
    half_h, half_s = q_rows // 2, num_seqs // 2
    kv_local = half.shape[0] - half_h
    assert sum(SEQ_GROUPS) == half_s
    order = tuple(n for _, _, n in PIECES) + SEQ_GROUPS
    chip_groups, groups = len(SEQ_GROUPS), len(order)
    width = w_o.shape[1]
    cols = width // 2
    chunks = cols // OUT_COLS
    total = chip_groups * chunks
    vmem = pl.BlockSpec(memory_space=pltpu.VMEM)
    anyspace = pl.BlockSpec(memory_space=pl.ANY)
    chunked = tuple(pltpu.VMEM((chunks, n, OUT_COLS), F32) for n in SEQ_GROUPS)
    parts = tuple(pltpu.VMEM((half_h, n, head_dim), F32) for n in SEQ_GROUPS)
    own_ml = pltpu.VMEM((chip_groups, 2 * half_h, 128), F32)
    piece_ml = pltpu.VMEM((len(PIECES), 2 * half_h, 128), F32)
    o_parts = tuple(pltpu.VMEM((n, half_h * head_dim), F32) for n in SEQ_GROUPS)
    ring = pltpu.VMEM((ATT_SLOTS, ATT_SEQS, rows, head_dim), BF16)
    dma = pltpu.SemaphoreType.DMA
    return pl.pallas_call(
        finish_kernel,
        out_shape=[
            jax.ShapeDtypeStruct((num_seqs, width), BF16),
            jax.ShapeDtypeStruct((2, num_seqs, kv_local, head_dim), BF16),
        ],
        in_specs=[anyspace] * 8,
        out_specs=[anyspace, vmem],
        scratch_shapes=[
            pltpu.SMEM((num_seqs,), jnp.int32),
            pltpu.VMEM((1, q_rows), F32),
            pltpu.VMEM((width // head_dim, head_dim), BF16),
            dma((3,)),
            tuple(pltpu.VMEM((4, chunks, n, OUT_COLS), BF16) for n in SEQ_GROUPS),
            pltpu.VMEM((w_o.shape[0], cols), BF16),
            tuple(pltpu.VMEM((n, cols), BF16) for n in SEQ_GROUPS),
            pltpu.VMEM((q_rows + 2 * kv_local, num_seqs, head_dim), F32),
            ring, ring,
            tuple(pltpu.VMEM((q_rows, n, head_dim), F32) for n in order),
            pltpu.VMEM((groups, 2 * q_rows, 128), F32),
            pltpu.VMEM((q_rows, 128), F32),
            pltpu.VMEM((width // head_dim, head_dim), F32),
            tuple(pltpu.VMEM((half_h, n, head_dim), F32) for n in order),
            pltpu.VMEM((groups, 2 * q_rows, 128), F32),
            parts, own_ml, parts, piece_ml, parts, piece_ml,
            o_parts, o_parts,
            tuple(pltpu.VMEM((n, q_rows * head_dim), BF16) for n in SEQ_GROUPS),
            chunked, chunked, chunked, chunked, chunked, chunked,
            dma((W_PARTS,)), dma((chip_groups,)), dma((ATT_SLOTS,)), dma((ATT_SLOTS,)),
            dma((2 * groups,)), dma((2 * groups,)), dma((2 * groups,)),
            dma((2 * groups,)), dma((2 * groups,)),
            dma((2 * len(PIECES),)), dma((2 * len(PIECES),)),
            dma((chip_groups,)), dma((chip_groups,)),
            *[dma((total,))] * 8,
            dma((4, total)),
        ],
        compiler_params=pltpu.CompilerParams(collective_id=1, has_side_effects=True, vmem_limit_bytes=62 << 20),
        name="finish",
    )(seq_lens, half, sinks, hidden, b_o.reshape(width // head_dim, head_dim), w_o, k_rows, v_rows)


LAST_PARTS = 8
LAST_UNROLL = 8


def last_kernel(lens_hbm, y_hbm, new_hbm, k_in, v_in, y_out, k_out, v_out, lens_ref, lens_sem, y_buf, new_ref, in_sem, out_sem, new_sem, k_sem, v_sem):
    num_seqs, ctx_local = k_out.shape[:2]
    base = lax.axis_index("sp") * ctx_local
    rows = y_hbm.shape[0] // LAST_PARTS
    new_copy = pltpu.make_async_copy(new_hbm, new_ref, new_sem)
    new_copy.start()
    lens_copy = pltpu.make_async_copy(lens_hbm, lens_ref, lens_sem)
    lens_copy.start()
    loads, stores = [], []
    for p in range(LAST_PARTS):
        at = pl.ds(p * rows, rows)
        loads.append(pltpu.make_async_copy(y_hbm.at[at], y_buf.at[at], in_sem.at[p]))
        stores.append(pltpu.make_async_copy(y_buf.at[at], y_out.at[at], out_sem.at[p]))
        loads[-1].start()

    def for_new_rows(act):
        def step(i, _):
            for b in (i * LAST_UNROLL + r for r in range(LAST_UNROLL)):
                n = lens_ref[b] - base

                @pl.when(jnp.logical_and(n >= 0, n < ctx_local))
                def _():
                    act(pltpu.make_async_copy(new_ref.at[0, b], k_out.at[b, n], k_sem))
                    act(pltpu.make_async_copy(new_ref.at[1, b], v_out.at[b, n], v_sem))

            return 0

        lax.fori_loop(0, num_seqs // LAST_UNROLL, step, 0)

    lens_copy.wait()
    new_copy.wait()
    for_new_rows(lambda c: c.start())
    for p in range(LAST_PARTS):
        loads[p].wait()
        stores[p].start()
    for_new_rows(lambda c: c.wait())
    for c in stores:
        c.wait()


def last(seq_lens, y, new, k_copy, v_copy):
    anyspace = pl.BlockSpec(memory_space=pl.ANY)
    dma = pltpu.SemaphoreType.DMA
    return pl.pallas_call(
        last_kernel,
        out_shape=[jax.ShapeDtypeStruct(a.shape, a.dtype) for a in (y, k_copy, v_copy)],
        in_specs=[anyspace] * 5,
        out_specs=[anyspace] * 3,
        scratch_shapes=[pltpu.SMEM(seq_lens.shape, jnp.int32), dma, pltpu.VMEM(y.shape, y.dtype), pltpu.VMEM(new.shape, new.dtype), dma((LAST_PARTS,)), dma((LAST_PARTS,)), dma, dma, dma],
        input_output_aliases={3: 1, 4: 2},
        compiler_params=pltpu.CompilerParams(vmem_limit_bytes=60 << 20),
        name="last",
    )(seq_lens, y, new, k_copy, v_copy)


def solution(mesh):
    cache_spec = P("dp", "sp", "tp", None)

    def block_step(hidden, seq_lens, rope_cos, rope_sin, k_cache, v_cache, norm_gain, w_qkv, b_qkv, sink_logits, w_o, b_o):
        num_seqs, ctx_local, kv_local, head_dim = k_cache.shape
        rows = (num_seqs, ctx_local * kv_local, head_dim)
        k_rows, v_rows = k_cache.reshape(rows), v_cache.reshape(rows)
        half, k_copy, v_copy = project(hidden, rope_cos, rope_sin, norm_gain, w_qkv, b_qkv, k_rows, v_rows)
        sinks = sink_logits.reshape(1, sink_logits.shape[0])
        y, new = finish(seq_lens, half, sinks, hidden, b_o, w_o, k_rows, v_rows)
        return last(seq_lens, y, new, k_copy.reshape(k_cache.shape), v_copy.reshape(v_cache.shape))

    return jax.shard_map(block_step, mesh=mesh, in_specs=(P("dp", None), P("dp"), P("dp", None), P("dp", None), cache_spec, cache_spec, P(None), P(None, "tp", None), P("tp", None), P("tp"), P("tp", None), P(None)), out_specs=(P("dp", None), cache_spec, cache_spec), check_vma=False)
```

```python
import functools

import jax
import jax.numpy as jnp
from jax import lax
from jax.experimental import pallas as pl
from jax.experimental.pallas import tpu as pltpu
from jax.sharding import PartitionSpec as P

NORM_EPS = 1e-5
F32 = jnp.float32
BF16 = jnp.bfloat16
MESH = pl.DeviceIdType.MESH


def sp_place():
    sp = lax.axis_index("sp")
    return lax.div(sp, 2), lax.rem(sp, 2)


def remote(src, dst, send_sem, recv_sem, where):
    return pltpu.make_async_remote_copy(src_ref=src, dst_ref=dst, send_sem=send_sem, recv_sem=recv_sem, device_id=where, device_id_type=MESH)


def sink_column(row_ref, count, halves, group):
    row = lax.broadcasted_iota(jnp.int32, (count, count), 0)
    per_half = count // halves
    part = group // halves
    head = lax.div(lax.rem(row, per_half), part) * group + lax.div(row, per_half) * part + lax.rem(row, part)
    same = head == lax.broadcasted_iota(jnp.int32, (count, count), 1)
    return jnp.sum(jnp.where(same, jnp.broadcast_to(row_ref[...], (count, count)), 0.0), axis=1, keepdims=True)


QKV_ROWS = 1024
QKV_SLOTS = 3
CACHE_SEQS = 16
CACHE_AHEAD = 2
CACHE_FIRST = 0
X_PARTS = 4


def project_kernel(x_hbm, gain_hbm, cos_hbm, sin_hbm, bias_hbm, w_ref, k_ref, v_ref, out_ref, k_out, v_out,
                   x_ref, gain_ref, cos_ref, sin_ref, bias_ref, x_sem, small_sem, normed, gain, heads, acc_q, acc_e, wq_buf, we_buf, k_buf, v_buf, wq_sem, we_sem, out_sem, k_in, v_in, k_back, v_back):
    _, core = sp_place()
    num_seqs, depth = x_ref.shape
    head_dim = acc_e.shape[2]
    q_cols = acc_q.shape[2]
    kv_local = acc_q.shape[0]
    per_core = q_cols // head_dim
    group = 2 * per_core
    steps = depth // QKV_ROWS
    x_rows = num_seqs // X_PARTS
    blocks = num_seqs // CACHE_SEQS

    def fetch(step, slot):
        rows = pl.ds(step * QKV_ROWS, QKV_ROWS)
        cq = pltpu.make_async_copy(w_ref.at[rows, :, pl.ds(pl.multiple_of(core * q_cols, 128), q_cols)], wq_buf.at[slot], wq_sem.at[slot])
        ce = pltpu.make_async_copy(w_ref.at[rows, :, pl.ds(pl.multiple_of((group + core) * head_dim, 128), head_dim)], we_buf.at[slot], we_sem.at[slot])
        return cq, ce

    def cache_in(i):
        at = pl.ds(i * CACHE_SEQS, CACHE_SEQS)
        return pltpu.make_async_copy(k_ref.at[at], k_buf.at[at], k_in.at[i]), pltpu.make_async_copy(v_ref.at[at], v_buf.at[at], v_in.at[i])

    def cache_back(i):
        at = pl.ds(i * CACHE_SEQS, CACHE_SEQS)
        return pltpu.make_async_copy(k_buf.at[at], k_out.at[at], k_back.at[i]), pltpu.make_async_copy(v_buf.at[at], v_out.at[at], v_back.at[i])

    small = [pltpu.make_async_copy(src, dst, small_sem.at[i]) for i, (src, dst) in enumerate(((gain_hbm, gain_ref), (cos_hbm, cos_ref), (sin_hbm, sin_ref), (bias_hbm, bias_ref)))]
    small[0].start()
    x_copies = []
    for p in range(X_PARTS):
        at = pl.ds(p * x_rows, x_rows)
        x_copies.append(pltpu.make_async_copy(x_hbm.at[at], x_ref.at[at], x_sem.at[p]))
        x_copies[-1].start()
    for c in fetch(0, 0):
        c.start()
    for i in range(CACHE_FIRST):
        for c in cache_in(i):
            c.start()
    for s in range(1, QKV_SLOTS - 1):
        for c in fetch(s, s):
            c.start()
    for i in range(CACHE_FIRST, CACHE_AHEAD):
        for c in cache_in(i):
            c.start()
    for c in small[1:]:
        c.start()

    small[0].wait()
    gain[...] = gain_ref[...].astype(F32)

    def norm_rows(r, _):
        rows = pl.ds(pl.multiple_of(r * 16, 16), 16)
        xw = x_ref[rows, :].astype(F32)
        inv = lax.rsqrt(jnp.mean(xw * xw, axis=-1, keepdims=True) + NORM_EPS)
        for t in range(depth // head_dim):
            cols = slice(t * head_dim, (t + 1) * head_dim)
            normed[rows, cols] = (xw[:, cols] * inv * gain[t : t + 1, :]).astype(BF16)
        return 0

    for p in range(X_PARTS):
        x_copies[p].wait()
        lax.fori_loop(p * x_rows // 16, (p + 1) * x_rows // 16, norm_rows, 0)
    for i in range(CACHE_FIRST):
        for c in cache_in(i):
            c.wait()
        for c in cache_back(i):
            c.start()
    acc_q[...] = jnp.zeros_like(acc_q)
    acc_e[...] = jnp.zeros_like(acc_e)

    def step_fn(step, _):
        slot = lax.rem(step, QKV_SLOTS)

        @pl.when(step + CACHE_AHEAD < blocks)
        def _():
            for c in cache_in(step + CACHE_AHEAD):
                c.start()

        for c in fetch(step, slot):
            c.wait()

        @pl.when(step + QKV_SLOTS - 1 < steps)
        def _():
            for c in fetch(step + QKV_SLOTS - 1, lax.rem(step + QKV_SLOTS - 1, QKV_SLOTS)):
                c.start()

        @pl.when(step + CACHE_FIRST < blocks)
        def _():
            for c in cache_in(step + CACHE_FIRST):
                c.wait()
            for c in cache_back(step + CACHE_FIRST):
                c.start()

        h = normed[:, pl.ds(pl.multiple_of(step * QKV_ROWS, 128), QKV_ROWS)]
        wq = jnp.swapaxes(wq_buf[slot], 0, 1)
        we = jnp.swapaxes(we_buf[slot], 0, 1)
        for k in range(kv_local):
            acc_q[k] += jnp.dot(h, wq[k], preferred_element_type=F32)
            acc_e[k] += jnp.dot(h, we[k], preferred_element_type=F32)
        return 0

    lax.fori_loop(0, steps, step_fn, 0)

    for c in small[1:]:
        c.wait()
    cos_t = cos_ref[...].T
    sin_t = sin_ref[...].T
    cos2 = jnp.concatenate([cos_t, cos_t], axis=1)
    sin2 = jnp.concatenate([-sin_t, sin_t], axis=1)
    is_key = core == 0
    cos_e = jnp.where(is_key, cos2, jnp.ones_like(cos2))
    sin_e = jnp.where(is_key, sin2, jnp.zeros_like(sin2))

    def rotate(v, c, s):
        r = v * c + pltpu.roll(v, head_dim // 2, 1) * s
        return r.astype(BF16).astype(F32)

    for k in range(kv_local):
        bias_q = bias_ref[k : k + 1, pl.ds(pl.multiple_of(core * q_cols, 128), q_cols)].astype(F32)
        for g in range(per_core):
            cols = slice(g * head_dim, (g + 1) * head_dim)
            heads[k * per_core + g] = rotate(acc_q[k, :, cols] + bias_q[:, cols], cos2, sin2)
        bias_e = bias_ref[k : k + 1, pl.ds(pl.multiple_of((group + core) * head_dim, 128), head_dim)].astype(F32)
        heads[kv_local * per_core + k] = rotate(acc_e[k] + bias_e, cos_e, sin_e)
    done = []
    for k in range(kv_local + 1):
        part = pl.ds(k * per_core, per_core)
        done.append(pltpu.make_async_copy(heads.at[part], out_ref.at[part], out_sem.at[k]))
        done[-1].start()
    for i in range(blocks):
        for c in cache_back(i):
            c.wait()
    for c in done:
        c.wait()


def project(hidden, rope_cos, rope_sin, norm_gain, w_qkv, b_qkv, k_rows, v_rows):
    num_seqs, depth = hidden.shape
    head_dim = k_rows.shape[2]
    kv_local = w_qkv.shape[1]
    per_core = (w_qkv.shape[2] // head_dim - 2) // 2
    rows = kv_local * (per_core + 1)
    blocks = num_seqs // CACHE_SEQS
    assert blocks <= depth // QKV_ROWS + CACHE_FIRST
    anyspace = pl.BlockSpec(memory_space=pl.ANY)
    dma = pltpu.SemaphoreType.DMA
    return pl.pallas_call(
        project_kernel,
        out_shape=[
            jax.ShapeDtypeStruct((rows, num_seqs, head_dim), F32),
            jax.ShapeDtypeStruct(k_rows.shape, BF16),
            jax.ShapeDtypeStruct(v_rows.shape, BF16),
        ],
        in_specs=[anyspace] * 8,
        out_specs=[anyspace] * 3,
        scratch_shapes=[
            pltpu.VMEM((num_seqs, depth), BF16),
            pltpu.VMEM((depth // head_dim, head_dim), BF16),
            pltpu.VMEM((head_dim // 2, num_seqs), F32),
            pltpu.VMEM((head_dim // 2, num_seqs), F32),
            pltpu.VMEM(b_qkv.shape, BF16),
            dma((X_PARTS,)),
            dma((4,)),
            pltpu.VMEM((num_seqs, depth), BF16),
            pltpu.VMEM((depth // head_dim, head_dim), F32),
            pltpu.VMEM((rows, num_seqs, head_dim), F32),
            pltpu.VMEM((kv_local, num_seqs, per_core * head_dim), F32),
            pltpu.VMEM((kv_local, num_seqs, head_dim), F32),
            pltpu.VMEM((QKV_SLOTS, QKV_ROWS, kv_local, per_core * head_dim), BF16),
            pltpu.VMEM((QKV_SLOTS, QKV_ROWS, kv_local, head_dim), BF16),
            pltpu.VMEM(k_rows.shape, BF16),
            pltpu.VMEM(v_rows.shape, BF16),
            dma((QKV_SLOTS,)), dma((QKV_SLOTS,)), dma((kv_local + 1,)),
            dma((blocks,)), dma((blocks,)), dma((blocks,)), dma((blocks,)),
        ],
        compiler_params=pltpu.CompilerParams(vmem_limit_bytes=60 << 20),
        name="project",
    )(hidden, norm_gain.reshape(depth // head_dim, head_dim), rope_cos.T, rope_sin.T, b_qkv, w_qkv, k_rows, v_rows)


ATT_SEQS = 8
ATT_SLOTS = 6
OUT_COLS = 512
SEQ_GROUPS = (24, 40)
PIECES = ((0, 0, 8), (0, 8, 16), (1, 0, 40))
W_PARTS = 8
LAG_Y = 3
LAG_X = 3
LAG_P = 1


def finish_kernel(lens_hbm, half_hbm, sink_hbm, hid_ref, bo_hbm, wo_ref, k_hbm, v_hbm, y_out, new_ref,
                  lens_ref, sink_ref, bo_ref, small_sem, y_parts, w_buf, x_buf, h_buf, k_ring, v_ring, num, ml, sink_col, bo_f32, r1, r1ml, own, own_ml, away, away_ml, r2, r2ml, o_buf, r3, o_all,
                  y_send, y_recv, z_buf, x_recv, p1, p2,
                  w_sem, x_sem, k_sem, v_sem, h_in, h_send, h_recv, s1_send, s1_recv, s2_send, s2_recv, s3_send, s3_recv,
                  y_ss, y_rs, x_ss, x_rs, p1_ss, p1_rs, p2_ss, p2_rs, o_sem):
    chip, core = sp_place()
    tp = lax.axis_index("tp")
    partner = {"sp": 2 * chip + (1 - core)}
    across_x = {"sp": 2 * (1 - chip) + core}
    across_y = {"tp": 1 - tp}
    q_rows, _, head_dim = num[0].shape
    chip_groups = len(SEQ_GROUPS)
    offsets = [sum(SEQ_GROUPS[:g]) for g in range(chip_groups)]
    num_seqs = h_buf.shape[1]
    kv_local = (h_buf.shape[0] - q_rows) // 2
    rows = k_ring.shape[2]
    ctx_local = rows // kv_local
    half_h = q_rows // 2
    half_s = num_seqs // 2
    part_h = half_h // kv_local
    cols = w_buf.shape[1]
    chunks = cols // OUT_COLS
    total = chip_groups * chunks
    mine = pl.multiple_of(core * half_h, half_h)
    theirs = pl.multiple_of((1 - core) * half_h, half_h)

    def seqs(which, g, first=0, count=None):
        return pl.ds(pl.multiple_of(which * half_s + offsets[g] + first, 8), SEQ_GROUPS[g] if count is None else count)

    small = [pltpu.make_async_copy(src, dst, small_sem.at[i]) for i, (src, dst) in enumerate(((lens_hbm, lens_ref), (sink_hbm, sink_ref), (bo_hbm, bo_ref)))]
    for c in small:
        c.start()
    barrier = pltpu.get_barrier_semaphore()
    for peer in (partner, across_x, across_y):
        pl.semaphore_signal(barrier, inc=1, device_id=peer, device_id_type=MESH)

    order = [(1 - chip, *piece) for piece in PIECES] + [(chip, g, 0, n) for g, n in enumerate(SEQ_GROUPS)]
    own_rows = (pl.ds(mine, half_h), pl.ds(pl.multiple_of(q_rows + kv_local * core, kv_local), kv_local))
    src_rows = (pl.ds(0, half_h), pl.ds(half_h, kv_local))
    h_local, h_remote = [], []
    for i, piece in enumerate(order):
        at = seqs(*piece)
        for j in range(2):
            h_local.append(pltpu.make_async_copy(half_hbm.at[src_rows[j], at], h_buf.at[own_rows[j], at], h_in.at[2 * i + j]))
            h_local[-1].start()
            h_remote.append(remote(half_hbm.at[src_rows[j], at], h_buf.at[own_rows[j], at], h_send.at[2 * i + j], h_recv.at[2 * i + j], partner))

    steps = num_seqs // ATT_SEQS
    counts = [n // ATT_SEQS for _, _, _, n in order]
    starts = [sum(counts[:i]) for i in range(len(counts))]

    def block(p):
        return lax.rem(p + (1 - chip) * (steps // 2), steps) * ATT_SEQS

    def kv_load(p):
        at = pl.ds(pl.multiple_of(block(p), ATT_SEQS), ATT_SEQS)
        slot = lax.rem(p, ATT_SLOTS)
        return pltpu.make_async_copy(k_hbm.at[at], k_ring.at[slot], k_sem.at[slot]), pltpu.make_async_copy(v_hbm.at[at], v_ring.at[slot], v_sem.at[slot])

    for p in range(ATT_SLOTS):
        for c in kv_load(p):
            c.start()
    my_cols = pl.ds(pl.multiple_of(core * cols, 128), cols)
    x_in = [pltpu.make_async_copy(hid_ref.at[seqs(chip, g), my_cols], x_buf[g], x_sem.at[g]) for g in range(chip_groups)]
    w_cols = cols // W_PARTS
    w_chunks = w_cols // OUT_COLS

    def w_copy(p):
        return pltpu.make_async_copy(wo_ref.at[:, pl.ds(pl.multiple_of(core * cols + p * w_cols, 128), w_cols)], w_buf.at[:, pl.ds(pl.multiple_of(p * w_cols, 128), w_cols)], w_sem.at[p])

    for c in small:
        c.wait()
    sink = sink_column(sink_ref, q_rows, 2, 2 * part_h)
    sink_col[...] = jnp.broadcast_to(sink, sink_col.shape)
    bo_f32[...] = bo_ref[...].astype(F32)
    pl.semaphore_wait(barrier, 3)
    for c in h_remote:
        c.start()

    base = lax.axis_index("sp") * ctx_local
    scale = head_dim**-0.5
    col = lax.broadcasted_iota(jnp.int32, (q_rows, rows), 1)
    kv_row = lax.div(lax.rem(lax.broadcasted_iota(jnp.int32, (q_rows, rows), 0), half_h), part_h)
    col_pos = jnp.where(lax.rem(col, kv_local) == kv_row, lax.div(col, kv_local), ctx_local * 1024)
    lane = lax.broadcasted_iota(jnp.int32, (q_rows, ml.shape[2]), 1)
    batch = range(ATT_SEQS)
    over_d = (((1,), (1,)), ((), ()))
    new_code = jnp.where(lax.broadcasted_iota(jnp.int32, (q_rows, 16), 1) == lax.div(lax.rem(lax.broadcasted_iota(jnp.int32, (q_rows, 16), 0), half_h), part_h), 1, 2)

    def attend(i, first, last, carry):
        def step_fn(t, carry):
            m_all, l_all = carry
            p = starts[i] + t
            slot = lax.rem(p, ATT_SLOTS)
            for c in kv_load(p):
                c.wait()
            start = block(p)
            heads = h_buf.at[:, pl.ds(pl.multiple_of(start, ATT_SEQS), ATT_SEQS)]
            rel = [lens_ref[start + s] - base for s in batch]
            inside = [jnp.where(jnp.logical_and(r >= 0, r < ctx_local), 1, 0) for r in rel]
            queries = [heads[0:q_rows, s, :].astype(BF16) for s in batch]
            new_k, new_v = ([jnp.concatenate([heads[lo : lo + kv_local, s, :]] * (16 // kv_local), axis=0).astype(BF16) for s in batch] for lo in (q_rows, q_rows + kv_local))
            logits = [lax.dot_general(queries[s], k_ring[slot, s], over_d, preferred_element_type=F32) for s in batch]
            extra = [lax.dot_general(queries[s], new_k[s], over_d, preferred_element_type=F32) for s in batch]
            logits = [jnp.where(col_pos < rel[s], logits[s] * scale, -jnp.inf) for s in batch]
            extra = [jnp.where(new_code == inside[s], extra[s] * scale, -jnp.inf) for s in batch]
            tops = [jnp.maximum(jnp.maximum(jnp.max(logits[s], axis=1, keepdims=True), jnp.max(extra[s], axis=1, keepdims=True)), sink) for s in batch]
            weights = [jnp.exp(logits[s] - tops[s]) for s in batch]
            extra = [jnp.exp(extra[s] - tops[s]) for s in batch]
            totals = [jnp.sum(weights[s], axis=1, keepdims=True) + jnp.sum(extra[s], axis=1, keepdims=True) for s in batch]
            sums = [jnp.dot(weights[s].astype(BF16), v_ring[slot, s], preferred_element_type=F32) for s in batch]
            sums = [sums[s] + jnp.dot(extra[s].astype(BF16), new_v[s], preferred_element_type=F32) for s in batch]
            out = num[i].at[:, pl.ds(pl.multiple_of(t * ATT_SEQS, ATT_SEQS), ATT_SEQS)]
            for s in batch:
                here = lane == order[i][2] + t * ATT_SEQS + s
                m_all = jnp.where(here, tops[s], m_all)
                l_all = jnp.where(here, totals[s], l_all)
                out[:, s, :] = sums[s]
            for s in batch:
                for j in range(2):
                    new_ref[j, start + s] = heads[q_rows + j * kv_local : q_rows + (j + 1) * kv_local, s, :].astype(BF16)

            @pl.when(p + ATT_SLOTS < steps)
            def _():
                for c in kv_load(p + ATT_SLOTS):
                    c.start()

            return m_all, l_all

        return lax.fori_loop(first, last, step_fn, carry)

    def heads_wait(i):
        for j in range(2):
            h_local[2 * i + j].wait()
            h_remote[2 * i + j].wait_recv()

    zero = jnp.zeros((q_rows, ml.shape[2]), F32)
    c1 = []

    def to_partner(i, carry):
        ml[i, 0:q_rows] = carry[0]
        ml[i, q_rows : 2 * q_rows] = carry[1]
        c1.append((
            remote(ml.at[i], r1ml.at[i], s1_send.at[2 * i], s1_recv.at[2 * i], partner),
            remote(num[i].at[pl.ds(theirs, half_h)], r1[i], s1_send.at[2 * i + 1], s1_recv.at[2 * i + 1], partner),
        ))
        for c in c1[-1]:
            c.start()

    def combine(i, dst, dst_ml):
        for c in c1[i]:
            c.wait_recv()
        m_a, l_a = ml[i, pl.ds(mine, half_h)], ml[i, pl.ds(q_rows + mine, half_h)]
        m_b, l_b = r1ml[i, pl.ds(mine, half_h)], r1ml[i, pl.ds(q_rows + mine, half_h)]
        m_chip = jnp.maximum(m_a, m_b)
        f_a = jnp.exp(m_a - m_chip)
        f_b = jnp.exp(m_b - m_chip)
        dst_ml[0:half_h] = m_chip
        dst_ml[half_h : 2 * half_h] = l_a * f_a + l_b * f_b
        f_a, f_b = f_a.T, f_b.T
        some = slice(order[i][2], order[i][2] + order[i][3])
        for h in range(half_h):
            dst[h, some] = num[i][mine + h] * f_a[some, h : h + 1] + r1[i][h] * f_b[some, h : h + 1]

    c2 = []

    def across(i):
        _, g, first, count = order[i]
        combine(i, away[g], away_ml.at[i])
        at = pl.ds(first, count)
        c2.append((
            remote(away_ml.at[i], r2ml.at[i], s2_send.at[2 * i], s2_recv.at[2 * i], across_x),
            remote(away[g].at[:, at], r2[g].at[:, at], s2_send.at[2 * i + 1], s2_recv.at[2 * i + 1], across_x),
        ))
        for c in c2[-1]:
            c.start()

    width = half_h * head_dim
    part_w = part_h * head_dim

    def o_place(which_half, k):
        return pl.ds(pl.multiple_of(2 * k * part_w + which_half * part_w, 128), part_w)

    def heads_start(g):
        m_a, l_a = own_ml[g, 0:half_h], own_ml[g, half_h : 2 * half_h]
        m_b, l_b = None, None
        for i, (group, first, _) in enumerate(PIECES):
            if group == g:
                for c in c2[i]:
                    c.wait_recv()
                m_i, l_i = r2ml[i, 0:half_h], r2ml[i, half_h : 2 * half_h]
                if m_b is None:
                    m_b, l_b = m_i, l_i
                else:
                    m_b = jnp.where(lane[0:half_h] < first, m_b, m_i)
                    l_b = jnp.where(lane[0:half_h] < first, l_b, l_i)
        m_top = jnp.maximum(m_a, m_b)
        f_a = jnp.exp(m_a - m_top)
        f_b = jnp.exp(m_b - m_top)
        den = l_a * f_a + l_b * f_b + jnp.exp(sink_col[pl.ds(mine, half_h)] - m_top)
        f_a, f_b = (f_a / den).T, (f_b / den).T
        for h in range(half_h):
            o_buf[g][:, h * head_dim : (h + 1) * head_dim] = own[g][h] * f_a[0 : SEQ_GROUPS[g], h : h + 1] + r2[g][h] * f_b[0 : SEQ_GROUPS[g], h : h + 1]
        c = remote(o_buf[g], r3[g], s3_send.at[g], s3_recv.at[g], partner)
        c.start()
        for k in range(kv_local):
            o_all[g][:, o_place(core, k)] = o_buf[g][:, k * part_w : (k + 1) * part_w].astype(BF16)
        return c

    def heads_end(g, c):
        c.wait_recv()
        for k in range(kv_local):
            o_all[g][:, o_place(1 - core, k)] = r3[g][:, k * part_w : (k + 1) * part_w].astype(BF16)

    def y_copy(g, j):
        t = g * chunks + j
        return remote(y_send[g].at[j], y_recv[g].at[j], y_ss.at[t], y_rs.at[t], across_y)

    def x_copy(g, j):
        t = g * chunks + j
        return remote(z_buf[g].at[j], x_recv[g].at[j], x_ss.at[t], x_rs.at[t], across_x)

    def p1_copy(g, j):
        t = g * chunks + j
        return remote(z_buf[g].at[j], p1[g].at[j], p1_ss.at[t], p1_rs.at[t], partner)

    def p2_copy(g, j):
        t = g * chunks + j
        return remote(x_recv[g].at[j], p2[g].at[j], p2_ss.at[t], p2_rs.at[t], partner)

    def out_copy(kind, g, j):
        which_seqs, which_cols = ((chip, core), (1 - chip, core), (chip, 1 - core), (1 - chip, 1 - core))[kind]
        cols_at = pl.ds(pl.multiple_of(which_cols * cols + j * OUT_COLS, 128), OUT_COLS)
        return pltpu.make_async_copy(y_parts[g].at[kind, j], y_out.at[seqs(which_seqs, g), cols_at], o_sem.at[kind, g * chunks + j])

    def put_out(kind, g, j, value):
        y_parts[g][kind, j] = value
        out_copy(kind, g, j).start()

    def multiply(g, j):
        if g == 0:
            @pl.when(lax.rem(j, w_chunks) == 0)
            def _():
                w_copy(lax.div(j, w_chunks)).wait()

        w = w_buf[:, pl.ds(pl.multiple_of(j * OUT_COLS, 128), OUT_COLS)]
        y_send[g][j] = jnp.dot(o_all[g][...], w, preferred_element_type=F32)
        y_copy(g, j).start()

    def add(g, j):
        y_copy(g, j).wait_recv()
        x_part = x_buf[g][:, pl.ds(pl.multiple_of(j * OUT_COLS, 128), OUT_COLS)].astype(F32)
        row = (core * cols + j * OUT_COLS) // head_dim
        bias = jnp.concatenate([bo_f32[pl.ds(row + i, 1), :] for i in range(OUT_COLS // head_dim)], axis=1)
        z = (x_part + (y_send[g][j] + y_recv[g][j]) + bias).astype(BF16)
        z_buf[g][j] = z.astype(F32)
        x_copy(g, j).start()
        p1_copy(g, j).start()
        put_out(0, g, j, z)

    def spread(g, j):
        x_copy(g, j).wait_recv()
        p2_copy(g, j).start()
        put_out(1, g, j, x_recv[g][j].astype(BF16))
        p1_copy(g, j).wait_recv()
        put_out(2, g, j, p1[g][j].astype(BF16))

    def receive(g, j):
        p2_copy(g, j).wait_recv()
        put_out(3, g, j, p2[g][j].astype(BF16))

    def body(t, _):
        for stage, lag in ((multiply, 0), (add, LAG_Y), (spread, LAG_Y + LAG_X), (receive, LAG_Y + LAG_X + LAG_P)):
            for g in range(chip_groups):
                j = t - lag - g * chunks

                @pl.when(jnp.logical_and(j >= 0, j < chunks))
                def _():
                    stage(g, j)

        return 0

    heads_wait(0)
    to_partner(0, attend(0, 0, counts[0], (zero, zero)))
    heads_wait(1)
    to_partner(1, attend(1, 0, counts[1], (zero, zero)))
    across(0)
    heads_wait(2)
    carry = attend(2, 0, 2, (zero, zero))
    across(1)
    for c in x_in:
        c.start()
    to_partner(2, attend(2, 2, counts[2], carry))
    w_copy(0).start()
    heads_wait(3)
    carry = attend(3, 0, counts[3], (zero, zero))
    across(2)
    w_copy(1).start()
    to_partner(3, carry)
    for p in range(2, W_PARTS):
        w_copy(p).start()
    heads_wait(4)
    to_partner(4, attend(4, 0, counts[4], (zero, zero)))
    combine(3, own[0], own_ml.at[0])
    combine(4, own[1], own_ml.at[1])

    c3 = [heads_start(0)]
    heads_end(0, c3[0])
    for c in x_in:
        c.wait()
    lax.fori_loop(0, chunks - 3, body, 0)
    c3.append(heads_start(1))
    lax.fori_loop(chunks - 3, chunks - 1, body, 0)
    heads_end(1, c3[1])
    lax.fori_loop(chunks - 1, total + LAG_Y + LAG_X + LAG_P, body, 0)

    for g in range(chip_groups):
        def tail(j, _):
            for copy in (y_copy, x_copy, p1_copy, p2_copy):
                copy(g, j).wait_send()
            for kind in range(4):
                out_copy(kind, g, j).wait()
            return 0

        lax.fori_loop(0, chunks, tail, 0)
    for c in (*h_remote, *(c for pair in c1 + c2 for c in pair), *c3):
        c.wait_send()


def finish(seq_lens, half, sinks, hidden, b_o, w_o, k_rows, v_rows):
    num_seqs, rows, head_dim = k_rows.shape
    q_rows = sinks.shape[1]
    half_h, half_s = q_rows // 2, num_seqs // 2
    kv_local = half.shape[0] - half_h
    assert sum(SEQ_GROUPS) == half_s
    order = tuple(n for _, _, n in PIECES) + SEQ_GROUPS
    chip_groups, groups = len(SEQ_GROUPS), len(order)
    width = w_o.shape[1]
    cols = width // 2
    chunks = cols // OUT_COLS
    total = chip_groups * chunks
    vmem = pl.BlockSpec(memory_space=pltpu.VMEM)
    anyspace = pl.BlockSpec(memory_space=pl.ANY)
    chunked = tuple(pltpu.VMEM((chunks, n, OUT_COLS), F32) for n in SEQ_GROUPS)
    parts = tuple(pltpu.VMEM((half_h, n, head_dim), F32) for n in SEQ_GROUPS)
    own_ml = pltpu.VMEM((chip_groups, 2 * half_h, 128), F32)
    piece_ml = pltpu.VMEM((len(PIECES), 2 * half_h, 128), F32)
    o_parts = tuple(pltpu.VMEM((n, half_h * head_dim), F32) for n in SEQ_GROUPS)
    ring = pltpu.VMEM((ATT_SLOTS, ATT_SEQS, rows, head_dim), BF16)
    dma = pltpu.SemaphoreType.DMA
    return pl.pallas_call(
        finish_kernel,
        out_shape=[
            jax.ShapeDtypeStruct((num_seqs, width), BF16),
            jax.ShapeDtypeStruct((2, num_seqs, kv_local, head_dim), BF16),
        ],
        in_specs=[anyspace] * 8,
        out_specs=[anyspace, vmem],
        scratch_shapes=[
            pltpu.SMEM((num_seqs,), jnp.int32),
            pltpu.VMEM((1, q_rows), F32),
            pltpu.VMEM((width // head_dim, head_dim), BF16),
            dma((3,)),
            tuple(pltpu.VMEM((4, chunks, n, OUT_COLS), BF16) for n in SEQ_GROUPS),
            pltpu.VMEM((w_o.shape[0], cols), BF16),
            tuple(pltpu.VMEM((n, cols), BF16) for n in SEQ_GROUPS),
            pltpu.VMEM((q_rows + 2 * kv_local, num_seqs, head_dim), F32),
            ring, ring,
            tuple(pltpu.VMEM((q_rows, n, head_dim), F32) for n in order),
            pltpu.VMEM((groups, 2 * q_rows, 128), F32),
            pltpu.VMEM((q_rows, 128), F32),
            pltpu.VMEM((width // head_dim, head_dim), F32),
            tuple(pltpu.VMEM((half_h, n, head_dim), F32) for n in order),
            pltpu.VMEM((groups, 2 * q_rows, 128), F32),
            parts, own_ml, parts, piece_ml, parts, piece_ml,
            o_parts, o_parts,
            tuple(pltpu.VMEM((n, q_rows * head_dim), BF16) for n in SEQ_GROUPS),
            chunked, chunked, chunked, chunked, chunked, chunked,
            dma((W_PARTS,)), dma((chip_groups,)), dma((ATT_SLOTS,)), dma((ATT_SLOTS,)),
            dma((2 * groups,)), dma((2 * groups,)), dma((2 * groups,)),
            dma((2 * groups,)), dma((2 * groups,)),
            dma((2 * len(PIECES),)), dma((2 * len(PIECES),)),
            dma((chip_groups,)), dma((chip_groups,)),
            *[dma((total,))] * 8,
            dma((4, total)),
        ],
        compiler_params=pltpu.CompilerParams(collective_id=1, has_side_effects=True, vmem_limit_bytes=62 << 20),
        name="finish",
    )(seq_lens, half, sinks, hidden, b_o.reshape(width // head_dim, head_dim), w_o, k_rows, v_rows)


LAST_PARTS = 8
LAST_UNROLL = 8


def last_kernel(lens_hbm, y_hbm, new_hbm, k_in, v_in, y_out, k_out, v_out, lens_ref, lens_sem, y_buf, new_ref, in_sem, out_sem, new_sem, k_sem, v_sem):
    num_seqs, ctx_local = k_out.shape[:2]
    base = lax.axis_index("sp") * ctx_local
    rows = y_hbm.shape[0] // LAST_PARTS
    new_copy = pltpu.make_async_copy(new_hbm, new_ref, new_sem)
    new_copy.start()
    lens_copy = pltpu.make_async_copy(lens_hbm, lens_ref, lens_sem)
    lens_copy.start()
    loads, stores = [], []
    for p in range(LAST_PARTS):
        at = pl.ds(p * rows, rows)
        loads.append(pltpu.make_async_copy(y_hbm.at[at], y_buf.at[at], in_sem.at[p]))
        stores.append(pltpu.make_async_copy(y_buf.at[at], y_out.at[at], out_sem.at[p]))
        loads[-1].start()

    def for_new_rows(act):
        def step(i, _):
            for b in (i * LAST_UNROLL + r for r in range(LAST_UNROLL)):
                n = lens_ref[b] - base

                @pl.when(jnp.logical_and(n >= 0, n < ctx_local))
                def _():
                    act(pltpu.make_async_copy(new_ref.at[0, b], k_out.at[b, n], k_sem))
                    act(pltpu.make_async_copy(new_ref.at[1, b], v_out.at[b, n], v_sem))

            return 0

        lax.fori_loop(0, num_seqs // LAST_UNROLL, step, 0)

    lens_copy.wait()
    new_copy.wait()
    for_new_rows(lambda c: c.start())
    for p in range(LAST_PARTS):
        loads[p].wait()
        stores[p].start()
    for_new_rows(lambda c: c.wait())
    for c in stores:
        c.wait()


def last(seq_lens, y, new, k_copy, v_copy):
    anyspace = pl.BlockSpec(memory_space=pl.ANY)
    dma = pltpu.SemaphoreType.DMA
    return pl.pallas_call(
        last_kernel,
        out_shape=[jax.ShapeDtypeStruct(a.shape, a.dtype) for a in (y, k_copy, v_copy)],
        in_specs=[anyspace] * 5,
        out_specs=[anyspace] * 3,
        scratch_shapes=[pltpu.SMEM(seq_lens.shape, jnp.int32), dma, pltpu.VMEM(y.shape, y.dtype), pltpu.VMEM(new.shape, new.dtype), dma((LAST_PARTS,)), dma((LAST_PARTS,)), dma, dma, dma],
        input_output_aliases={3: 1, 4: 2},
        compiler_params=pltpu.CompilerParams(vmem_limit_bytes=60 << 20),
        name="last",
    )(seq_lens, y, new, k_copy, v_copy)


def solution(mesh):
    cache_spec = P("dp", "sp", "tp", None)

    def block_step(hidden, seq_lens, rope_cos, rope_sin, k_cache, v_cache, norm_gain, w_qkv, b_qkv, sink_logits, w_o, b_o):
        num_seqs, ctx_local, kv_local, head_dim = k_cache.shape
        rows = (num_seqs, ctx_local * kv_local, head_dim)
        k_rows, v_rows = k_cache.reshape(rows), v_cache.reshape(rows)
        half, k_copy, v_copy = project(hidden, rope_cos, rope_sin, norm_gain, w_qkv, b_qkv, k_rows, v_rows)
        sinks = sink_logits.reshape(1, sink_logits.shape[0])
        y, new = finish(seq_lens, half, sinks, hidden, b_o, w_o, k_rows, v_rows)
        return last(seq_lens, y, new, k_copy.reshape(k_cache.shape), v_copy.reshape(v_cache.shape))

    return jax.shard_map(block_step, mesh=mesh, in_specs=(P("dp", None), P("dp"), P("dp", None), P("dp", None), cache_spec, cache_spec, P(None), P(None, "tp", None), P("tp", None), P("tp"), P("tp", None), P(None)), out_specs=(P("dp", None), cache_spec, cache_spec), check_vma=False)
```
